32 devices in a mesh: seq: 2 (over core), fsdp: 16 (over z, y, x).
Axes of the slice: x: 2, y: 2, z: 4, core: 2. Of those that a mesh axis runs over, the one named last changes fastest.
Arguments:
- token_ids: int32 [2, 16, 1024], P(None, 'fsdp', 'seq'), may hold values from 0 to 31999
- lengths: int32 [2, 16], P(None, 'fsdp'), may hold values from 256 to 1024, as said below
- loss_positions: int32 [2, 16, 32], P(None, 'fsdp', 'seq'), may hold values from 0 to 511, as said below
- loss_targets: int32 [2, 16, 32], P(None, 'fsdp', 'seq'), may hold values from 0 to 31999
- attention_in: float32 [1, 768, 2316], P(None, ('seq', 'fsdp'))
- attention_in_moment: float32 [1, 768, 2316], P(None, ('seq', 'fsdp')), may hold values from -0.00010681152 to 0.00010681152
- attention_in_average: float32 [1, 768, 2316], P(None, ('seq', 'fsdp')), may hold values from -0.21875 to 0.21875
- attention_out: float32 [1, 768, 768], P(None, ('seq', 'fsdp')), may hold values from -0.875 to 0.875
- attention_out_moment: float32 [1, 768, 768], P(None, ('seq', 'fsdp')), may hold values from -0.00010681152 to 0.00010681152
- attention_out_average: float32 [1, 768, 768], P(None, ('seq', 'fsdp')), may hold values from -0.875 to 0.875
- feed_in: float32 [1, 768, 4096], P(None, ('seq', 'fsdp')), may hold values from -0.21875 to 0.21875
- feed_in_moment: float32 [1, 768, 4096], P(None, ('seq', 'fsdp')), may hold values from -0.00010681152 to 0.00010681152
- feed_in_average: float32 [1, 768, 4096], P(None, ('seq', 'fsdp')), may hold values from -0.21875 to 0.21875
- feed_out: float32 [1, 2048, 768], P(None, ('seq', 'fsdp')), may hold values from -0.125 to 0.125
- feed_out_moment: float32 [1, 2048, 768], P(None, ('seq', 'fsdp')), may hold values from -0.00010681152 to 0.00010681152
- feed_out_average: float32 [1, 2048, 768], P(None, ('seq', 'fsdp')), may hold values from -0.125 to 0.125
- embedding: float32 [32000, 768], P(None, ('seq', 'fsdp'))
- embedding_moment: float32 [32000, 768], P(None, ('seq', 'fsdp')), may hold values from -0.00010681152 to 0.00010681152
- embedding_average: float32 [32000, 768], P(None, ('seq', 'fsdp')), may hold values from -6 to 6
- unembedding: float32 [32000, 768], P(('seq', 'fsdp'))
- unembedding_moment: float32 [32000, 768], P(('seq', 'fsdp')), may hold values from -0.00010681152 to 0.00010681152
- unembedding_average: float32 [32000, 768], P(('seq', 'fsdp')), may hold values from -0.4375 to 0.4375
- gains_biases: float32 [2316], replicated
- gains_biases_moment: float32 [2316], replicated, may hold values from -0.0009765625 to 0.0009765625
- gains_biases_average: float32 [2316], replicated, may hold values from -6 to 6
Outputs:
- loss_value: float32 [], replicated
- grad_norm: float32 [], replicated
- attention_in_new: float32 [1, 768, 2316], P(None, ('seq', 'fsdp'))
- attention_in_moment_new: float32 [1, 768, 2316], P(None, ('seq', 'fsdp'))
- attention_in_average_new: float32 [1, 768, 2316], P(None, ('seq', 'fsdp'))
- attention_out_new: float32 [1, 768, 768], P(None, ('seq', 'fsdp'))
- attention_out_moment_new: float32 [1, 768, 768], P(None, ('seq', 'fsdp'))
- attention_out_average_new: float32 [1, 768, 768], P(None, ('seq', 'fsdp'))
- feed_in_new: float32 [1, 768, 4096], P(None, ('seq', 'fsdp'))
- feed_in_moment_new: float32 [1, 768, 4096], P(None, ('seq', 'fsdp'))
- feed_in_average_new: float32 [1, 768, 4096], P(None, ('seq', 'fsdp'))
- feed_out_new: float32 [1, 2048, 768], P(None, ('seq', 'fsdp'))
- feed_out_moment_new: float32 [1, 2048, 768], P(None, ('seq', 'fsdp'))
- feed_out_average_new: float32 [1, 2048, 768], P(None, ('seq', 'fsdp'))
- embedding_new: float32 [32000, 768], P(None, ('seq', 'fsdp'))
- embedding_moment_new: float32 [32000, 768], P(None, ('seq', 'fsdp'))
- embedding_average_new: float32 [32000, 768], P(None, ('seq', 'fsdp'))
- unembedding_new: float32 [32000, 768], P(('seq', 'fsdp'))
- unembedding_moment_new: float32 [32000, 768], P(('seq', 'fsdp'))
- unembedding_average_new: float32 [32000, 768], P(('seq', 'fsdp'))
- gains_biases_new: float32 [2316], replicated
- gains_biases_moment_new: float32 [2316], replicated
- gains_biases_average_new: float32 [2316], replicated
The draws below stay inside these ranges and needn't reach their ends.
Inputs may be any that keep to these rules, and one draw needn't show every extreme that they name: Each slot holds one sequence of lengths[m, g] tokens at its start, the rest is padding; in each micro-batch one slot is full and another holds 256 tokens. `loss_positions`: column c names a token of the part c // 16 of the slot, counted from that part's start; the 16 positions of one part rise strictly.
All inputs are finite; a program needn't handle non-finite values.
Results may differ from the reference program's by a relative error of at most 0.0025.
The reference program's roundings to bfloat16 on the way count: a program that leaves them out, or rounds other values in their place, can miss the bound.
Values may be sent and summed in bfloat16 or wider, within the bound.
A program may use at most 256 MiB of HBM per device.

```python
import math
import jax
import jax.numpy as jnp
import numpy as np
from jax import lax

D = 768
H = 12
HD = 64
FF = 2048
V = 32000
LAYERS = 1
MICRO = 2
SLOT = 1024
LOSS_DEV = 16
HALF = 512
SEQS = 16
LOSS_SEQ = 32
SMALL = 2316
N_SEQ = 2
N_FSDP = 16


def draw_lengths(key, part):
    base_draw = jax.random.randint(key, (MICRO, SEQS), SLOT // 4, SLOT + 1)
    pick_full = jax.random.randint(jax.random.fold_in(key, 1), (MICRO, 1), 0, SEQS)
    pick_short = (pick_full + 1 + jax.random.randint(jax.random.fold_in(key, 2), (MICRO, 1), 0, SEQS - 1)) % SEQS
    column = jnp.arange(SEQS)[None, :]
    result = jnp.where(column == pick_short, SLOT // 4, base_draw)
    result = jnp.where(column == pick_full, SLOT, result)
    return result.astype(jnp.int32)


def draw_loss_positions(key, part):
    stride = HALF // LOSS_DEV
    offsets = jax.random.randint(key, (MICRO, SEQS, LOSS_SEQ), 0, stride)
    column = jnp.arange(LOSS_SEQ)
    result = (column % LOSS_DEV)[None, None, :] * stride + offsets
    pick_seq = jax.random.randint(jax.random.fold_in(key, 1), (), 0, SEQS)
    seq_ids = jnp.arange(SEQS)[None, :, None]
    result = jnp.where((seq_ids == pick_seq) & (column[None, None, :] == 0), 0, result)
    result = jnp.where((seq_ids == pick_seq) & (column[None, None, :] == LOSS_SEQ - 1), HALF - 1, result)
    return result.astype(jnp.int32)


def draw_attention_in(key, part):
    base_draw = jax.random.normal(key, (LAYERS, D, 3 * D + H), jnp.float32)
    column = jnp.arange(3 * D + H)
    factor = jnp.where(column >= 3 * D, 3.0, 1.0) * D ** (-0.5)
    return base_draw * factor[None, None, :]


def common_feature(key):
    return jax.random.normal(jax.random.fold_in(key, 9137), (D,), jnp.float32)


def draw_embedding(key, part):
    base_draw = jax.random.normal(jax.random.fold_in(key, 5), (V, D), jnp.float32)
    return base_draw + common_feature(key)[None, :]


def draw_unembedding(key, part):
    base_draw = jax.random.normal(jax.random.fold_in(key, 6), (V, D), jnp.float32) * (D // 4) ** (-0.5)
    block_size = V // (N_SEQ * N_FSDP)
    row_block = jnp.arange(V) // block_size
    lift = jnp.where(row_block % 2 == 0, 2.0, -1.0) / D
    return base_draw + lift[:, None] * common_feature(key)[None, :]


def draw_gains_biases(key, part):
    gains = jax.random.uniform(key, ((2 * LAYERS + 1) * D,), jnp.float32, 0.6, 1.4)
    biases = jax.random.uniform(jax.random.fold_in(key, 1), (LAYERS * H,), jnp.float32, 3.0, 9.0)
    return jnp.concatenate([gains, biases])


def set_ends(drawn, rng, smallest, top_value):
    spot = [jax.random.randint(jax.random.fold_in(rng, axis), (), 0, length) for axis, length in enumerate(drawn.shape)]
    widest = drawn.shape.index(max(drawn.shape))
    neighbour = spot[:widest] + [(spot[widest] + 1) % drawn.shape[widest]] + spot[widest + 1:]
    return drawn.at[tuple(spot)].set(smallest).at[tuple(neighbour)].set(top_value)


def steps_of(rng, extent, cuts, smallest, high):
    level, own = 1.0, jax.random.fold_in(rng, 6)
    for axis_at, shards_of in cuts:
        draws = jnp.exp(jax.random.uniform(jax.random.fold_in(own, axis_at), (shards_of,), jnp.float32, smallest / len(cuts), high / len(cuts)))
        level = level * jnp.repeat(draws, extent[axis_at] // shards_of).reshape([-1 if axis == axis_at else 1 for axis in range(len(extent))])
    return level


def rank_table(count, skew):
    weights = [(1 << 20) // math.isqrt(rank ** skew) + 1 for rank in range(1, count + 1)]
    deviation = 1 + sum(weights) // (1 << 30)
    return np.cumsum(np.array([max(1, weight // deviation) for weight in weights]))


def skewed_ids(own_key, shape, number_of, lean):
    table = rank_table(number_of, lean)
    lot = jax.random.randint(jax.random.fold_in(own_key, 1), shape, 0, int(table[number_of - 1]))
    grade = jnp.searchsorted(jnp.asarray(table, jnp.int32), lot, side="right")
    return jax.random.permutation(jax.random.fold_in(own_key, 2), number_of)[grade].astype(jnp.int32)


def bell_draw(stream_key, dims, width, most, cuts=(), kind=jnp.bfloat16):
    array = width * jax.random.normal(stream_key, dims, jnp.float32)
    if cuts:
        array = array * steps_of(stream_key, dims, cuts, -0.22, 0.18)
    return jnp.clip(array, -most, most).astype(kind)


def setup_inputs(seed: int = 0) -> dict:
    arg_keys = jax.random.split(jax.random.key(seed), 26)
    token_ids = set_ends(skewed_ids(arg_keys[0], (MICRO, SEQS, SLOT), V, 2), jax.random.fold_in(arg_keys[0], 3), 0, V - 1).astype(jnp.int32)
    lengths = draw_lengths(jax.random.fold_in(arg_keys[25], 71), 0)
    loss_positions = draw_loss_positions(jax.random.fold_in(arg_keys[25], 71), 0)
    loss_targets = set_ends(skewed_ids(arg_keys[3], (MICRO, SEQS, LOSS_SEQ), V, 2), jax.random.fold_in(arg_keys[3], 3), 0, V - 1).astype(jnp.int32)
    attention_in = draw_attention_in(jax.random.fold_in(arg_keys[25], 71), 0)
    attention_in_moment = bell_draw(arg_keys[5], (LAYERS, D, 3 * D + H), (0.055 * (LAYERS * (4 * D * D + D * H + 3 * D * FF) + 2 * V * D) ** -0.5), 0.00010681152, ((1, 32),), jnp.float32)
    attention_in_average = bell_draw(arg_keys[6], (LAYERS, D, 3 * D + H), D ** -0.5, 0.21875, ((1, 32),), jnp.float32)
    attention_out = bell_draw(arg_keys[7], (LAYERS, D, D), (D // 16) ** -0.5, 0.875, ((1, 32),), jnp.float32)
    attention_out_moment = bell_draw(arg_keys[8], (LAYERS, D, D), (0.055 * (LAYERS * (4 * D * D + D * H + 3 * D * FF) + 2 * V * D) ** -0.5), 0.00010681152, ((1, 32),), jnp.float32)
    attention_out_average = bell_draw(arg_keys[9], (LAYERS, D, D), (D // 16) ** -0.5, 0.875, ((1, 32),), jnp.float32)
    feed_in = bell_draw(arg_keys[10], (LAYERS, D, 2 * FF), D ** -0.5, 0.21875, ((1, 32),), jnp.float32)
    feed_in_moment = bell_draw(arg_keys[11], (LAYERS, D, 2 * FF), (0.055 * (LAYERS * (4 * D * D + D * H + 3 * D * FF) + 2 * V * D) ** -0.5), 0.00010681152, ((1, 32),), jnp.float32)
    feed_in_average = bell_draw(arg_keys[12], (LAYERS, D, 2 * FF), D ** -0.5, 0.21875, ((1, 32),), jnp.float32)
    feed_out = bell_draw(arg_keys[13], (LAYERS, FF, D), FF ** -0.5, 0.125, ((1, 32),), jnp.float32)
    feed_out_moment = bell_draw(arg_keys[14], (LAYERS, FF, D), (0.055 * (LAYERS * (4 * D * D + D * H + 3 * D * FF) + 2 * V * D) ** -0.5), 0.00010681152, ((1, 32),), jnp.float32)
    feed_out_average = bell_draw(arg_keys[15], (LAYERS, FF, D), FF ** -0.5, 0.125, ((1, 32),), jnp.float32)
    embedding = draw_embedding(jax.random.fold_in(arg_keys[25], 71), 0)
    embedding_moment = bell_draw(arg_keys[17], (V, D), (0.055 * (LAYERS * (4 * D * D + D * H + 3 * D * FF) + 2 * V * D) ** -0.5), 0.00010681152, ((1, 32),), jnp.float32)
    embedding_average = bell_draw(arg_keys[18], (V, D), 1.0, 6.0, ((1, 32),), jnp.float32)
    unembedding = draw_unembedding(jax.random.fold_in(arg_keys[25], 71), 0)
    unembedding_moment = bell_draw(arg_keys[20], (V, D), (0.055 * (LAYERS * (4 * D * D + D * H + 3 * D * FF) + 2 * V * D) ** -0.5), 0.00010681152, ((0, 32),), jnp.float32)
    unembedding_average = bell_draw(arg_keys[21], (V, D), (D // 4) ** -0.5, 0.4375, ((0, 32),), jnp.float32)
    gains_biases = draw_gains_biases(jax.random.fold_in(arg_keys[25], 71), 0)
    gains_biases_moment = bell_draw(arg_keys[23], (SMALL,), (0.55 * (LAYERS * (4 * D * D + D * H + 3 * D * FF) + 2 * V * D) ** -0.5), 0.0009765625, (), jnp.float32)
    gains_biases_average = bell_draw(arg_keys[24], (SMALL,), 1.0, 6.0, (), jnp.float32)
    return {"token_ids": token_ids, "lengths": lengths, "loss_positions": loss_positions, "loss_targets": loss_targets, "attention_in": attention_in, "attention_in_moment": attention_in_moment, "attention_in_average": attention_in_average, "attention_out": attention_out, "attention_out_moment": attention_out_moment, "attention_out_average": attention_out_average, "feed_in": feed_in, "feed_in_moment": feed_in_moment, "feed_in_average": feed_in_average, "feed_out": feed_out, "feed_out_moment": feed_out_moment, "feed_out_average": feed_out_average, "embedding": embedding, "embedding_moment": embedding_moment, "embedding_average": embedding_average, "unembedding": unembedding, "unembedding_moment": unembedding_moment, "unembedding_average": unembedding_average, "gains_biases": gains_biases, "gains_biases_moment": gains_biases_moment, "gains_biases_average": gains_biases_average}


@jax.custom_vjp
def low(v):
    return lax.optimization_barrier(v.astype(jnp.bfloat16)).astype(jnp.float32)

@jax.custom_vjp
def low_back(v):
    return v

def low_keep(v):
    return (low(v), None)

def low_pass(kept, grad):
    return (grad,)

def back_keep(v):
    return (v, None)

def back_low(kept, grad):
    return (low(grad),)
low.defvjp(low_keep, low_pass)
low_back.defvjp(back_keep, back_low)
epsilon = 1e-06
smooth = 0.1
z_weight = 0.005
clip_limit = 0.5
moment = 0.9
average = 0.9
rate_layer = 200.0
rate_head = 1000.0
rate_embed = 5000.0
highest = lax.Precision.HIGHEST

def matmul(left_side, right_side):
    return jnp.dot(left_side, right_side, precision=highest, preferred_element_type=jnp.float32)

def rms_scale(values, gain_row):
    return values * lax.rsqrt(lax.optimization_barrier(jnp.mean(values * values, axis=-1, keepdims=True)) + epsilon) * gain_row

def sequence_loss(lowered, gain_rows, biases, token_row, length, positions, targets, weight):
    attention_in, attention_out, feed_in, feed_out, embed_low, head_low = lowered
    residual = low_back(jnp.take(embed_low, token_row, axis=0))
    places = jnp.arange(SLOT)
    causal = places[:, None] >= places[None, :]
    for layer_index in range(LAYERS):
        normed = low(rms_scale(residual, gain_rows[2 * layer_index]))
        project = matmul(normed, attention_in[layer_index])
        project = jnp.concatenate([project[:, :3 * D], project[:, 3 * D:] + biases[layer_index]], axis=1)
        project = low_back(low(project))
        query_rows = project[:, :D].reshape(SLOT, H, HD)
        key_rows = project[:, D:2 * D].reshape(SLOT, H, HD)
        value_rows = project[:, 2 * D:3 * D].reshape(SLOT, H, HD)
        decay_sum = jnp.cumsum(jax.nn.log_sigmoid(project[:, 3 * D:]), axis=0).T
        scores = jnp.einsum('ihd,jhd->hij', query_rows, key_rows, precision=highest) * HD ** (-0.5)
        scores = low_back(scores + decay_sum[:, :, None] - decay_sum[:, None, :])
        scores = jnp.where(causal[None], scores, -1e+30)
        log_total = jax.nn.logsumexp(scores, axis=-1, keepdims=True)
        attention = low(jnp.exp(scores - log_total))
        mixed_heads = jnp.einsum('hij,jhd->ihd', attention, value_rows, precision=highest).reshape(SLOT, D)
        mixed_heads = low_back(low(mixed_heads))
        residual = residual + low_back(matmul(mixed_heads, attention_out[layer_index]))
        normed = low(rms_scale(residual, gain_rows[2 * layer_index + 1]))
        gate_up = low_back(matmul(normed, feed_in[layer_index]))
        hidden = low(jax.nn.silu(gate_up[:, :FF]) * gate_up[:, FF:])
        residual = residual + low_back(matmul(hidden, feed_out[layer_index]))
    halves = jnp.arange(LOSS_SEQ) // LOSS_DEV
    places_all = positions + halves * HALF
    loss_rows = jnp.take(residual, places_all, axis=0)
    final_rows = low(rms_scale(loss_rows, gain_rows[2 * LAYERS]))
    logits = low_back(matmul(final_rows, head_low.T))
    row_total = jax.nn.logsumexp(logits, axis=-1)
    target_logit = jnp.take_along_axis(logits, targets[:, None], axis=1)[:, 0]
    per_row = row_total - (1.0 - smooth) * target_logit - smooth * lax.optimization_barrier(jnp.mean(logits, axis=-1)) + z_weight * row_total * row_total
    counted = places_all < length
    return jnp.sum(jnp.where(counted, per_row, 0.0)) * weight

def apply_update(weight_old, grad_full, moment_old, average_old, factor, rate):
    clipped = factor * grad_full
    moment_new = moment * moment_old + clipped
    weight_new = weight_old - rate * (clipped + moment * moment_new)
    average_new = average * average_old + (1.0 - average) * weight_new
    return (weight_new, moment_new, average_new)

def reference(token_ids, lengths, loss_positions, loss_targets, attention_in, attention_in_moment, attention_in_average, attention_out, attention_out_moment, attention_out_average, feed_in, feed_in_moment, feed_in_average, feed_out, feed_out_moment, feed_out_average, embedding, embedding_moment, embedding_average, unembedding, unembedding_moment, unembedding_average, gains_biases, gains_biases_moment, gains_biases_average):
    halves = jnp.arange(LOSS_SEQ) // LOSS_DEV
    counted = loss_positions + halves[None, None, :] * HALF < lengths[:, :, None]
    counts = lax.optimization_barrier(jnp.sum(counted.astype(jnp.int32), axis=(1, 2)))
    scales = 1.0 / (MICRO * counts.astype(jnp.float32))
    seq_scale = jnp.broadcast_to(scales[:, None], (MICRO, SEQS)).reshape(MICRO * SEQS)
    flat_tokens = token_ids.reshape(MICRO * SEQS, SLOT)
    flat_lengths = lengths.reshape(MICRO * SEQS)
    flat_positions = loss_positions.reshape(MICRO * SEQS, LOSS_SEQ)
    flat_targets = loss_targets.reshape(MICRO * SEQS, LOSS_SEQ)

    def step_loss(params):
        lowered = tuple((low(matrix_one) for matrix_one in params[:6]))
        gain_rows = params[6][:(2 * LAYERS + 1) * D].reshape(2 * LAYERS + 1, D)
        biases = params[6][(2 * LAYERS + 1) * D:].reshape(LAYERS, H)
        checked = jax.checkpoint(sequence_loss)

        def advance(running, sequence_item):
            token_row, length, positions, targets, weight = sequence_item
            return (running + checked(lowered, gain_rows, biases, token_row, length, positions, targets, weight), None)
        summed, unused = lax.scan(advance, jnp.zeros((), jnp.float32), (flat_tokens, flat_lengths, flat_positions, flat_targets, seq_scale))
        return summed
    params = (attention_in, attention_out, feed_in, feed_out, embedding, unembedding, gains_biases)
    loss_value, pullback = jax.vjp(step_loss, params)
    grads = pullback(jnp.ones((), jnp.float32))[0]
    square_sum = jnp.zeros((), jnp.float32)
    for grad_part in grads:
        square_sum = square_sum + jnp.sum(grad_part * grad_part)
    grad_norm = jnp.sqrt(square_sum)
    factor = jnp.minimum(1.0, clip_limit / grad_norm)
    first = apply_update(attention_in, grads[0], attention_in_moment, attention_in_average, factor, rate_layer)
    second = apply_update(attention_out, grads[1], attention_out_moment, attention_out_average, factor, rate_layer)
    third = apply_update(feed_in, grads[2], feed_in_moment, feed_in_average, factor, rate_layer)
    fourth = apply_update(feed_out, grads[3], feed_out_moment, feed_out_average, factor, rate_layer)
    fifth = apply_update(embedding, grads[4], embedding_moment, embedding_average, factor, rate_embed)
    sixth = apply_update(unembedding, grads[5], unembedding_moment, unembedding_average, factor, rate_head)
    seventh = apply_update(gains_biases, grads[6], gains_biases_moment, gains_biases_average, factor, rate_layer)
    return (loss_value, grad_norm, first[0], first[1], first[2], second[0], second[1], second[2], third[0], third[1], third[2], fourth[0], fourth[1], fourth[2], fifth[0], fifth[1], fifth[2], sixth[0], sixth[1], sixth[2], seventh[0], seventh[1], seventh[2])
```

```python
import functools

import jax
import jax.numpy as jnp
from jax import lax
from jax.experimental import pallas as pl
from jax.experimental.pallas import tpu as pltpu
from jax.sharding import PartitionSpec as P

D = 768
H = 12
HD = 64
FF = 2048
V = 32000


epsilon = 1e-06
smooth = 0.1
z_weight = 0.005
clip_limit = 0.5
moment = 0.9
average = 0.9
rate_layer = 200.0
rate_head = 1000.0
rate_embed = 5000.0
negative = -1e30
both = ("seq", "fsdp")
highest = lax.Precision.HIGHEST
MESH = pl.DeviceIdType.MESH


def dot(left_side, right_side, left_axis, right_axis, precision=None):
    return lax.dot_general(
        left_side,
        right_side,
        (((left_axis,), (right_axis,)), ((), ())),
        precision=precision,
        preferred_element_type=jnp.float32,
    )


def line_of(fsdp_count):
    return 4 if fsdp_count % 4 == 0 else 1


def gather_kernel(cores, fsdp, x_ref, o_ref, send_sem, recv_sem):
    plane = line_of(fsdp)
    lines = fsdp // plane
    core = lax.axis_index("seq")
    spot = lax.axis_index("fsdp")
    high, low = spot // plane, spot % plane
    line_peers = [((high + k) % lines) * plane + low for k in range(1, lines)]
    plane_peers = [high * plane + (low + k) % plane for k in range(1, plane)]
    core_peers = [(core + k) % cores for k in range(1, cores)]
    peers = [(core, p) for p in line_peers + plane_peers] + [(c, spot) for c in core_peers]

    barrier = pltpu.get_barrier_semaphore()
    for peer in peers:
        pl.semaphore_signal(barrier, inc=1, device_id=peer, device_id_type=MESH)
    pl.semaphore_wait(barrier, len(peers))

    sent = []

    def send(source_ref, block, peer):
        copy = pltpu.make_async_remote_copy(
            src_ref=source_ref,
            dst_ref=o_ref.at[block],
            send_sem=send_sem.at[len(sent)],
            recv_sem=recv_sem.at[block],
            device_id=peer,
            device_id_type=MESH,
        )
        copy.start()
        sent.append(copy)

    def arrived(block):
        pltpu.make_async_copy(o_ref.at[block], o_ref.at[block], recv_sem.at[block]).wait()

    mine = core * fsdp + spot
    for p in line_peers:
        send(x_ref, mine, (core, p))
    for p in plane_peers:
        send(x_ref, mine, (core, p))
    for c in core_peers:
        send(x_ref, mine, (c, spot))
    o_ref[mine] = x_ref[...]
    for k in range(1, lines):
        block = core * fsdp + ((high + lines - k) % lines) * plane + low
        arrived(block)
        for p in plane_peers:
            send(o_ref.at[block], block, (core, p))
        for c in core_peers:
            send(o_ref.at[block], block, (c, spot))
    for m in range(lines):
        for k in range(1, plane):
            block = core * fsdp + ((high + lines - m) % lines) * plane + (low + plane - k) % plane
            arrived(block)
            for c in core_peers:
                send(o_ref.at[block], block, (c, spot))
    for c in core_peers:
        for m in range(lines):
            for k in range(plane):
                block = c * fsdp + ((high + lines - m) % lines) * plane + (low + plane - k) % plane
                arrived(block)
    for copy in sent:
        copy.wait_send()


def gather_rows(array, collective):
    cores, fsdp = lax.axis_size("seq"), lax.axis_size("fsdp")
    count = cores * fsdp
    return pl.pallas_call(
        functools.partial(gather_kernel, cores, fsdp),
        out_shape=jax.ShapeDtypeStruct((count,) + array.shape, array.dtype),
        in_specs=[pl.BlockSpec(memory_space=pltpu.VMEM)],
        out_specs=pl.BlockSpec(memory_space=pltpu.VMEM),
        scratch_shapes=[
            pltpu.SemaphoreType.DMA((count,)),
            pltpu.SemaphoreType.DMA((count,)),
        ],
        compiler_params=pltpu.CompilerParams(collective_id=collective, has_side_effects=True),
        name="gather_rows",
    )(array)


def other_core(arrays):
    return lax.ppermute(arrays, "seq", [(0, 1), (1, 0)])


def norm_forward(values, gain_row):
    inverse = lax.rsqrt(jnp.mean(values * values, axis=-1, keepdims=True) + epsilon)
    return (values * inverse * gain_row, inverse)


def norm_backward(values, inverse, gain_row, grad_out):
    scaled = grad_out * gain_row
    grad_gain = jnp.sum(grad_out * values * inverse, axis=0)
    grad_in = inverse * scaled - values * inverse**3 * jnp.mean(
        values * scaled, axis=-1, keepdims=True
    )
    return (grad_in, grad_gain)


def apply_update(weight_old, grad_full, moment_old, average_old, factor, rate):
    clipped = factor * grad_full
    moment_new = moment * moment_old + clipped
    weight_new = weight_old - rate * (clipped + moment * moment_new)
    average_new = average * average_old + (1.0 - average) * weight_new
    return (weight_new, moment_new, average_new)


def on_device(
    token_ids,
    lengths,
    loss_positions,
    loss_targets,
    attention_in,
    attention_in_moment,
    attention_in_average,
    attention_out,
    attention_out_moment,
    attention_out_average,
    feed_in,
    feed_in_moment,
    feed_in_average,
    feed_out,
    feed_out_moment,
    feed_out_average,
    embedding,
    embedding_moment,
    embedding_average,
    unembedding,
    unembedding_moment,
    unembedding_average,
    gains_biases,
    gains_biases_moment,
    gains_biases_average,
):
    low = jnp.bfloat16
    wide = jnp.float32
    devices_all = lax.axis_size(both)
    seq_index = lax.axis_index("seq")
    device = lax.axis_index(both)
    micros, _, half = token_ids.shape
    loss_dev = loss_positions.shape[2]
    tokens = micros * half
    rows = micros * loss_dev
    rows_all = devices_all * rows
    vocab_here = unembedding.shape[0]
    features = D // devices_all
    gate_here = FF // devices_all
    gain_rows = gains_biases[: 3 * D].reshape(3, D)
    bias_row = gains_biases[3 * D :]
    second = seq_index.astype(wide)

    positions = loss_positions[:, 0]
    targets = loss_targets[:, 0]
    counted = (seq_index * half + positions < lengths[:, :1]).astype(jnp.int32)
    labels = jnp.concatenate([targets.reshape(-1), counted.reshape(-1)])
    ids_block = jnp.concatenate([token_ids.reshape(-1), labels])
    pad = -ids_block.shape[0] % 1024
    ids_block = jnp.pad(ids_block, (0, pad)).reshape(-1, 128)
    ids_all = gather_rows(ids_block, 1).reshape(devices_all, -1)
    all_tokens = ids_all[:, :tokens]
    all_targets = ids_all[:, tokens : tokens + rows].reshape(-1)
    all_counted = ids_all[:, tokens + rows : tokens + 2 * rows]

    w_in = lax.all_gather(attention_in[0].astype(low), both, axis=0, tiled=True)
    w_out = lax.all_gather(attention_out[0].astype(low), both, axis=0, tiled=True)
    w_feed = lax.all_gather(feed_in[0].astype(low), both, axis=0, tiled=True)
    w_down = lax.all_gather(feed_out[0].astype(low), both, axis=0, tiled=True)
    head_low = unembedding.astype(low)

    looked = jnp.take(embedding.astype(low), all_tokens, axis=0)
    arrived = lax.all_to_all(
        jnp.swapaxes(looked, 1, 2), both, split_axis=0, concat_axis=0, tiled=True
    )
    x_t = arrived.reshape(D, tokens)
    x_wide = x_t.astype(wide)
    inverse_one = lax.rsqrt(jnp.mean(x_wide * x_wide, axis=0, keepdims=True) + epsilon)
    normed_t = (x_wide * inverse_one * gain_rows[0][:, None]).astype(low)

    project_t = dot(w_in[:, D:], normed_t, 0, 0)
    kv_t = project_t[: 2 * D].astype(low)
    forget_t = (project_t[2 * D :] + bias_row[:, None]).astype(low).astype(wide)
    pick = [
        (positions[m][:, None] == jnp.arange(half)[None, :]).astype(low) for m in range(micros)
    ]

    def per_micro(array, m):
        return array[:, m * half : (m + 1) * half]

    x_rows = jnp.concatenate([dot(pick[m], per_micro(x_t, m), 1, 1) for m in range(micros)])
    normed_rows = jnp.concatenate(
        [dot(pick[m], per_micro(normed_t, m), 1, 1) for m in range(micros)]
    ).astype(low)
    q_rows = dot(normed_rows, w_in[:, :D], 1, 0).astype(low)

    upper = (jnp.arange(half)[:, None] <= jnp.arange(half)[None, :]).astype(wide)
    log_gate = jax.nn.log_sigmoid(forget_t).reshape(H, micros, half)
    decay_own = lax.dot_general(
        log_gate, upper, (((2,), (0,)), ((), ())), precision=highest, preferred_element_type=wide
    )
    total_own = decay_own[:, :, -1]
    decay_rows = jnp.stack(
        [dot(pick[m].astype(wide), decay_own[:, m], 1, 1, highest) for m in range(micros)]
    )
    q_own = q_rows.reshape(micros, loss_dev, H, HD)
    q_far, decay_far, total_far, place_far = other_core((q_own, decay_rows, total_own, positions))
    shift_own = second * total_far
    shift_far = (1.0 - second) * total_own
    key_decay = decay_own + shift_own[:, :, None]
    row_decay = jnp.concatenate(
        [decay_rows + shift_own.T[:, None], decay_far + shift_far.T[:, None]], axis=1
    )
    q_all = jnp.concatenate([q_own, q_far], axis=1)
    places = jnp.concatenate(
        [positions + seq_index * half, place_far + (1 - seq_index) * half], axis=1
    )
    key_places = seq_index * half + jnp.arange(half)
    keys_t = kv_t[:D].reshape(H, HD, tokens)
    values_t = kv_t[D:].reshape(H, HD, tokens)

    scores = []
    for m in range(micros):
        keys_m = keys_t[:, :, m * half : (m + 1) * half]
        raw = jnp.einsum("rhd,hdj->hrj", q_all[m], keys_m, preferred_element_type=wide)
        part = raw * HD ** (-0.5) + row_decay[m].T[:, :, None] - key_decay[:, m][:, None, :]
        causal = places[m][:, None] >= key_places[None, :]
        scores.append(jnp.where(causal[None], part, negative))
    scores = jnp.stack(scores)
    peak_own = jnp.max(scores, axis=-1)
    spread_own = jnp.sum(jnp.exp(scores - peak_own[..., None]), axis=-1)
    peak_far, spread_far = other_core((peak_own, spread_own))

    def swap_rows(array):
        return jnp.concatenate([array[:, :, loss_dev:], array[:, :, :loss_dev]], axis=2)

    peak_far, spread_far = swap_rows(peak_far), swap_rows(spread_far)
    peak = jnp.maximum(peak_own, peak_far)
    log_total = peak + jnp.log(
        spread_own * jnp.exp(peak_own - peak) + spread_far * jnp.exp(peak_far - peak)
    )
    probs = jnp.exp(scores - log_total[..., None])
    probs_low = probs.astype(low)
    probs_rest = (probs - probs_low.astype(wide)).astype(low)

    def mix(weights):
        return jnp.stack(
            [
                jnp.einsum(
                    "hrj,hdj->rhd",
                    weights[m],
                    values_t[:, :, m * half : (m + 1) * half],
                    preferred_element_type=wide,
                )
                for m in range(micros)
            ]
        )

    mixed_part = mix(probs_low)
    rest_part = mix(probs_rest)
    mixed_far, rest_far = other_core((mixed_part[:, loss_dev:], rest_part[:, loss_dev:]))
    mixed_sum = mixed_part[:, :loss_dev] + mixed_far
    mixed_full = mixed_sum + rest_part[:, :loss_dev] + rest_far
    mixed_rows = mixed_sum.reshape(rows, D).astype(low)

    middle = x_rows + dot(mixed_rows, w_out, 1, 0)
    normed_two, inverse_two = norm_forward(middle, gain_rows[1])
    normed_two = normed_two.astype(low)
    gate_up = dot(normed_two, w_feed, 1, 0)
    gate_half, up_half = gate_up[:, :FF], gate_up[:, FF:]
    gate_sigmoid = jax.nn.sigmoid(gate_half)
    hidden = (gate_half * gate_sigmoid * up_half).astype(low)
    final_in = middle + dot(hidden, w_down, 1, 0)
    final_normed, final_inverse = norm_forward(final_in, gain_rows[2])

    final_all = gather_rows(final_normed.astype(low), 2).reshape(rows_all, D)
    logits = dot(final_all, head_low, 1, 1)
    vocab_ids = device * vocab_here + jnp.arange(vocab_here)
    target_hits = all_targets[:, None] == vocab_ids[None, :]
    row_peak = jnp.max(logits, axis=1)
    exp_sum = jnp.sum(jnp.exp(logits - row_peak[:, None]), axis=1)
    target_part = jnp.sum(jnp.where(target_hits, logits, 0.0), axis=1)
    logit_sum = jnp.sum(logits, axis=1)
    stats = jnp.stack([row_peak, exp_sum, target_part, logit_sum])
    stats_all = gather_rows(stats.reshape(-1, 128), 3).reshape(devices_all, 4, rows_all)
    peak_all = jnp.max(stats_all[:, 0], axis=0)
    spread_all = jnp.sum(stats_all[:, 1] * jnp.exp(stats_all[:, 0] - peak_all), axis=0)
    target_all = jnp.sum(stats_all[:, 2], axis=0)
    logit_all = jnp.sum(stats_all[:, 3], axis=0)
    total_all = peak_all + jnp.log(spread_all)
    per_row = (
        total_all
        - (1.0 - smooth) * target_all
        - smooth * logit_all / V
        + z_weight * total_all * total_all
    )
    weights_row = all_counted.astype(wide).reshape(devices_all, micros, loss_dev)
    counts = jnp.sum(weights_row, axis=(0, 2))
    weights_row = (weights_row / (micros * counts)[None, :, None]).reshape(-1)
    loss_value = jnp.sum(weights_row * per_row)
    soft_rows = jnp.exp(logits - total_all[:, None])
    grad_logits = (
        weights_row[:, None]
        * (
            soft_rows * (1.0 + 2.0 * z_weight * total_all)[:, None]
            - (1.0 - smooth) * target_hits.astype(wide)
            - smooth / V
        )
    ).astype(low)
    head_grad = dot(grad_logits, final_all, 0, 0)
    grad_final = lax.psum_scatter(
        dot(grad_logits, head_low, 1, 0), both, scatter_dimension=0, tiled=True
    )

    grad_rows, gain_grad_final = norm_backward(final_in, final_inverse, gain_rows[2], grad_final)
    grad_branch = grad_rows.astype(low)
    grad_hidden = dot(grad_branch, w_down, 1, 1)
    grad_gate = grad_hidden * up_half * gate_sigmoid * (1.0 + gate_half * (1.0 - gate_sigmoid))
    grad_up = grad_hidden * gate_half * gate_sigmoid
    grad_gate_up = jnp.concatenate([grad_gate, grad_up], axis=1).astype(low)
    grad_two, gain_grad_two = norm_backward(
        middle, inverse_two, gain_rows[1], dot(grad_gate_up, w_feed, 1, 1)
    )
    grad_middle = grad_rows + grad_two
    grad_mid_low = grad_middle.astype(low)
    grad_mixed = dot(grad_mid_low, w_out, 1, 1).astype(low)

    normed_two_all = lax.all_gather(normed_two, both, axis=0, tiled=True)
    grad_branch_all = lax.all_gather(grad_branch, both, axis=0, tiled=True)
    hidden_columns = lax.all_to_all(
        hidden.reshape(rows, devices_all, gate_here), both, split_axis=1, concat_axis=0, tiled=True
    ).reshape(rows_all, gate_here)
    grad_down = dot(hidden_columns, grad_branch_all, 0, 0)
    gate_up_columns = lax.all_to_all(
        grad_gate_up.reshape(rows, 2, devices_all, gate_here),
        both,
        split_axis=2,
        concat_axis=0,
        tiled=True,
    ).reshape(rows_all, 2 * gate_here)
    grad_feed_columns = dot(normed_two_all, gate_up_columns, 0, 0)
    grad_feed = lax.all_to_all(
        grad_feed_columns.reshape(devices_all, features, 2 * gate_here),
        both,
        split_axis=0,
        concat_axis=0,
        tiled=True,
    )
    grad_feed = (
        grad_feed.reshape(devices_all, features, 2, gate_here)
        .transpose(1, 2, 0, 3)
        .reshape(features, 2 * FF)
    )
    grad_out = lax.psum_scatter(
        dot(mixed_rows, grad_mid_low, 0, 0), both, scatter_dimension=0, tiled=True
    )

    grad_own = grad_mixed.reshape(micros, loss_dev, H, HD)
    inner_own = jnp.sum(grad_own.astype(wide) * mixed_full, axis=-1)
    grad_far, inner_far = other_core((grad_own, inner_own))
    grad_heads = jnp.concatenate([grad_own, grad_far], axis=1)
    inner_sum = jnp.concatenate([inner_own, inner_far], axis=1)
    query_parts, score_rows = [], []
    grad_keys, grad_values, score_columns = [], [], []
    for m in range(micros):
        keys_m = keys_t[:, :, m * half : (m + 1) * half]
        values_m = values_t[:, :, m * half : (m + 1) * half]
        grad_probs = jnp.einsum("rhd,hdj->hrj", grad_heads[m], values_m, preferred_element_type=wide)
        grad_scores = (probs[m] * (grad_probs - inner_sum[m].T[:, :, None])).astype(low)
        query_parts.append(
            jnp.einsum("hrj,hdj->rhd", grad_scores, keys_m, preferred_element_type=wide)
        )
        grad_keys.append(
            jnp.einsum("hrj,rhd->hdj", grad_scores, q_all[m], preferred_element_type=wide)
            * HD ** (-0.5)
        )
        grad_values.append(
            jnp.einsum("hrj,rhd->hdj", probs_low[m], grad_heads[m], preferred_element_type=wide)
        )
        score_wide = grad_scores.astype(wide)
        score_rows.append(jnp.sum(score_wide, axis=-1))
        score_columns.append(jnp.sum(score_wide, axis=1))
    query_parts = jnp.stack(query_parts)
    score_rows = jnp.stack(score_rows).transpose(0, 2, 1)
    query_far, score_far = other_core((query_parts[:, loss_dev:], score_rows[:, loss_dev:]))
    grad_query = ((query_parts[:, :loss_dev] + query_far) * HD ** (-0.5)).astype(low)
    grad_query = grad_query.reshape(rows, D)
    rows_sum = score_rows[:, :loss_dev] + score_far
    later = (1.0 - second) * jnp.sum(score_rows[:, loss_dev:], axis=1)
    grad_log = []
    for m in range(micros):
        placed = dot(rows_sum[m], pick[m].astype(wide), 0, 0, highest)
        change = placed - score_columns[m]
        suffix = dot(change, upper, 1, 1, highest)
        grad_log.append(suffix + later[m][:, None])
    grad_log = jnp.concatenate(grad_log, axis=1)
    grad_forget = (grad_log * jax.nn.sigmoid(-forget_t)).astype(low)
    query_t = jnp.concatenate(
        [
            dot(grad_query[m * loss_dev : (m + 1) * loss_dev], pick[m], 0, 0).astype(low)
            for m in range(micros)
        ],
        axis=1,
    )
    keys_part = jnp.concatenate(grad_keys, axis=2).reshape(D, tokens).astype(low)
    values_part = jnp.concatenate(grad_values, axis=2).reshape(D, tokens).astype(low)
    grad_project = jnp.concatenate([query_t, keys_part, values_part, grad_forget], axis=0)
    grad_bias = jnp.sum(grad_forget.astype(wide), axis=1)
    grad_in = lax.psum_scatter(
        dot(normed_t, grad_project, 1, 1), both, scatter_dimension=0, tiled=True
    )
    grad_normed = dot(w_in, grad_project, 1, 0)
    scaled = grad_normed * gain_rows[0][:, None]
    gain_grad_one = jnp.sum(grad_normed * x_wide * inverse_one, axis=1)
    grad_one = inverse_one * scaled - x_wide * inverse_one**3 * jnp.mean(
        x_wide * scaled, axis=0, keepdims=True
    )
    middle_t = jnp.concatenate(
        [
            dot(
                grad_middle[m * loss_dev : (m + 1) * loss_dev],
                pick[m].astype(wide),
                0,
                0,
                highest,
            )
            for m in range(micros)
        ],
        axis=1,
    )
    grad_embed = (middle_t + grad_one).astype(low).reshape(devices_all, features, tokens)
    moved = lax.all_to_all(grad_embed, both, split_axis=0, concat_axis=0, tiled=True)
    embed_grad = jax.ops.segment_sum(
        jnp.swapaxes(moved, 1, 2).reshape(-1, features).astype(wide),
        all_tokens.reshape(-1),
        num_segments=V,
    )

    owned_grads = [grad_in[None], grad_out[None], grad_feed[None], grad_down[None]]
    owned_grads = owned_grads + [embed_grad, head_grad]
    square_sum = jnp.zeros((), wide)
    for grad_part in owned_grads:
        square_sum = square_sum + jnp.sum(grad_part * grad_part)
    small_grad = jnp.concatenate(
        [gain_grad_one, gain_grad_two, gain_grad_final, grad_bias, square_sum[None]]
    )
    small_count = small_grad.shape[0]
    small_grad = jnp.pad(small_grad, (0, -small_count % 1024)).reshape(-1, 128)
    small_sum = jnp.sum(gather_rows(small_grad, 4), axis=0).reshape(-1)
    small_total, square_total = small_sum[: small_count - 1], small_sum[small_count - 1]
    grad_norm = jnp.sqrt(square_total + jnp.sum(small_total * small_total))
    factor = jnp.minimum(1.0, clip_limit / grad_norm)
    updates = (
        (attention_in, owned_grads[0], attention_in_moment, attention_in_average, rate_layer),
        (attention_out, owned_grads[1], attention_out_moment, attention_out_average, rate_layer),
        (feed_in, owned_grads[2], feed_in_moment, feed_in_average, rate_layer),
        (feed_out, owned_grads[3], feed_out_moment, feed_out_average, rate_layer),
        (embedding, embed_grad, embedding_moment, embedding_average, rate_embed),
        (unembedding, head_grad, unembedding_moment, unembedding_average, rate_head),
        (gains_biases, small_total, gains_biases_moment, gains_biases_average, rate_layer),
    )
    results = [loss_value, grad_norm]
    for weight, grad_full, moment_old, average_old, rate in updates:
        results.extend(apply_update(weight, grad_full, moment_old, average_old, factor, rate))
    return tuple(results)


def solution(mesh):
    rows = P(None, both, None)
    tables = (rows,) * 12 + (P(None, both),) * 3 + (P(both, None),) * 3 + (P(),) * 3
    return jax.shard_map(
        on_device,
        mesh=mesh,
        in_specs=(
            P(None, "fsdp", "seq"),
            P(None, "fsdp"),
            P(None, "fsdp", "seq"),
            P(None, "fsdp", "seq"),
        )
        + tables,
        out_specs=(P(), P()) + tables,
        check_vma=False,
    )
```

```python
import functools

import jax
import jax.numpy as jnp
from jax import lax
from jax.experimental import pallas as pl
from jax.experimental.pallas import tpu as pltpu
from jax.sharding import PartitionSpec as P

D = 768
H = 12
HD = 64
FF = 2048
V = 32000


epsilon = 1e-06
smooth = 0.1
z_weight = 0.005
clip_limit = 0.5
moment = 0.9
average = 0.9
rate_layer = 200.0
rate_head = 1000.0
rate_embed = 5000.0
negative = -1e30
both = ("seq", "fsdp")
highest = lax.Precision.HIGHEST
MESH = pl.DeviceIdType.MESH


def dot(left_side, right_side, left_axis, right_axis, precision=None):
    return lax.dot_general(
        left_side,
        right_side,
        (((left_axis,), (right_axis,)), ((), ())),
        precision=precision,
        preferred_element_type=jnp.float32,
    )


def line_of(fsdp_count):
    return 4 if fsdp_count % 4 == 0 else 1


def gather_kernel(cores, fsdp, x_ref, o_ref, send_sem, recv_sem):
    plane = line_of(fsdp)
    lines = fsdp // plane
    core = lax.axis_index("seq")
    spot = lax.axis_index("fsdp")
    high, low = spot // plane, spot % plane
    line_peers = [((high + k) % lines) * plane + low for k in range(1, lines)]
    plane_peers = [high * plane + (low + k) % plane for k in range(1, plane)]
    core_peers = [(core + k) % cores for k in range(1, cores)]
    peers = [(core, p) for p in line_peers + plane_peers] + [(c, spot) for c in core_peers]

    barrier = pltpu.get_barrier_semaphore()
    for peer in peers:
        pl.semaphore_signal(barrier, inc=1, device_id=peer, device_id_type=MESH)
    pl.semaphore_wait(barrier, len(peers))

    sent = []

    def send(source_ref, block, peer):
        copy = pltpu.make_async_remote_copy(
            src_ref=source_ref,
            dst_ref=o_ref.at[block],
            send_sem=send_sem.at[len(sent)],
            recv_sem=recv_sem.at[block],
            device_id=peer,
            device_id_type=MESH,
        )
        copy.start()
        sent.append(copy)

    def arrived(block):
        pltpu.make_async_copy(o_ref.at[block], o_ref.at[block], recv_sem.at[block]).wait()

    mine = core * fsdp + spot
    for p in line_peers:
        send(x_ref, mine, (core, p))
    for p in plane_peers:
        send(x_ref, mine, (core, p))
    for c in core_peers:
        send(x_ref, mine, (c, spot))
    o_ref[mine] = x_ref[...]
    for k in range(1, lines):
        block = core * fsdp + ((high + lines - k) % lines) * plane + low
        arrived(block)
        for p in plane_peers:
            send(o_ref.at[block], block, (core, p))
        for c in core_peers:
            send(o_ref.at[block], block, (c, spot))
    for m in range(lines):
        for k in range(1, plane):
            block = core * fsdp + ((high + lines - m) % lines) * plane + (low + plane - k) % plane
            arrived(block)
            for c in core_peers:
                send(o_ref.at[block], block, (c, spot))
    for c in core_peers:
        for m in range(lines):
            for k in range(plane):
                block = c * fsdp + ((high + lines - m) % lines) * plane + (low + plane - k) % plane
                arrived(block)
    for copy in sent:
        copy.wait_send()


def gather_rows(array, collective):
    cores, fsdp = lax.axis_size("seq"), lax.axis_size("fsdp")
    count = cores * fsdp
    return pl.pallas_call(
        functools.partial(gather_kernel, cores, fsdp),
        out_shape=jax.ShapeDtypeStruct((count,) + array.shape, array.dtype),
        in_specs=[pl.BlockSpec(memory_space=pltpu.VMEM)],
        out_specs=pl.BlockSpec(memory_space=pltpu.VMEM),
        scratch_shapes=[
            pltpu.SemaphoreType.DMA((count,)),
            pltpu.SemaphoreType.DMA((count,)),
        ],
        compiler_params=pltpu.CompilerParams(collective_id=collective, has_side_effects=True),
        name="gather_rows",
    )(array)


def exchange_kernel(cores, fsdp, x_ref, o_ref, send_sem, recv_sem, own_sem):
    count = cores * fsdp
    mine = lax.axis_index("seq") * fsdp + lax.axis_index("fsdp")

    def place(step):
        other = lax.rem(mine + step, count)
        return other, (other // fsdp, lax.rem(other, fsdp))

    barrier = pltpu.get_barrier_semaphore()

    def greet(step, _):
        pl.semaphore_signal(barrier, inc=1, device_id=place(step)[1], device_id_type=MESH)
        return 0

    lax.fori_loop(1, count, greet, 0)
    pl.semaphore_wait(barrier, count - 1)
    own = pltpu.make_async_copy(x_ref.at[mine], o_ref.at[mine], own_sem)
    own.start()

    def copy_to(step):
        other, peer = place(step)
        return pltpu.make_async_remote_copy(
            src_ref=x_ref.at[other],
            dst_ref=o_ref.at[mine],
            send_sem=send_sem.at[step],
            recv_sem=recv_sem.at[step],
            device_id=peer,
            device_id_type=MESH,
        )

    def start(step, _):
        copy_to(step).start()
        return 0

    lax.fori_loop(1, count, start, 0)
    own.wait()

    def finish(step, _):
        source = lax.rem(mine + count - step, count)
        pltpu.make_async_copy(o_ref.at[source], o_ref.at[source], recv_sem.at[step]).wait()
        copy_to(step).wait_send()
        return 0

    lax.fori_loop(1, count, finish, 0)


def exchange(array, collective):
    cores, fsdp = lax.axis_size("seq"), lax.axis_size("fsdp")
    return pl.pallas_call(
        functools.partial(exchange_kernel, cores, fsdp),
        out_shape=jax.ShapeDtypeStruct(array.shape, array.dtype),
        in_specs=[pl.BlockSpec(memory_space=pltpu.VMEM)],
        out_specs=pl.BlockSpec(memory_space=pltpu.VMEM),
        scratch_shapes=[
            pltpu.SemaphoreType.DMA((cores * fsdp,)),
            pltpu.SemaphoreType.DMA((cores * fsdp,)),
            pltpu.SemaphoreType.DMA,
        ],
        compiler_params=pltpu.CompilerParams(collective_id=collective, has_side_effects=True),
        name="exchange",
    )(array)


def reduce_kernel(
    cores,
    fsdp,
    x_ref,
    o_ref,
    from_core,
    from_plane,
    from_line,
    core_sum,
    plane_sum,
    send_sem,
    recv_sem,
):
    plane = line_of(fsdp)
    lines = fsdp // plane
    core = lax.axis_index("seq")
    spot = lax.axis_index("fsdp")
    high, low = spot // plane, lax.rem(spot, plane)
    far = 1 - core
    peers = [(far, spot)]
    peers += [(core, lax.rem(high + k, lines) * plane + low) for k in range(1, lines)]
    peers += [(core, high * plane + lax.rem(low + k, plane)) for k in range(1, plane)]
    barrier = pltpu.get_barrier_semaphore()
    for peer in peers:
        pl.semaphore_signal(barrier, inc=1, device_id=peer, device_id_type=MESH)
    pl.semaphore_wait(barrier, len(peers))
    sent = []

    def send(source_ref, target_ref, slot, peer):
        copy = pltpu.make_async_remote_copy(
            src_ref=source_ref,
            dst_ref=target_ref,
            send_sem=send_sem.at[slot],
            recv_sem=recv_sem.at[slot],
            device_id=peer,
            device_id_type=MESH,
        )
        copy.start()
        sent.append(copy)
        return copy

    first = []
    for k in list(range(1, plane)) + [0]:
        spot_low = lax.rem(low + k, plane)
        first.append(
            (k, spot_low, send(x_ref.at[far, :, spot_low], from_core.at[spot_low], k, (far, spot)))
        )
    second = []
    for k, spot_low, copy in first:
        copy.wait_recv()
        core_sum[spot_low] = x_ref[core, :, spot_low] + from_core[spot_low]
        if k:
            target = from_plane.at[k - 1]
            peer = (core, high * plane + spot_low)
            second.append((k, send(core_sum.at[spot_low], target, plane + k - 1, peer)))
    plane_sum[...] = core_sum[low]
    for k, copy in second:
        copy.wait_recv()
        plane_sum[...] += from_plane[k - 1]
    third = []
    for k in range(1, lines):
        line = lax.rem(high + k, lines)
        slot = 2 * plane + k - 2
        peer = (core, line * plane + low)
        third.append((k, send(plane_sum.at[line], from_line.at[k - 1], slot, peer)))
    total = plane_sum[high]
    for k, copy in third:
        copy.wait_recv()
        total = total + from_line[k - 1]
    o_ref[...] = total
    for copy in sent:
        copy.wait_send()


def reduce_rows(array, collective):
    cores, fsdp = lax.axis_size("seq"), lax.axis_size("fsdp")
    plane = line_of(fsdp)
    lines = fsdp // plane
    rows, columns = array.shape[0] // (cores * fsdp), array.shape[1]
    kind = array.dtype
    slots = 2 * plane + lines - 2
    return pl.pallas_call(
        functools.partial(reduce_kernel, cores, fsdp),
        out_shape=jax.ShapeDtypeStruct((rows, columns), kind),
        in_specs=[pl.BlockSpec(memory_space=pltpu.VMEM)],
        out_specs=pl.BlockSpec(memory_space=pltpu.VMEM),
        scratch_shapes=[
            pltpu.VMEM((plane, lines, rows, columns), kind),
            pltpu.VMEM((plane - 1, lines, rows, columns), kind),
            pltpu.VMEM((lines - 1, rows, columns), kind),
            pltpu.VMEM((plane, lines, rows, columns), kind),
            pltpu.VMEM((lines, rows, columns), kind),
            pltpu.SemaphoreType.DMA((slots,)),
            pltpu.SemaphoreType.DMA((slots,)),
        ],
        compiler_params=pltpu.CompilerParams(
            collective_id=collective, has_side_effects=True, vmem_limit_bytes=60 * 1024 * 1024
        ),
        name="reduce_rows",
    )(array.reshape(cores, lines, plane, rows, columns))


def lookup_kernel(unroll, builds, live_ref, ids_ref, own_ref, o_ref, table, stage):
    sources, features, tokens = o_ref.shape
    micros = live_ref.shape[0] // sources
    half = tokens // micros

    def build(step, _):
        for u in range(builds):
            at = pl.multiple_of((step * builds + u) * 128, 128)
            block = own_ref[:, pl.ds(at, 128)].astype(jnp.bfloat16).astype(jnp.float32)
            table[pl.ds(at, 128), pl.ds(0, features)] = block.T
        return 0

    lax.fori_loop(0, table.shape[0] // 128 // builds, build, 0)
    stage[...] = jnp.zeros_like(stage)

    def source(which, _):
        def fetch(first, step, _):
            at = first + step * unroll
            ids = [ids_ref[which * tokens + at + u] for u in range(unroll)]
            for u in range(unroll):
                stage[pl.ds(at + u, 1), :] = table[pl.ds(ids[u], 1), :]
            return 0

        for m in range(micros):
            live = live_ref[which * micros + m]
            lax.fori_loop(
                0, (live + unroll - 1) // unroll, functools.partial(fetch, m * half), 0
            )
        for c in range(tokens // 128):
            block = stage[pl.ds(c * 128, 128), :].T
            o_ref[which, :, pl.ds(c * 128, 128)] = block[:features].astype(jnp.bfloat16)
        return 0

    lax.fori_loop(0, sources, source, 0)


def lookup(live, ids, table_t):
    sources, tokens = ids.shape
    features, vocab = table_t.shape
    return pl.pallas_call(
        functools.partial(lookup_kernel, 64, 10),
        out_shape=jax.ShapeDtypeStruct((sources, features, tokens), jnp.bfloat16),
        in_specs=[
            pl.BlockSpec(memory_space=pltpu.SMEM),
            pl.BlockSpec(memory_space=pltpu.SMEM),
            pl.BlockSpec(memory_space=pltpu.VMEM),
        ],
        out_specs=pl.BlockSpec(memory_space=pltpu.VMEM),
        scratch_shapes=[
            pltpu.VMEM((vocab, 128), jnp.float32),
            pltpu.VMEM((tokens, 128), jnp.float32),
        ],
        compiler_params=pltpu.CompilerParams(vmem_limit_bytes=48 * 1024 * 1024),
        name="lookup",
    )(live.reshape(-1), ids.reshape(-1), table_t)


row_bits = 13
row_count = 1 << row_bits


def scatter_kernel(unroll, live_ref, rows_ref, ids_ref, g_ref, o_ref, spread, *sums):
    sources, features, tokens = g_ref.shape
    micros = live_ref.shape[0] // sources
    half = tokens // micros
    vocab = o_ref.shape[1]
    groups = 4

    def clear(step, _):
        for one in sums:
            one[pl.ds(pl.multiple_of(step * 256, 256), 256)] = jnp.zeros((256, 128), jnp.float32)
        return 0

    lax.fori_loop(0, row_count // 256, clear, 0)
    blank = jnp.zeros((128 // groups - features, 128), jnp.float32)
    group = lax.broadcasted_iota(jnp.int32, (128, 128), 0) // (128 // groups)

    def source(which, _):
        for c in range(tokens // 128):
            block = g_ref[which, :, pl.ds(c * 128, 128)].astype(jnp.float32)
            block = jnp.concatenate([block, blank] * groups, axis=0)
            chosen = ids_ref[which, :, pl.ds(c * 128, 128)] >> row_bits
            spread[pl.ds(c * 128, 128), :] = jnp.where(group == chosen, block, 0.0).T

        def add(first, step, _):
            at = first + step * unroll
            rows = [rows_ref[which * tokens + at + u] for u in range(unroll)]
            for u in range(unroll):
                one = sums[u % len(sums)]
                one[pl.ds(rows[u], 1), :] += spread[pl.ds(at + u, 1), :]
            return 0

        for m in range(micros):
            live = live_ref[which * micros + m]
            lax.fori_loop(0, (live + unroll - 1) // unroll, functools.partial(add, m * half), 0)
        return 0

    lax.fori_loop(0, sources, source, 0)

    def finish(step, _):
        for u in range(2):
            at = pl.multiple_of((step * 2 + u) * 128, 128)
            total = sums[0][pl.ds(at, 128)]
            for one in sums[1:]:
                total = total + one[pl.ds(at, 128)]
            total = total.T
            for k in range(groups):
                part = total[k * (128 // groups) : k * (128 // groups) + features]
                if (k + 1) * row_count <= vocab:
                    o_ref[:, pl.ds(k * row_count + at, 128)] = part
                elif k * row_count < vocab:

                    @pl.when(k * row_count + at + 128 <= vocab)
                    def _():
                        o_ref[:, pl.ds(k * row_count + at, 128)] = part

        return 0

    lax.fori_loop(0, row_count // 256, finish, 0)


def scatter_add(live, ids, grads, vocab):
    sources, features, tokens = grads.shape
    return pl.pallas_call(
        functools.partial(scatter_kernel, 32),
        out_shape=jax.ShapeDtypeStruct((features, vocab), jnp.float32),
        in_specs=[
            pl.BlockSpec(memory_space=pltpu.SMEM),
            pl.BlockSpec(memory_space=pltpu.SMEM),
            pl.BlockSpec(memory_space=pltpu.VMEM),
            pl.BlockSpec(memory_space=pltpu.VMEM),
        ],
        out_specs=pl.BlockSpec(memory_space=pltpu.VMEM),
        scratch_shapes=[pltpu.VMEM((tokens, 128), jnp.float32)]
        + [pltpu.VMEM((row_count, 128), jnp.float32)] * 8,
        compiler_params=pltpu.CompilerParams(vmem_limit_bytes=60 * 1024 * 1024),
        name="scatter_add",
    )(
        live.reshape(-1),
        (ids & (row_count - 1)).reshape(-1),
        ids.reshape(sources, 1, tokens),
        grads,
    )


def other_core(arrays):
    return lax.ppermute(arrays, "seq", [(0, 1), (1, 0)])


def norm_forward(values, gain_row):
    inverse = lax.rsqrt(jnp.mean(values * values, axis=-1, keepdims=True) + epsilon)
    return (values * inverse * gain_row, inverse)


def norm_backward(values, inverse, gain_row, grad_out):
    scaled = grad_out * gain_row
    grad_gain = jnp.sum(grad_out * values * inverse, axis=0)
    grad_in = inverse * scaled - values * inverse**3 * jnp.mean(
        values * scaled, axis=-1, keepdims=True
    )
    return (grad_in, grad_gain)


def apply_update(weight_old, grad_full, moment_old, average_old, factor, rate):
    clipped = factor * grad_full
    moment_new = moment * moment_old + clipped
    weight_new = weight_old - rate * (clipped + moment * moment_new)
    average_new = average * average_old + (1.0 - average) * weight_new
    return (weight_new, moment_new, average_new)


def on_device(
    token_ids,
    lengths,
    loss_positions,
    loss_targets,
    attention_in,
    attention_in_moment,
    attention_in_average,
    attention_out,
    attention_out_moment,
    attention_out_average,
    feed_in,
    feed_in_moment,
    feed_in_average,
    feed_out,
    feed_out_moment,
    feed_out_average,
    embedding,
    embedding_moment,
    embedding_average,
    unembedding,
    unembedding_moment,
    unembedding_average,
    gains_biases,
    gains_biases_moment,
    gains_biases_average,
):
    low = jnp.bfloat16
    wide = jnp.float32
    devices_all = lax.axis_size(both)
    seq_index = lax.axis_index("seq")
    device = lax.axis_index(both)
    micros, _, half = token_ids.shape
    loss_dev = loss_positions.shape[2]
    tokens = micros * half
    rows = micros * loss_dev
    rows_all = devices_all * rows
    vocab_here = unembedding.shape[0]
    features = D // devices_all
    gate_here = FF // devices_all
    gain_rows = gains_biases[: 3 * D].reshape(3, D)
    bias_row = gains_biases[3 * D :]
    second = seq_index.astype(wide)

    positions = loss_positions[:, 0]
    targets = loss_targets[:, 0]
    counted = (seq_index * half + positions < lengths[:, :1]).astype(jnp.int32)
    live = jnp.clip(lengths[:, 0] - seq_index * half, 0, half)
    labels = jnp.concatenate([targets.reshape(-1), counted.reshape(-1), live])
    ids_block = jnp.concatenate([token_ids.reshape(-1), labels])
    pad = -ids_block.shape[0] % 1024
    ids_block = jnp.pad(ids_block, (0, pad)).reshape(-1, 128)
    ids_all = gather_rows(ids_block, 1).reshape(devices_all, -1)
    all_tokens = ids_all[:, :tokens]
    all_targets = ids_all[:, tokens : tokens + rows].reshape(-1)
    all_counted = ids_all[:, tokens + rows : tokens + 2 * rows]
    all_live = ids_all[:, tokens + 2 * rows : tokens + 2 * rows + micros]

    w_in = lax.all_gather(attention_in[0].astype(low), both, axis=0, tiled=True)
    w_out = lax.all_gather(attention_out[0].astype(low), both, axis=0, tiled=True)
    w_feed = lax.all_gather(feed_in[0].astype(low), both, axis=0, tiled=True)
    w_down = lax.all_gather(feed_out[0].astype(low), both, axis=0, tiled=True)
    head_low = unembedding.astype(low)

    arrived = exchange(lookup(all_live, all_tokens, embedding.T), 5)
    x_t = arrived.reshape(D, tokens)
    x_wide = x_t.astype(wide)
    inverse_one = lax.rsqrt(jnp.mean(x_wide * x_wide, axis=0, keepdims=True) + epsilon)
    normed_t = (x_wide * inverse_one * gain_rows[0][:, None]).astype(low)

    project_t = dot(w_in[:, D:], normed_t, 0, 0)
    kv_t = project_t[: 2 * D].astype(low)
    forget_t = (project_t[2 * D :] + bias_row[:, None]).astype(low).astype(wide)
    pick = [
        (positions[m][:, None] == jnp.arange(half)[None, :]).astype(low) for m in range(micros)
    ]

    def per_micro(array, m):
        return array[:, m * half : (m + 1) * half]

    x_rows = jnp.concatenate([dot(pick[m], per_micro(x_t, m), 1, 1) for m in range(micros)])
    normed_rows = jnp.concatenate(
        [dot(pick[m], per_micro(normed_t, m), 1, 1) for m in range(micros)]
    ).astype(low)
    q_rows = dot(normed_rows, w_in[:, :D], 1, 0).astype(low)

    upper = (jnp.arange(half)[:, None] <= jnp.arange(half)[None, :]).astype(wide)
    log_gate = jax.nn.log_sigmoid(forget_t).reshape(H, micros, half)
    decay_own = lax.dot_general(
        log_gate, upper, (((2,), (0,)), ((), ())), precision=highest, preferred_element_type=wide
    )
    total_own = decay_own[:, :, -1]
    decay_rows = jnp.stack(
        [dot(pick[m].astype(wide), decay_own[:, m], 1, 1, highest) for m in range(micros)]
    )
    q_own = q_rows.reshape(micros, loss_dev, H, HD)
    q_far, decay_far, total_far, place_far = other_core((q_own, decay_rows, total_own, positions))
    shift_own = second * total_far
    shift_far = (1.0 - second) * total_own
    key_decay = decay_own + shift_own[:, :, None]
    row_decay = jnp.concatenate(
        [decay_rows + shift_own.T[:, None], decay_far + shift_far.T[:, None]], axis=1
    )
    q_all = jnp.concatenate([q_own, q_far], axis=1)
    places = jnp.concatenate(
        [positions + seq_index * half, place_far + (1 - seq_index) * half], axis=1
    )
    key_places = seq_index * half + jnp.arange(half)
    keys_t = kv_t[:D].reshape(H, HD, tokens)
    values_t = kv_t[D:].reshape(H, HD, tokens)

    scores = []
    for m in range(micros):
        keys_m = keys_t[:, :, m * half : (m + 1) * half]
        raw = jnp.einsum("rhd,hdj->hrj", q_all[m], keys_m, preferred_element_type=wide)
        part = raw * HD ** (-0.5) + row_decay[m].T[:, :, None] - key_decay[:, m][:, None, :]
        causal = places[m][:, None] >= key_places[None, :]
        scores.append(jnp.where(causal[None], part, negative))
    scores = jnp.stack(scores)
    peak_own = jnp.max(scores, axis=-1)
    spread_own = jnp.sum(jnp.exp(scores - peak_own[..., None]), axis=-1)
    peak_far, spread_far = other_core((peak_own, spread_own))

    def swap_rows(array):
        return jnp.concatenate([array[:, :, loss_dev:], array[:, :, :loss_dev]], axis=2)

    peak_far, spread_far = swap_rows(peak_far), swap_rows(spread_far)
    peak = jnp.maximum(peak_own, peak_far)
    log_total = peak + jnp.log(
        spread_own * jnp.exp(peak_own - peak) + spread_far * jnp.exp(peak_far - peak)
    )
    probs = jnp.exp(scores - log_total[..., None])
    probs_low = probs.astype(low)
    probs_rest = (probs - probs_low.astype(wide)).astype(low)

    def mix(weights):
        return jnp.stack(
            [
                jnp.einsum(
                    "hrj,hdj->rhd",
                    weights[m],
                    values_t[:, :, m * half : (m + 1) * half],
                    preferred_element_type=wide,
                )
                for m in range(micros)
            ]
        )

    mixed_part = mix(probs_low)
    rest_part = mix(probs_rest)
    mixed_far, rest_far = other_core((mixed_part[:, loss_dev:], rest_part[:, loss_dev:]))
    mixed_sum = mixed_part[:, :loss_dev] + mixed_far
    mixed_full = mixed_sum + rest_part[:, :loss_dev] + rest_far
    mixed_rows = mixed_sum.reshape(rows, D).astype(low)

    middle = x_rows + dot(mixed_rows, w_out, 1, 0)
    normed_two, inverse_two = norm_forward(middle, gain_rows[1])
    normed_two = normed_two.astype(low)
    gate_up = dot(normed_two, w_feed, 1, 0)
    gate_half, up_half = gate_up[:, :FF], gate_up[:, FF:]
    gate_sigmoid = jax.nn.sigmoid(gate_half)
    hidden = (gate_half * gate_sigmoid * up_half).astype(low)
    final_in = middle + dot(hidden, w_down, 1, 0)
    final_normed, final_inverse = norm_forward(final_in, gain_rows[2])

    final_all = gather_rows(final_normed.astype(low), 2).reshape(rows_all, D)
    logits = dot(final_all, head_low, 1, 1)
    vocab_ids = device * vocab_here + jnp.arange(vocab_here)
    target_hits = all_targets[:, None] == vocab_ids[None, :]
    row_peak = jnp.max(logits, axis=1)
    exp_sum = jnp.sum(jnp.exp(logits - row_peak[:, None]), axis=1)
    target_part = jnp.sum(jnp.where(target_hits, logits, 0.0), axis=1)
    logit_sum = jnp.sum(logits, axis=1)
    stats = jnp.stack([row_peak, exp_sum, target_part, logit_sum])
    stats_all = gather_rows(stats.reshape(-1, 128), 3).reshape(devices_all, 4, rows_all)
    peak_all = jnp.max(stats_all[:, 0], axis=0)
    spread_all = jnp.sum(stats_all[:, 1] * jnp.exp(stats_all[:, 0] - peak_all), axis=0)
    target_all = jnp.sum(stats_all[:, 2], axis=0)
    logit_all = jnp.sum(stats_all[:, 3], axis=0)
    total_all = peak_all + jnp.log(spread_all)
    per_row = (
        total_all
        - (1.0 - smooth) * target_all
        - smooth * logit_all / V
        + z_weight * total_all * total_all
    )
    weights_row = all_counted.astype(wide).reshape(devices_all, micros, loss_dev)
    counts = jnp.sum(weights_row, axis=(0, 2))
    weights_row = (weights_row / (micros * counts)[None, :, None]).reshape(-1)
    loss_value = jnp.sum(weights_row * per_row)
    soft_rows = jnp.exp(logits - total_all[:, None])
    grad_logits = (
        weights_row[:, None]
        * (
            soft_rows * (1.0 + 2.0 * z_weight * total_all)[:, None]
            - (1.0 - smooth) * target_hits.astype(wide)
            - smooth / V
        )
    ).astype(low)
    head_grad = dot(grad_logits, final_all, 0, 0)
    grad_final = reduce_rows(dot(grad_logits, head_low, 1, 0), 7)

    grad_rows, gain_grad_final = norm_backward(final_in, final_inverse, gain_rows[2], grad_final)
    grad_branch = grad_rows.astype(low)
    grad_hidden = dot(grad_branch, w_down, 1, 1)
    grad_gate = grad_hidden * up_half * gate_sigmoid * (1.0 + gate_half * (1.0 - gate_sigmoid))
    grad_up = grad_hidden * gate_half * gate_sigmoid
    grad_gate_up = jnp.concatenate([grad_gate, grad_up], axis=1).astype(low)
    grad_two, gain_grad_two = norm_backward(
        middle, inverse_two, gain_rows[1], dot(grad_gate_up, w_feed, 1, 1)
    )
    grad_middle = grad_rows + grad_two
    grad_mid_low = grad_middle.astype(low)
    grad_mixed = dot(grad_mid_low, w_out, 1, 1).astype(low)

    normed_two_all = lax.all_gather(normed_two, both, axis=0, tiled=True)
    grad_branch_all = lax.all_gather(grad_branch, both, axis=0, tiled=True)
    hidden_columns = lax.all_to_all(
        hidden.reshape(rows, devices_all, gate_here), both, split_axis=1, concat_axis=0, tiled=True
    ).reshape(rows_all, gate_here)
    grad_down = dot(hidden_columns, grad_branch_all, 0, 0)
    gate_up_columns = lax.all_to_all(
        grad_gate_up.reshape(rows, 2, devices_all, gate_here),
        both,
        split_axis=2,
        concat_axis=0,
        tiled=True,
    ).reshape(rows_all, 2 * gate_here)
    grad_feed_columns = dot(normed_two_all, gate_up_columns, 0, 0)
    grad_feed = lax.all_to_all(
        grad_feed_columns.reshape(devices_all, features, 2 * gate_here),
        both,
        split_axis=0,
        concat_axis=0,
        tiled=True,
    )
    grad_feed = (
        grad_feed.reshape(devices_all, features, 2, gate_here)
        .transpose(1, 2, 0, 3)
        .reshape(features, 2 * FF)
    )
    grad_out = lax.psum_scatter(
        dot(mixed_rows, grad_mid_low, 0, 0), both, scatter_dimension=0, tiled=True
    )

    grad_own = grad_mixed.reshape(micros, loss_dev, H, HD)
    inner_own = jnp.sum(grad_own.astype(wide) * mixed_full, axis=-1)
    grad_far, inner_far = other_core((grad_own, inner_own))
    grad_heads = jnp.concatenate([grad_own, grad_far], axis=1)
    inner_sum = jnp.concatenate([inner_own, inner_far], axis=1)
    query_parts, score_rows = [], []
    grad_keys, grad_values, score_columns = [], [], []
    for m in range(micros):
        keys_m = keys_t[:, :, m * half : (m + 1) * half]
        values_m = values_t[:, :, m * half : (m + 1) * half]
        grad_probs = jnp.einsum("rhd,hdj->hrj", grad_heads[m], values_m, preferred_element_type=wide)
        grad_scores = (probs[m] * (grad_probs - inner_sum[m].T[:, :, None])).astype(low)
        query_parts.append(
            jnp.einsum("hrj,hdj->rhd", grad_scores, keys_m, preferred_element_type=wide)
        )
        grad_keys.append(
            jnp.einsum("hrj,rhd->hdj", grad_scores, q_all[m], preferred_element_type=wide)
            * HD ** (-0.5)
        )
        grad_values.append(
            jnp.einsum("hrj,rhd->hdj", probs_low[m], grad_heads[m], preferred_element_type=wide)
        )
        score_wide = grad_scores.astype(wide)
        score_rows.append(jnp.sum(score_wide, axis=-1))
        score_columns.append(jnp.sum(score_wide, axis=1))
    query_parts = jnp.stack(query_parts)
    score_rows = jnp.stack(score_rows).transpose(0, 2, 1)
    query_far, score_far = other_core((query_parts[:, loss_dev:], score_rows[:, loss_dev:]))
    grad_query = ((query_parts[:, :loss_dev] + query_far) * HD ** (-0.5)).astype(low)
    grad_query = grad_query.reshape(rows, D)
    rows_sum = score_rows[:, :loss_dev] + score_far
    later = (1.0 - second) * jnp.sum(score_rows[:, loss_dev:], axis=1)
    grad_log = []
    for m in range(micros):
        placed = dot(rows_sum[m], pick[m].astype(wide), 0, 0, highest)
        change = placed - score_columns[m]
        suffix = dot(change, upper, 1, 1, highest)
        grad_log.append(suffix + later[m][:, None])
    grad_log = jnp.concatenate(grad_log, axis=1)
    grad_forget = (grad_log * jax.nn.sigmoid(-forget_t)).astype(low)
    query_t = jnp.concatenate(
        [
            dot(grad_query[m * loss_dev : (m + 1) * loss_dev], pick[m], 0, 0).astype(low)
            for m in range(micros)
        ],
        axis=1,
    )
    keys_part = jnp.concatenate(grad_keys, axis=2).reshape(D, tokens).astype(low)
    values_part = jnp.concatenate(grad_values, axis=2).reshape(D, tokens).astype(low)
    grad_project = jnp.concatenate([query_t, keys_part, values_part, grad_forget], axis=0)
    grad_bias = jnp.sum(grad_forget.astype(wide), axis=1)
    grad_in = lax.psum_scatter(
        dot(normed_t, grad_project, 1, 1), both, scatter_dimension=0, tiled=True
    )
    grad_normed = dot(w_in, grad_project, 1, 0)
    scaled = grad_normed * gain_rows[0][:, None]
    gain_grad_one = jnp.sum(grad_normed * x_wide * inverse_one, axis=1)
    grad_one = inverse_one * scaled - x_wide * inverse_one**3 * jnp.mean(
        x_wide * scaled, axis=0, keepdims=True
    )
    middle_t = jnp.concatenate(
        [
            dot(
                grad_middle[m * loss_dev : (m + 1) * loss_dev],
                pick[m].astype(wide),
                0,
                0,
                highest,
            )
            for m in range(micros)
        ],
        axis=1,
    )
    grad_embed = (middle_t + grad_one).astype(low).reshape(devices_all, features, tokens)
    moved = exchange(grad_embed, 6)
    embed_grad = scatter_add(all_live, all_tokens, moved, V).T

    owned_grads = [grad_in[None], grad_out[None], grad_feed[None], grad_down[None]]
    owned_grads = owned_grads + [embed_grad, head_grad]
    square_sum = jnp.zeros((), wide)
    for grad_part in owned_grads:
        square_sum = square_sum + jnp.sum(grad_part * grad_part)
    small_grad = jnp.concatenate(
        [gain_grad_one, gain_grad_two, gain_grad_final, grad_bias, square_sum[None]]
    )
    small_count = small_grad.shape[0]
    small_grad = jnp.pad(small_grad, (0, -small_count % 1024)).reshape(-1, 128)
    small_sum = jnp.sum(gather_rows(small_grad, 4), axis=0).reshape(-1)
    small_total, square_total = small_sum[: small_count - 1], small_sum[small_count - 1]
    grad_norm = jnp.sqrt(square_total + jnp.sum(small_total * small_total))
    factor = jnp.minimum(1.0, clip_limit / grad_norm)
    updates = (
        (attention_in, owned_grads[0], attention_in_moment, attention_in_average, rate_layer),
        (attention_out, owned_grads[1], attention_out_moment, attention_out_average, rate_layer),
        (feed_in, owned_grads[2], feed_in_moment, feed_in_average, rate_layer),
        (feed_out, owned_grads[3], feed_out_moment, feed_out_average, rate_layer),
        (embedding, embed_grad, embedding_moment, embedding_average, rate_embed),
        (unembedding, head_grad, unembedding_moment, unembedding_average, rate_head),
        (gains_biases, small_total, gains_biases_moment, gains_biases_average, rate_layer),
    )
    results = [loss_value, grad_norm]
    for weight, grad_full, moment_old, average_old, rate in updates:
        results.extend(apply_update(weight, grad_full, moment_old, average_old, factor, rate))
    return tuple(results)


def solution(mesh):
    rows = P(None, both, None)
    tables = (rows,) * 12 + (P(None, both),) * 3 + (P(both, None),) * 3 + (P(),) * 3
    return jax.shard_map(
        on_device,
        mesh=mesh,
        in_specs=(
            P(None, "fsdp", "seq"),
            P(None, "fsdp"),
            P(None, "fsdp", "seq"),
            P(None, "fsdp", "seq"),
        )
        + tables,
        out_specs=(P(), P()) + tables,
        check_vma=False,
    )
```

```python
import functools

import jax
import jax.numpy as jnp
from jax import lax
from jax.experimental import pallas as pl
from jax.experimental.pallas import tpu as pltpu
from jax.sharding import PartitionSpec as P

D = 768
H = 12
HD = 64
FF = 2048
V = 32000


epsilon = 1e-06
smooth = 0.1
z_weight = 0.005
clip_limit = 0.5
moment = 0.9
average = 0.9
rate_layer = 200.0
rate_head = 1000.0
rate_embed = 5000.0
negative = -1e30
both = ("seq", "fsdp")
highest = lax.Precision.HIGHEST
MESH = pl.DeviceIdType.MESH


def dot(left_side, right_side, left_axis, right_axis, precision=None):
    return lax.dot_general(
        left_side,
        right_side,
        (((left_axis,), (right_axis,)), ((), ())),
        precision=precision,
        preferred_element_type=jnp.float32,
    )


def line_of(fsdp_count):
    return 4 if fsdp_count % 4 == 0 else 1


def gather_kernel(cores, fsdp, x_ref, o_ref, send_sem, recv_sem):
    plane = line_of(fsdp)
    lines = fsdp // plane
    core = lax.axis_index("seq")
    spot = lax.axis_index("fsdp")
    high, low = spot // plane, spot % plane
    line_peers = [((high + k) % lines) * plane + low for k in range(1, lines)]
    plane_peers = [high * plane + (low + k) % plane for k in range(1, plane)]
    core_peers = [(core + k) % cores for k in range(1, cores)]
    peers = [(core, p) for p in line_peers + plane_peers] + [(c, spot) for c in core_peers]

    barrier = pltpu.get_barrier_semaphore()
    for peer in peers:
        pl.semaphore_signal(barrier, inc=1, device_id=peer, device_id_type=MESH)
    pl.semaphore_wait(barrier, len(peers))

    sent = []

    def send(source_ref, block, peer):
        copy = pltpu.make_async_remote_copy(
            src_ref=source_ref,
            dst_ref=o_ref.at[block],
            send_sem=send_sem.at[len(sent)],
            recv_sem=recv_sem.at[block],
            device_id=peer,
            device_id_type=MESH,
        )
        copy.start()
        sent.append(copy)

    def arrived(block):
        pltpu.make_async_copy(o_ref.at[block], o_ref.at[block], recv_sem.at[block]).wait()

    mine = core * fsdp + spot
    for p in line_peers:
        send(x_ref, mine, (core, p))
    for p in plane_peers:
        send(x_ref, mine, (core, p))
    for c in core_peers:
        send(x_ref, mine, (c, spot))
    o_ref[mine] = x_ref[...]
    for k in range(1, lines):
        block = core * fsdp + ((high + lines - k) % lines) * plane + low
        arrived(block)
        for p in plane_peers:
            send(o_ref.at[block], block, (core, p))
        for c in core_peers:
            send(o_ref.at[block], block, (c, spot))
    for m in range(lines):
        for k in range(1, plane):
            block = core * fsdp + ((high + lines - m) % lines) * plane + (low + plane - k) % plane
            arrived(block)
            for c in core_peers:
                send(o_ref.at[block], block, (c, spot))
    for c in core_peers:
        for m in range(lines):
            for k in range(plane):
                block = c * fsdp + ((high + lines - m) % lines) * plane + (low + plane - k) % plane
                arrived(block)
    for copy in sent:
        copy.wait_send()


def label_kernel(
    cores, fsdp, tokens_ref, lengths_ref, places_ref, targets_ref, o_ref, packed, send_sem, recv_sem
):
    micros, half = tokens_ref.shape
    chunks = half // 128
    start = lax.axis_index("seq") * half
    packed[...] = jnp.zeros_like(packed)
    for m in range(micros):
        for c in range(chunks):
            packed[pl.ds(m * chunks + c, 1), :] = tokens_ref[pl.ds(m, 1), pl.ds(c * 128, 128)]
    base = micros * chunks
    length = lengths_ref[...]
    counted = (start + places_ref[...] < length).astype(jnp.int32)
    live = jnp.clip(length - start, 0, half)
    count = places_ref.shape[1]
    packed[pl.ds(base, micros), pl.ds(0, count)] = targets_ref[...]
    packed[pl.ds(base + micros, micros), pl.ds(0, count)] = counted
    packed[pl.ds(base + 2 * micros, micros), :] = jnp.broadcast_to(live, (micros, 128))
    gather_kernel(cores, fsdp, packed, o_ref, send_sem, recv_sem)


def gather_labels(tokens, lengths, places, targets, collective):
    cores, fsdp = lax.axis_size("seq"), lax.axis_size("fsdp")
    count = cores * fsdp
    micros, half = tokens.shape
    rows = micros * (half // 128) + 3 * micros
    rows = -(-rows // 8) * 8
    return pl.pallas_call(
        functools.partial(label_kernel, cores, fsdp),
        out_shape=jax.ShapeDtypeStruct((count, rows, 128), jnp.int32),
        in_specs=[pl.BlockSpec(memory_space=pltpu.VMEM)] * 4,
        out_specs=pl.BlockSpec(memory_space=pltpu.VMEM),
        scratch_shapes=[
            pltpu.VMEM((rows, 128), jnp.int32),
            pltpu.SemaphoreType.DMA((count,)),
            pltpu.SemaphoreType.DMA((count,)),
        ],
        compiler_params=pltpu.CompilerParams(collective_id=collective, has_side_effects=True),
        name="gather_labels",
    )(tokens, lengths, places, targets)


def gather_rows(array, collective):
    cores, fsdp = lax.axis_size("seq"), lax.axis_size("fsdp")
    count = cores * fsdp
    return pl.pallas_call(
        functools.partial(gather_kernel, cores, fsdp),
        out_shape=jax.ShapeDtypeStruct((count,) + array.shape, array.dtype),
        in_specs=[pl.BlockSpec(memory_space=pltpu.VMEM)],
        out_specs=pl.BlockSpec(memory_space=pltpu.VMEM),
        scratch_shapes=[
            pltpu.SemaphoreType.DMA((count,)),
            pltpu.SemaphoreType.DMA((count,)),
        ],
        compiler_params=pltpu.CompilerParams(collective_id=collective, has_side_effects=True),
        name="gather_rows",
    )(array)


def exchange_kernel(cores, fsdp, x_ref, o_ref, send_sem, recv_sem, own_sem):
    count = cores * fsdp
    mine = lax.axis_index("seq") * fsdp + lax.axis_index("fsdp")

    def place(step):
        other = lax.rem(mine + step, count)
        return other, (other // fsdp, lax.rem(other, fsdp))

    barrier = pltpu.get_barrier_semaphore()

    def greet(step, _):
        pl.semaphore_signal(barrier, inc=1, device_id=place(step)[1], device_id_type=MESH)
        return 0

    lax.fori_loop(1, count, greet, 0)
    pl.semaphore_wait(barrier, count - 1)
    own = pltpu.make_async_copy(x_ref.at[mine], o_ref.at[mine], own_sem)
    own.start()

    def copy_to(step):
        other, peer = place(step)
        return pltpu.make_async_remote_copy(
            src_ref=x_ref.at[other],
            dst_ref=o_ref.at[mine],
            send_sem=send_sem.at[step],
            recv_sem=recv_sem.at[step],
            device_id=peer,
            device_id_type=MESH,
        )

    def start(step, _):
        copy_to(step).start()
        return 0

    lax.fori_loop(1, count, start, 0)
    own.wait()

    def finish(step, _):
        source = lax.rem(mine + count - step, count)
        pltpu.make_async_copy(o_ref.at[source], o_ref.at[source], recv_sem.at[step]).wait()
        copy_to(step).wait_send()
        return 0

    lax.fori_loop(1, count, finish, 0)


def exchange(array, collective):
    cores, fsdp = lax.axis_size("seq"), lax.axis_size("fsdp")
    return pl.pallas_call(
        functools.partial(exchange_kernel, cores, fsdp),
        out_shape=jax.ShapeDtypeStruct(array.shape, array.dtype),
        in_specs=[pl.BlockSpec(memory_space=pltpu.VMEM)],
        out_specs=pl.BlockSpec(memory_space=pltpu.VMEM),
        scratch_shapes=[
            pltpu.SemaphoreType.DMA((cores * fsdp,)),
            pltpu.SemaphoreType.DMA((cores * fsdp,)),
            pltpu.SemaphoreType.DMA,
        ],
        compiler_params=pltpu.CompilerParams(collective_id=collective, has_side_effects=True),
        name="exchange",
    )(array)


def reduce_kernel(
    fsdp, x_ref, o_ref, from_core, from_plane, from_line, core_sum, plane_sum, send_sem, recv_sem
):
    plane = line_of(fsdp)
    lines = fsdp // plane
    core = lax.axis_index("seq")
    spot = lax.axis_index("fsdp")
    high, low = spot // plane, lax.rem(spot, plane)
    far = 1 - core
    peers = [(far, spot)]
    peers += [(core, lax.rem(high + k, lines) * plane + low) for k in range(1, lines)]
    peers += [(core, high * plane + lax.rem(low + k, plane)) for k in range(1, plane)]
    barrier = pltpu.get_barrier_semaphore()
    for peer in peers:
        pl.semaphore_signal(barrier, inc=1, device_id=peer, device_id_type=MESH)
    pl.semaphore_wait(barrier, len(peers))
    sent = []

    def send(source_ref, target_ref, slot, peer):
        copy = pltpu.make_async_remote_copy(
            src_ref=source_ref,
            dst_ref=target_ref,
            send_sem=send_sem.at[slot],
            recv_sem=recv_sem.at[slot],
            device_id=peer,
            device_id_type=MESH,
        )
        copy.start()
        sent.append(copy)
        return copy

    first = []
    for k in list(range(1, plane)) + [0]:
        spot_low = lax.rem(low + k, plane)
        first.append(
            (k, spot_low, send(x_ref.at[far, :, spot_low], from_core.at[spot_low], k, (far, spot)))
        )
    second = []
    for k, spot_low, copy in first:
        copy.wait_recv()
        core_sum[spot_low] = x_ref[core, :, spot_low] + from_core[spot_low]
        if k:
            target = from_plane.at[k - 1]
            peer = (core, high * plane + spot_low)
            second.append((k, send(core_sum.at[spot_low], target, plane + k - 1, peer)))
    plane_sum[...] = core_sum[low]
    for k, copy in second:
        copy.wait_recv()
        plane_sum[...] += from_plane[k - 1]
    third = []
    for k in range(1, lines):
        line = lax.rem(high + k, lines)
        slot = 2 * plane + k - 2
        peer = (core, line * plane + low)
        third.append((k, send(plane_sum.at[line], from_line.at[k - 1], slot, peer)))
    total = plane_sum[high]
    for k, copy in third:
        copy.wait_recv()
        total = total + from_line[k - 1]
    o_ref[...] = total
    for copy in sent:
        copy.wait_send()


def reduce_rows(array, collective):
    cores, fsdp = lax.axis_size("seq"), lax.axis_size("fsdp")
    plane = line_of(fsdp)
    lines = fsdp // plane
    rows, columns = array.shape[0] // (cores * fsdp), array.shape[1]
    kind = array.dtype
    slots = 2 * plane + lines - 2
    return pl.pallas_call(
        functools.partial(reduce_kernel, fsdp),
        out_shape=jax.ShapeDtypeStruct((rows, columns), kind),
        in_specs=[pl.BlockSpec(memory_space=pltpu.VMEM)],
        out_specs=pl.BlockSpec(memory_space=pltpu.VMEM),
        scratch_shapes=[
            pltpu.VMEM((plane, lines, rows, columns), kind),
            pltpu.VMEM((plane - 1, lines, rows, columns), kind),
            pltpu.VMEM((lines - 1, rows, columns), kind),
            pltpu.VMEM((plane, lines, rows, columns), kind),
            pltpu.VMEM((lines, rows, columns), kind),
            pltpu.SemaphoreType.DMA((slots,)),
            pltpu.SemaphoreType.DMA((slots,)),
        ],
        compiler_params=pltpu.CompilerParams(
            collective_id=collective, has_side_effects=True, vmem_limit_bytes=60 * 1024 * 1024
        ),
        name="reduce_rows",
    )(array.reshape(cores, lines, plane, rows, columns))


def lookup_kernel(unroll, builds, live_ref, ids_ref, own_ref, o_ref, table, stage):
    sources, features, tokens = o_ref.shape
    micros = live_ref.shape[0] // sources
    half = tokens // micros

    def build(step, _):
        for u in range(builds):
            at = pl.multiple_of((step * builds + u) * 128, 128)
            block = own_ref[:, pl.ds(at, 128)].astype(jnp.bfloat16).astype(jnp.float32)
            table[pl.ds(at, 128), pl.ds(0, features)] = block.T
        return 0

    lax.fori_loop(0, table.shape[0] // 128 // builds, build, 0)
    stage[...] = jnp.zeros_like(stage)

    def source(which, _):
        def fetch(first, step, _):
            at = first + step * unroll
            ids = [ids_ref[which * tokens + at + u] for u in range(unroll)]
            for u in range(unroll):
                stage[pl.ds(at + u, 1), :] = table[pl.ds(ids[u], 1), :]
            return 0

        for m in range(micros):
            live = live_ref[which * micros + m]
            lax.fori_loop(
                0, (live + unroll - 1) // unroll, functools.partial(fetch, m * half), 0
            )
        for c in range(tokens // 128):
            block = stage[pl.ds(c * 128, 128), :].T
            o_ref[which, :, pl.ds(c * 128, 128)] = block[:features].astype(jnp.bfloat16)
        return 0

    lax.fori_loop(0, sources, source, 0)


def lookup(live, ids, table_t):
    sources, tokens = ids.shape
    features, vocab = table_t.shape
    return pl.pallas_call(
        functools.partial(lookup_kernel, 64, 10),
        out_shape=jax.ShapeDtypeStruct((sources, features, tokens), jnp.bfloat16),
        in_specs=[
            pl.BlockSpec(memory_space=pltpu.SMEM),
            pl.BlockSpec(memory_space=pltpu.SMEM),
            pl.BlockSpec(memory_space=pltpu.VMEM),
        ],
        out_specs=pl.BlockSpec(memory_space=pltpu.VMEM),
        scratch_shapes=[
            pltpu.VMEM((vocab, 128), jnp.float32),
            pltpu.VMEM((tokens, 128), jnp.float32),
        ],
        compiler_params=pltpu.CompilerParams(vmem_limit_bytes=48 * 1024 * 1024),
        name="lookup",
    )(live.reshape(-1), ids.reshape(-1), table_t)


row_bits = 13
row_count = 1 << row_bits


def scatter_kernel(unroll, live_ref, rows_ref, ids_ref, g_ref, o_ref, spread, *sums):
    sources, features, tokens = g_ref.shape
    micros = live_ref.shape[0] // sources
    half = tokens // micros
    vocab = o_ref.shape[1]
    groups = 4

    def clear(step, _):
        for one in sums:
            one[pl.ds(pl.multiple_of(step * 256, 256), 256)] = jnp.zeros((256, 128), jnp.float32)
        return 0

    lax.fori_loop(0, row_count // 256, clear, 0)
    blank = jnp.zeros((128 // groups - features, 128), jnp.float32)
    group = lax.broadcasted_iota(jnp.int32, (128, 128), 0) // (128 // groups)

    def source(which, _):
        for c in range(tokens // 128):
            block = g_ref[which, :, pl.ds(c * 128, 128)].astype(jnp.float32)
            block = jnp.concatenate([block, blank] * groups, axis=0)
            chosen = ids_ref[which, :, pl.ds(c * 128, 128)] >> row_bits
            spread[pl.ds(c * 128, 128), :] = jnp.where(group == chosen, block, 0.0).T

        def add(first, step, _):
            at = first + step * unroll
            rows = [rows_ref[which * tokens + at + u] for u in range(unroll)]
            for u in range(unroll):
                one = sums[u % len(sums)]
                one[pl.ds(rows[u], 1), :] += spread[pl.ds(at + u, 1), :]
            return 0

        for m in range(micros):
            live = live_ref[which * micros + m]
            lax.fori_loop(0, (live + unroll - 1) // unroll, functools.partial(add, m * half), 0)
        return 0

    lax.fori_loop(0, sources, source, 0)

    def finish(step, _):
        for u in range(2):
            at = pl.multiple_of((step * 2 + u) * 128, 128)
            total = sums[0][pl.ds(at, 128)]
            for one in sums[1:]:
                total = total + one[pl.ds(at, 128)]
            total = total.T
            for k in range(groups):
                part = total[k * (128 // groups) : k * (128 // groups) + features]
                if (k + 1) * row_count <= vocab:
                    o_ref[:, pl.ds(k * row_count + at, 128)] = part
                elif k * row_count < vocab:

                    @pl.when(k * row_count + at + 128 <= vocab)
                    def _():
                        o_ref[:, pl.ds(k * row_count + at, 128)] = part

        return 0

    lax.fori_loop(0, row_count // 256, finish, 0)


def scatter_add(live, ids, grads, vocab):
    sources, features, tokens = grads.shape
    return pl.pallas_call(
        functools.partial(scatter_kernel, 32),
        out_shape=jax.ShapeDtypeStruct((features, vocab), jnp.float32),
        in_specs=[
            pl.BlockSpec(memory_space=pltpu.SMEM),
            pl.BlockSpec(memory_space=pltpu.SMEM),
            pl.BlockSpec(memory_space=pltpu.VMEM),
            pl.BlockSpec(memory_space=pltpu.VMEM),
        ],
        out_specs=pl.BlockSpec(memory_space=pltpu.VMEM),
        scratch_shapes=[pltpu.VMEM((tokens, 128), jnp.float32)]
        + [pltpu.VMEM((row_count, 128), jnp.float32)] * 8,
        compiler_params=pltpu.CompilerParams(vmem_limit_bytes=60 * 1024 * 1024),
        name="scatter_add",
    )(
        live.reshape(-1),
        (ids & (row_count - 1)).reshape(-1),
        ids.reshape(sources, 1, tokens),
        grads,
    )


def other_core(arrays):
    return lax.ppermute(arrays, "seq", [(0, 1), (1, 0)])


def norm_forward(values, gain_row):
    inverse = lax.rsqrt(jnp.mean(values * values, axis=-1, keepdims=True) + epsilon)
    return (values * inverse * gain_row, inverse)


def norm_backward(values, inverse, gain_row, grad_out):
    scaled = grad_out * gain_row
    grad_gain = jnp.sum(grad_out * values * inverse, axis=0)
    grad_in = inverse * scaled - values * inverse**3 * jnp.mean(
        values * scaled, axis=-1, keepdims=True
    )
    return (grad_in, grad_gain)


def apply_update(weight_old, grad_full, moment_old, average_old, factor, rate):
    clipped = factor * grad_full
    moment_new = moment * moment_old + clipped
    weight_new = weight_old - rate * (clipped + moment * moment_new)
    average_new = average * average_old + (1.0 - average) * weight_new
    return (weight_new, moment_new, average_new)


def step(
    token_ids,
    lengths,
    loss_positions,
    loss_targets,
    attention_in,
    attention_in_moment,
    attention_in_average,
    attention_out,
    attention_out_moment,
    attention_out_average,
    feed_in,
    feed_in_moment,
    feed_in_average,
    feed_out,
    feed_out_moment,
    feed_out_average,
    embedding,
    embedding_moment,
    embedding_average,
    unembedding,
    unembedding_moment,
    unembedding_average,
    gains_biases,
    gains_biases_moment,
    gains_biases_average,
):
    low = jnp.bfloat16
    wide = jnp.float32
    devices_all = lax.axis_size(both)
    seq_index = lax.axis_index("seq")
    device = lax.axis_index(both)
    micros, _, half = token_ids.shape
    loss_dev = loss_positions.shape[2]
    tokens = micros * half
    rows = micros * loss_dev
    rows_all = devices_all * rows
    vocab_here = unembedding.shape[0]
    features = D // devices_all
    gate_here = FF // devices_all
    gain_rows = gains_biases[: 3 * D].reshape(3, D)
    bias_row = gains_biases[3 * D :]
    second = seq_index.astype(wide)

    positions = loss_positions[:, 0]
    targets = loss_targets[:, 0]
    ids_all = gather_labels(token_ids[:, 0], lengths, positions, targets, 1)
    base = tokens // 128
    all_tokens = ids_all[:, :base].reshape(devices_all, tokens)
    all_targets = ids_all[:, base : base + micros, :loss_dev].reshape(-1)
    all_counted = ids_all[:, base + micros : base + 2 * micros, :loss_dev]
    all_live = ids_all[:, base + 2 * micros : base + 3 * micros, 0]

    down_here = feed_out.shape[1]
    pieces = -(-down_here // features)
    down_pad = jnp.pad(feed_out[0], ((0, pieces * features - down_here), (0, 0)))
    down_pad = [down_pad[k * features : (k + 1) * features] for k in range(pieces)]
    packed = jnp.concatenate([feed_in[0]] + down_pad + [attention_out[0], attention_in[0]], axis=1)
    w_all = lax.all_gather(packed.astype(low), both, axis=0, tiled=True)
    down_at = 2 * FF
    out_at = down_at + pieces * D
    w_feed = w_all[:, :down_at]
    w_out = w_all[:, out_at : out_at + D]
    w_in = w_all[:, out_at + D :]
    w_down = jnp.swapaxes(w_all[:, down_at:out_at].reshape(devices_all, features, pieces, D), 1, 2)
    w_down = w_down.reshape(devices_all, pieces * features, D)[:, :down_here].reshape(FF, D)
    head_low = unembedding.astype(low)

    arrived = exchange(lookup(all_live, all_tokens, embedding.T), 5)
    x_t = arrived.reshape(D, tokens)
    x_wide = x_t.astype(wide)
    inverse_one = lax.rsqrt(jnp.mean(x_wide * x_wide, axis=0, keepdims=True) + epsilon)
    normed_t = (x_wide * inverse_one * gain_rows[0][:, None]).astype(low)

    project_t = dot(w_in[:, D:], normed_t, 0, 0)
    kv_t = project_t[: 2 * D].astype(low)
    forget_t = (project_t[2 * D :] + bias_row[:, None]).astype(low).astype(wide)
    pick = [
        (positions[m][:, None] == jnp.arange(half)[None, :]).astype(low) for m in range(micros)
    ]

    def per_micro(array, m):
        return array[:, m * half : (m + 1) * half]

    x_rows = jnp.concatenate([dot(pick[m], per_micro(x_t, m), 1, 1) for m in range(micros)])
    normed_rows = jnp.concatenate(
        [dot(pick[m], per_micro(normed_t, m), 1, 1) for m in range(micros)]
    ).astype(low)
    q_rows = dot(normed_rows, w_in[:, :D], 1, 0).astype(low)

    upper = (jnp.arange(half)[:, None] <= jnp.arange(half)[None, :]).astype(wide)
    log_gate = jax.nn.log_sigmoid(forget_t).reshape(H, micros, half)
    decay_own = lax.dot_general(
        log_gate, upper, (((2,), (0,)), ((), ())), precision=highest, preferred_element_type=wide
    )
    total_own = decay_own[:, :, -1]
    decay_rows = jnp.stack(
        [dot(pick[m].astype(wide), decay_own[:, m], 1, 1, highest) for m in range(micros)]
    )
    q_own = q_rows.reshape(micros, loss_dev, H, HD)
    q_far, decay_far, total_far, place_far = other_core((q_own, decay_rows, total_own, positions))
    shift_own = second * total_far
    shift_far = (1.0 - second) * total_own
    key_decay = decay_own + shift_own[:, :, None]
    row_decay = jnp.concatenate(
        [decay_rows + shift_own.T[:, None], decay_far + shift_far.T[:, None]], axis=1
    )
    q_all = jnp.concatenate([q_own, q_far], axis=1)
    places = jnp.concatenate(
        [positions + seq_index * half, place_far + (1 - seq_index) * half], axis=1
    )
    key_places = seq_index * half + jnp.arange(half)
    keys_t = kv_t[:D].reshape(H, HD, tokens)
    values_t = kv_t[D:].reshape(H, HD, tokens)

    scores = []
    for m in range(micros):
        keys_m = keys_t[:, :, m * half : (m + 1) * half]
        raw = jnp.einsum("rhd,hdj->hrj", q_all[m], keys_m, preferred_element_type=wide)
        part = raw * HD ** (-0.5) + row_decay[m].T[:, :, None] - key_decay[:, m][:, None, :]
        causal = places[m][:, None] >= key_places[None, :]
        scores.append(jnp.where(causal[None], part, negative))
    scores = jnp.stack(scores)
    peak_own = jnp.max(scores, axis=-1)
    spread_own = jnp.sum(jnp.exp(scores - peak_own[..., None]), axis=-1)
    peak_far, spread_far = other_core((peak_own, spread_own))

    def swap_rows(array):
        return jnp.concatenate([array[:, :, loss_dev:], array[:, :, :loss_dev]], axis=2)

    peak_far, spread_far = swap_rows(peak_far), swap_rows(spread_far)
    peak = jnp.maximum(peak_own, peak_far)
    log_total = peak + jnp.log(
        spread_own * jnp.exp(peak_own - peak) + spread_far * jnp.exp(peak_far - peak)
    )
    probs = jnp.exp(scores - log_total[..., None])
    probs_low = probs.astype(low)
    probs_rest = (probs - probs_low.astype(wide)).astype(low)

    def mix(weights):
        return jnp.stack(
            [
                jnp.einsum(
                    "hrj,hdj->rhd",
                    weights[m],
                    values_t[:, :, m * half : (m + 1) * half],
                    preferred_element_type=wide,
                )
                for m in range(micros)
            ]
        )

    mixed_part = mix(probs_low)
    rest_part = mix(probs_rest)
    mixed_far, rest_far = other_core((mixed_part[:, loss_dev:], rest_part[:, loss_dev:]))
    mixed_sum = mixed_part[:, :loss_dev] + mixed_far
    mixed_full = mixed_sum + rest_part[:, :loss_dev] + rest_far
    mixed_rows = mixed_sum.reshape(rows, D).astype(low)

    middle = x_rows + dot(mixed_rows, w_out, 1, 0)
    normed_two, inverse_two = norm_forward(middle, gain_rows[1])
    normed_two = normed_two.astype(low)
    gate_up = dot(normed_two, w_feed, 1, 0)
    gate_half, up_half = gate_up[:, :FF], gate_up[:, FF:]
    gate_sigmoid = jax.nn.sigmoid(gate_half)
    hidden = (gate_half * gate_sigmoid * up_half).astype(low)
    final_in = middle + dot(hidden, w_down, 1, 0)
    final_normed, final_inverse = norm_forward(final_in, gain_rows[2])

    final_all = gather_rows(final_normed.astype(low), 2).reshape(rows_all, D)
    logits = dot(final_all, head_low, 1, 1)
    vocab_ids = device * vocab_here + jnp.arange(vocab_here)
    target_hits = all_targets[:, None] == vocab_ids[None, :]
    row_peak = jnp.max(logits, axis=1)
    exp_sum = jnp.sum(jnp.exp(logits - row_peak[:, None]), axis=1)
    target_part = jnp.sum(jnp.where(target_hits, logits, 0.0), axis=1)
    logit_sum = jnp.sum(logits, axis=1)
    stats = jnp.stack([row_peak, exp_sum, target_part, logit_sum])
    stats_all = gather_rows(stats.reshape(-1, 128), 3).reshape(devices_all, 4, rows_all)
    peak_all = jnp.max(stats_all[:, 0], axis=0)
    spread_all = jnp.sum(stats_all[:, 1] * jnp.exp(stats_all[:, 0] - peak_all), axis=0)
    target_all = jnp.sum(stats_all[:, 2], axis=0)
    logit_all = jnp.sum(stats_all[:, 3], axis=0)
    total_all = peak_all + jnp.log(spread_all)
    per_row = (
        total_all
        - (1.0 - smooth) * target_all
        - smooth * logit_all / V
        + z_weight * total_all * total_all
    )
    weights_row = all_counted.astype(wide).reshape(devices_all, micros, loss_dev)
    counts = jnp.sum(weights_row, axis=(0, 2))
    weights_row = (weights_row / (micros * counts)[None, :, None]).reshape(-1)
    loss_value = jnp.sum(weights_row * per_row)
    soft_rows = jnp.exp(logits - total_all[:, None])
    grad_logits = (
        weights_row[:, None]
        * (
            soft_rows * (1.0 + 2.0 * z_weight * total_all)[:, None]
            - (1.0 - smooth) * target_hits.astype(wide)
            - smooth / V
        )
    ).astype(low)
    head_grad = dot(grad_logits, final_all, 0, 0)
    grad_final = reduce_rows(dot(grad_logits, head_low, 1, 0), 7)

    grad_rows, gain_grad_final = norm_backward(final_in, final_inverse, gain_rows[2], grad_final)
    grad_branch = grad_rows.astype(low)
    grad_hidden = dot(grad_branch, w_down, 1, 1)
    grad_gate = grad_hidden * up_half * gate_sigmoid * (1.0 + gate_half * (1.0 - gate_sigmoid))
    grad_up = grad_hidden * gate_half * gate_sigmoid
    grad_gate_up = jnp.concatenate([grad_gate, grad_up], axis=1).astype(low)
    grad_two, gain_grad_two = norm_backward(
        middle, inverse_two, gain_rows[1], dot(grad_gate_up, w_feed, 1, 1)
    )
    grad_middle = grad_rows + grad_two
    grad_mid_low = grad_middle.astype(low)
    grad_mixed = dot(grad_mid_low, w_out, 1, 1).astype(low)

    rows_all_packed = lax.all_gather(
        jnp.concatenate([normed_two, grad_branch, grad_mid_low], axis=1), both, axis=0, tiled=True
    )
    columns_packed = lax.all_to_all(
        jnp.concatenate(
            [
                hidden.reshape(rows, devices_all, gate_here),
                mixed_rows.reshape(rows, devices_all, features),
            ],
            axis=2,
        ),
        both,
        split_axis=1,
        concat_axis=0,
        tiled=True,
    )
    gate_up_columns = lax.all_to_all(
        grad_gate_up.reshape(rows, 2, devices_all, gate_here),
        both,
        split_axis=2,
        concat_axis=0,
        tiled=True,
    )

    grad_own = grad_mixed.reshape(micros, loss_dev, H, HD)
    inner_own = jnp.sum(grad_own.astype(wide) * mixed_full, axis=-1)
    grad_far, inner_far = other_core((grad_own, inner_own))
    grad_heads = jnp.concatenate([grad_own, grad_far], axis=1)
    inner_sum = jnp.concatenate([inner_own, inner_far], axis=1)
    query_parts, score_rows = [], []
    grad_keys, grad_values, score_columns = [], [], []
    for m in range(micros):
        keys_m = keys_t[:, :, m * half : (m + 1) * half]
        values_m = values_t[:, :, m * half : (m + 1) * half]
        grad_probs = jnp.einsum("rhd,hdj->hrj", grad_heads[m], values_m, preferred_element_type=wide)
        grad_scores = (probs[m] * (grad_probs - inner_sum[m].T[:, :, None])).astype(low)
        query_parts.append(
            jnp.einsum("hrj,hdj->rhd", grad_scores, keys_m, preferred_element_type=wide)
        )
        grad_keys.append(
            jnp.einsum("hrj,rhd->hdj", grad_scores, q_all[m], preferred_element_type=wide)
            * HD ** (-0.5)
        )
        grad_values.append(
            jnp.einsum("hrj,rhd->hdj", probs_low[m], grad_heads[m], preferred_element_type=wide)
        )
        score_wide = grad_scores.astype(wide)
        score_rows.append(jnp.sum(score_wide, axis=-1))
        score_columns.append(jnp.sum(score_wide, axis=1))
    query_parts = jnp.stack(query_parts)
    score_rows = jnp.stack(score_rows).transpose(0, 2, 1)
    query_far, score_far = other_core((query_parts[:, loss_dev:], score_rows[:, loss_dev:]))
    grad_query = ((query_parts[:, :loss_dev] + query_far) * HD ** (-0.5)).astype(low)
    grad_query = grad_query.reshape(rows, D)
    rows_sum = score_rows[:, :loss_dev] + score_far
    later = (1.0 - second) * jnp.sum(score_rows[:, loss_dev:], axis=1)
    grad_log = []
    for m in range(micros):
        placed = dot(rows_sum[m], pick[m].astype(wide), 0, 0, highest)
        change = placed - score_columns[m]
        suffix = dot(change, upper, 1, 1, highest)
        grad_log.append(suffix + later[m][:, None])
    grad_log = jnp.concatenate(grad_log, axis=1)
    grad_forget = (grad_log * jax.nn.sigmoid(-forget_t)).astype(low)
    query_t = jnp.concatenate(
        [
            dot(grad_query[m * loss_dev : (m + 1) * loss_dev], pick[m], 0, 0).astype(low)
            for m in range(micros)
        ],
        axis=1,
    )
    keys_part = jnp.concatenate(grad_keys, axis=2).reshape(D, tokens).astype(low)
    values_part = jnp.concatenate(grad_values, axis=2).reshape(D, tokens).astype(low)
    grad_project = jnp.concatenate([query_t, keys_part, values_part, grad_forget], axis=0)
    grad_bias = jnp.sum(grad_forget.astype(wide), axis=1)
    grad_in = lax.psum_scatter(
        dot(normed_t, grad_project, 1, 1), both, scatter_dimension=0, tiled=True
    )
    grad_normed = dot(w_in, grad_project, 1, 0)
    scaled = grad_normed * gain_rows[0][:, None]
    gain_grad_one = jnp.sum(grad_normed * x_wide * inverse_one, axis=1)
    grad_one = inverse_one * scaled - x_wide * inverse_one**3 * jnp.mean(
        x_wide * scaled, axis=0, keepdims=True
    )
    middle_t = jnp.concatenate(
        [
            dot(
                grad_middle[m * loss_dev : (m + 1) * loss_dev],
                pick[m].astype(wide),
                0,
                0,
                highest,
            )
            for m in range(micros)
        ],
        axis=1,
    )
    grad_embed = (middle_t + grad_one).astype(low).reshape(devices_all, features, tokens)
    moved = lax.all_to_all(grad_embed, both, split_axis=0, concat_axis=0, tiled=True)
    rows_all_packed, columns_packed, gate_up_columns, _ = lax.optimization_barrier(
        (rows_all_packed, columns_packed, gate_up_columns, grad_embed[:1, :1, :1])
    )
    columns_packed = columns_packed.reshape(rows_all, gate_here + features)
    gate_up_columns = gate_up_columns.reshape(rows_all, 2 * gate_here)
    grad_feed_columns = dot(rows_all_packed[:, :D], gate_up_columns, 0, 0)
    grad_down = dot(columns_packed[:, :gate_here], rows_all_packed[:, D : 2 * D], 0, 0)
    grad_out = dot(columns_packed[:, gate_here:], rows_all_packed[:, 2 * D :], 0, 0)
    grad_feed = lax.all_to_all(
        grad_feed_columns.reshape(devices_all, features, 2 * gate_here),
        both,
        split_axis=0,
        concat_axis=0,
        tiled=True,
    )
    grad_feed = (
        grad_feed.reshape(devices_all, features, 2, gate_here)
        .transpose(1, 2, 0, 3)
        .reshape(features, 2 * FF)
    )
    embed_grad = scatter_add(all_live, all_tokens, moved, V).T

    grad_in, _ = lax.optimization_barrier((grad_in, embed_grad[:1, :1]))
    owned_grads = [grad_in[None], grad_out[None], grad_feed[None], grad_down[None]]
    owned_grads = owned_grads + [embed_grad, head_grad]
    square_sum = jnp.zeros((), wide)
    for grad_part in owned_grads:
        square_sum = square_sum + jnp.sum(grad_part * grad_part)
    small_grad = jnp.concatenate(
        [gain_grad_one, gain_grad_two, gain_grad_final, grad_bias, square_sum[None]]
    )
    small_count = small_grad.shape[0]
    small_grad = jnp.pad(small_grad, (0, -small_count % 1024)).reshape(-1, 128)
    small_sum = jnp.sum(gather_rows(small_grad, 4), axis=0).reshape(-1)
    small_total, square_total = small_sum[: small_count - 1], small_sum[small_count - 1]
    grad_norm = jnp.sqrt(square_total + jnp.sum(small_total * small_total))
    factor = jnp.minimum(1.0, clip_limit / grad_norm)
    updates = (
        (attention_in, owned_grads[0], attention_in_moment, attention_in_average, rate_layer),
        (attention_out, owned_grads[1], attention_out_moment, attention_out_average, rate_layer),
        (feed_in, owned_grads[2], feed_in_moment, feed_in_average, rate_layer),
        (feed_out, owned_grads[3], feed_out_moment, feed_out_average, rate_layer),
        (embedding, embed_grad, embedding_moment, embedding_average, rate_embed),
        (unembedding, head_grad, unembedding_moment, unembedding_average, rate_head),
        (gains_biases, small_total, gains_biases_moment, gains_biases_average, rate_layer),
    )
    results = [loss_value, grad_norm]
    for weight, grad_full, moment_old, average_old, rate in updates:
        results.extend(apply_update(weight, grad_full, moment_old, average_old, factor, rate))
    return tuple(results)


def solution(mesh):
    rows = P(None, both, None)
    tables = (rows,) * 12 + (P(None, both),) * 3 + (P(both, None),) * 3 + (P(),) * 3
    return jax.shard_map(
        step,
        mesh=mesh,
        in_specs=(
            P(None, "fsdp", "seq"),
            P(None, "fsdp"),
            P(None, "fsdp", "seq"),
            P(None, "fsdp", "seq"),
        )
        + tables,
        out_specs=(P(), P()) + tables,
        check_vma=False,
    )
```

```python
import functools

import jax
import jax.numpy as jnp
from jax import lax
from jax.experimental import pallas as pl
from jax.experimental.pallas import tpu as pltpu
from jax.sharding import PartitionSpec as P

D = 768
H = 12
HD = 64
FF = 2048
V = 32000


epsilon = 1e-06
smooth = 0.1
z_weight = 0.005
clip_limit = 0.5
moment = 0.9
average = 0.9
rate_layer = 200.0
rate_head = 1000.0
rate_embed = 5000.0
negative = -1e30
both = ("seq", "fsdp")
highest = lax.Precision.HIGHEST
MESH = pl.DeviceIdType.MESH


def dot(left_side, right_side, left_axis, right_axis, precision=None):
    return lax.dot_general(
        left_side,
        right_side,
        (((left_axis,), (right_axis,)), ((), ())),
        precision=precision,
        preferred_element_type=jnp.float32,
    )


def line_of(fsdp_count):
    return 4 if fsdp_count % 4 == 0 else 1


def gather_kernel(cores, fsdp, x_ref, o_ref, send_sem, recv_sem):
    plane = line_of(fsdp)
    lines = fsdp // plane
    core = lax.axis_index("seq")
    spot = lax.axis_index("fsdp")
    high, low = spot // plane, spot % plane
    line_peers = [((high + k) % lines) * plane + low for k in range(1, lines)]
    plane_peers = [high * plane + (low + k) % plane for k in range(1, plane)]
    core_peers = [(core + k) % cores for k in range(1, cores)]
    peers = [(core, p) for p in line_peers + plane_peers] + [(c, spot) for c in core_peers]

    barrier = pltpu.get_barrier_semaphore()
    for peer in peers:
        pl.semaphore_signal(barrier, inc=1, device_id=peer, device_id_type=MESH)
    pl.semaphore_wait(barrier, len(peers))

    sent = []

    def send(source_ref, block, peer):
        copy = pltpu.make_async_remote_copy(
            src_ref=source_ref,
            dst_ref=o_ref.at[block],
            send_sem=send_sem.at[len(sent)],
            recv_sem=recv_sem.at[block],
            device_id=peer,
            device_id_type=MESH,
        )
        copy.start()
        sent.append(copy)

    def arrived(block):
        pltpu.make_async_copy(o_ref.at[block], o_ref.at[block], recv_sem.at[block]).wait()

    mine = core * fsdp + spot
    for p in line_peers:
        send(x_ref, mine, (core, p))
    for p in plane_peers:
        send(x_ref, mine, (core, p))
    for c in core_peers:
        send(x_ref, mine, (c, spot))
    o_ref[mine] = x_ref[...]
    for k in range(1, lines):
        block = core * fsdp + ((high + lines - k) % lines) * plane + low
        arrived(block)
        for p in plane_peers:
            send(o_ref.at[block], block, (core, p))
        for c in core_peers:
            send(o_ref.at[block], block, (c, spot))
    for m in range(lines):
        for k in range(1, plane):
            block = core * fsdp + ((high + lines - m) % lines) * plane + (low + plane - k) % plane
            arrived(block)
            for c in core_peers:
                send(o_ref.at[block], block, (c, spot))
    for c in core_peers:
        for m in range(lines):
            for k in range(plane):
                block = c * fsdp + ((high + lines - m) % lines) * plane + (low + plane - k) % plane
                arrived(block)
    for copy in sent:
        copy.wait_send()


def label_kernel(
    cores, fsdp, tokens_ref, lengths_ref, places_ref, targets_ref, o_ref, packed, send_sem, recv_sem
):
    micros, half = tokens_ref.shape
    chunks = half // 128
    start = lax.axis_index("seq") * half
    packed[...] = jnp.zeros_like(packed)
    for m in range(micros):
        for c in range(chunks):
            packed[pl.ds(m * chunks + c, 1), :] = tokens_ref[pl.ds(m, 1), pl.ds(c * 128, 128)]
    base = micros * chunks
    length = lengths_ref[...]
    counted = (start + places_ref[...] < length).astype(jnp.int32)
    live = jnp.clip(length - start, 0, half)
    count = places_ref.shape[1]
    packed[pl.ds(base, micros), pl.ds(0, count)] = targets_ref[...]
    packed[pl.ds(base + micros, micros), pl.ds(0, count)] = counted
    packed[pl.ds(base + 2 * micros, micros), :] = jnp.broadcast_to(live, (micros, 128))
    gather_kernel(cores, fsdp, packed, o_ref, send_sem, recv_sem)


def gather_labels(tokens, lengths, places, targets, collective):
    cores, fsdp = lax.axis_size("seq"), lax.axis_size("fsdp")
    count = cores * fsdp
    micros, half = tokens.shape
    rows = micros * (half // 128) + 3 * micros
    rows = -(-rows // 8) * 8
    return pl.pallas_call(
        functools.partial(label_kernel, cores, fsdp),
        out_shape=jax.ShapeDtypeStruct((count, rows, 128), jnp.int32),
        in_specs=[pl.BlockSpec(memory_space=pltpu.VMEM)] * 4,
        out_specs=pl.BlockSpec(memory_space=pltpu.VMEM),
        scratch_shapes=[
            pltpu.VMEM((rows, 128), jnp.int32),
            pltpu.SemaphoreType.DMA((count,)),
            pltpu.SemaphoreType.DMA((count,)),
        ],
        compiler_params=pltpu.CompilerParams(collective_id=collective, has_side_effects=True),
        name="gather_labels",
    )(tokens, lengths, places, targets)


def gather_rows(array, collective):
    cores, fsdp = lax.axis_size("seq"), lax.axis_size("fsdp")
    count = cores * fsdp
    return pl.pallas_call(
        functools.partial(gather_kernel, cores, fsdp),
        out_shape=jax.ShapeDtypeStruct((count,) + array.shape, array.dtype),
        in_specs=[pl.BlockSpec(memory_space=pltpu.VMEM)],
        out_specs=pl.BlockSpec(memory_space=pltpu.VMEM),
        scratch_shapes=[
            pltpu.SemaphoreType.DMA((count,)),
            pltpu.SemaphoreType.DMA((count,)),
        ],
        compiler_params=pltpu.CompilerParams(collective_id=collective, has_side_effects=True),
        name="gather_rows",
    )(array)


def exchange_kernel(cores, fsdp, x_ref, o_ref, send_sem, recv_sem, own_sem):
    count = cores * fsdp
    mine = lax.axis_index("seq") * fsdp + lax.axis_index("fsdp")

    def place(step):
        other = lax.rem(mine + step, count)
        return other, (other // fsdp, lax.rem(other, fsdp))

    barrier = pltpu.get_barrier_semaphore()

    def greet(step, _):
        pl.semaphore_signal(barrier, inc=1, device_id=place(step)[1], device_id_type=MESH)
        return 0

    lax.fori_loop(1, count, greet, 0)
    pl.semaphore_wait(barrier, count - 1)
    own = pltpu.make_async_copy(x_ref.at[mine], o_ref.at[mine], own_sem)
    own.start()

    def copy_to(step):
        other, peer = place(step)
        return pltpu.make_async_remote_copy(
            src_ref=x_ref.at[other],
            dst_ref=o_ref.at[mine],
            send_sem=send_sem.at[step],
            recv_sem=recv_sem.at[step],
            device_id=peer,
            device_id_type=MESH,
        )

    def start(step, _):
        copy_to(step).start()
        return 0

    lax.fori_loop(1, count, start, 0)
    own.wait()

    def finish(step, _):
        source = lax.rem(mine + count - step, count)
        pltpu.make_async_copy(o_ref.at[source], o_ref.at[source], recv_sem.at[step]).wait()
        copy_to(step).wait_send()
        return 0

    lax.fori_loop(1, count, finish, 0)


def exchange(array, collective):
    cores, fsdp = lax.axis_size("seq"), lax.axis_size("fsdp")
    return pl.pallas_call(
        functools.partial(exchange_kernel, cores, fsdp),
        out_shape=jax.ShapeDtypeStruct(array.shape, array.dtype),
        in_specs=[pl.BlockSpec(memory_space=pltpu.VMEM)],
        out_specs=pl.BlockSpec(memory_space=pltpu.VMEM),
        scratch_shapes=[
            pltpu.SemaphoreType.DMA((cores * fsdp,)),
            pltpu.SemaphoreType.DMA((cores * fsdp,)),
            pltpu.SemaphoreType.DMA,
        ],
        compiler_params=pltpu.CompilerParams(collective_id=collective, has_side_effects=True),
        name="exchange",
    )(array)


def reduce_kernel(
    fsdp, x_ref, o_ref, from_core, from_plane, from_line, core_sum, plane_sum, send_sem, recv_sem
):
    plane = line_of(fsdp)
    lines = fsdp // plane
    core = lax.axis_index("seq")
    spot = lax.axis_index("fsdp")
    high, low = spot // plane, lax.rem(spot, plane)
    far = 1 - core
    peers = [(far, spot)]
    peers += [(core, lax.rem(high + k, lines) * plane + low) for k in range(1, lines)]
    peers += [(core, high * plane + lax.rem(low + k, plane)) for k in range(1, plane)]
    barrier = pltpu.get_barrier_semaphore()
    for peer in peers:
        pl.semaphore_signal(barrier, inc=1, device_id=peer, device_id_type=MESH)
    pl.semaphore_wait(barrier, len(peers))
    sent = []

    def send(source_ref, target_ref, slot, peer):
        copy = pltpu.make_async_remote_copy(
            src_ref=source_ref,
            dst_ref=target_ref,
            send_sem=send_sem.at[slot],
            recv_sem=recv_sem.at[slot],
            device_id=peer,
            device_id_type=MESH,
        )
        copy.start()
        sent.append(copy)
        return copy

    first = []
    for k in list(range(1, plane)) + [0]:
        spot_low = lax.rem(low + k, plane)
        first.append(
            (k, spot_low, send(x_ref.at[far, :, spot_low], from_core.at[spot_low], k, (far, spot)))
        )
    second = []
    for k, spot_low, copy in first:
        copy.wait_recv()
        core_sum[spot_low] = x_ref[core, :, spot_low] + from_core[spot_low]
        if k:
            target = from_plane.at[k - 1]
            peer = (core, high * plane + spot_low)
            second.append((k, send(core_sum.at[spot_low], target, plane + k - 1, peer)))
    plane_sum[...] = core_sum[low]
    for k, copy in second:
        copy.wait_recv()
        plane_sum[...] += from_plane[k - 1]
    third = []
    for k in range(1, lines):
        line = lax.rem(high + k, lines)
        slot = 2 * plane + k - 2
        peer = (core, line * plane + low)
        third.append((k, send(plane_sum.at[line], from_line.at[k - 1], slot, peer)))
    total = plane_sum[high]
    for k, copy in third:
        copy.wait_recv()
        total = total + from_line[k - 1]
    o_ref[...] = total
    for copy in sent:
        copy.wait_send()


def reduce_rows(array, collective):
    cores, fsdp = lax.axis_size("seq"), lax.axis_size("fsdp")
    plane = line_of(fsdp)
    lines = fsdp // plane
    rows, columns = array.shape[0] // (cores * fsdp), array.shape[1]
    kind = array.dtype
    slots = 2 * plane + lines - 2
    return pl.pallas_call(
        functools.partial(reduce_kernel, fsdp),
        out_shape=jax.ShapeDtypeStruct((rows, columns), kind),
        in_specs=[pl.BlockSpec(memory_space=pltpu.VMEM)],
        out_specs=pl.BlockSpec(memory_space=pltpu.VMEM),
        scratch_shapes=[
            pltpu.VMEM((plane, lines, rows, columns), kind),
            pltpu.VMEM((plane - 1, lines, rows, columns), kind),
            pltpu.VMEM((lines - 1, rows, columns), kind),
            pltpu.VMEM((plane, lines, rows, columns), kind),
            pltpu.VMEM((lines, rows, columns), kind),
            pltpu.SemaphoreType.DMA((slots,)),
            pltpu.SemaphoreType.DMA((slots,)),
        ],
        compiler_params=pltpu.CompilerParams(
            collective_id=collective, has_side_effects=True, vmem_limit_bytes=60 * 1024 * 1024
        ),
        name="reduce_rows",
    )(array.reshape(cores, lines, plane, rows, columns))


def lookup_kernel(unroll, builds, live_ref, ids_ref, own_ref, o_ref, table, stage):
    sources, features, tokens = o_ref.shape
    micros = live_ref.shape[0] // sources
    half = tokens // micros

    def build(step, _):
        for u in range(builds):
            at = pl.multiple_of((step * builds + u) * 128, 128)
            block = own_ref[:, pl.ds(at, 128)].astype(jnp.bfloat16).astype(jnp.float32)
            table[pl.ds(at, 128), pl.ds(0, features)] = block.T
        return 0

    lax.fori_loop(0, table.shape[0] // 128 // builds, build, 0)
    stage[...] = jnp.zeros_like(stage)

    def source(which, _):
        def fetch(first, step, _):
            at = first + step * unroll
            ids = [ids_ref[which * tokens + at + u] for u in range(unroll)]
            for u in range(unroll):
                stage[pl.ds(at + u, 1), :] = table[pl.ds(ids[u], 1), :]
            return 0

        for m in range(micros):
            live = live_ref[which * micros + m]
            lax.fori_loop(
                0, (live + unroll - 1) // unroll, functools.partial(fetch, m * half), 0
            )
        for c in range(tokens // 128):
            block = stage[pl.ds(c * 128, 128), :].T
            o_ref[which, :, pl.ds(c * 128, 128)] = block[:features].astype(jnp.bfloat16)
        return 0

    lax.fori_loop(0, sources, source, 0)


def lookup(live, ids, table_t):
    sources, tokens = ids.shape
    features, vocab = table_t.shape
    return pl.pallas_call(
        functools.partial(lookup_kernel, 64, 10),
        out_shape=jax.ShapeDtypeStruct((sources, features, tokens), jnp.bfloat16),
        in_specs=[
            pl.BlockSpec(memory_space=pltpu.SMEM),
            pl.BlockSpec(memory_space=pltpu.SMEM),
            pl.BlockSpec(memory_space=pltpu.VMEM),
        ],
        out_specs=pl.BlockSpec(memory_space=pltpu.VMEM),
        scratch_shapes=[
            pltpu.VMEM((vocab, 128), jnp.float32),
            pltpu.VMEM((tokens, 128), jnp.float32),
        ],
        compiler_params=pltpu.CompilerParams(vmem_limit_bytes=48 * 1024 * 1024),
        name="lookup",
    )(live.reshape(-1), ids.reshape(-1), table_t)


row_bits = 13
row_count = 1 << row_bits


def scatter_kernel(unroll, live_ref, rows_ref, ids_ref, g_ref, o_ref, spread, *sums):
    sources, features, tokens = g_ref.shape
    micros = live_ref.shape[0] // sources
    half = tokens // micros
    vocab = o_ref.shape[1]
    groups = 4

    def clear(step, _):
        for one in sums:
            one[pl.ds(pl.multiple_of(step * 256, 256), 256)] = jnp.zeros((256, 128), jnp.float32)
        return 0

    lax.fori_loop(0, row_count // 256, clear, 0)
    blank = jnp.zeros((128 // groups - features, 128), jnp.float32)
    group = lax.broadcasted_iota(jnp.int32, (128, 128), 0) // (128 // groups)

    def source(which, _):
        for c in range(tokens // 128):
            block = g_ref[which, :, pl.ds(c * 128, 128)].astype(jnp.float32)
            block = jnp.concatenate([block, blank] * groups, axis=0)
            chosen = ids_ref[which, :, pl.ds(c * 128, 128)] >> row_bits
            spread[pl.ds(c * 128, 128), :] = jnp.where(group == chosen, block, 0.0).T

        def add(first, step, _):
            at = first + step * unroll
            rows = [rows_ref[which * tokens + at + u] for u in range(unroll)]
            for u in range(unroll):
                one = sums[u % len(sums)]
                one[pl.ds(rows[u], 1), :] += spread[pl.ds(at + u, 1), :]
            return 0

        for m in range(micros):
            live = live_ref[which * micros + m]
            lax.fori_loop(0, (live + unroll - 1) // unroll, functools.partial(add, m * half), 0)
        return 0

    lax.fori_loop(0, sources, source, 0)

    def finish(step, _):
        for u in range(2):
            at = pl.multiple_of((step * 2 + u) * 128, 128)
            total = sums[0][pl.ds(at, 128)]
            for one in sums[1:]:
                total = total + one[pl.ds(at, 128)]
            total = total.T
            for k in range(groups):
                part = total[k * (128 // groups) : k * (128 // groups) + features]
                if (k + 1) * row_count <= vocab:
                    o_ref[:, pl.ds(k * row_count + at, 128)] = part
                elif k * row_count < vocab:

                    @pl.when(k * row_count + at + 128 <= vocab)
                    def _():
                        o_ref[:, pl.ds(k * row_count + at, 128)] = part

        return 0

    lax.fori_loop(0, row_count // 256, finish, 0)


def scatter_add(live, ids, grads, vocab):
    sources, features, tokens = grads.shape
    return pl.pallas_call(
        functools.partial(scatter_kernel, 32),
        out_shape=jax.ShapeDtypeStruct((features, vocab), jnp.float32),
        in_specs=[
            pl.BlockSpec(memory_space=pltpu.SMEM),
            pl.BlockSpec(memory_space=pltpu.SMEM),
            pl.BlockSpec(memory_space=pltpu.VMEM),
            pl.BlockSpec(memory_space=pltpu.VMEM),
        ],
        out_specs=pl.BlockSpec(memory_space=pltpu.VMEM),
        scratch_shapes=[pltpu.VMEM((tokens, 128), jnp.float32)]
        + [pltpu.VMEM((row_count, 128), jnp.float32)] * 8,
        compiler_params=pltpu.CompilerParams(vmem_limit_bytes=60 * 1024 * 1024),
        name="scatter_add",
    )(
        live.reshape(-1),
        (ids & (row_count - 1)).reshape(-1),
        ids.reshape(sources, 1, tokens),
        grads,
    )


def spread_kernel(hidden_ref, mixed_ref, spread_ref, packed_ref):
    count = packed_ref.shape[0]
    per = hidden_ref.shape[1] // count
    features = mixed_ref.shape[1] // count
    spread_ref[...] = jnp.zeros_like(spread_ref)
    packed_ref[...] = jnp.zeros_like(packed_ref)
    for d in range(count):
        block = hidden_ref[:, pl.ds(d * per, per)]
        packed_ref[d, :, pl.ds(0, per)] = block
        packed_ref[d, :, pl.ds(per, features)] = mixed_ref[:, pl.ds(d * features, features)]
        for k in range(-(-per // features)):
            width = min(features, per - k * features)
            at = (k * count + d) * features
            spread_ref[:, pl.ds(at, width)] = block[:, k * features : k * features + width]


def spread_columns(hidden, mixed, count):
    rows = hidden.shape[0]
    per, features = hidden.shape[1] // count, mixed.shape[1] // count
    pieces = -(-per // features)
    return pl.pallas_call(
        spread_kernel,
        out_shape=(
            jax.ShapeDtypeStruct((rows, pieces * count * features), hidden.dtype),
            jax.ShapeDtypeStruct((count, rows, 128), hidden.dtype),
        ),
        in_specs=[pl.BlockSpec(memory_space=pltpu.VMEM)] * 2,
        out_specs=(pl.BlockSpec(memory_space=pltpu.VMEM),) * 2,
        name="spread_columns",
    )(hidden, mixed)


def collect_kernel(count, spread_ref, o_ref):
    per = o_ref.shape[1] // count
    features = spread_ref.shape[2] // count
    for d in range(count):
        for k in range(spread_ref.shape[0]):
            width = min(features, per - k * features)
            part = spread_ref[k, :, pl.ds(d * features, width)]
            o_ref[:, pl.ds(d * per + k * features, width)] = part


def collect_columns(parts, columns, count):
    return pl.pallas_call(
        functools.partial(collect_kernel, count),
        out_shape=jax.ShapeDtypeStruct((parts.shape[1], columns), parts.dtype),
        in_specs=[pl.BlockSpec(memory_space=pltpu.VMEM)],
        out_specs=pl.BlockSpec(memory_space=pltpu.VMEM),
        name="collect_columns",
    )(parts)


def other_core(arrays):
    return lax.ppermute(arrays, "seq", [(0, 1), (1, 0)])


def norm_forward(values, gain_row):
    inverse = lax.rsqrt(jnp.mean(values * values, axis=-1, keepdims=True) + epsilon)
    return (values * inverse * gain_row, inverse)


def norm_backward(values, inverse, gain_row, grad_out):
    scaled = grad_out * gain_row
    grad_gain = jnp.sum(grad_out * values * inverse, axis=0)
    grad_in = inverse * scaled - values * inverse**3 * jnp.mean(
        values * scaled, axis=-1, keepdims=True
    )
    return (grad_in, grad_gain)


def apply_update(weight_old, grad_full, moment_old, average_old, factor, rate):
    clipped = factor * grad_full
    moment_new = moment * moment_old + clipped
    weight_new = weight_old - rate * (clipped + moment * moment_new)
    average_new = average * average_old + (1.0 - average) * weight_new
    return (weight_new, moment_new, average_new)


def step(
    token_ids,
    lengths,
    loss_positions,
    loss_targets,
    attention_in,
    attention_in_moment,
    attention_in_average,
    attention_out,
    attention_out_moment,
    attention_out_average,
    feed_in,
    feed_in_moment,
    feed_in_average,
    feed_out,
    feed_out_moment,
    feed_out_average,
    embedding,
    embedding_moment,
    embedding_average,
    unembedding,
    unembedding_moment,
    unembedding_average,
    gains_biases,
    gains_biases_moment,
    gains_biases_average,
):
    low = jnp.bfloat16
    wide = jnp.float32
    devices_all = lax.axis_size(both)
    seq_index = lax.axis_index("seq")
    device = lax.axis_index(both)
    micros, _, half = token_ids.shape
    loss_dev = loss_positions.shape[2]
    tokens = micros * half
    rows = micros * loss_dev
    rows_all = devices_all * rows
    vocab_here = unembedding.shape[0]
    features = D // devices_all
    gate_here = FF // devices_all
    gain_rows = gains_biases[: 3 * D].reshape(3, D)
    bias_row = gains_biases[3 * D :]
    second = seq_index.astype(wide)

    positions = loss_positions[:, 0]
    targets = loss_targets[:, 0]
    ids_all = gather_labels(token_ids[:, 0], lengths, positions, targets, 1)
    base = tokens // 128
    all_tokens = ids_all[:, :base].reshape(devices_all, tokens)
    all_targets = ids_all[:, base : base + micros, :loss_dev].reshape(-1)
    all_counted = ids_all[:, base + micros : base + 2 * micros, :loss_dev]
    all_live = ids_all[:, base + 2 * micros : base + 3 * micros, 0]

    down_here = feed_out.shape[1]
    pieces = -(-down_here // features)
    down_pad = jnp.pad(feed_out[0], ((0, pieces * features - down_here), (0, 0)))
    down_pad = [down_pad[k * features : (k + 1) * features] for k in range(pieces)]
    packed = jnp.concatenate([feed_in[0]] + down_pad + [attention_out[0], attention_in[0]], axis=1)
    w_all = lax.all_gather(packed.astype(low), both, axis=0, tiled=True)
    down_at = 2 * FF
    out_at = down_at + pieces * D
    w_feed = w_all[:, :down_at]
    w_out = w_all[:, out_at : out_at + D]
    w_in = w_all[:, out_at + D :]
    w_down = [w_all[:, down_at + k * D : down_at + (k + 1) * D] for k in range(pieces)]
    head_low = unembedding.astype(low)

    arrived = exchange(lookup(all_live, all_tokens, embedding.T), 5)
    x_t = arrived.reshape(D, tokens)
    pick = [
        (positions[m][:, None] == jnp.arange(half)[None, :]).astype(low) for m in range(micros)
    ]
    x_wide, inverse_one, normed_t, keys_t, values_t, forget_t = [], [], [], [], [], []
    for m in range(micros):
        x_wide.append(x_t[:, m * half : (m + 1) * half].astype(wide))
        inverse_one.append(
            lax.rsqrt(jnp.mean(x_wide[m] * x_wide[m], axis=0, keepdims=True) + epsilon)
        )
        normed_t.append((x_wide[m] * inverse_one[m] * gain_rows[0][:, None]).astype(low))

        project_t = dot(w_in[:, D:], normed_t[m], 0, 0)
        keys_t.append(project_t[:D].astype(low).reshape(H, HD, half))
        values_t.append(project_t[D : 2 * D].astype(low).reshape(H, HD, half))
        forget_t.append((project_t[2 * D :] + bias_row[:, None]).astype(low).astype(wide))
    x_rows = jnp.concatenate([dot(pick[m], x_wide[m].astype(low), 1, 1) for m in range(micros)])
    normed_rows = jnp.concatenate(
        [dot(pick[m], normed_t[m], 1, 1) for m in range(micros)]
    ).astype(low)
    q_rows = dot(normed_rows, w_in[:, :D], 1, 0).astype(low)

    upper = (jnp.arange(half)[:, None] <= jnp.arange(half)[None, :]).astype(wide)
    log_gate = jax.nn.log_sigmoid(jnp.stack(forget_t, axis=1))
    decay_own = lax.dot_general(
        log_gate, upper, (((2,), (0,)), ((), ())), precision=highest, preferred_element_type=wide
    )
    total_own = decay_own[:, :, -1]
    decay_rows = jnp.stack(
        [dot(pick[m].astype(wide), decay_own[:, m], 1, 1, highest) for m in range(micros)]
    )
    q_own = q_rows.reshape(micros, loss_dev, H, HD)
    q_far, decay_far, total_far, place_far = other_core((q_own, decay_rows, total_own, positions))
    shift_own = second * total_far
    shift_far = (1.0 - second) * total_own
    key_decay = decay_own + shift_own[:, :, None]
    row_decay = jnp.concatenate(
        [decay_rows + shift_own.T[:, None], decay_far + shift_far.T[:, None]], axis=1
    )
    q_all = jnp.concatenate([q_own, q_far], axis=1)
    places = jnp.concatenate(
        [positions + seq_index * half, place_far + (1 - seq_index) * half], axis=1
    )
    key_places = seq_index * half + jnp.arange(half)

    scores = []
    for m in range(micros):
        raw = jnp.einsum("rhd,hdj->hrj", q_all[m], keys_t[m], preferred_element_type=wide)
        part = raw * HD ** (-0.5) + row_decay[m].T[:, :, None] - key_decay[:, m][:, None, :]
        causal = places[m][:, None] >= key_places[None, :]
        scores.append(jnp.where(causal[None], part, negative))
    scores = jnp.stack(scores)
    peak_own = jnp.max(scores, axis=-1)
    spread_own = jnp.sum(jnp.exp(scores - peak_own[..., None]), axis=-1)
    peak_far, spread_far = other_core((peak_own, spread_own))

    def swap_rows(array):
        return jnp.concatenate([array[:, :, loss_dev:], array[:, :, :loss_dev]], axis=2)

    peak_far, spread_far = swap_rows(peak_far), swap_rows(spread_far)
    peak = jnp.maximum(peak_own, peak_far)
    log_total = peak + jnp.log(
        spread_own * jnp.exp(peak_own - peak) + spread_far * jnp.exp(peak_far - peak)
    )
    probs = jnp.exp(scores - log_total[..., None])
    probs_low = probs.astype(low)
    probs_rest = (probs - probs_low.astype(wide)).astype(low)

    def mix(weights):
        return jnp.stack(
            [
                jnp.einsum(
                    "hrj,hdj->rhd",
                    weights[m],
                    values_t[m],
                    preferred_element_type=wide,
                )
                for m in range(micros)
            ]
        )

    mixed_part = mix(probs_low)
    rest_part = mix(probs_rest)
    mixed_far, rest_far = other_core((mixed_part[:, loss_dev:], rest_part[:, loss_dev:]))
    mixed_sum = mixed_part[:, :loss_dev] + mixed_far
    mixed_full = mixed_sum + rest_part[:, :loss_dev] + rest_far
    mixed_rows = mixed_sum.reshape(rows, D).astype(low)

    middle = x_rows + dot(mixed_rows, w_out, 1, 0)
    normed_two, inverse_two = norm_forward(middle, gain_rows[1])
    normed_two = normed_two.astype(low)
    gate_up = dot(normed_two, w_feed, 1, 0)
    gate_half, up_half = gate_up[:, :FF], gate_up[:, FF:]
    gate_sigmoid = jax.nn.sigmoid(gate_half)
    hidden = (gate_half * gate_sigmoid * up_half).astype(low)
    hidden_spread, columns_packed = spread_columns(hidden, mixed_rows, devices_all)
    final_in = middle
    for k in range(pieces):
        final_in = final_in + dot(hidden_spread[:, k * D : (k + 1) * D], w_down[k], 1, 0)
    final_normed, final_inverse = norm_forward(final_in, gain_rows[2])

    final_all = gather_rows(final_normed.astype(low), 2).reshape(rows_all, D)
    logits = dot(final_all, head_low, 1, 1)
    vocab_ids = device * vocab_here + jnp.arange(vocab_here)
    target_hits = all_targets[:, None] == vocab_ids[None, :]
    row_peak = jnp.max(logits, axis=1)
    exp_sum = jnp.sum(jnp.exp(logits - row_peak[:, None]), axis=1)
    target_part = jnp.sum(jnp.where(target_hits, logits, 0.0), axis=1)
    logit_sum = jnp.sum(logits, axis=1)
    stats = jnp.stack([row_peak, exp_sum, target_part, logit_sum])
    stats_all = gather_rows(stats.reshape(-1, 128), 3).reshape(devices_all, 4, rows_all)
    peak_all = jnp.max(stats_all[:, 0], axis=0)
    spread_all = jnp.sum(stats_all[:, 1] * jnp.exp(stats_all[:, 0] - peak_all), axis=0)
    target_all = jnp.sum(stats_all[:, 2], axis=0)
    logit_all = jnp.sum(stats_all[:, 3], axis=0)
    total_all = peak_all + jnp.log(spread_all)
    per_row = (
        total_all
        - (1.0 - smooth) * target_all
        - smooth * logit_all / V
        + z_weight * total_all * total_all
    )
    weights_row = all_counted.astype(wide).reshape(devices_all, micros, loss_dev)
    counts = jnp.sum(weights_row, axis=(0, 2))
    weights_row = (weights_row / (micros * counts)[None, :, None]).reshape(-1)
    loss_value = jnp.sum(weights_row * per_row)
    soft_rows = jnp.exp(logits - total_all[:, None])
    grad_logits = (
        weights_row[:, None]
        * (
            soft_rows * (1.0 + 2.0 * z_weight * total_all)[:, None]
            - (1.0 - smooth) * target_hits.astype(wide)
            - smooth / V
        )
    ).astype(low)
    head_grad = dot(grad_logits, final_all, 0, 0)
    grad_final = reduce_rows(dot(grad_logits, head_low, 1, 0), 7)

    grad_rows, gain_grad_final = norm_backward(final_in, final_inverse, gain_rows[2], grad_final)
    grad_branch = grad_rows.astype(low)
    grad_hidden = jnp.stack([dot(grad_branch, w_down[k], 1, 1) for k in range(pieces)])
    grad_hidden = collect_columns(grad_hidden, FF, devices_all)
    grad_gate = grad_hidden * up_half * gate_sigmoid * (1.0 + gate_half * (1.0 - gate_sigmoid))
    grad_up = grad_hidden * gate_half * gate_sigmoid
    grad_gate_up = jnp.concatenate([grad_gate, grad_up], axis=1).astype(low)
    grad_two, gain_grad_two = norm_backward(
        middle, inverse_two, gain_rows[1], dot(grad_gate_up, w_feed, 1, 1)
    )
    grad_middle = grad_rows + grad_two
    grad_mid_low = grad_middle.astype(low)
    grad_mixed = dot(grad_mid_low, w_out, 1, 1).astype(low)

    rows_all_packed = lax.all_gather(
        jnp.concatenate([normed_two, grad_branch, grad_mid_low], axis=1), both, axis=0, tiled=True
    )
    columns_packed = lax.all_to_all(
        columns_packed, both, split_axis=0, concat_axis=0, tiled=True
    )
    feed_here = 2 * FF // devices_all
    gate_up_columns = lax.all_to_all(
        jnp.swapaxes(grad_gate_up.reshape(rows, devices_all, feed_here), 0, 1),
        both,
        split_axis=0,
        concat_axis=0,
        tiled=True,
    )

    grad_own = grad_mixed.reshape(micros, loss_dev, H, HD)
    inner_own = jnp.sum(grad_own.astype(wide) * mixed_full, axis=-1)
    grad_far, inner_far = other_core((grad_own, inner_own))
    grad_heads = jnp.concatenate([grad_own, grad_far], axis=1)
    inner_sum = jnp.concatenate([inner_own, inner_far], axis=1)
    query_parts, score_rows = [], []
    grad_keys, grad_values, score_columns = [], [], []
    for m in range(micros):
        grad_probs = jnp.einsum(
            "rhd,hdj->hrj", grad_heads[m], values_t[m], preferred_element_type=wide
        )
        grad_scores = (probs[m] * (grad_probs - inner_sum[m].T[:, :, None])).astype(low)
        query_parts.append(
            jnp.einsum("hrj,hdj->rhd", grad_scores, keys_t[m], preferred_element_type=wide)
        )
        grad_keys.append(
            jnp.einsum("hrj,rhd->hdj", grad_scores, q_all[m], preferred_element_type=wide)
            * HD ** (-0.5)
        )
        grad_values.append(
            jnp.einsum("hrj,rhd->hdj", probs_low[m], grad_heads[m], preferred_element_type=wide)
        )
        score_wide = grad_scores.astype(wide)
        score_rows.append(jnp.sum(score_wide, axis=-1))
        score_columns.append(jnp.sum(score_wide, axis=1))
    query_parts = jnp.stack(query_parts)
    score_rows = jnp.stack(score_rows).transpose(0, 2, 1)
    query_far, score_far = other_core((query_parts[:, loss_dev:], score_rows[:, loss_dev:]))
    grad_query = ((query_parts[:, :loss_dev] + query_far) * HD ** (-0.5)).astype(low)
    grad_query = grad_query.reshape(rows, D)
    rows_sum = score_rows[:, :loss_dev] + score_far
    later = (1.0 - second) * jnp.sum(score_rows[:, loss_dev:], axis=1)
    grad_in_sum, gain_grad_one, grad_bias, grad_embed = 0.0, 0.0, 0.0, []
    projects = []
    for m in range(micros):
        placed = dot(rows_sum[m], pick[m].astype(wide), 0, 0, highest)
        change = placed - score_columns[m]
        grad_log = dot(change, upper, 1, 1, highest) + later[m][:, None]
        grad_forget = (grad_log * jax.nn.sigmoid(-forget_t[m])).astype(low)
        grad_bias = grad_bias + jnp.sum(grad_forget.astype(wide), axis=1)
        query_t = dot(grad_query[m * loss_dev : (m + 1) * loss_dev], pick[m], 0, 0).astype(low)
        keys_part = grad_keys[m].astype(low).reshape(D, half)
        values_part = grad_values[m].astype(low).reshape(D, half)
        projects.append(jnp.concatenate([query_t, keys_part, values_part, grad_forget], axis=0))
        grad_in_sum = grad_in_sum + dot(normed_t[m], projects[m], 1, 1)
    grad_in = lax.psum_scatter(grad_in_sum, both, scatter_dimension=0, tiled=True)
    for m in range(micros):
        grad_normed = dot(w_in, projects[m], 1, 0)
        scaled = grad_normed * gain_rows[0][:, None]
        gain_grad_one = gain_grad_one + jnp.sum(grad_normed * x_wide[m] * inverse_one[m], axis=1)
        grad_one = inverse_one[m] * scaled - x_wide[m] * inverse_one[m] ** 3 * jnp.mean(
            x_wide[m] * scaled, axis=0, keepdims=True
        )
        middle_t = dot(
            grad_middle[m * loss_dev : (m + 1) * loss_dev], pick[m].astype(wide), 0, 0, highest
        )
        grad_embed.append((middle_t + grad_one).astype(low))
    grad_embed = jnp.concatenate(grad_embed, axis=1).reshape(devices_all, features, tokens)
    moved = lax.all_to_all(grad_embed, both, split_axis=0, concat_axis=0, tiled=True)
    rows_all_packed, columns_packed, gate_up_columns, _ = lax.optimization_barrier(
        (rows_all_packed, columns_packed, gate_up_columns, grad_embed[:1, :1, :1])
    )
    columns_packed = columns_packed.reshape(rows_all, 128)
    gate_up_columns = gate_up_columns.reshape(rows_all, feed_here)
    grad_feed_columns = dot(rows_all_packed[:, :D], gate_up_columns, 0, 0)
    grad_down = dot(columns_packed[:, :gate_here], rows_all_packed[:, D : 2 * D], 0, 0)
    out_columns = columns_packed[:, gate_here : gate_here + features]
    grad_out = dot(out_columns, rows_all_packed[:, 2 * D :], 0, 0)
    grad_feed = lax.all_to_all(
        grad_feed_columns.reshape(devices_all, features, feed_here),
        both,
        split_axis=0,
        concat_axis=0,
        tiled=True,
    )
    grad_feed = jnp.swapaxes(grad_feed, 0, 1).reshape(features, 2 * FF)
    embed_grad = scatter_add(all_live, all_tokens, moved, V).T

    grad_in, _ = lax.optimization_barrier((grad_in, embed_grad[:1, :1]))
    owned_grads = [grad_in[None], grad_out[None], grad_feed[None], grad_down[None]]
    owned_grads = owned_grads + [embed_grad, head_grad]
    square_sum = jnp.zeros((), wide)
    for grad_part in owned_grads:
        square_sum = square_sum + jnp.sum(grad_part * grad_part)
    small_grad = jnp.concatenate(
        [gain_grad_one, gain_grad_two, gain_grad_final, grad_bias, square_sum[None]]
    )
    small_count = small_grad.shape[0]
    small_grad = jnp.pad(small_grad, (0, -small_count % 1024)).reshape(-1, 128)
    small_sum = jnp.sum(gather_rows(small_grad, 4), axis=0).reshape(-1)
    small_total, square_total = small_sum[: small_count - 1], small_sum[small_count - 1]
    grad_norm = jnp.sqrt(square_total + jnp.sum(small_total * small_total))
    factor = jnp.minimum(1.0, clip_limit / grad_norm)
    updates = (
        (attention_in, owned_grads[0], attention_in_moment, attention_in_average, rate_layer),
        (attention_out, owned_grads[1], attention_out_moment, attention_out_average, rate_layer),
        (feed_in, owned_grads[2], feed_in_moment, feed_in_average, rate_layer),
        (feed_out, owned_grads[3], feed_out_moment, feed_out_average, rate_layer),
        (embedding, embed_grad, embedding_moment, embedding_average, rate_embed),
        (unembedding, head_grad, unembedding_moment, unembedding_average, rate_head),
        (gains_biases, small_total, gains_biases_moment, gains_biases_average, rate_layer),
    )
    results = [loss_value, grad_norm]
    for weight, grad_full, moment_old, average_old, rate in updates:
        results.extend(apply_update(weight, grad_full, moment_old, average_old, factor, rate))
    return tuple(results)


def solution(mesh):
    rows = P(None, both, None)
    tables = (rows,) * 12 + (P(None, both),) * 3 + (P(both, None),) * 3 + (P(),) * 3
    return jax.shard_map(
        step,
        mesh=mesh,
        in_specs=(
            P(None, "fsdp", "seq"),
            P(None, "fsdp"),
            P(None, "fsdp", "seq"),
            P(None, "fsdp", "seq"),
        )
        + tables,
        out_specs=(P(), P()) + tables,
        check_vma=False,
    )
```

```python
import functools
import math

import jax
import jax.numpy as jnp
from jax import lax
from jax.experimental import pallas as pl
from jax.experimental.pallas import tpu as pltpu
from jax.sharding import PartitionSpec as P

D = 768
H = 12
HD = 64
FF = 2048
V = 32000


epsilon = 1e-06
smooth = 0.1
z_weight = 0.005
clip_limit = 0.5
moment = 0.9
average = 0.9
rate_layer = 200.0
rate_head = 1000.0
rate_embed = 5000.0
negative = -1e30
both = ("seq", "fsdp")
highest = lax.Precision.HIGHEST
MESH = pl.DeviceIdType.MESH


def dot(left_side, right_side, left_axis, right_axis, precision=None):
    return lax.dot_general(
        left_side,
        right_side,
        (((left_axis,), (right_axis,)), ((), ())),
        precision=precision,
        preferred_element_type=jnp.float32,
    )


def room(*arrays):
    total = 1 << 20
    for array in arrays:
        shape, size = array.shape, jnp.dtype(array.dtype).itemsize
        tile = 32 // size
        total += (
            math.prod(shape[:-2]) * (-(-shape[-2] // tile) * tile) * (-(-shape[-1] // 128) * 128)
        ) * size
    return total


def line_of(fsdp_count):
    return 4 if fsdp_count % 4 == 0 else 1


def gather_kernel(cores, fsdp, x_ref, o_ref, send_sem, recv_sem):
    plane = line_of(fsdp)
    lines = fsdp // plane
    core = lax.axis_index("seq")
    spot = lax.axis_index("fsdp")
    high, low = spot // plane, spot % plane
    line_peers = [((high + k) % lines) * plane + low for k in range(1, lines)]
    plane_peers = [high * plane + (low + k) % plane for k in range(1, plane)]
    core_peers = [(core + k) % cores for k in range(1, cores)]
    peers = [(core, p) for p in line_peers + plane_peers] + [(c, spot) for c in core_peers]

    barrier = pltpu.get_barrier_semaphore()
    for peer in peers:
        pl.semaphore_signal(barrier, inc=1, device_id=peer, device_id_type=MESH)
    pl.semaphore_wait(barrier, len(peers))

    sent = []

    def send(source_ref, block, peer):
        copy = pltpu.make_async_remote_copy(
            src_ref=source_ref,
            dst_ref=o_ref.at[block],
            send_sem=send_sem.at[len(sent)],
            recv_sem=recv_sem.at[block],
            device_id=peer,
            device_id_type=MESH,
        )
        copy.start()
        sent.append(copy)

    def arrived(block):
        pltpu.make_async_copy(o_ref.at[block], o_ref.at[block], recv_sem.at[block]).wait()

    mine = core * fsdp + spot
    for p in line_peers:
        send(x_ref, mine, (core, p))
    for p in plane_peers:
        send(x_ref, mine, (core, p))
    for c in core_peers:
        send(x_ref, mine, (c, spot))
    o_ref[mine] = x_ref[...]
    for k in range(1, lines):
        block = core * fsdp + ((high + lines - k) % lines) * plane + low
        arrived(block)
        for p in plane_peers:
            send(o_ref.at[block], block, (core, p))
        for c in core_peers:
            send(o_ref.at[block], block, (c, spot))
    for m in range(lines):
        for k in range(1, plane):
            block = core * fsdp + ((high + lines - m) % lines) * plane + (low + plane - k) % plane
            arrived(block)
            for c in core_peers:
                send(o_ref.at[block], block, (c, spot))
    for c in core_peers:
        for m in range(lines):
            for k in range(plane):
                block = c * fsdp + ((high + lines - m) % lines) * plane + (low + plane - k) % plane
                arrived(block)
    for copy in sent:
        copy.wait_send()


def label_kernel(
    cores, fsdp, tokens_ref, lengths_ref, places_ref, targets_ref, o_ref, packed, send_sem, recv_sem
):
    micros, half = tokens_ref.shape
    chunks = half // 128
    start = lax.axis_index("seq") * half
    packed[...] = jnp.zeros_like(packed)
    for m in range(micros):
        for c in range(chunks):
            packed[pl.ds(m * chunks + c, 1), :] = tokens_ref[pl.ds(m, 1), pl.ds(c * 128, 128)]
    base = micros * chunks
    length = lengths_ref[...]
    counted = (start + places_ref[...] < length).astype(jnp.int32)
    live = jnp.clip(length - start, 0, half)
    count = places_ref.shape[1]
    packed[pl.ds(base, micros), pl.ds(0, count)] = targets_ref[...]
    packed[pl.ds(base + micros, micros), pl.ds(0, count)] = counted
    packed[pl.ds(base + 2 * micros, micros), :] = jnp.broadcast_to(live, (micros, 128))
    gather_kernel(cores, fsdp, packed, o_ref, send_sem, recv_sem)


def gather_labels(tokens, lengths, places, targets, collective):
    cores, fsdp = lax.axis_size("seq"), lax.axis_size("fsdp")
    count = cores * fsdp
    micros, half = tokens.shape
    rows = micros * (half // 128) + 3 * micros
    rows = -(-rows // 8) * 8
    result = jax.ShapeDtypeStruct((count, rows, 128), jnp.int32)
    return pl.pallas_call(
        functools.partial(label_kernel, cores, fsdp),
        out_shape=result,
        in_specs=[pl.BlockSpec(memory_space=pltpu.VMEM)] * 4,
        out_specs=pl.BlockSpec(memory_space=pltpu.VMEM),
        scratch_shapes=[
            pltpu.VMEM((rows, 128), jnp.int32),
            pltpu.SemaphoreType.DMA((count,)),
            pltpu.SemaphoreType.DMA((count,)),
        ],
        compiler_params=pltpu.CompilerParams(
            collective_id=collective, has_side_effects=True, vmem_limit_bytes=room(result)
        ),
        name="gather_labels",
    )(tokens, lengths, places, targets)


def gather_rows(array, collective):
    cores, fsdp = lax.axis_size("seq"), lax.axis_size("fsdp")
    count = cores * fsdp
    result = jax.ShapeDtypeStruct((count,) + array.shape, array.dtype)
    return pl.pallas_call(
        functools.partial(gather_kernel, cores, fsdp),
        out_shape=result,
        in_specs=[pl.BlockSpec(memory_space=pltpu.VMEM)],
        out_specs=pl.BlockSpec(memory_space=pltpu.VMEM),
        scratch_shapes=[
            pltpu.SemaphoreType.DMA((count,)),
            pltpu.SemaphoreType.DMA((count,)),
        ],
        compiler_params=pltpu.CompilerParams(
            collective_id=collective,
            has_side_effects=True,
            vmem_limit_bytes=room(array, result),
        ),
        name="gather_rows",
    )(array)


def exchange_kernel(cores, fsdp, x_ref, o_ref, send_sem, recv_sem, own_sem):
    count = cores * fsdp
    mine = lax.axis_index("seq") * fsdp + lax.axis_index("fsdp")

    def place(step):
        other = lax.rem(mine + step, count)
        return other, (other // fsdp, lax.rem(other, fsdp))

    barrier = pltpu.get_barrier_semaphore()

    def greet(step, _):
        pl.semaphore_signal(barrier, inc=1, device_id=place(step)[1], device_id_type=MESH)
        return 0

    lax.fori_loop(1, count, greet, 0)
    pl.semaphore_wait(barrier, count - 1)
    own = pltpu.make_async_copy(x_ref.at[mine], o_ref.at[mine], own_sem)
    own.start()

    def copy_to(step):
        other, peer = place(step)
        return pltpu.make_async_remote_copy(
            src_ref=x_ref.at[other],
            dst_ref=o_ref.at[mine],
            send_sem=send_sem.at[step],
            recv_sem=recv_sem.at[step],
            device_id=peer,
            device_id_type=MESH,
        )

    def start(step, _):
        copy_to(step).start()
        return 0

    lax.fori_loop(1, count, start, 0)
    own.wait()

    def finish(step, _):
        source = lax.rem(mine + count - step, count)
        pltpu.make_async_copy(o_ref.at[source], o_ref.at[source], recv_sem.at[step]).wait()
        copy_to(step).wait_send()
        return 0

    lax.fori_loop(1, count, finish, 0)


def exchange(array, collective):
    cores, fsdp = lax.axis_size("seq"), lax.axis_size("fsdp")
    return pl.pallas_call(
        functools.partial(exchange_kernel, cores, fsdp),
        out_shape=jax.ShapeDtypeStruct(array.shape, array.dtype),
        in_specs=[pl.BlockSpec(memory_space=pltpu.VMEM)],
        out_specs=pl.BlockSpec(memory_space=pltpu.VMEM),
        scratch_shapes=[
            pltpu.SemaphoreType.DMA((cores * fsdp,)),
            pltpu.SemaphoreType.DMA((cores * fsdp,)),
            pltpu.SemaphoreType.DMA,
        ],
        compiler_params=pltpu.CompilerParams(
            collective_id=collective,
            has_side_effects=True,
            vmem_limit_bytes=room(array, array),
        ),
        name="exchange",
    )(array)


def reduce_kernel(
    fsdp, x_ref, o_ref, from_core, from_plane, from_line, core_sum, plane_sum, send_sem, recv_sem
):
    plane = line_of(fsdp)
    lines = fsdp // plane
    core = lax.axis_index("seq")
    spot = lax.axis_index("fsdp")
    high, low = spot // plane, lax.rem(spot, plane)
    far = 1 - core
    peers = [(far, spot)]
    peers += [(core, lax.rem(high + k, lines) * plane + low) for k in range(1, lines)]
    peers += [(core, high * plane + lax.rem(low + k, plane)) for k in range(1, plane)]
    barrier = pltpu.get_barrier_semaphore()
    for peer in peers:
        pl.semaphore_signal(barrier, inc=1, device_id=peer, device_id_type=MESH)
    pl.semaphore_wait(barrier, len(peers))
    sent = []

    def send(source_ref, target_ref, slot, peer):
        copy = pltpu.make_async_remote_copy(
            src_ref=source_ref,
            dst_ref=target_ref,
            send_sem=send_sem.at[slot],
            recv_sem=recv_sem.at[slot],
            device_id=peer,
            device_id_type=MESH,
        )
        copy.start()
        sent.append(copy)
        return copy

    first = []
    for k in list(range(1, plane)) + [0]:
        spot_low = lax.rem(low + k, plane)
        first.append(
            (k, spot_low, send(x_ref.at[far, :, spot_low], from_core.at[spot_low], k, (far, spot)))
        )
    second = []
    for k, spot_low, copy in first:
        copy.wait_recv()
        core_sum[spot_low] = x_ref[core, :, spot_low] + from_core[spot_low]
        if k:
            target = from_plane.at[k - 1]
            peer = (core, high * plane + spot_low)
            second.append((k, send(core_sum.at[spot_low], target, plane + k - 1, peer)))
    plane_sum[...] = core_sum[low]
    for k, copy in second:
        copy.wait_recv()
        plane_sum[...] += from_plane[k - 1]
    third = []
    for k in range(1, lines):
        line = lax.rem(high + k, lines)
        slot = 2 * plane + k - 2
        peer = (core, line * plane + low)
        third.append((k, send(plane_sum.at[line], from_line.at[k - 1], slot, peer)))
    total = plane_sum[high]
    for k, copy in third:
        copy.wait_recv()
        total = total + from_line[k - 1]
    o_ref[...] = total
    for copy in sent:
        copy.wait_send()


def reduce_rows(array, collective):
    cores, fsdp = lax.axis_size("seq"), lax.axis_size("fsdp")
    plane = line_of(fsdp)
    lines = fsdp // plane
    rows, columns = array.shape[0] // (cores * fsdp), array.shape[1]
    kind = array.dtype
    slots = 2 * plane + lines - 2
    return pl.pallas_call(
        functools.partial(reduce_kernel, fsdp),
        out_shape=jax.ShapeDtypeStruct((rows, columns), kind),
        in_specs=[pl.BlockSpec(memory_space=pltpu.VMEM)],
        out_specs=pl.BlockSpec(memory_space=pltpu.VMEM),
        scratch_shapes=[
            pltpu.VMEM((plane, lines, rows, columns), kind),
            pltpu.VMEM((plane - 1, lines, rows, columns), kind),
            pltpu.VMEM((lines - 1, rows, columns), kind),
            pltpu.VMEM((plane, lines, rows, columns), kind),
            pltpu.VMEM((lines, rows, columns), kind),
            pltpu.SemaphoreType.DMA((slots,)),
            pltpu.SemaphoreType.DMA((slots,)),
        ],
        compiler_params=pltpu.CompilerParams(
            collective_id=collective,
            has_side_effects=True,
            vmem_limit_bytes=room(array, array, array),
        ),
        name="reduce_rows",
    )(array.reshape(cores, lines, plane, rows, columns))


def lookup_kernel(unroll, builds, live_ref, ids_ref, own_ref, o_ref, table, stage):
    sources, features, tokens = o_ref.shape
    micros = live_ref.shape[0] // sources
    half = tokens // micros

    def build(step, _):
        for u in range(builds):
            at = pl.multiple_of((step * builds + u) * 128, 128)
            block = own_ref[:, pl.ds(at, 128)].astype(jnp.bfloat16).astype(jnp.float32)
            table[pl.ds(at, 128), pl.ds(0, features)] = block.T
        return 0

    lax.fori_loop(0, table.shape[0] // 128 // builds, build, 0)
    stage[...] = jnp.zeros_like(stage)

    def source(which, _):
        def fetch(first, step, _):
            at = first + step * unroll
            ids = [ids_ref[which * tokens + at + u] for u in range(unroll)]
            for u in range(unroll):
                stage[pl.ds(at + u, 1), :] = table[pl.ds(ids[u], 1), :]
            return 0

        for m in range(micros):
            live = live_ref[which * micros + m]
            lax.fori_loop(
                0, (live + unroll - 1) // unroll, functools.partial(fetch, m * half), 0
            )
        for c in range(tokens // 128):
            block = stage[pl.ds(c * 128, 128), :].T
            o_ref[which, :, pl.ds(c * 128, 128)] = block[:features].astype(jnp.bfloat16)
        return 0

    lax.fori_loop(0, sources, source, 0)


def lookup(live, ids, table_t):
    sources, tokens = ids.shape
    features, vocab = table_t.shape
    return pl.pallas_call(
        functools.partial(lookup_kernel, 64, 10),
        out_shape=jax.ShapeDtypeStruct((sources, features, tokens), jnp.bfloat16),
        in_specs=[
            pl.BlockSpec(memory_space=pltpu.SMEM),
            pl.BlockSpec(memory_space=pltpu.SMEM),
            pl.BlockSpec(memory_space=pltpu.VMEM),
        ],
        out_specs=pl.BlockSpec(memory_space=pltpu.VMEM),
        scratch_shapes=[
            pltpu.VMEM((vocab, 128), jnp.float32),
            pltpu.VMEM((tokens, 128), jnp.float32),
        ],
        compiler_params=pltpu.CompilerParams(vmem_limit_bytes=32 * 1024 * 1024),
        name="lookup",
    )(live.reshape(-1), ids.reshape(-1), table_t)


row_bits = 13
row_count = 1 << row_bits


def scatter_kernel(unroll, live_ref, rows_ref, ids_ref, g_ref, o_ref, spread, *sums):
    sources, features, tokens = g_ref.shape
    micros = live_ref.shape[0] // sources
    half = tokens // micros
    vocab = o_ref.shape[1]
    groups = 4

    def clear(step, _):
        for one in sums:
            one[pl.ds(pl.multiple_of(step * 256, 256), 256)] = jnp.zeros((256, 128), jnp.float32)
        return 0

    lax.fori_loop(0, row_count // 256, clear, 0)
    blank = jnp.zeros((128 // groups - features, 128), jnp.float32)
    group = lax.broadcasted_iota(jnp.int32, (128, 128), 0) // (128 // groups)

    def source(which, _):
        for c in range(tokens // 128):
            block = g_ref[which, :, pl.ds(c * 128, 128)].astype(jnp.float32)
            block = jnp.concatenate([block, blank] * groups, axis=0)
            chosen = ids_ref[which, :, pl.ds(c * 128, 128)] >> row_bits
            spread[pl.ds(c * 128, 128), :] = jnp.where(group == chosen, block, 0.0).T

        def add(first, step, _):
            at = first + step * unroll
            rows = [rows_ref[which * tokens + at + u] for u in range(unroll)]
            for u in range(unroll):
                one = sums[u % len(sums)]
                one[pl.ds(rows[u], 1), :] += spread[pl.ds(at + u, 1), :]
            return 0

        for m in range(micros):
            live = live_ref[which * micros + m]
            lax.fori_loop(0, (live + unroll - 1) // unroll, functools.partial(add, m * half), 0)
        return 0

    lax.fori_loop(0, sources, source, 0)

    def finish(step, _):
        for u in range(2):
            at = pl.multiple_of((step * 2 + u) * 128, 128)
            total = sums[0][pl.ds(at, 128)]
            for one in sums[1:]:
                total = total + one[pl.ds(at, 128)]
            total = total.T
            for k in range(groups):
                part = total[k * (128 // groups) : k * (128 // groups) + features]
                if (k + 1) * row_count <= vocab:
                    o_ref[:, pl.ds(k * row_count + at, 128)] = part
                elif k * row_count < vocab:

                    @pl.when(k * row_count + at + 128 <= vocab)
                    def _():
                        o_ref[:, pl.ds(k * row_count + at, 128)] = part

        return 0

    lax.fori_loop(0, row_count // 256, finish, 0)


def scatter_add(live, ids, grads, vocab):
    sources, features, tokens = grads.shape
    return pl.pallas_call(
        functools.partial(scatter_kernel, 32),
        out_shape=jax.ShapeDtypeStruct((features, vocab), jnp.float32),
        in_specs=[
            pl.BlockSpec(memory_space=pltpu.SMEM),
            pl.BlockSpec(memory_space=pltpu.SMEM),
            pl.BlockSpec(memory_space=pltpu.VMEM),
            pl.BlockSpec(memory_space=pltpu.VMEM),
        ],
        out_specs=pl.BlockSpec(memory_space=pltpu.VMEM),
        scratch_shapes=[pltpu.VMEM((tokens, 128), jnp.float32)]
        + [pltpu.VMEM((row_count, 128), jnp.float32)] * 8,
        compiler_params=pltpu.CompilerParams(vmem_limit_bytes=44 * 1024 * 1024),
        name="scatter_add",
    )(
        live.reshape(-1),
        (ids & (row_count - 1)).reshape(-1),
        ids.reshape(sources, 1, tokens),
        grads,
    )


def spread_kernel(count, hidden_ref, spread_ref):
    per = hidden_ref.shape[1] // count
    features = spread_ref.shape[1] // (-(-per // (D // count)) * count)
    spread_ref[...] = jnp.zeros_like(spread_ref)
    for d in range(count):
        block = hidden_ref[:, pl.ds(d * per, per)]
        for k in range(-(-per // features)):
            width = min(features, per - k * features)
            at = (k * count + d) * features
            spread_ref[:, pl.ds(at, width)] = block[:, k * features : k * features + width]


def spread_columns(hidden, count):
    rows = hidden.shape[0]
    pieces = -(-(hidden.shape[1] // count) // (D // count))
    result = jax.ShapeDtypeStruct((rows, pieces * D), hidden.dtype)
    return pl.pallas_call(
        functools.partial(spread_kernel, count),
        out_shape=result,
        in_specs=[pl.BlockSpec(memory_space=pltpu.VMEM)],
        out_specs=pl.BlockSpec(memory_space=pltpu.VMEM),
        compiler_params=pltpu.CompilerParams(vmem_limit_bytes=room(hidden, result)),
        name="spread_columns",
    )(hidden)


def pack_kernel(hidden_ref, middle_ref, packed_ref):
    count = packed_ref.shape[0]
    per = hidden_ref.shape[1] // count
    features = middle_ref.shape[1] // count
    packed_ref[...] = jnp.zeros_like(packed_ref)
    for d in range(count):
        packed_ref[d, :, pl.ds(0, per)] = hidden_ref[:, pl.ds(d * per, per)]
        packed_ref[d, :, pl.ds(per, features)] = middle_ref[:, pl.ds(d * features, features)]


def pack_columns(hidden, middle, count):
    result = jax.ShapeDtypeStruct((count, hidden.shape[0], 128), hidden.dtype)
    return pl.pallas_call(
        pack_kernel,
        out_shape=result,
        in_specs=[pl.BlockSpec(memory_space=pltpu.VMEM)] * 2,
        out_specs=pl.BlockSpec(memory_space=pltpu.VMEM),
        compiler_params=pltpu.CompilerParams(vmem_limit_bytes=room(hidden, middle, result)),
        name="pack_columns",
    )(hidden, middle)


def collect_kernel(count, spread_ref, o_ref):
    per = o_ref.shape[1] // count
    features = spread_ref.shape[2] // count
    for d in range(count):
        for k in range(spread_ref.shape[0]):
            width = min(features, per - k * features)
            part = spread_ref[k, :, pl.ds(d * features, width)]
            o_ref[:, pl.ds(d * per + k * features, width)] = part


def collect_columns(parts, columns, count):
    return pl.pallas_call(
        functools.partial(collect_kernel, count),
        out_shape=jax.ShapeDtypeStruct((parts.shape[1], columns), parts.dtype),
        in_specs=[pl.BlockSpec(memory_space=pltpu.VMEM)],
        out_specs=pl.BlockSpec(memory_space=pltpu.VMEM),
        compiler_params=pltpu.CompilerParams(vmem_limit_bytes=room(parts, parts)),
        name="collect_columns",
    )(parts)


def other_core(arrays):
    return lax.ppermute(arrays, "seq", [(0, 1), (1, 0)])


def norm_forward(values, gain_row):
    inverse = lax.rsqrt(jnp.mean(values * values, axis=-1, keepdims=True) + epsilon)
    return (values * inverse * gain_row, inverse)


def norm_backward(values, inverse, gain_row, grad_out):
    scaled = grad_out * gain_row
    grad_gain = jnp.sum(grad_out * values * inverse, axis=0)
    grad_in = inverse * scaled - values * inverse**3 * jnp.mean(
        values * scaled, axis=-1, keepdims=True
    )
    return (grad_in, grad_gain)


def apply_update(weight_old, grad_full, moment_old, average_old, factor, rate):
    clipped = factor * grad_full
    moment_new = moment * moment_old + clipped
    weight_new = weight_old - rate * (clipped + moment * moment_new)
    average_new = average * average_old + (1.0 - average) * weight_new
    return (weight_new, moment_new, average_new)


def step(
    token_ids,
    lengths,
    loss_positions,
    loss_targets,
    attention_in,
    attention_in_moment,
    attention_in_average,
    attention_out,
    attention_out_moment,
    attention_out_average,
    feed_in,
    feed_in_moment,
    feed_in_average,
    feed_out,
    feed_out_moment,
    feed_out_average,
    embedding,
    embedding_moment,
    embedding_average,
    unembedding,
    unembedding_moment,
    unembedding_average,
    gains_biases,
    gains_biases_moment,
    gains_biases_average,
):
    low = jnp.bfloat16
    wide = jnp.float32
    devices_all = lax.axis_size(both)
    seq_index = lax.axis_index("seq")
    device = lax.axis_index(both)
    micros, _, half = token_ids.shape
    loss_dev = loss_positions.shape[2]
    tokens = micros * half
    rows = micros * loss_dev
    rows_all = devices_all * rows
    vocab_here = unembedding.shape[0]
    features = D // devices_all
    gate_here = FF // devices_all
    gain_rows = gains_biases[: 3 * D].reshape(3, D)
    bias_row = gains_biases[3 * D :]
    second = seq_index.astype(wide)

    positions = loss_positions[:, 0]
    targets = loss_targets[:, 0]
    ids_all = gather_labels(token_ids[:, 0], lengths, positions, targets, 1)
    base = tokens // 128
    all_tokens = ids_all[:, :base].reshape(devices_all, tokens)
    all_targets = ids_all[:, base : base + micros, :loss_dev].reshape(-1)
    all_counted = ids_all[:, base + micros : base + 2 * micros, :loss_dev]
    all_live = ids_all[:, base + 2 * micros : base + 3 * micros, 0]

    down_here = feed_out.shape[1]
    pieces = -(-down_here // features)
    down_pad = jnp.pad(feed_out[0], ((0, pieces * features - down_here), (0, 0)))
    down_pad = [down_pad[k * features : (k + 1) * features] for k in range(pieces)]
    packed = jnp.concatenate([feed_in[0]] + down_pad + [attention_out[0], attention_in[0]], axis=1)
    w_all = lax.all_gather(packed.astype(low), both, axis=0, tiled=True)
    down_at = 2 * FF
    out_at = down_at + pieces * D
    w_feed = w_all[:, :down_at]
    w_out = w_all[:, out_at : out_at + D]
    w_in = w_all[:, out_at + D :]
    w_down = [w_all[:, down_at + k * D : down_at + (k + 1) * D] for k in range(pieces)]
    head_low = unembedding.astype(low)

    arrived = exchange(lookup(all_live, all_tokens, embedding.T), 5)
    x_t = arrived.reshape(D, tokens)
    pick = [
        (positions[m][:, None] == jnp.arange(half)[None, :]).astype(low) for m in range(micros)
    ]
    x_wide, inverse_one, normed_t, keys_t, values_t, forget_t = [], [], [], [], [], []
    for m in range(micros):
        x_wide.append(x_t[:, m * half : (m + 1) * half].astype(wide))
        inverse_one.append(
            lax.rsqrt(jnp.mean(x_wide[m] * x_wide[m], axis=0, keepdims=True) + epsilon)
        )
        normed_t.append((x_wide[m] * inverse_one[m] * gain_rows[0][:, None]).astype(low))

        project_t = dot(w_in[:, D:], normed_t[m], 0, 0)
        keys_t.append(project_t[:D].astype(low).reshape(H, HD, half))
        values_t.append(project_t[D : 2 * D].astype(low).reshape(H, HD, half))
        forget_t.append((project_t[2 * D :] + bias_row[:, None]).astype(low).astype(wide))
    x_rows = jnp.concatenate([dot(pick[m], x_wide[m].astype(low), 1, 1) for m in range(micros)])
    normed_rows = jnp.concatenate(
        [dot(pick[m], normed_t[m], 1, 1) for m in range(micros)]
    ).astype(low)
    q_rows = dot(normed_rows, w_in[:, :D], 1, 0).astype(low)

    upper = (jnp.arange(half)[:, None] <= jnp.arange(half)[None, :]).astype(wide)
    log_gate = jax.nn.log_sigmoid(jnp.stack(forget_t, axis=1))
    decay_own = lax.dot_general(
        log_gate, upper, (((2,), (0,)), ((), ())), precision=highest, preferred_element_type=wide
    )
    total_own = decay_own[:, :, -1]
    decay_rows = jnp.stack(
        [dot(pick[m].astype(wide), decay_own[:, m], 1, 1, highest) for m in range(micros)]
    )
    q_own = q_rows.reshape(micros, loss_dev, H, HD)
    q_far, decay_far, total_far, place_far = other_core((q_own, decay_rows, total_own, positions))
    shift_own = second * total_far
    shift_far = (1.0 - second) * total_own
    key_decay = decay_own + shift_own[:, :, None]
    row_decay = jnp.concatenate(
        [decay_rows + shift_own.T[:, None], decay_far + shift_far.T[:, None]], axis=1
    )
    q_all = jnp.concatenate([q_own, q_far], axis=1)
    places = jnp.concatenate(
        [positions + seq_index * half, place_far + (1 - seq_index) * half], axis=1
    )
    key_places = seq_index * half + jnp.arange(half)

    scores = []
    for m in range(micros):
        raw = jnp.einsum("rhd,hdj->hrj", q_all[m], keys_t[m], preferred_element_type=wide)
        part = raw * HD ** (-0.5) + row_decay[m].T[:, :, None] - key_decay[:, m][:, None, :]
        causal = places[m][:, None] >= key_places[None, :]
        scores.append(jnp.where(causal[None], part, negative))
    scores = jnp.stack(scores)
    peak_own = jnp.max(scores, axis=-1)
    spread_own = jnp.sum(jnp.exp(scores - peak_own[..., None]), axis=-1)
    peak_far, spread_far = other_core((peak_own, spread_own))

    def swap_rows(array):
        return jnp.concatenate([array[:, :, loss_dev:], array[:, :, :loss_dev]], axis=2)

    peak_far, spread_far = swap_rows(peak_far), swap_rows(spread_far)
    peak = jnp.maximum(peak_own, peak_far)
    log_total = peak + jnp.log(
        spread_own * jnp.exp(peak_own - peak) + spread_far * jnp.exp(peak_far - peak)
    )
    probs = jnp.exp(scores - log_total[..., None])
    probs_low = probs.astype(low)
    probs_rest = (probs - probs_low.astype(wide)).astype(low)

    def mix(weights):
        return jnp.stack(
            [
                jnp.einsum(
                    "hrj,hdj->rhd",
                    weights[m],
                    values_t[m],
                    preferred_element_type=wide,
                )
                for m in range(micros)
            ]
        )

    mixed_part = mix(probs_low)
    rest_part = mix(probs_rest)
    mixed_far, rest_far = other_core((mixed_part[:, loss_dev:], rest_part[:, loss_dev:]))
    mixed_sum = mixed_part[:, :loss_dev] + mixed_far
    mixed_full = mixed_sum + rest_part[:, :loss_dev] + rest_far
    mixed_rows = mixed_sum.reshape(rows, D).astype(low)

    middle = x_rows + dot(mixed_rows, w_out, 1, 0)
    normed_two, inverse_two = norm_forward(middle, gain_rows[1])
    normed_two = normed_two.astype(low)
    gate_up = dot(normed_two, w_feed, 1, 0)
    gate_half, up_half = gate_up[:, :FF], gate_up[:, FF:]
    gate_sigmoid = jax.nn.sigmoid(gate_half)
    hidden = (gate_half * gate_sigmoid * up_half).astype(low)
    hidden_spread = spread_columns(hidden, devices_all)
    early_packed = lax.all_gather(
        jnp.concatenate([normed_two, mixed_rows], axis=1), both, axis=0, tiled=True
    )
    final_in = middle
    for k in range(pieces):
        final_in = final_in + dot(hidden_spread[:, k * D : (k + 1) * D], w_down[k], 1, 0)
    final_normed, final_inverse = norm_forward(final_in, gain_rows[2])

    final_all = gather_rows(final_normed.astype(low), 2).reshape(rows_all, D)
    logits = dot(final_all, head_low, 1, 1)
    vocab_ids = device * vocab_here + jnp.arange(vocab_here)
    target_hits = all_targets[:, None] == vocab_ids[None, :]
    row_peak = jnp.max(logits, axis=1)
    exp_sum = jnp.sum(jnp.exp(logits - row_peak[:, None]), axis=1)
    target_part = jnp.sum(jnp.where(target_hits, logits, 0.0), axis=1)
    logit_sum = jnp.sum(logits, axis=1)
    stats = jnp.stack([row_peak, exp_sum, target_part, logit_sum])
    stats_all = gather_rows(stats.reshape(-1, 128), 3).reshape(devices_all, 4, rows_all)
    peak_all = jnp.max(stats_all[:, 0], axis=0)
    spread_all = jnp.sum(stats_all[:, 1] * jnp.exp(stats_all[:, 0] - peak_all), axis=0)
    target_all = jnp.sum(stats_all[:, 2], axis=0)
    logit_all = jnp.sum(stats_all[:, 3], axis=0)
    total_all = peak_all + jnp.log(spread_all)
    per_row = (
        total_all
        - (1.0 - smooth) * target_all
        - smooth * logit_all / V
        + z_weight * total_all * total_all
    )
    weights_row = all_counted.astype(wide).reshape(devices_all, micros, loss_dev)
    counts = jnp.sum(weights_row, axis=(0, 2))
    weights_row = (weights_row / (micros * counts)[None, :, None]).reshape(-1)
    loss_value = jnp.sum(weights_row * per_row)
    soft_rows = jnp.exp(logits - total_all[:, None])
    grad_logits = (
        weights_row[:, None]
        * (
            soft_rows * (1.0 + 2.0 * z_weight * total_all)[:, None]
            - (1.0 - smooth) * target_hits.astype(wide)
            - smooth / V
        )
    ).astype(low)
    head_grad = dot(grad_logits, final_all, 0, 0)
    grad_final = reduce_rows(dot(grad_logits, head_low, 1, 0), 7)

    grad_rows, gain_grad_final = norm_backward(final_in, final_inverse, gain_rows[2], grad_final)
    grad_branch = grad_rows.astype(low)
    grad_hidden = jnp.stack([dot(grad_branch, w_down[k], 1, 1) for k in range(pieces)])
    grad_hidden = collect_columns(grad_hidden, FF, devices_all)
    grad_gate = grad_hidden * up_half * gate_sigmoid * (1.0 + gate_half * (1.0 - gate_sigmoid))
    grad_up = grad_hidden * gate_half * gate_sigmoid
    grad_gate_up = jnp.concatenate([grad_gate, grad_up], axis=1).astype(low)
    grad_two, gain_grad_two = norm_backward(
        middle, inverse_two, gain_rows[1], dot(grad_gate_up, w_feed, 1, 1)
    )
    grad_middle = grad_rows + grad_two
    grad_mid_low = grad_middle.astype(low)
    grad_mixed = dot(grad_mid_low, w_out, 1, 1).astype(low)

    branch_all = lax.all_gather(grad_branch, both, axis=0, tiled=True)
    columns_packed = lax.all_to_all(
        pack_columns(hidden, grad_mid_low, devices_all),
        both,
        split_axis=0,
        concat_axis=0,
        tiled=True,
    )
    feed_here = 2 * FF // devices_all
    gate_up_columns = lax.all_to_all(
        jnp.swapaxes(grad_gate_up.reshape(rows, devices_all, feed_here), 0, 1),
        both,
        split_axis=0,
        concat_axis=0,
        tiled=True,
    )

    grad_own = grad_mixed.reshape(micros, loss_dev, H, HD)
    inner_own = jnp.sum(grad_own.astype(wide) * mixed_full, axis=-1)
    grad_far, inner_far = other_core((grad_own, inner_own))
    grad_heads = jnp.concatenate([grad_own, grad_far], axis=1)
    inner_sum = jnp.concatenate([inner_own, inner_far], axis=1)
    query_parts, score_rows = [], []
    grad_keys, grad_values, score_columns = [], [], []
    for m in range(micros):
        grad_probs = jnp.einsum(
            "rhd,hdj->hrj", grad_heads[m], values_t[m], preferred_element_type=wide
        )
        grad_scores = (probs[m] * (grad_probs - inner_sum[m].T[:, :, None])).astype(low)
        query_parts.append(
            jnp.einsum("hrj,hdj->rhd", grad_scores, keys_t[m], preferred_element_type=wide)
        )
        grad_keys.append(
            jnp.einsum("hrj,rhd->hdj", grad_scores, q_all[m], preferred_element_type=wide)
            * HD ** (-0.5)
        )
        grad_values.append(
            jnp.einsum("hrj,rhd->hdj", probs_low[m], grad_heads[m], preferred_element_type=wide)
        )
        score_wide = grad_scores.astype(wide)
        score_rows.append(jnp.sum(score_wide, axis=-1))
        score_columns.append(jnp.sum(score_wide, axis=1))
    query_parts = jnp.stack(query_parts)
    score_rows = jnp.stack(score_rows).transpose(0, 2, 1)
    query_far, score_far = other_core((query_parts[:, loss_dev:], score_rows[:, loss_dev:]))
    grad_query = ((query_parts[:, :loss_dev] + query_far) * HD ** (-0.5)).astype(low)
    grad_query = grad_query.reshape(rows, D)
    rows_sum = score_rows[:, :loss_dev] + score_far
    later = (1.0 - second) * jnp.sum(score_rows[:, loss_dev:], axis=1)
    grad_in_sum, gain_grad_one, grad_bias, grad_embed = 0.0, 0.0, 0.0, []
    projects = []
    for m in range(micros):
        placed = dot(rows_sum[m], pick[m].astype(wide), 0, 0, highest)
        change = placed - score_columns[m]
        grad_log = dot(change, upper, 1, 1, highest) + later[m][:, None]
        grad_forget = (grad_log * jax.nn.sigmoid(-forget_t[m])).astype(low)
        grad_bias = grad_bias + jnp.sum(grad_forget.astype(wide), axis=1)
        query_t = dot(grad_query[m * loss_dev : (m + 1) * loss_dev], pick[m], 0, 0).astype(low)
        keys_part = grad_keys[m].astype(low).reshape(D, half)
        values_part = grad_values[m].astype(low).reshape(D, half)
        projects.append(jnp.concatenate([query_t, keys_part, values_part, grad_forget], axis=0))
        grad_in_sum = grad_in_sum + dot(normed_t[m], projects[m], 1, 1)
    grad_in = lax.psum_scatter(grad_in_sum, both, scatter_dimension=0, tiled=True)
    for m in range(micros):
        grad_normed = dot(w_in, projects[m], 1, 0)
        scaled = grad_normed * gain_rows[0][:, None]
        gain_grad_one = gain_grad_one + jnp.sum(grad_normed * x_wide[m] * inverse_one[m], axis=1)
        grad_one = inverse_one[m] * scaled - x_wide[m] * inverse_one[m] ** 3 * jnp.mean(
            x_wide[m] * scaled, axis=0, keepdims=True
        )
        middle_t = dot(
            grad_middle[m * loss_dev : (m + 1) * loss_dev], pick[m].astype(wide), 0, 0, highest
        )
        grad_embed.append((middle_t + grad_one).astype(low))
    grad_embed = jnp.concatenate(grad_embed, axis=1).reshape(devices_all, features, tokens)
    moved = lax.all_to_all(grad_embed, both, split_axis=0, concat_axis=0, tiled=True)
    early_packed, branch_all, columns_packed, gate_up_columns, _ = lax.optimization_barrier(
        (early_packed, branch_all, columns_packed, gate_up_columns, grad_embed[:1, :1, :1])
    )
    columns_packed = columns_packed.reshape(rows_all, 128)
    gate_up_columns = gate_up_columns.reshape(rows_all, feed_here)
    feed_columns = dot(early_packed[:, :D], gate_up_columns, 0, 0)
    middle_columns = columns_packed[:, gate_here : gate_here + features]
    out_columns = dot(early_packed[:, D:], middle_columns, 0, 0)
    grad_down = dot(columns_packed[:, :gate_here], branch_all, 0, 0)
    grad_feed = lax.all_to_all(
        jnp.concatenate([feed_columns, out_columns], axis=1).reshape(
            devices_all, features, feed_here + features
        ),
        both,
        split_axis=0,
        concat_axis=0,
        tiled=True,
    )
    grad_feed = jnp.swapaxes(grad_feed, 0, 1)
    grad_out = grad_feed[:, :, feed_here:].reshape(features, D)
    grad_feed = grad_feed[:, :, :feed_here].reshape(features, 2 * FF)
    embed_grad = scatter_add(all_live, all_tokens, moved, V).T

    grad_in, _ = lax.optimization_barrier((grad_in, embed_grad[:1, :1]))
    owned_grads = [grad_in[None], grad_out[None], grad_feed[None], grad_down[None]]
    owned_grads = owned_grads + [embed_grad, head_grad]
    square_sum = jnp.zeros((), wide)
    for grad_part in owned_grads:
        square_sum = square_sum + jnp.sum(grad_part * grad_part)
    small_grad = jnp.concatenate(
        [gain_grad_one, gain_grad_two, gain_grad_final, grad_bias, square_sum[None]]
    )
    small_count = small_grad.shape[0]
    small_grad = jnp.pad(small_grad, (0, -small_count % 1024)).reshape(-1, 128)
    small_sum = jnp.sum(gather_rows(small_grad, 4), axis=0).reshape(-1)
    small_total, square_total = small_sum[: small_count - 1], small_sum[small_count - 1]
    grad_norm = jnp.sqrt(square_total + jnp.sum(small_total * small_total))
    factor = jnp.minimum(1.0, clip_limit / grad_norm)
    updates = (
        (attention_in, owned_grads[0], attention_in_moment, attention_in_average, rate_layer),
        (attention_out, owned_grads[1], attention_out_moment, attention_out_average, rate_layer),
        (feed_in, owned_grads[2], feed_in_moment, feed_in_average, rate_layer),
        (feed_out, owned_grads[3], feed_out_moment, feed_out_average, rate_layer),
        (embedding, embed_grad, embedding_moment, embedding_average, rate_embed),
        (unembedding, head_grad, unembedding_moment, unembedding_average, rate_head),
        (gains_biases, small_total, gains_biases_moment, gains_biases_average, rate_layer),
    )
    results = [loss_value, grad_norm]
    for weight, grad_full, moment_old, average_old, rate in updates:
        results.extend(apply_update(weight, grad_full, moment_old, average_old, factor, rate))
    return tuple(results)


def solution(mesh):
    rows = P(None, both, None)
    tables = (rows,) * 12 + (P(None, both),) * 3 + (P(both, None),) * 3 + (P(),) * 3
    return jax.shard_map(
        step,
        mesh=mesh,
        in_specs=(
            P(None, "fsdp", "seq"),
            P(None, "fsdp"),
            P(None, "fsdp", "seq"),
            P(None, "fsdp", "seq"),
        )
        + tables,
        out_specs=(P(), P()) + tables,
        check_vma=False,
    )
```

```python
import functools
import math

import jax
import jax.numpy as jnp
from jax import lax
from jax.experimental import pallas as pl
from jax.experimental.pallas import tpu as pltpu
from jax.sharding import PartitionSpec as P

D = 768
H = 12
HD = 64
FF = 2048
V = 32000


epsilon = 1e-06
smooth = 0.1
z_weight = 0.005
clip_limit = 0.5
moment = 0.9
average = 0.9
rate_layer = 200.0
rate_head = 1000.0
rate_embed = 5000.0
negative = -1e30
both = ("seq", "fsdp")
highest = lax.Precision.HIGHEST
MESH = pl.DeviceIdType.MESH


def dot(left_side, right_side, left_axis, right_axis, precision=None):
    return lax.dot_general(
        left_side,
        right_side,
        (((left_axis,), (right_axis,)), ((), ())),
        precision=precision,
        preferred_element_type=jnp.float32,
    )


def room(*arrays):
    total = 1 << 20
    for array in arrays:
        shape, size = array.shape, jnp.dtype(array.dtype).itemsize
        tile = 32 // size
        total += (
            math.prod(shape[:-2]) * (-(-shape[-2] // tile) * tile) * (-(-shape[-1] // 128) * 128)
        ) * size
    return total


def line_of(fsdp_count):
    return 4 if fsdp_count % 4 == 0 else 1


def gather_kernel(cores, fsdp, x_ref, o_ref, send_sem, recv_sem):
    plane = line_of(fsdp)
    lines = fsdp // plane
    core = lax.axis_index("seq")
    spot = lax.axis_index("fsdp")
    high, low = spot // plane, spot % plane
    line_peers = [((high + k) % lines) * plane + low for k in range(1, lines)]
    plane_peers = [high * plane + (low + k) % plane for k in range(1, plane)]
    core_peers = [(core + k) % cores for k in range(1, cores)]
    peers = [(core, p) for p in line_peers + plane_peers] + [(c, spot) for c in core_peers]

    barrier = pltpu.get_barrier_semaphore()
    for peer in peers:
        pl.semaphore_signal(barrier, inc=1, device_id=peer, device_id_type=MESH)
    pl.semaphore_wait(barrier, len(peers))

    sent = []

    def send(source_ref, block, peer):
        copy = pltpu.make_async_remote_copy(
            src_ref=source_ref,
            dst_ref=o_ref.at[block],
            send_sem=send_sem.at[len(sent)],
            recv_sem=recv_sem.at[block],
            device_id=peer,
            device_id_type=MESH,
        )
        copy.start()
        sent.append(copy)

    def arrived(block):
        pltpu.make_async_copy(o_ref.at[block], o_ref.at[block], recv_sem.at[block]).wait()

    mine = core * fsdp + spot
    for p in line_peers:
        send(x_ref, mine, (core, p))
    for p in plane_peers:
        send(x_ref, mine, (core, p))
    for c in core_peers:
        send(x_ref, mine, (c, spot))
    o_ref[mine] = x_ref[...]
    for k in range(1, lines):
        block = core * fsdp + ((high + lines - k) % lines) * plane + low
        arrived(block)
        for p in plane_peers:
            send(o_ref.at[block], block, (core, p))
        for c in core_peers:
            send(o_ref.at[block], block, (c, spot))
    for m in range(lines):
        for k in range(1, plane):
            block = core * fsdp + ((high + lines - m) % lines) * plane + (low + plane - k) % plane
            arrived(block)
            for c in core_peers:
                send(o_ref.at[block], block, (c, spot))
    for c in core_peers:
        for m in range(lines):
            for k in range(plane):
                block = c * fsdp + ((high + lines - m) % lines) * plane + (low + plane - k) % plane
                arrived(block)
    for copy in sent:
        copy.wait_send()


def label_kernel(
    cores, fsdp, tokens_ref, lengths_ref, places_ref, targets_ref, o_ref, packed, send_sem, recv_sem
):
    micros, half = tokens_ref.shape
    chunks = half // 128
    start = lax.axis_index("seq") * half
    packed[...] = jnp.zeros_like(packed)
    for m in range(micros):
        for c in range(chunks):
            packed[pl.ds(m * chunks + c, 1), :] = tokens_ref[pl.ds(m, 1), pl.ds(c * 128, 128)]
    base = micros * chunks
    length = lengths_ref[...]
    counted = (start + places_ref[...] < length).astype(jnp.int32)
    live = jnp.clip(length - start, 0, half)
    count = places_ref.shape[1]
    packed[pl.ds(base, micros), pl.ds(0, count)] = targets_ref[...]
    packed[pl.ds(base + micros, micros), pl.ds(0, count)] = counted
    packed[pl.ds(base + 2 * micros, micros), :] = jnp.broadcast_to(live, (micros, 128))
    gather_kernel(cores, fsdp, packed, o_ref, send_sem, recv_sem)


def gather_labels(tokens, lengths, places, targets, collective):
    cores, fsdp = lax.axis_size("seq"), lax.axis_size("fsdp")
    count = cores * fsdp
    micros, half = tokens.shape
    rows = micros * (half // 128) + 3 * micros
    rows = -(-rows // 8) * 8
    result = jax.ShapeDtypeStruct((count, rows, 128), jnp.int32)
    return pl.pallas_call(
        functools.partial(label_kernel, cores, fsdp),
        out_shape=result,
        in_specs=[pl.BlockSpec(memory_space=pltpu.VMEM)] * 4,
        out_specs=pl.BlockSpec(memory_space=pltpu.VMEM),
        scratch_shapes=[
            pltpu.VMEM((rows, 128), jnp.int32),
            pltpu.SemaphoreType.DMA((count,)),
            pltpu.SemaphoreType.DMA((count,)),
        ],
        compiler_params=pltpu.CompilerParams(
            collective_id=collective, has_side_effects=True, vmem_limit_bytes=room(result)
        ),
        name="gather_labels",
    )(tokens, lengths, places, targets)


def gather_rows(array, collective):
    cores, fsdp = lax.axis_size("seq"), lax.axis_size("fsdp")
    count = cores * fsdp
    result = jax.ShapeDtypeStruct((count,) + array.shape, array.dtype)
    return pl.pallas_call(
        functools.partial(gather_kernel, cores, fsdp),
        out_shape=result,
        in_specs=[pl.BlockSpec(memory_space=pltpu.VMEM)],
        out_specs=pl.BlockSpec(memory_space=pltpu.VMEM),
        scratch_shapes=[
            pltpu.SemaphoreType.DMA((count,)),
            pltpu.SemaphoreType.DMA((count,)),
        ],
        compiler_params=pltpu.CompilerParams(
            collective_id=collective,
            has_side_effects=True,
            vmem_limit_bytes=room(array, result),
        ),
        name="gather_rows",
    )(array)


def exchange_kernel(cores, fsdp, x_ref, o_ref, send_sem, recv_sem, own_sem):
    count = cores * fsdp
    mine = lax.axis_index("seq") * fsdp + lax.axis_index("fsdp")

    def place(step):
        other = lax.rem(mine + step, count)
        return other, (other // fsdp, lax.rem(other, fsdp))

    barrier = pltpu.get_barrier_semaphore()

    def greet(step, _):
        pl.semaphore_signal(barrier, inc=1, device_id=place(step)[1], device_id_type=MESH)
        return 0

    lax.fori_loop(1, count, greet, 0)
    pl.semaphore_wait(barrier, count - 1)
    own = pltpu.make_async_copy(x_ref.at[mine], o_ref.at[mine], own_sem)
    own.start()

    def copy_to(step):
        other, peer = place(step)
        return pltpu.make_async_remote_copy(
            src_ref=x_ref.at[other],
            dst_ref=o_ref.at[mine],
            send_sem=send_sem.at[step],
            recv_sem=recv_sem.at[step],
            device_id=peer,
            device_id_type=MESH,
        )

    def start(step, _):
        copy_to(step).start()
        return 0

    lax.fori_loop(1, count, start, 0)
    own.wait()

    def finish(step, _):
        source = lax.rem(mine + count - step, count)
        pltpu.make_async_copy(o_ref.at[source], o_ref.at[source], recv_sem.at[step]).wait()
        copy_to(step).wait_send()
        return 0

    lax.fori_loop(1, count, finish, 0)


def exchange(array, collective):
    cores, fsdp = lax.axis_size("seq"), lax.axis_size("fsdp")
    return pl.pallas_call(
        functools.partial(exchange_kernel, cores, fsdp),
        out_shape=jax.ShapeDtypeStruct(array.shape, array.dtype),
        in_specs=[pl.BlockSpec(memory_space=pltpu.VMEM)],
        out_specs=pl.BlockSpec(memory_space=pltpu.VMEM),
        scratch_shapes=[
            pltpu.SemaphoreType.DMA((cores * fsdp,)),
            pltpu.SemaphoreType.DMA((cores * fsdp,)),
            pltpu.SemaphoreType.DMA,
        ],
        compiler_params=pltpu.CompilerParams(
            collective_id=collective,
            has_side_effects=True,
            vmem_limit_bytes=room(array, array),
        ),
        name="exchange",
    )(array)


def reduce_kernel(
    fsdp, x_ref, o_ref, from_core, from_plane, from_line, core_sum, plane_sum, send_sem, recv_sem
):
    plane = line_of(fsdp)
    lines = fsdp // plane
    core = lax.axis_index("seq")
    spot = lax.axis_index("fsdp")
    high, low = spot // plane, lax.rem(spot, plane)
    far = 1 - core
    peers = [(far, spot)]
    peers += [(core, lax.rem(high + k, lines) * plane + low) for k in range(1, lines)]
    peers += [(core, high * plane + lax.rem(low + k, plane)) for k in range(1, plane)]
    barrier = pltpu.get_barrier_semaphore()
    for peer in peers:
        pl.semaphore_signal(barrier, inc=1, device_id=peer, device_id_type=MESH)
    pl.semaphore_wait(barrier, len(peers))
    sent = []

    def send(source_ref, target_ref, slot, peer):
        copy = pltpu.make_async_remote_copy(
            src_ref=source_ref,
            dst_ref=target_ref,
            send_sem=send_sem.at[slot],
            recv_sem=recv_sem.at[slot],
            device_id=peer,
            device_id_type=MESH,
        )
        copy.start()
        sent.append(copy)
        return copy

    first = []
    for k in list(range(1, plane)) + [0]:
        spot_low = lax.rem(low + k, plane)
        first.append(
            (k, spot_low, send(x_ref.at[far, :, spot_low], from_core.at[spot_low], k, (far, spot)))
        )
    second = []
    for k, spot_low, copy in first:
        copy.wait_recv()
        core_sum[spot_low] = x_ref[core, :, spot_low] + from_core[spot_low]
        if k:
            target = from_plane.at[k - 1]
            peer = (core, high * plane + spot_low)
            second.append((k, send(core_sum.at[spot_low], target, plane + k - 1, peer)))
    plane_sum[...] = core_sum[low]
    for k, copy in second:
        copy.wait_recv()
        plane_sum[...] += from_plane[k - 1]
    third = []
    for k in range(1, lines):
        line = lax.rem(high + k, lines)
        slot = 2 * plane + k - 2
        peer = (core, line * plane + low)
        third.append((k, send(plane_sum.at[line], from_line.at[k - 1], slot, peer)))
    total = plane_sum[high]
    for k, copy in third:
        copy.wait_recv()
        total = total + from_line[k - 1]
    o_ref[...] = total
    for copy in sent:
        copy.wait_send()


def reduce_rows(array, collective):
    cores, fsdp = lax.axis_size("seq"), lax.axis_size("fsdp")
    plane = line_of(fsdp)
    lines = fsdp // plane
    rows, columns = array.shape[0] // (cores * fsdp), array.shape[1]
    kind = array.dtype
    slots = 2 * plane + lines - 2
    return pl.pallas_call(
        functools.partial(reduce_kernel, fsdp),
        out_shape=jax.ShapeDtypeStruct((rows, columns), kind),
        in_specs=[pl.BlockSpec(memory_space=pltpu.VMEM)],
        out_specs=pl.BlockSpec(memory_space=pltpu.VMEM),
        scratch_shapes=[
            pltpu.VMEM((plane, lines, rows, columns), kind),
            pltpu.VMEM((plane - 1, lines, rows, columns), kind),
            pltpu.VMEM((lines - 1, rows, columns), kind),
            pltpu.VMEM((plane, lines, rows, columns), kind),
            pltpu.VMEM((lines, rows, columns), kind),
            pltpu.SemaphoreType.DMA((slots,)),
            pltpu.SemaphoreType.DMA((slots,)),
        ],
        compiler_params=pltpu.CompilerParams(
            collective_id=collective,
            has_side_effects=True,
            vmem_limit_bytes=room(array, array, array),
        ),
        name="reduce_rows",
    )(array.reshape(cores, lines, plane, rows, columns))


def lookup_kernel(unroll, builds, live_ref, ids_ref, own_ref, o_ref, table, stage):
    sources, features, tokens = o_ref.shape
    micros = live_ref.shape[0] // sources
    half = tokens // micros

    def build(step, _):
        for u in range(builds):
            at = pl.multiple_of((step * builds + u) * 128, 128)
            block = own_ref[:, pl.ds(at, 128)].astype(jnp.bfloat16).astype(jnp.float32)
            table[pl.ds(at, 128), pl.ds(0, features)] = block.T
        return 0

    lax.fori_loop(0, table.shape[0] // 128 // builds, build, 0)
    stage[...] = jnp.zeros_like(stage)

    def source(which, _):
        def fetch(first, step, _):
            at = first + step * unroll
            ids = [ids_ref[which * tokens + at + u] for u in range(unroll)]
            for u in range(unroll):
                stage[pl.ds(at + u, 1), :] = table[pl.ds(ids[u], 1), :]
            return 0

        for m in range(micros):
            live = live_ref[which * micros + m]
            lax.fori_loop(
                0, (live + unroll - 1) // unroll, functools.partial(fetch, m * half), 0
            )
        for c in range(tokens // 128):
            block = stage[pl.ds(c * 128, 128), :].T
            o_ref[which, :, pl.ds(c * 128, 128)] = block[:features].astype(jnp.bfloat16)
        return 0

    lax.fori_loop(0, sources, source, 0)


def lookup(live, ids, table_t):
    sources, tokens = ids.shape
    features, vocab = table_t.shape
    return pl.pallas_call(
        functools.partial(lookup_kernel, 64, 10),
        out_shape=jax.ShapeDtypeStruct((sources, features, tokens), jnp.bfloat16),
        in_specs=[
            pl.BlockSpec(memory_space=pltpu.SMEM),
            pl.BlockSpec(memory_space=pltpu.SMEM),
            pl.BlockSpec(memory_space=pltpu.VMEM),
        ],
        out_specs=pl.BlockSpec(memory_space=pltpu.VMEM),
        scratch_shapes=[
            pltpu.VMEM((vocab, 128), jnp.float32),
            pltpu.VMEM((tokens, 128), jnp.float32),
        ],
        compiler_params=pltpu.CompilerParams(vmem_limit_bytes=32 * 1024 * 1024),
        name="lookup",
    )(live.reshape(-1), ids.reshape(-1), table_t)


row_bits = 13
row_count = 1 << row_bits


def scatter_kernel(unroll, live_ref, rows_ref, ids_ref, g_ref, o_ref, spread, *sums):
    sources, features, tokens = g_ref.shape
    micros = live_ref.shape[0] // sources
    half = tokens // micros
    vocab = o_ref.shape[1]
    groups = 4

    def clear(step, _):
        for one in sums:
            one[pl.ds(pl.multiple_of(step * 256, 256), 256)] = jnp.zeros((256, 128), jnp.float32)
        return 0

    lax.fori_loop(0, row_count // 256, clear, 0)
    blank = jnp.zeros((128 // groups - features, 128), jnp.float32)
    group = lax.broadcasted_iota(jnp.int32, (128, 128), 0) // (128 // groups)

    def source(which, _):
        for c in range(tokens // 128):
            block = g_ref[which, :, pl.ds(c * 128, 128)].astype(jnp.float32)
            block = jnp.concatenate([block, blank] * groups, axis=0)
            chosen = ids_ref[which, :, pl.ds(c * 128, 128)] >> row_bits
            spread[pl.ds(c * 128, 128), :] = jnp.where(group == chosen, block, 0.0).T

        def add(first, step, _):
            at = first + step * unroll
            rows = [rows_ref[which * tokens + at + u] for u in range(unroll)]
            for u in range(unroll):
                one = sums[u % len(sums)]
                one[pl.ds(rows[u], 1), :] += spread[pl.ds(at + u, 1), :]
            return 0

        for m in range(micros):
            live = live_ref[which * micros + m]
            lax.fori_loop(0, (live + unroll - 1) // unroll, functools.partial(add, m * half), 0)
        return 0

    lax.fori_loop(0, sources, source, 0)

    def finish(step, _):
        for u in range(2):
            at = pl.multiple_of((step * 2 + u) * 128, 128)
            total = sums[0][pl.ds(at, 128)]
            for one in sums[1:]:
                total = total + one[pl.ds(at, 128)]
            total = total.T
            for k in range(groups):
                part = total[k * (128 // groups) : k * (128 // groups) + features]
                if (k + 1) * row_count <= vocab:
                    o_ref[:, pl.ds(k * row_count + at, 128)] = part
                elif k * row_count < vocab:

                    @pl.when(k * row_count + at + 128 <= vocab)
                    def _():
                        o_ref[:, pl.ds(k * row_count + at, 128)] = part

        return 0

    lax.fori_loop(0, row_count // 256, finish, 0)


def scatter_add(live, ids, grads, vocab):
    sources, features, tokens = grads.shape
    return pl.pallas_call(
        functools.partial(scatter_kernel, 32),
        out_shape=jax.ShapeDtypeStruct((features, vocab), jnp.float32),
        in_specs=[
            pl.BlockSpec(memory_space=pltpu.SMEM),
            pl.BlockSpec(memory_space=pltpu.SMEM),
            pl.BlockSpec(memory_space=pltpu.VMEM),
            pl.BlockSpec(memory_space=pltpu.VMEM),
        ],
        out_specs=pl.BlockSpec(memory_space=pltpu.VMEM),
        scratch_shapes=[pltpu.VMEM((tokens, 128), jnp.float32)]
        + [pltpu.VMEM((row_count, 128), jnp.float32)] * 8,
        compiler_params=pltpu.CompilerParams(vmem_limit_bytes=44 * 1024 * 1024),
        cost_estimate=pl.CostEstimate(
            flops=40 * 10**9, bytes_accessed=8 * 10**6, transcendentals=0
        ),
        name="scatter_add",
    )(
        live.reshape(-1),
        (ids & (row_count - 1)).reshape(-1),
        ids.reshape(sources, 1, tokens),
        grads,
    )


def spread_kernel(count, hidden_ref, spread_ref):
    per = hidden_ref.shape[1] // count
    features = spread_ref.shape[1] // (-(-per // (D // count)) * count)
    spread_ref[...] = jnp.zeros_like(spread_ref)
    for d in range(count):
        block = hidden_ref[:, pl.ds(d * per, per)]
        for k in range(-(-per // features)):
            width = min(features, per - k * features)
            at = (k * count + d) * features
            spread_ref[:, pl.ds(at, width)] = block[:, k * features : k * features + width]


def spread_columns(hidden, count):
    rows = hidden.shape[0]
    pieces = -(-(hidden.shape[1] // count) // (D // count))
    result = jax.ShapeDtypeStruct((rows, pieces * D), hidden.dtype)
    return pl.pallas_call(
        functools.partial(spread_kernel, count),
        out_shape=result,
        in_specs=[pl.BlockSpec(memory_space=pltpu.VMEM)],
        out_specs=pl.BlockSpec(memory_space=pltpu.VMEM),
        compiler_params=pltpu.CompilerParams(vmem_limit_bytes=room(hidden, result)),
        name="spread_columns",
    )(hidden)


def pack_kernel(*refs):
    packed_ref = refs[-1]
    count = packed_ref.shape[0]
    packed_ref[...] = jnp.zeros_like(packed_ref)
    at = 0
    for x_ref in refs[:-1]:
        width = x_ref.shape[1] // count
        for d in range(count):
            packed_ref[d, :, pl.ds(at, width)] = x_ref[:, pl.ds(d * width, width)]
        at += width


def pack_columns(arrays, count):
    width = -(-sum(array.shape[1] for array in arrays) // (128 * count)) * 128
    result = jax.ShapeDtypeStruct((count, arrays[0].shape[0], width), arrays[0].dtype)
    return pl.pallas_call(
        pack_kernel,
        out_shape=result,
        in_specs=[pl.BlockSpec(memory_space=pltpu.VMEM)] * len(arrays),
        out_specs=pl.BlockSpec(memory_space=pltpu.VMEM),
        compiler_params=pltpu.CompilerParams(vmem_limit_bytes=room(*arrays, result)),
        name="pack_columns",
    )(*arrays)


def collect_kernel(count, spread_ref, o_ref):
    per = o_ref.shape[1] // count
    features = spread_ref.shape[2] // count
    for d in range(count):
        for k in range(spread_ref.shape[0]):
            width = min(features, per - k * features)
            part = spread_ref[k, :, pl.ds(d * features, width)]
            o_ref[:, pl.ds(d * per + k * features, width)] = part


def collect_columns(parts, columns, count):
    return pl.pallas_call(
        functools.partial(collect_kernel, count),
        out_shape=jax.ShapeDtypeStruct((parts.shape[1], columns), parts.dtype),
        in_specs=[pl.BlockSpec(memory_space=pltpu.VMEM)],
        out_specs=pl.BlockSpec(memory_space=pltpu.VMEM),
        compiler_params=pltpu.CompilerParams(vmem_limit_bytes=room(parts, parts)),
        name="collect_columns",
    )(parts)


def unpack_kernel(widths, x_ref, *o_refs):
    count = x_ref.shape[0]
    at = 0
    for width, o_ref in zip(widths, o_refs):
        for d in range(count):
            o_ref[:, pl.ds(d * width, width)] = x_ref[d, :, pl.ds(at, width)]
        at += width


def unpack_columns(blocks, widths):
    count, rows, _ = blocks.shape
    results = tuple(jax.ShapeDtypeStruct((rows, count * w), blocks.dtype) for w in widths)
    return pl.pallas_call(
        functools.partial(unpack_kernel, widths),
        out_shape=results,
        in_specs=[pl.BlockSpec(memory_space=pltpu.VMEM)],
        out_specs=tuple(pl.BlockSpec(memory_space=pltpu.VMEM) for _ in widths),
        compiler_params=pltpu.CompilerParams(vmem_limit_bytes=room(blocks, *results)),
        name="unpack_columns",
    )(blocks)


def update_kernel(rates, factor_ref, *refs):
    count = len(rates)
    inputs, outputs = refs[: 4 * count], refs[4 * count : 7 * count]
    staged, sems = refs[7 * count : 10 * count], refs[10 * count]
    factor = factor_ref[0]
    copies = []
    for p, rate in enumerate(rates):
        rows, columns = inputs[4 * p].shape
        wide = rows < 32 and columns > 8192
        size, total = (3200, columns) if wide else (40 if rows % 40 == 0 else rows, rows)
        parts = total // size
        weight_ref, moment_ref, average_ref, grad_ref = inputs[4 * p : 4 * p + 4]

        def span(step, wide=wide, size=size):
            at = pl.ds(pl.multiple_of(step * size, 128 if wide else 8), size)
            return (slice(None), at) if wide else (at, slice(None))

        def compute(where, p=p, rate=rate, refs=(weight_ref, moment_ref, average_ref, grad_ref)):
            new = apply_update(refs[0][where], refs[3][where], refs[1][where], refs[2][where], factor, rate)
            for k in range(3):
                staged[3 * p + k][where] = new[k]

        if parts == 1:
            compute((slice(None), slice(None)))
        else:

            def body(step, _, compute=compute, span=span):
                compute(span(step))
                return 0

            lax.fori_loop(0, parts, body, 0)
        for k in range(3):
            at = 3 * p + k
            copies.append(pltpu.make_async_copy(staged[at], outputs[at], sems.at[at]))
            copies[-1].start()
    for copy in copies:
        copy.wait()


def update_all(factor, params, rates):
    flat = [array for param in params for array in param]
    shapes = [param[0].shape for param in params for _ in range(3)]
    results = tuple(jax.ShapeDtypeStruct(shape, jnp.float32) for shape in shapes)
    new = pl.pallas_call(
        functools.partial(update_kernel, rates),
        out_shape=results,
        in_specs=[pl.BlockSpec(memory_space=pltpu.SMEM)]
        + [pl.BlockSpec(memory_space=pltpu.VMEM)] * len(flat),
        out_specs=tuple(pl.BlockSpec(memory_space=pl.ANY) for _ in shapes),
        scratch_shapes=[pltpu.VMEM(shape, jnp.float32) for shape in shapes]
        + [pltpu.SemaphoreType.DMA((len(shapes),))],
        compiler_params=pltpu.CompilerParams(vmem_limit_bytes=room(*results, *flat)),
        name="update_all",
    )(factor.reshape(1), *flat)
    return [new[3 * p : 3 * p + 3] for p in range(len(params))]


def other_core(arrays):
    return lax.ppermute(arrays, "seq", [(0, 1), (1, 0)])


def norm_forward(values, gain_row):
    inverse = lax.rsqrt(jnp.mean(values * values, axis=-1, keepdims=True) + epsilon)
    return (values * inverse * gain_row, inverse)


def norm_backward(values, inverse, gain_row, grad_out):
    scaled = grad_out * gain_row
    grad_gain = jnp.sum(grad_out * values * inverse, axis=0)
    grad_in = inverse * scaled - values * inverse**3 * jnp.mean(
        values * scaled, axis=-1, keepdims=True
    )
    return (grad_in, grad_gain)


def apply_update(weight_old, grad_full, moment_old, average_old, factor, rate):
    clipped = factor * grad_full
    moment_new = moment * moment_old + clipped
    weight_new = weight_old - rate * (clipped + moment * moment_new)
    average_new = average * average_old + (1.0 - average) * weight_new
    return (weight_new, moment_new, average_new)


def step(
    token_ids,
    lengths,
    loss_positions,
    loss_targets,
    attention_in,
    attention_in_moment,
    attention_in_average,
    attention_out,
    attention_out_moment,
    attention_out_average,
    feed_in,
    feed_in_moment,
    feed_in_average,
    feed_out,
    feed_out_moment,
    feed_out_average,
    embedding,
    embedding_moment,
    embedding_average,
    unembedding,
    unembedding_moment,
    unembedding_average,
    gains_biases,
    gains_biases_moment,
    gains_biases_average,
):
    low = jnp.bfloat16
    wide = jnp.float32
    devices_all = lax.axis_size(both)
    seq_index = lax.axis_index("seq")
    device = lax.axis_index(both)
    micros, _, half = token_ids.shape
    loss_dev = loss_positions.shape[2]
    tokens = micros * half
    rows = micros * loss_dev
    rows_all = devices_all * rows
    vocab_here = unembedding.shape[0]
    features = D // devices_all
    gate_here = FF // devices_all
    gain_rows = gains_biases[: 3 * D].reshape(3, D)
    bias_row = gains_biases[3 * D :]
    second = seq_index.astype(wide)

    positions = loss_positions[:, 0]
    targets = loss_targets[:, 0]
    ids_all = gather_labels(token_ids[:, 0], lengths, positions, targets, 1)
    base = tokens // 128
    all_tokens = ids_all[:, :base].reshape(devices_all, tokens)
    all_targets = ids_all[:, base : base + micros, :loss_dev].reshape(-1)
    all_counted = ids_all[:, base + micros : base + 2 * micros, :loss_dev]
    all_live = ids_all[:, base + 2 * micros : base + 3 * micros, 0]

    down_here = feed_out.shape[1]
    pieces = -(-down_here // features)
    down_pad = jnp.pad(feed_out[0], ((0, pieces * features - down_here), (0, 0)))
    down_pad = [down_pad[k * features : (k + 1) * features] for k in range(pieces)]
    packed = jnp.concatenate([feed_in[0]] + down_pad + [attention_out[0], attention_in[0]], axis=1)
    w_all = lax.all_gather(packed.astype(low), both, axis=0, tiled=True)
    down_at = 2 * FF
    out_at = down_at + pieces * D
    w_feed = w_all[:, :down_at]
    w_out = w_all[:, out_at : out_at + D]
    w_in = w_all[:, out_at + D :]
    w_down = [w_all[:, down_at + k * D : down_at + (k + 1) * D] for k in range(pieces)]
    head_low = unembedding.astype(low)

    arrived = exchange(lookup(all_live, all_tokens, embedding.T), 5)
    x_t = arrived.reshape(D, tokens)
    pick = [
        (positions[m][:, None] == jnp.arange(half)[None, :]).astype(low) for m in range(micros)
    ]
    x_wide, inverse_one, normed_t, keys_t, values_t, forget_t = [], [], [], [], [], []
    for m in range(micros):
        x_wide.append(x_t[:, m * half : (m + 1) * half].astype(wide))
        inverse_one.append(
            lax.rsqrt(jnp.mean(x_wide[m] * x_wide[m], axis=0, keepdims=True) + epsilon)
        )
        normed_t.append((x_wide[m] * inverse_one[m] * gain_rows[0][:, None]).astype(low))

        project_t = dot(w_in[:, D:], normed_t[m], 0, 0)
        keys_t.append(project_t[:D].astype(low).reshape(H, HD, half))
        values_t.append(project_t[D : 2 * D].astype(low).reshape(H, HD, half))
        forget_t.append((project_t[2 * D :] + bias_row[:, None]).astype(low).astype(wide))
    x_rows = jnp.concatenate([dot(pick[m], x_wide[m].astype(low), 1, 1) for m in range(micros)])
    normed_rows = jnp.concatenate(
        [dot(pick[m], normed_t[m], 1, 1) for m in range(micros)]
    ).astype(low)
    q_rows = dot(normed_rows, w_in[:, :D], 1, 0).astype(low)

    upper = (jnp.arange(half)[:, None] <= jnp.arange(half)[None, :]).astype(wide)
    log_gate = jax.nn.log_sigmoid(jnp.stack(forget_t, axis=1))
    decay_own = lax.dot_general(
        log_gate, upper, (((2,), (0,)), ((), ())), precision=highest, preferred_element_type=wide
    )
    total_own = decay_own[:, :, -1]
    decay_rows = jnp.stack(
        [dot(pick[m].astype(wide), decay_own[:, m], 1, 1, highest) for m in range(micros)]
    )
    q_own = q_rows.reshape(micros, loss_dev, H, HD)
    q_far, decay_far, total_far, place_far = other_core((q_own, decay_rows, total_own, positions))
    shift_own = second * total_far
    shift_far = (1.0 - second) * total_own
    key_decay = decay_own + shift_own[:, :, None]
    row_decay = jnp.concatenate(
        [decay_rows + shift_own.T[:, None], decay_far + shift_far.T[:, None]], axis=1
    )
    q_all = jnp.concatenate([q_own, q_far], axis=1)
    places = jnp.concatenate(
        [positions + seq_index * half, place_far + (1 - seq_index) * half], axis=1
    )
    key_places = seq_index * half + jnp.arange(half)

    scores = []
    for m in range(micros):
        raw = jnp.einsum("rhd,hdj->hrj", q_all[m], keys_t[m], preferred_element_type=wide)
        part = raw * HD ** (-0.5) + row_decay[m].T[:, :, None] - key_decay[:, m][:, None, :]
        causal = places[m][:, None] >= key_places[None, :]
        scores.append(jnp.where(causal[None], part, negative))
    scores = jnp.stack(scores)
    peak_own = jnp.max(scores, axis=-1)
    spread_own = jnp.sum(jnp.exp(scores - peak_own[..., None]), axis=-1)
    peak_far, spread_far = other_core((peak_own, spread_own))

    def swap_rows(array):
        return jnp.concatenate([array[:, :, loss_dev:], array[:, :, :loss_dev]], axis=2)

    peak_far, spread_far = swap_rows(peak_far), swap_rows(spread_far)
    peak = jnp.maximum(peak_own, peak_far)
    log_total = peak + jnp.log(
        spread_own * jnp.exp(peak_own - peak) + spread_far * jnp.exp(peak_far - peak)
    )
    probs = jnp.exp(scores - log_total[..., None])
    probs_low = probs.astype(low)
    probs_rest = (probs - probs_low.astype(wide)).astype(low)

    def mix(weights):
        return jnp.stack(
            [
                jnp.einsum(
                    "hrj,hdj->rhd",
                    weights[m],
                    values_t[m],
                    preferred_element_type=wide,
                )
                for m in range(micros)
            ]
        )

    mixed_part = mix(probs_low)
    rest_part = mix(probs_rest)
    mixed_far, rest_far = other_core((mixed_part[:, loss_dev:], rest_part[:, loss_dev:]))
    mixed_sum = mixed_part[:, :loss_dev] + mixed_far
    mixed_full = mixed_sum + rest_part[:, :loss_dev] + rest_far
    mixed_rows = mixed_sum.reshape(rows, D).astype(low)

    middle = x_rows + dot(mixed_rows, w_out, 1, 0)
    normed_two, inverse_two = norm_forward(middle, gain_rows[1])
    normed_two = normed_two.astype(low)
    gate_up = dot(normed_two, w_feed, 1, 0)
    gate_half, up_half = gate_up[:, :FF], gate_up[:, FF:]
    gate_sigmoid = jax.nn.sigmoid(gate_half)
    hidden = (gate_half * gate_sigmoid * up_half).astype(low)
    hidden_spread = spread_columns(hidden, devices_all)
    early_packed = lax.all_gather(
        jnp.concatenate([normed_two, mixed_rows, normed_rows], axis=1),
        both,
        axis=0,
        tiled=True,
    )
    final_in = middle
    for k in range(pieces):
        final_in = final_in + dot(hidden_spread[:, k * D : (k + 1) * D], w_down[k], 1, 0)
    final_normed, final_inverse = norm_forward(final_in, gain_rows[2])

    final_all = gather_rows(final_normed.astype(low), 2).reshape(rows_all, D)
    logits = dot(final_all, head_low, 1, 1)
    vocab_ids = device * vocab_here + jnp.arange(vocab_here)
    target_hits = all_targets[:, None] == vocab_ids[None, :]
    row_peak = jnp.max(logits, axis=1)
    exp_sum = jnp.sum(jnp.exp(logits - row_peak[:, None]), axis=1)
    target_part = jnp.sum(jnp.where(target_hits, logits, 0.0), axis=1)
    logit_sum = jnp.sum(logits, axis=1)
    stats = jnp.stack([row_peak, exp_sum, target_part, logit_sum])
    stats_all = gather_rows(stats.reshape(-1, 128), 3).reshape(devices_all, 4, rows_all)
    peak_all = jnp.max(stats_all[:, 0], axis=0)
    spread_all = jnp.sum(stats_all[:, 1] * jnp.exp(stats_all[:, 0] - peak_all), axis=0)
    target_all = jnp.sum(stats_all[:, 2], axis=0)
    logit_all = jnp.sum(stats_all[:, 3], axis=0)
    total_all = peak_all + jnp.log(spread_all)
    per_row = (
        total_all
        - (1.0 - smooth) * target_all
        - smooth * logit_all / V
        + z_weight * total_all * total_all
    )
    weights_row = all_counted.astype(wide).reshape(devices_all, micros, loss_dev)
    counts = jnp.sum(weights_row, axis=(0, 2))
    weights_row = (weights_row / (micros * counts)[None, :, None]).reshape(-1)
    loss_value = jnp.sum(weights_row * per_row)
    soft_rows = jnp.exp(logits - total_all[:, None])
    grad_logits = (
        weights_row[:, None]
        * (
            soft_rows * (1.0 + 2.0 * z_weight * total_all)[:, None]
            - (1.0 - smooth) * target_hits.astype(wide)
            - smooth / V
        )
    ).astype(low)
    grad_final = reduce_rows(dot(grad_logits, head_low, 1, 0), 7)

    grad_rows, gain_grad_final = norm_backward(final_in, final_inverse, gain_rows[2], grad_final)
    grad_branch = grad_rows.astype(low)
    grad_hidden = jnp.stack([dot(grad_branch, w_down[k], 1, 1) for k in range(pieces)])
    grad_hidden = collect_columns(grad_hidden, FF, devices_all)
    grad_gate = grad_hidden * up_half * gate_sigmoid * (1.0 + gate_half * (1.0 - gate_sigmoid))
    grad_up = grad_hidden * gate_half * gate_sigmoid
    grad_gate_up = jnp.concatenate([grad_gate, grad_up], axis=1).astype(low)
    grad_two, gain_grad_two = norm_backward(
        middle, inverse_two, gain_rows[1], dot(grad_gate_up, w_feed, 1, 1)
    )
    grad_middle = grad_rows + grad_two
    grad_mid_low = grad_middle.astype(low)
    grad_mixed = dot(grad_mid_low, w_out, 1, 1).astype(low)

    branch_all = lax.all_gather(grad_branch, both, axis=0, tiled=True)
    feed_here = 2 * FF // devices_all
    grad_own = grad_mixed.reshape(micros, loss_dev, H, HD)
    inner_own = jnp.sum(grad_own.astype(wide) * mixed_full, axis=-1)
    grad_far, inner_far = other_core((grad_own, inner_own))
    grad_heads = jnp.concatenate([grad_own, grad_far], axis=1)
    inner_sum = jnp.concatenate([inner_own, inner_far], axis=1)
    query_parts, score_rows = [], []
    grad_keys, grad_values, score_columns = [], [], []
    for m in range(micros):
        grad_probs = jnp.einsum(
            "rhd,hdj->hrj", grad_heads[m], values_t[m], preferred_element_type=wide
        )
        grad_scores = (probs[m] * (grad_probs - inner_sum[m].T[:, :, None])).astype(low)
        query_parts.append(
            jnp.einsum("hrj,hdj->rhd", grad_scores, keys_t[m], preferred_element_type=wide)
        )
        grad_keys.append(
            jnp.einsum("hrj,rhd->hdj", grad_scores, q_all[m], preferred_element_type=wide)
            * HD ** (-0.5)
        )
        grad_values.append(
            jnp.einsum("hrj,rhd->hdj", probs_low[m], grad_heads[m], preferred_element_type=wide)
        )
        score_wide = grad_scores.astype(wide)
        score_rows.append(jnp.sum(score_wide, axis=-1))
        score_columns.append(jnp.sum(score_wide, axis=1))
    query_parts = jnp.stack(query_parts)
    score_rows = jnp.stack(score_rows).transpose(0, 2, 1)
    query_far, score_far = other_core((query_parts[:, loss_dev:], score_rows[:, loss_dev:]))
    grad_query = ((query_parts[:, :loss_dev] + query_far) * HD ** (-0.5)).astype(low)
    grad_query = grad_query.reshape(rows, D)
    columns_packed = lax.all_to_all(
        pack_columns((grad_gate_up, hidden, grad_mid_low, grad_query), devices_all),
        both,
        split_axis=0,
        concat_axis=0,
        tiled=True,
    )
    rows_sum = score_rows[:, :loss_dev] + score_far
    later = (1.0 - second) * jnp.sum(score_rows[:, loss_dev:], axis=1)
    grad_in_sum, gain_grad_one, grad_bias, grad_embed = 0.0, 0.0, 0.0, []
    projects = []
    for m in range(micros):
        placed = dot(rows_sum[m], pick[m].astype(wide), 0, 0, highest)
        change = placed - score_columns[m]
        grad_log = dot(change, upper, 1, 1, highest) + later[m][:, None]
        grad_forget = (grad_log * jax.nn.sigmoid(-forget_t[m])).astype(low)
        grad_bias = grad_bias + jnp.sum(grad_forget.astype(wide), axis=1)
        query_t = dot(grad_query[m * loss_dev : (m + 1) * loss_dev], pick[m], 0, 0).astype(low)
        keys_part = grad_keys[m].astype(low).reshape(D, half)
        values_part = grad_values[m].astype(low).reshape(D, half)
        grad_forget = lax.optimization_barrier(jnp.pad(grad_forget, ((0, -H % 128), (0, 0))))
        projects.append(jnp.concatenate([query_t, keys_part, values_part, grad_forget], axis=0))
        grad_in_sum = grad_in_sum + dot(normed_t[m], projects[m][D:], 1, 1)
    grad_in = lax.psum_scatter(grad_in_sum, both, scatter_dimension=0, tiled=True)
    for m in range(micros):
        grad_normed = dot(w_in, projects[m][: 3 * D + H], 1, 0)
        scaled = grad_normed * gain_rows[0][:, None]
        gain_grad_one = gain_grad_one + jnp.sum(grad_normed * x_wide[m] * inverse_one[m], axis=1)
        grad_one = inverse_one[m] * scaled - x_wide[m] * inverse_one[m] ** 3 * jnp.mean(
            x_wide[m] * scaled, axis=0, keepdims=True
        )
        middle_t = dot(
            grad_middle[m * loss_dev : (m + 1) * loss_dev], pick[m].astype(wide), 0, 0, highest
        )
        grad_embed.append((middle_t + grad_one).astype(low))
    grad_embed = jnp.concatenate(grad_embed, axis=1).reshape(devices_all, features, tokens)
    moved = lax.all_to_all(grad_embed, both, split_axis=0, concat_axis=0, tiled=True)
    early_packed, branch_all, columns_packed, _ = lax.optimization_barrier(
        (early_packed, branch_all, columns_packed, grad_embed[:1, :1, :1])
    )
    late_logits, _ = lax.optimization_barrier((grad_logits, grad_embed[:1, :1, :1]))
    head_grad = lax.optimization_barrier(dot(late_logits, final_all, 0, 0))
    columns_packed = columns_packed.reshape(rows_all, -1)

    def columns_of(first, width):
        return columns_packed[:, first : first + width]

    feed_columns = dot(early_packed[:, :D], columns_of(0, feed_here), 0, 0)
    out_columns = columns_of(feed_here + gate_here, features)
    out_columns = dot(early_packed[:, D : 2 * D], out_columns, 0, 0)
    query_columns = columns_of(feed_here + gate_here + features, features)
    query_columns = dot(early_packed[:, 2 * D :], query_columns, 0, 0)
    grad_down = lax.optimization_barrier(dot(columns_of(feed_here, gate_here), branch_all, 0, 0))
    grad_feed = lax.all_to_all(
        jnp.concatenate([feed_columns, out_columns, query_columns], axis=1).reshape(
            devices_all, features, feed_here + 2 * features
        ),
        both,
        split_axis=0,
        concat_axis=0,
        tiled=True,
    )
    grad_feed, grad_out, grad_q = unpack_columns(grad_feed, (feed_here, features, features))
    embed_grad = scatter_add(all_live, all_tokens, moved, V)

    grad_in, _ = lax.optimization_barrier((grad_in, embed_grad[:1, :1]))
    grad_in = jnp.concatenate([grad_q, grad_in[:, : 2 * D + H]], axis=1)
    owned_grads = [grad_in, grad_out, grad_feed, grad_down, embed_grad, head_grad]
    square_sum = jnp.zeros((), wide)
    for grad_part in owned_grads:
        square_sum = square_sum + jnp.sum(grad_part * grad_part)
    small_grad = jnp.concatenate(
        [gain_grad_one, gain_grad_two, gain_grad_final, grad_bias, square_sum[None]]
    )
    small_count = small_grad.shape[0]
    small_grad = jnp.pad(small_grad, (0, -small_count % 1024)).reshape(-1, 128)
    small_sum = jnp.sum(gather_rows(small_grad, 4), axis=0).reshape(-1)
    small_total, square_total = small_sum[: small_count - 1], small_sum[small_count - 1]
    grad_norm = jnp.sqrt(square_total + jnp.sum(small_total * small_total))
    factor = jnp.minimum(1.0, clip_limit / grad_norm)
    layer = rate_layer
    news = update_all(
        factor,
        (
            (attention_in[0], attention_in_moment[0], attention_in_average[0], grad_in),
            (attention_out[0], attention_out_moment[0], attention_out_average[0], grad_out),
            (feed_in[0], feed_in_moment[0], feed_in_average[0], grad_feed),
            (feed_out[0], feed_out_moment[0], feed_out_average[0], grad_down),
            (embedding.T, embedding_moment.T, embedding_average.T, embed_grad),
            (unembedding, unembedding_moment, unembedding_average, head_grad),
        ),
        (layer, layer, layer, layer, rate_embed, rate_head),
    )
    results = [loss_value, grad_norm]
    for new in news[:4]:
        results.extend(array[None] for array in new)
    results.extend(array.T for array in news[4])
    results.extend(news[5])
    results.extend(
        apply_update(
            gains_biases, small_total, gains_biases_moment, gains_biases_average, factor, layer
        )
    )
    return tuple(results)


def solution(mesh):
    rows = P(None, both, None)
    tables = (rows,) * 12 + (P(None, both),) * 3 + (P(both, None),) * 3 + (P(),) * 3
    return jax.shard_map(
        step,
        mesh=mesh,
        in_specs=(
            P(None, "fsdp", "seq"),
            P(None, "fsdp"),
            P(None, "fsdp", "seq"),
            P(None, "fsdp", "seq"),
        )
        + tables,
        out_specs=(P(), P()) + tables,
        check_vma=False,
    )
```

```python
import functools
import math

import jax
import jax.numpy as jnp
from jax import lax
from jax.experimental import pallas as pl
from jax.experimental.pallas import tpu as pltpu
from jax.sharding import PartitionSpec as P

D = 768
H = 12
HD = 64
FF = 2048
V = 32000


epsilon = 1e-06
smooth = 0.1
z_weight = 0.005
clip_limit = 0.5
moment = 0.9
average = 0.9
rate_layer = 200.0
rate_head = 1000.0
rate_embed = 5000.0
negative = -1e30
both = ("seq", "fsdp")
highest = lax.Precision.HIGHEST
MESH = pl.DeviceIdType.MESH


def dot(left_side, right_side, left_axis, right_axis, precision=None):
    return lax.dot_general(
        left_side,
        right_side,
        (((left_axis,), (right_axis,)), ((), ())),
        precision=precision,
        preferred_element_type=jnp.float32,
    )


def room(*arrays):
    total = 1 << 20
    for array in arrays:
        shape, size = array.shape, jnp.dtype(array.dtype).itemsize
        tile = 32 // size
        total += (
            math.prod(shape[:-2]) * (-(-shape[-2] // tile) * tile) * (-(-shape[-1] // 128) * 128)
        ) * size
    return total


def line_of(fsdp_count):
    return 4 if fsdp_count % 4 == 0 else 1


def gather_kernel(cores, fsdp, x_ref, o_ref, send_sem, recv_sem):
    plane = line_of(fsdp)
    lines = fsdp // plane
    core = lax.axis_index("seq")
    spot = lax.axis_index("fsdp")
    high, low = spot // plane, spot % plane
    line_peers = [((high + k) % lines) * plane + low for k in range(1, lines)]
    plane_peers = [high * plane + (low + k) % plane for k in range(1, plane)]
    core_peers = [(core + k) % cores for k in range(1, cores)]
    peers = [(core, p) for p in line_peers + plane_peers] + [(c, spot) for c in core_peers]

    barrier = pltpu.get_barrier_semaphore()
    for peer in peers:
        pl.semaphore_signal(barrier, inc=1, device_id=peer, device_id_type=MESH)
    pl.semaphore_wait(barrier, len(peers))

    sent = []

    def send(source_ref, block, peer):
        copy = pltpu.make_async_remote_copy(
            src_ref=source_ref,
            dst_ref=o_ref.at[block],
            send_sem=send_sem.at[len(sent)],
            recv_sem=recv_sem.at[block],
            device_id=peer,
            device_id_type=MESH,
        )
        copy.start()
        sent.append(copy)

    def arrived(block):
        pltpu.make_async_copy(o_ref.at[block], o_ref.at[block], recv_sem.at[block]).wait()

    mine = core * fsdp + spot
    for p in line_peers:
        send(x_ref, mine, (core, p))
    for p in plane_peers:
        send(x_ref, mine, (core, p))
    for c in core_peers:
        send(x_ref, mine, (c, spot))
    o_ref[mine] = x_ref[...]
    for k in range(1, lines):
        block = core * fsdp + ((high + lines - k) % lines) * plane + low
        arrived(block)
        for p in plane_peers:
            send(o_ref.at[block], block, (core, p))
        for c in core_peers:
            send(o_ref.at[block], block, (c, spot))
    for m in range(lines):
        for k in range(1, plane):
            block = core * fsdp + ((high + lines - m) % lines) * plane + (low + plane - k) % plane
            arrived(block)
            for c in core_peers:
                send(o_ref.at[block], block, (c, spot))
    for c in core_peers:
        for m in range(lines):
            for k in range(plane):
                block = c * fsdp + ((high + lines - m) % lines) * plane + (low + plane - k) % plane
                arrived(block)
    for copy in sent:
        copy.wait_send()


def label_kernel(
    cores, fsdp, tokens_ref, lengths_ref, places_ref, targets_ref, o_ref, packed, send_sem, recv_sem
):
    micros, half = tokens_ref.shape
    chunks = half // 128
    start = lax.axis_index("seq") * half
    packed[...] = jnp.zeros_like(packed)
    for m in range(micros):
        for c in range(chunks):
            packed[pl.ds(m * chunks + c, 1), :] = tokens_ref[pl.ds(m, 1), pl.ds(c * 128, 128)]
    base = micros * chunks
    length = lengths_ref[...]
    counted = (start + places_ref[...] < length).astype(jnp.int32)
    live = jnp.clip(length - start, 0, half)
    count = places_ref.shape[1]
    packed[pl.ds(base, micros), pl.ds(0, count)] = targets_ref[...]
    packed[pl.ds(base + micros, micros), pl.ds(0, count)] = counted
    packed[pl.ds(base + 2 * micros, micros), :] = jnp.broadcast_to(live, (micros, 128))
    gather_kernel(cores, fsdp, packed, o_ref, send_sem, recv_sem)


def gather_labels(tokens, lengths, places, targets, collective):
    cores, fsdp = lax.axis_size("seq"), lax.axis_size("fsdp")
    count = cores * fsdp
    micros, half = tokens.shape
    rows = micros * (half // 128) + 3 * micros
    rows = -(-rows // 8) * 8
    result = jax.ShapeDtypeStruct((count, rows, 128), jnp.int32)
    return pl.pallas_call(
        functools.partial(label_kernel, cores, fsdp),
        out_shape=result,
        in_specs=[pl.BlockSpec(memory_space=pltpu.VMEM)] * 4,
        out_specs=pl.BlockSpec(memory_space=pltpu.VMEM),
        scratch_shapes=[
            pltpu.VMEM((rows, 128), jnp.int32),
            pltpu.SemaphoreType.DMA((count,)),
            pltpu.SemaphoreType.DMA((count,)),
        ],
        compiler_params=pltpu.CompilerParams(
            collective_id=collective, has_side_effects=True, vmem_limit_bytes=room(result)
        ),
        name="gather_labels",
    )(tokens, lengths, places, targets)


def gather_rows(array, collective):
    cores, fsdp = lax.axis_size("seq"), lax.axis_size("fsdp")
    count = cores * fsdp
    result = jax.ShapeDtypeStruct((count,) + array.shape, array.dtype)
    return pl.pallas_call(
        functools.partial(gather_kernel, cores, fsdp),
        out_shape=result,
        in_specs=[pl.BlockSpec(memory_space=pltpu.VMEM)],
        out_specs=pl.BlockSpec(memory_space=pltpu.VMEM),
        scratch_shapes=[
            pltpu.SemaphoreType.DMA((count,)),
            pltpu.SemaphoreType.DMA((count,)),
        ],
        compiler_params=pltpu.CompilerParams(
            collective_id=collective,
            has_side_effects=True,
            vmem_limit_bytes=room(array, result),
        ),
        name="gather_rows",
    )(array)


def exchange_kernel(cores, fsdp, x_ref, o_ref, send_sem, recv_sem, own_sem):
    count = cores * fsdp
    mine = lax.axis_index("seq") * fsdp + lax.axis_index("fsdp")

    def place(step):
        other = lax.rem(mine + step, count)
        return other, (other // fsdp, lax.rem(other, fsdp))

    barrier = pltpu.get_barrier_semaphore()

    def greet(step, _):
        pl.semaphore_signal(barrier, inc=1, device_id=place(step)[1], device_id_type=MESH)
        return 0

    lax.fori_loop(1, count, greet, 0)
    pl.semaphore_wait(barrier, count - 1)
    own = pltpu.make_async_copy(x_ref.at[mine], o_ref.at[mine], own_sem)
    own.start()

    def copy_to(step):
        other, peer = place(step)
        return pltpu.make_async_remote_copy(
            src_ref=x_ref.at[other],
            dst_ref=o_ref.at[mine],
            send_sem=send_sem.at[step],
            recv_sem=recv_sem.at[step],
            device_id=peer,
            device_id_type=MESH,
        )

    def start(step, _):
        copy_to(step).start()
        return 0

    lax.fori_loop(1, count, start, 0)
    own.wait()

    def finish(step, _):
        source = lax.rem(mine + count - step, count)
        pltpu.make_async_copy(o_ref.at[source], o_ref.at[source], recv_sem.at[step]).wait()
        copy_to(step).wait_send()
        return 0

    lax.fori_loop(1, count, finish, 0)


def exchange(array, collective):
    cores, fsdp = lax.axis_size("seq"), lax.axis_size("fsdp")
    return pl.pallas_call(
        functools.partial(exchange_kernel, cores, fsdp),
        out_shape=jax.ShapeDtypeStruct(array.shape, array.dtype),
        in_specs=[pl.BlockSpec(memory_space=pltpu.VMEM)],
        out_specs=pl.BlockSpec(memory_space=pltpu.VMEM),
        scratch_shapes=[
            pltpu.SemaphoreType.DMA((cores * fsdp,)),
            pltpu.SemaphoreType.DMA((cores * fsdp,)),
            pltpu.SemaphoreType.DMA,
        ],
        compiler_params=pltpu.CompilerParams(
            collective_id=collective,
            has_side_effects=True,
            vmem_limit_bytes=room(array, array),
        ),
        name="exchange",
    )(array)


def reduce_kernel(
    fsdp, x_ref, o_ref, from_core, from_plane, from_line, core_sum, plane_sum, send_sem, recv_sem
):
    plane = line_of(fsdp)
    lines = fsdp // plane
    core = lax.axis_index("seq")
    spot = lax.axis_index("fsdp")
    high, low = spot // plane, lax.rem(spot, plane)
    far = 1 - core
    peers = [(far, spot)]
    peers += [(core, lax.rem(high + k, lines) * plane + low) for k in range(1, lines)]
    peers += [(core, high * plane + lax.rem(low + k, plane)) for k in range(1, plane)]
    barrier = pltpu.get_barrier_semaphore()
    for peer in peers:
        pl.semaphore_signal(barrier, inc=1, device_id=peer, device_id_type=MESH)
    pl.semaphore_wait(barrier, len(peers))
    sent = []

    def send(source_ref, target_ref, slot, peer):
        copy = pltpu.make_async_remote_copy(
            src_ref=source_ref,
            dst_ref=target_ref,
            send_sem=send_sem.at[slot],
            recv_sem=recv_sem.at[slot],
            device_id=peer,
            device_id_type=MESH,
        )
        copy.start()
        sent.append(copy)
        return copy

    first = []
    for k in list(range(1, plane)) + [0]:
        spot_low = lax.rem(low + k, plane)
        first.append(
            (k, spot_low, send(x_ref.at[far, :, spot_low], from_core.at[spot_low], k, (far, spot)))
        )
    second = []
    for k, spot_low, copy in first:
        copy.wait_recv()
        core_sum[spot_low] = x_ref[core, :, spot_low] + from_core[spot_low]
        if k:
            target = from_plane.at[k - 1]
            peer = (core, high * plane + spot_low)
            second.append((k, send(core_sum.at[spot_low], target, plane + k - 1, peer)))
    plane_sum[...] = core_sum[low]
    for k, copy in second:
        copy.wait_recv()
        plane_sum[...] += from_plane[k - 1]
    third = []
    for k in range(1, lines):
        line = lax.rem(high + k, lines)
        slot = 2 * plane + k - 2
        peer = (core, line * plane + low)
        third.append((k, send(plane_sum.at[line], from_line.at[k - 1], slot, peer)))
    total = plane_sum[high]
    for k, copy in third:
        copy.wait_recv()
        total = total + from_line[k - 1]
    o_ref[...] = total
    for copy in sent:
        copy.wait_send()


def reduce_rows(array, collective):
    cores, fsdp = lax.axis_size("seq"), lax.axis_size("fsdp")
    plane = line_of(fsdp)
    lines = fsdp // plane
    rows, columns = array.shape[0] // (cores * fsdp), array.shape[1]
    kind = array.dtype
    slots = 2 * plane + lines - 2
    return pl.pallas_call(
        functools.partial(reduce_kernel, fsdp),
        out_shape=jax.ShapeDtypeStruct((rows, columns), kind),
        in_specs=[pl.BlockSpec(memory_space=pltpu.VMEM)],
        out_specs=pl.BlockSpec(memory_space=pltpu.VMEM),
        scratch_shapes=[
            pltpu.VMEM((plane, lines, rows, columns), kind),
            pltpu.VMEM((plane - 1, lines, rows, columns), kind),
            pltpu.VMEM((lines - 1, rows, columns), kind),
            pltpu.VMEM((plane, lines, rows, columns), kind),
            pltpu.VMEM((lines, rows, columns), kind),
            pltpu.SemaphoreType.DMA((slots,)),
            pltpu.SemaphoreType.DMA((slots,)),
        ],
        compiler_params=pltpu.CompilerParams(
            collective_id=collective,
            has_side_effects=True,
            vmem_limit_bytes=room(array, array, array),
        ),
        name="reduce_rows",
    )(array.reshape(cores, lines, plane, rows, columns))


def lookup_kernel(unroll, builds, live_ref, ids_ref, own_ref, o_ref, table, stage):
    sources, features, tokens = o_ref.shape
    micros = live_ref.shape[0] // sources
    half = tokens // micros

    def build(step, _):
        for u in range(builds):
            at = pl.multiple_of((step * builds + u) * 128, 128)
            block = own_ref[:, pl.ds(at, 128)].astype(jnp.bfloat16).astype(jnp.float32)
            table[pl.ds(at, 128), pl.ds(0, features)] = block.T
        return 0

    lax.fori_loop(0, table.shape[0] // 128 // builds, build, 0)
    stage[...] = jnp.zeros_like(stage)

    def source(which, _):
        def fetch(first, step, _):
            at = first + step * unroll
            ids = [ids_ref[which * tokens + at + u] for u in range(unroll)]
            for u in range(unroll):
                stage[pl.ds(at + u, 1), :] = table[pl.ds(ids[u], 1), :]
            return 0

        for m in range(micros):
            live = live_ref[which * micros + m]
            lax.fori_loop(
                0, (live + unroll - 1) // unroll, functools.partial(fetch, m * half), 0
            )
        for c in range(tokens // 128):
            block = stage[pl.ds(c * 128, 128), :].T
            o_ref[which, :, pl.ds(c * 128, 128)] = block[:features].astype(jnp.bfloat16)
        return 0

    lax.fori_loop(0, sources, source, 0)


def lookup(live, ids, table_t):
    sources, tokens = ids.shape
    features, vocab = table_t.shape
    return pl.pallas_call(
        functools.partial(lookup_kernel, 64, 10),
        out_shape=jax.ShapeDtypeStruct((sources, features, tokens), jnp.bfloat16),
        in_specs=[
            pl.BlockSpec(memory_space=pltpu.SMEM),
            pl.BlockSpec(memory_space=pltpu.SMEM),
            pl.BlockSpec(memory_space=pltpu.VMEM),
        ],
        out_specs=pl.BlockSpec(memory_space=pltpu.VMEM),
        scratch_shapes=[
            pltpu.VMEM((vocab, 128), jnp.float32),
            pltpu.VMEM((tokens, 128), jnp.float32),
        ],
        compiler_params=pltpu.CompilerParams(vmem_limit_bytes=32 * 1024 * 1024),
        name="lookup",
    )(live.reshape(-1), ids.reshape(-1), table_t)


row_bits = 13
row_count = 1 << row_bits


def scatter_kernel(unroll, live_ref, rows_ref, ids_ref, g_ref, o_ref, spread, *sums):
    sources, features, tokens = g_ref.shape
    micros = live_ref.shape[0] // sources
    half = tokens // micros
    vocab = o_ref.shape[1]
    groups = 4

    def clear(step, _):
        for one in sums:
            one[pl.ds(pl.multiple_of(step * 256, 256), 256)] = jnp.zeros((256, 128), jnp.float32)
        return 0

    lax.fori_loop(0, row_count // 256, clear, 0)
    blank = jnp.zeros((128 // groups - features, 128), jnp.float32)
    group = lax.broadcasted_iota(jnp.int32, (128, 128), 0) // (128 // groups)

    def source(which, _):
        for c in range(tokens // 128):
            block = g_ref[which, :, pl.ds(c * 128, 128)].astype(jnp.float32)
            block = jnp.concatenate([block, blank] * groups, axis=0)
            chosen = ids_ref[which, :, pl.ds(c * 128, 128)] >> row_bits
            spread[pl.ds(c * 128, 128), :] = jnp.where(group == chosen, block, 0.0).T

        def add(first, step, _):
            at = first + step * unroll
            rows = [rows_ref[which * tokens + at + u] for u in range(unroll)]
            for u in range(unroll):
                one = sums[u % len(sums)]
                one[pl.ds(rows[u], 1), :] += spread[pl.ds(at + u, 1), :]
            return 0

        for m in range(micros):
            live = live_ref[which * micros + m]
            lax.fori_loop(0, (live + unroll - 1) // unroll, functools.partial(add, m * half), 0)
        return 0

    lax.fori_loop(0, sources, source, 0)

    def finish(step, _):
        for u in range(2):
            at = pl.multiple_of((step * 2 + u) * 128, 128)
            total = sums[0][pl.ds(at, 128)]
            for one in sums[1:]:
                total = total + one[pl.ds(at, 128)]
            total = total.T
            for k in range(groups):
                part = total[k * (128 // groups) : k * (128 // groups) + features]
                if (k + 1) * row_count <= vocab:
                    o_ref[:, pl.ds(k * row_count + at, 128)] = part
                elif k * row_count < vocab:

                    @pl.when(k * row_count + at + 128 <= vocab)
                    def _():
                        o_ref[:, pl.ds(k * row_count + at, 128)] = part

        return 0

    lax.fori_loop(0, row_count // 256, finish, 0)


def scatter_add(live, ids, grads, vocab):
    sources, features, tokens = grads.shape
    return pl.pallas_call(
        functools.partial(scatter_kernel, 32),
        out_shape=jax.ShapeDtypeStruct((features, vocab), jnp.float32),
        in_specs=[
            pl.BlockSpec(memory_space=pltpu.SMEM),
            pl.BlockSpec(memory_space=pltpu.SMEM),
            pl.BlockSpec(memory_space=pltpu.VMEM),
            pl.BlockSpec(memory_space=pltpu.VMEM),
        ],
        out_specs=pl.BlockSpec(memory_space=pltpu.VMEM),
        scratch_shapes=[pltpu.VMEM((tokens, 128), jnp.float32)]
        + [pltpu.VMEM((row_count, 128), jnp.float32)] * 8,
        compiler_params=pltpu.CompilerParams(vmem_limit_bytes=44 * 1024 * 1024),
        cost_estimate=pl.CostEstimate(
            flops=40 * 10**9, bytes_accessed=8 * 10**6, transcendentals=0
        ),
        name="scatter_add",
    )(
        live.reshape(-1),
        (ids & (row_count - 1)).reshape(-1),
        ids.reshape(sources, 1, tokens),
        grads,
    )


def spread_kernel(count, hidden_ref, spread_ref):
    per = hidden_ref.shape[1] // count
    features = spread_ref.shape[1] // (-(-per // (D // count)) * count)
    spread_ref[...] = jnp.zeros_like(spread_ref)
    for d in range(count):
        block = hidden_ref[:, pl.ds(d * per, per)]
        for k in range(-(-per // features)):
            width = min(features, per - k * features)
            at = (k * count + d) * features
            spread_ref[:, pl.ds(at, width)] = block[:, k * features : k * features + width]


def spread_columns(hidden, count):
    rows = hidden.shape[0]
    pieces = -(-(hidden.shape[1] // count) // (D // count))
    result = jax.ShapeDtypeStruct((rows, pieces * D), hidden.dtype)
    return pl.pallas_call(
        functools.partial(spread_kernel, count),
        out_shape=result,
        in_specs=[pl.BlockSpec(memory_space=pltpu.VMEM)],
        out_specs=pl.BlockSpec(memory_space=pltpu.VMEM),
        compiler_params=pltpu.CompilerParams(vmem_limit_bytes=room(hidden, result)),
        name="spread_columns",
    )(hidden)


def pack_kernel(*refs):
    packed_ref = refs[-1]
    count = packed_ref.shape[0]
    packed_ref[...] = jnp.zeros_like(packed_ref)
    at = 0
    for x_ref in refs[:-1]:
        width = x_ref.shape[1] // count
        for d in range(count):
            packed_ref[d, :, pl.ds(at, width)] = x_ref[:, pl.ds(d * width, width)]
        at += width


def pack_columns(arrays, count):
    width = -(-sum(array.shape[1] for array in arrays) // (128 * count)) * 128
    result = jax.ShapeDtypeStruct((count, arrays[0].shape[0], width), arrays[0].dtype)
    return pl.pallas_call(
        pack_kernel,
        out_shape=result,
        in_specs=[pl.BlockSpec(memory_space=pltpu.VMEM)] * len(arrays),
        out_specs=pl.BlockSpec(memory_space=pltpu.VMEM),
        compiler_params=pltpu.CompilerParams(vmem_limit_bytes=room(*arrays, result)),
        name="pack_columns",
    )(*arrays)


def collect_kernel(count, spread_ref, o_ref):
    per = o_ref.shape[1] // count
    features = spread_ref.shape[2] // count
    for d in range(count):
        for k in range(spread_ref.shape[0]):
            width = min(features, per - k * features)
            part = spread_ref[k, :, pl.ds(d * features, width)]
            o_ref[:, pl.ds(d * per + k * features, width)] = part


def collect_columns(parts, columns, count):
    return pl.pallas_call(
        functools.partial(collect_kernel, count),
        out_shape=jax.ShapeDtypeStruct((parts.shape[1], columns), parts.dtype),
        in_specs=[pl.BlockSpec(memory_space=pltpu.VMEM)],
        out_specs=pl.BlockSpec(memory_space=pltpu.VMEM),
        compiler_params=pltpu.CompilerParams(vmem_limit_bytes=room(parts, parts)),
        name="collect_columns",
    )(parts)


def pack_grads_kernel(down_ref, *refs):
    o_ref = refs[-1]
    count, features, _ = o_ref.shape
    down_here = down_ref.shape[1] // count
    o_ref[...] = jnp.zeros_like(o_ref)
    for d in range(count):
        at = 0
        for x_ref in refs[:-1]:
            width = x_ref.shape[1]
            o_ref[d, :, pl.ds(at, width)] = x_ref[pl.ds(d * features, features), :]
            at += width
        o_ref[d, :, pl.ds(at, down_here)] = down_ref[:, pl.ds(d * down_here, down_here)]


def pack_grads(down, columns, count):
    width = sum(x.shape[1] for x in columns) + down.shape[1] // count
    width = -(-width // 128) * 128
    result = jax.ShapeDtypeStruct((count, down.shape[0], width), jnp.float32)
    return pl.pallas_call(
        pack_grads_kernel,
        out_shape=result,
        in_specs=[pl.BlockSpec(memory_space=pltpu.VMEM)] * (1 + len(columns)),
        out_specs=pl.BlockSpec(memory_space=pltpu.VMEM),
        compiler_params=pltpu.CompilerParams(vmem_limit_bytes=room(down, *columns, result)),
        name="pack_grads",
    )(down, *columns)


def unpack_kernel(widths, x_ref, *refs):
    o_refs, down_ref, turned = refs[: len(widths)], refs[len(widths)], refs[-1]
    count, features, _ = x_ref.shape
    down_here = down_ref.shape[0]
    at = 0
    for width, o_ref in zip(widths, o_refs):
        for d in range(count):
            o_ref[:, pl.ds(d * width, width)] = x_ref[d, :, pl.ds(at, width)]
        at += width
    turned[...] = jnp.zeros_like(turned)
    for d in range(count):
        turned[pl.ds(d * features, features), pl.ds(0, down_here)] = x_ref[
            d, :, pl.ds(at, down_here)
        ]
    for c in range(D // 128):
        block = turned[pl.ds(c * 128, 128), :].T
        down_ref[:, pl.ds(c * 128, 128)] = block[:down_here]


def unpack_columns(blocks, widths, down_here):
    count, rows, _ = blocks.shape
    results = tuple(jax.ShapeDtypeStruct((rows, count * w), blocks.dtype) for w in widths)
    results += (jax.ShapeDtypeStruct((down_here, D), blocks.dtype),)
    turned = jax.ShapeDtypeStruct((D, 128), blocks.dtype)
    return pl.pallas_call(
        functools.partial(unpack_kernel, widths),
        out_shape=results,
        in_specs=[pl.BlockSpec(memory_space=pltpu.VMEM)],
        out_specs=tuple(pl.BlockSpec(memory_space=pltpu.VMEM) for _ in results),
        scratch_shapes=[pltpu.VMEM(turned.shape, turned.dtype)],
        compiler_params=pltpu.CompilerParams(vmem_limit_bytes=room(blocks, turned, *results)),
        name="unpack_columns",
    )(blocks)


def update_kernel(rates, factor_ref, *refs):
    count = len(rates)
    inputs, outputs = refs[: 4 * count], refs[4 * count : 7 * count]
    staged, sems = refs[7 * count : 10 * count], refs[10 * count]
    factor = factor_ref[0]
    copies = []
    for p, rate in enumerate(rates):
        rows, columns = inputs[4 * p].shape
        wide = rows < 32 and columns > 8192
        size, total = (3200, columns) if wide else (40 if rows % 40 == 0 else rows, rows)
        parts = total // size
        weight_ref, moment_ref, average_ref, grad_ref = inputs[4 * p : 4 * p + 4]

        def span(step, wide=wide, size=size):
            at = pl.ds(pl.multiple_of(step * size, 128 if wide else 8), size)
            return (slice(None), at) if wide else (at, slice(None))

        def compute(where, p=p, rate=rate, refs=(weight_ref, moment_ref, average_ref, grad_ref)):
            new = apply_update(refs[0][where], refs[3][where], refs[1][where], refs[2][where], factor, rate)
            for k in range(3):
                staged[3 * p + k][where] = new[k]

        if parts == 1:
            compute((slice(None), slice(None)))
        else:

            def body(step, _, compute=compute, span=span):
                compute(span(step))
                return 0

            lax.fori_loop(0, parts, body, 0)
        for k in range(3):
            at = 3 * p + k
            copies.append(pltpu.make_async_copy(staged[at], outputs[at], sems.at[at]))
            copies[-1].start()
    for copy in copies:
        copy.wait()


def update_all(factor, params, rates):
    flat = [array for param in params for array in param]
    shapes = [param[0].shape for param in params for _ in range(3)]
    results = tuple(jax.ShapeDtypeStruct(shape, jnp.float32) for shape in shapes)
    new = pl.pallas_call(
        functools.partial(update_kernel, rates),
        out_shape=results,
        in_specs=[pl.BlockSpec(memory_space=pltpu.SMEM)]
        + [pl.BlockSpec(memory_space=pltpu.VMEM)] * len(flat),
        out_specs=tuple(pl.BlockSpec(memory_space=pl.ANY) for _ in shapes),
        scratch_shapes=[pltpu.VMEM(shape, jnp.float32) for shape in shapes]
        + [pltpu.SemaphoreType.DMA((len(shapes),))],
        compiler_params=pltpu.CompilerParams(vmem_limit_bytes=room(*results, *flat)),
        name="update_all",
    )(factor.reshape(1), *flat)
    return [new[3 * p : 3 * p + 3] for p in range(len(params))]


def other_core(arrays):
    return lax.ppermute(arrays, "seq", [(0, 1), (1, 0)])


def norm_forward(values, gain_row):
    inverse = lax.rsqrt(jnp.mean(values * values, axis=-1, keepdims=True) + epsilon)
    return (values * inverse * gain_row, inverse)


def norm_backward(values, inverse, gain_row, grad_out):
    scaled = grad_out * gain_row
    grad_gain = jnp.sum(grad_out * values * inverse, axis=0)
    grad_in = inverse * scaled - values * inverse**3 * jnp.mean(
        values * scaled, axis=-1, keepdims=True
    )
    return (grad_in, grad_gain)


def apply_update(weight_old, grad_full, moment_old, average_old, factor, rate):
    clipped = factor * grad_full
    moment_new = moment * moment_old + clipped
    weight_new = weight_old - rate * (clipped + moment * moment_new)
    average_new = average * average_old + (1.0 - average) * weight_new
    return (weight_new, moment_new, average_new)


def step(
    token_ids,
    lengths,
    loss_positions,
    loss_targets,
    attention_in,
    attention_in_moment,
    attention_in_average,
    attention_out,
    attention_out_moment,
    attention_out_average,
    feed_in,
    feed_in_moment,
    feed_in_average,
    feed_out,
    feed_out_moment,
    feed_out_average,
    embedding,
    embedding_moment,
    embedding_average,
    unembedding,
    unembedding_moment,
    unembedding_average,
    gains_biases,
    gains_biases_moment,
    gains_biases_average,
):
    low = jnp.bfloat16
    wide = jnp.float32
    devices_all = lax.axis_size(both)
    seq_index = lax.axis_index("seq")
    device = lax.axis_index(both)
    micros, _, half = token_ids.shape
    loss_dev = loss_positions.shape[2]
    tokens = micros * half
    rows = micros * loss_dev
    rows_all = devices_all * rows
    vocab_here = unembedding.shape[0]
    features = D // devices_all
    gate_here = FF // devices_all
    gain_rows = gains_biases[: 3 * D].reshape(3, D)
    bias_row = gains_biases[3 * D :]
    second = seq_index.astype(wide)

    positions = loss_positions[:, 0]
    targets = loss_targets[:, 0]
    ids_all = gather_labels(token_ids[:, 0], lengths, positions, targets, 1)
    base = tokens // 128
    all_tokens = ids_all[:, :base].reshape(devices_all, tokens)
    all_targets = ids_all[:, base : base + micros, :loss_dev].reshape(-1)
    all_counted = ids_all[:, base + micros : base + 2 * micros, :loss_dev]
    all_live = ids_all[:, base + 2 * micros : base + 3 * micros, 0]

    down_here = feed_out.shape[1]
    pieces = -(-down_here // features)
    down_pad = jnp.pad(feed_out[0], ((0, pieces * features - down_here), (0, 0)))
    down_pad = [down_pad[k * features : (k + 1) * features] for k in range(pieces)]
    packed = jnp.concatenate([feed_in[0]] + down_pad + [attention_out[0], attention_in[0]], axis=1)
    w_all = lax.all_gather(packed.astype(low), both, axis=0, tiled=True)
    down_at = 2 * FF
    out_at = down_at + pieces * D
    w_feed = w_all[:, :down_at]
    w_out = w_all[:, out_at : out_at + D]
    w_in = w_all[:, out_at + D :]
    w_down = [w_all[:, down_at + k * D : down_at + (k + 1) * D] for k in range(pieces)]
    head_low = unembedding.astype(low)

    arrived = exchange(lookup(all_live, all_tokens, embedding.T), 5)
    x_t = arrived.reshape(D, tokens)
    pick = [
        (positions[m][:, None] == jnp.arange(half)[None, :]).astype(low) for m in range(micros)
    ]
    x_wide, inverse_one, normed_t, keys_t, values_t, forget_t = [], [], [], [], [], []
    for m in range(micros):
        x_wide.append(x_t[:, m * half : (m + 1) * half].astype(wide))
        inverse_one.append(
            lax.rsqrt(jnp.mean(x_wide[m] * x_wide[m], axis=0, keepdims=True) + epsilon)
        )
        normed_t.append((x_wide[m] * inverse_one[m] * gain_rows[0][:, None]).astype(low))

        project_t = dot(w_in[:, D:], normed_t[m], 0, 0)
        keys_t.append(project_t[:D].astype(low).reshape(H, HD, half))
        values_t.append(project_t[D : 2 * D].astype(low).reshape(H, HD, half))
        forget_t.append((project_t[2 * D :] + bias_row[:, None]).astype(low).astype(wide))
    x_rows = jnp.concatenate([dot(pick[m], x_wide[m].astype(low), 1, 1) for m in range(micros)])
    normed_rows = jnp.concatenate(
        [dot(pick[m], normed_t[m], 1, 1) for m in range(micros)]
    ).astype(low)
    q_rows = dot(normed_rows, w_in[:, :D], 1, 0).astype(low)

    upper = (jnp.arange(half)[:, None] <= jnp.arange(half)[None, :]).astype(wide)
    log_gate = jax.nn.log_sigmoid(jnp.stack(forget_t, axis=1))
    decay_own = lax.dot_general(
        log_gate, upper, (((2,), (0,)), ((), ())), precision=highest, preferred_element_type=wide
    )
    total_own = decay_own[:, :, -1]
    decay_rows = jnp.stack(
        [dot(pick[m].astype(wide), decay_own[:, m], 1, 1, highest) for m in range(micros)]
    )
    q_own = q_rows.reshape(micros, loss_dev, H, HD)
    q_far, decay_far, total_far, place_far = other_core((q_own, decay_rows, total_own, positions))
    shift_own = second * total_far
    shift_far = (1.0 - second) * total_own
    key_decay = decay_own + shift_own[:, :, None]
    row_decay = jnp.concatenate(
        [decay_rows + shift_own.T[:, None], decay_far + shift_far.T[:, None]], axis=1
    )
    q_all = jnp.concatenate([q_own, q_far], axis=1)
    places = jnp.concatenate(
        [positions + seq_index * half, place_far + (1 - seq_index) * half], axis=1
    )
    key_places = seq_index * half + jnp.arange(half)

    scores = []
    for m in range(micros):
        raw = jnp.einsum("rhd,hdj->hrj", q_all[m], keys_t[m], preferred_element_type=wide)
        part = raw * HD ** (-0.5) + row_decay[m].T[:, :, None] - key_decay[:, m][:, None, :]
        causal = places[m][:, None] >= key_places[None, :]
        scores.append(jnp.where(causal[None], part, negative))
    scores = jnp.stack(scores)
    peak_own = jnp.max(scores, axis=-1)
    spread_own = jnp.sum(jnp.exp(scores - peak_own[..., None]), axis=-1)
    peak_far, spread_far = other_core((peak_own, spread_own))

    def swap_rows(array):
        return jnp.concatenate([array[:, :, loss_dev:], array[:, :, :loss_dev]], axis=2)

    peak_far, spread_far = swap_rows(peak_far), swap_rows(spread_far)
    peak = jnp.maximum(peak_own, peak_far)
    log_total = peak + jnp.log(
        spread_own * jnp.exp(peak_own - peak) + spread_far * jnp.exp(peak_far - peak)
    )
    probs = jnp.exp(scores - log_total[..., None])
    probs_low = probs.astype(low)
    probs_rest = (probs - probs_low.astype(wide)).astype(low)

    def mix(weights):
        return jnp.stack(
            [
                jnp.einsum(
                    "hrj,hdj->rhd",
                    weights[m],
                    values_t[m],
                    preferred_element_type=wide,
                )
                for m in range(micros)
            ]
        )

    mixed_part = mix(probs_low)
    rest_part = mix(probs_rest)
    mixed_far, rest_far = other_core((mixed_part[:, loss_dev:], rest_part[:, loss_dev:]))
    mixed_sum = mixed_part[:, :loss_dev] + mixed_far
    mixed_full = mixed_sum + rest_part[:, :loss_dev] + rest_far
    mixed_rows = mixed_sum.reshape(rows, D).astype(low)

    middle = x_rows + dot(mixed_rows, w_out, 1, 0)
    normed_two, inverse_two = norm_forward(middle, gain_rows[1])
    normed_two = normed_two.astype(low)
    gate_up = dot(normed_two, w_feed, 1, 0)
    gate_half, up_half = gate_up[:, :FF], gate_up[:, FF:]
    gate_sigmoid = jax.nn.sigmoid(gate_half)
    hidden = (gate_half * gate_sigmoid * up_half).astype(low)
    hidden_spread = spread_columns(hidden, devices_all)
    early_packed = lax.all_gather(
        jnp.concatenate([normed_two, mixed_rows, normed_rows, hidden], axis=1),
        both,
        axis=0,
        tiled=True,
    )
    final_in = middle
    for k in range(pieces):
        final_in = final_in + dot(hidden_spread[:, k * D : (k + 1) * D], w_down[k], 1, 0)
    final_normed, final_inverse = norm_forward(final_in, gain_rows[2])

    final_all = gather_rows(final_normed.astype(low), 2).reshape(rows_all, D)
    logits = dot(final_all, head_low, 1, 1)
    vocab_ids = device * vocab_here + jnp.arange(vocab_here)
    target_hits = all_targets[:, None] == vocab_ids[None, :]
    row_peak = jnp.max(logits, axis=1)
    exp_sum = jnp.sum(jnp.exp(logits - row_peak[:, None]), axis=1)
    target_part = jnp.sum(jnp.where(target_hits, logits, 0.0), axis=1)
    logit_sum = jnp.sum(logits, axis=1)
    stats = jnp.stack([row_peak, exp_sum, target_part, logit_sum])
    stats_all = gather_rows(stats.reshape(-1, 128), 3).reshape(devices_all, 4, rows_all)
    peak_all = jnp.max(stats_all[:, 0], axis=0)
    spread_all = jnp.sum(stats_all[:, 1] * jnp.exp(stats_all[:, 0] - peak_all), axis=0)
    target_all = jnp.sum(stats_all[:, 2], axis=0)
    logit_all = jnp.sum(stats_all[:, 3], axis=0)
    total_all = peak_all + jnp.log(spread_all)
    per_row = (
        total_all
        - (1.0 - smooth) * target_all
        - smooth * logit_all / V
        + z_weight * total_all * total_all
    )
    weights_row = all_counted.astype(wide).reshape(devices_all, micros, loss_dev)
    counts = jnp.sum(weights_row, axis=(0, 2))
    weights_row = (weights_row / (micros * counts)[None, :, None]).reshape(-1)
    loss_value = jnp.sum(weights_row * per_row)
    soft_rows = jnp.exp(logits - total_all[:, None])
    grad_logits = (
        weights_row[:, None]
        * (
            soft_rows * (1.0 + 2.0 * z_weight * total_all)[:, None]
            - (1.0 - smooth) * target_hits.astype(wide)
            - smooth / V
        )
    ).astype(low)
    grad_final = reduce_rows(dot(grad_logits, head_low, 1, 0), 7)

    grad_rows, gain_grad_final = norm_backward(final_in, final_inverse, gain_rows[2], grad_final)
    grad_branch = grad_rows.astype(low)
    grad_hidden = jnp.stack([dot(grad_branch, w_down[k], 1, 1) for k in range(pieces)])
    grad_hidden = collect_columns(grad_hidden, FF, devices_all)
    grad_gate = grad_hidden * up_half * gate_sigmoid * (1.0 + gate_half * (1.0 - gate_sigmoid))
    grad_up = grad_hidden * gate_half * gate_sigmoid
    grad_gate_up = jnp.concatenate([grad_gate, grad_up], axis=1).astype(low)
    grad_two, gain_grad_two = norm_backward(
        middle, inverse_two, gain_rows[1], dot(grad_gate_up, w_feed, 1, 1)
    )
    grad_middle = grad_rows + grad_two
    grad_mid_low = grad_middle.astype(low)
    grad_mixed = dot(grad_mid_low, w_out, 1, 1).astype(low)

    feed_here = 2 * FF // devices_all
    grad_own = grad_mixed.reshape(micros, loss_dev, H, HD)
    inner_own = jnp.sum(grad_own.astype(wide) * mixed_full, axis=-1)
    grad_far, inner_far = other_core((grad_own, inner_own))
    grad_heads = jnp.concatenate([grad_own, grad_far], axis=1)
    inner_sum = jnp.concatenate([inner_own, inner_far], axis=1)
    query_parts, score_rows = [], []
    grad_keys, grad_values, score_columns = [], [], []
    for m in range(micros):
        grad_probs = jnp.einsum(
            "rhd,hdj->hrj", grad_heads[m], values_t[m], preferred_element_type=wide
        )
        grad_scores = (probs[m] * (grad_probs - inner_sum[m].T[:, :, None])).astype(low)
        query_parts.append(
            jnp.einsum("hrj,hdj->rhd", grad_scores, keys_t[m], preferred_element_type=wide)
        )
        grad_keys.append(
            jnp.einsum("hrj,rhd->hdj", grad_scores, q_all[m], preferred_element_type=wide)
            * HD ** (-0.5)
        )
        grad_values.append(
            jnp.einsum("hrj,rhd->hdj", probs_low[m], grad_heads[m], preferred_element_type=wide)
        )
        score_wide = grad_scores.astype(wide)
        score_rows.append(jnp.sum(score_wide, axis=-1))
        score_columns.append(jnp.sum(score_wide, axis=1))
    query_parts = jnp.stack(query_parts)
    score_rows = jnp.stack(score_rows).transpose(0, 2, 1)
    query_far, score_far = other_core((query_parts[:, loss_dev:], score_rows[:, loss_dev:]))
    grad_query = ((query_parts[:, :loss_dev] + query_far) * HD ** (-0.5)).astype(low)
    grad_query = grad_query.reshape(rows, D)
    columns_packed = lax.all_to_all(
        pack_columns((grad_gate_up, grad_mid_low, grad_query, grad_branch), devices_all),
        both,
        split_axis=0,
        concat_axis=0,
        tiled=True,
    )
    rows_sum = score_rows[:, :loss_dev] + score_far
    later = (1.0 - second) * jnp.sum(score_rows[:, loss_dev:], axis=1)
    grad_in_sum, gain_grad_one, grad_bias, grad_embed = 0.0, 0.0, 0.0, []
    projects = []
    for m in range(micros):
        placed = dot(rows_sum[m], pick[m].astype(wide), 0, 0, highest)
        change = placed - score_columns[m]
        grad_log = dot(change, upper, 1, 1, highest) + later[m][:, None]
        grad_forget = (grad_log * jax.nn.sigmoid(-forget_t[m])).astype(low)
        grad_bias = grad_bias + jnp.sum(grad_forget.astype(wide), axis=1)
        query_t = dot(grad_query[m * loss_dev : (m + 1) * loss_dev], pick[m], 0, 0).astype(low)
        keys_part = grad_keys[m].astype(low).reshape(D, half)
        values_part = grad_values[m].astype(low).reshape(D, half)
        grad_forget = lax.optimization_barrier(jnp.pad(grad_forget, ((0, -H % 128), (0, 0))))
        projects.append(jnp.concatenate([query_t, keys_part, values_part, grad_forget], axis=0))
        grad_in_sum = grad_in_sum + dot(normed_t[m], projects[m][D:], 1, 1)
    grad_in = lax.psum_scatter(grad_in_sum, both, scatter_dimension=0, tiled=True)
    for m in range(micros):
        grad_normed = dot(w_in, projects[m][: 3 * D + H], 1, 0)
        scaled = grad_normed * gain_rows[0][:, None]
        gain_grad_one = gain_grad_one + jnp.sum(grad_normed * x_wide[m] * inverse_one[m], axis=1)
        grad_one = inverse_one[m] * scaled - x_wide[m] * inverse_one[m] ** 3 * jnp.mean(
            x_wide[m] * scaled, axis=0, keepdims=True
        )
        middle_t = dot(
            grad_middle[m * loss_dev : (m + 1) * loss_dev], pick[m].astype(wide), 0, 0, highest
        )
        grad_embed.append((middle_t + grad_one).astype(low))
    grad_embed = jnp.concatenate(grad_embed, axis=1).reshape(devices_all, features, tokens)
    moved = lax.all_to_all(grad_embed, both, split_axis=0, concat_axis=0, tiled=True)
    early_packed, columns_packed, _ = lax.optimization_barrier(
        (early_packed, columns_packed, grad_embed[:1, :1, :1])
    )
    late_logits, _ = lax.optimization_barrier((grad_logits, grad_embed[:1, :1, :1]))
    head_grad = lax.optimization_barrier(dot(late_logits, final_all, 0, 0))
    columns_packed = columns_packed.reshape(rows_all, -1)

    def columns_of(first, width):
        return columns_packed[:, first : first + width]

    feed_columns = dot(early_packed[:, :D], columns_of(0, feed_here), 0, 0)
    out_columns = columns_of(feed_here, features)
    out_columns = dot(early_packed[:, D : 2 * D], out_columns, 0, 0)
    query_columns = columns_of(feed_here + features, features)
    query_columns = dot(early_packed[:, 2 * D : 3 * D], query_columns, 0, 0)
    down_rows = columns_of(feed_here + 2 * features, features)
    down_rows = dot(down_rows, early_packed[:, 3 * D :], 0, 0)
    moved_grads = lax.all_to_all(
        pack_grads(down_rows, (feed_columns, out_columns, query_columns), devices_all),
        both,
        split_axis=0,
        concat_axis=0,
        tiled=True,
    )
    grad_feed, grad_out, grad_q, grad_down = unpack_columns(
        moved_grads, (feed_here, features, features), gate_here
    )
    embed_grad = scatter_add(all_live, all_tokens, moved, V)

    grad_in, _ = lax.optimization_barrier((grad_in, embed_grad[:1, :1]))
    grad_in = jnp.concatenate([grad_q, grad_in[:, : 2 * D + H]], axis=1)
    owned_grads = [grad_in, grad_out, grad_feed, grad_down, embed_grad, head_grad]
    square_sum = jnp.zeros((), wide)
    for grad_part in owned_grads:
        square_sum = square_sum + jnp.sum(grad_part * grad_part)
    small_grad = jnp.concatenate(
        [gain_grad_one, gain_grad_two, gain_grad_final, grad_bias, square_sum[None]]
    )
    small_count = small_grad.shape[0]
    small_grad = jnp.pad(small_grad, (0, -small_count % 1024)).reshape(-1, 128)
    small_sum = jnp.sum(gather_rows(small_grad, 4), axis=0).reshape(-1)
    small_total, square_total = small_sum[: small_count - 1], small_sum[small_count - 1]
    grad_norm = jnp.sqrt(square_total + jnp.sum(small_total * small_total))
    factor = jnp.minimum(1.0, clip_limit / grad_norm)
    layer = rate_layer
    news = update_all(
        factor,
        (
            (attention_in[0], attention_in_moment[0], attention_in_average[0], grad_in),
            (attention_out[0], attention_out_moment[0], attention_out_average[0], grad_out),
            (feed_in[0], feed_in_moment[0], feed_in_average[0], grad_feed),
            (feed_out[0], feed_out_moment[0], feed_out_average[0], grad_down),
            (embedding.T, embedding_moment.T, embedding_average.T, embed_grad),
            (unembedding, unembedding_moment, unembedding_average, head_grad),
        ),
        (layer, layer, layer, layer, rate_embed, rate_head),
    )
    results = [loss_value, grad_norm]
    for new in news[:4]:
        results.extend(array[None] for array in new)
    results.extend(array.T for array in news[4])
    results.extend(news[5])
    results.extend(
        apply_update(
            gains_biases, small_total, gains_biases_moment, gains_biases_average, factor, layer
        )
    )
    return tuple(results)


def solution(mesh):
    rows = P(None, both, None)
    tables = (rows,) * 12 + (P(None, both),) * 3 + (P(both, None),) * 3 + (P(),) * 3
    return jax.shard_map(
        step,
        mesh=mesh,
        in_specs=(
            P(None, "fsdp", "seq"),
            P(None, "fsdp"),
            P(None, "fsdp", "seq"),
            P(None, "fsdp", "seq"),
        )
        + tables,
        out_specs=(P(), P()) + tables,
        check_vma=False,
    )
```

```python
import functools
import math

import jax
import jax.numpy as jnp
from jax import lax
from jax.experimental import pallas as pl
from jax.experimental.pallas import tpu as pltpu
from jax.sharding import PartitionSpec as P

D = 768
H = 12
HD = 64
FF = 2048
V = 32000


epsilon = 1e-06
smooth = 0.1
z_weight = 0.005
clip_limit = 0.5
moment = 0.9
average = 0.9
rate_layer = 200.0
rate_head = 1000.0
rate_embed = 5000.0
negative = -1e30
both = ("seq", "fsdp")
highest = lax.Precision.HIGHEST
MESH = pl.DeviceIdType.MESH


def dot(left_side, right_side, left_axis, right_axis, precision=None):
    return lax.dot_general(
        left_side,
        right_side,
        (((left_axis,), (right_axis,)), ((), ())),
        precision=precision,
        preferred_element_type=jnp.float32,
    )


def room(*arrays):
    total = 1 << 20
    for array in arrays:
        shape, size = array.shape, jnp.dtype(array.dtype).itemsize
        tile = 32 // size
        total += (
            math.prod(shape[:-2]) * (-(-shape[-2] // tile) * tile) * (-(-shape[-1] // 128) * 128)
        ) * size
    return total


def line_of(fsdp_count):
    return 4 if fsdp_count % 4 == 0 else 1


def gather_kernel(cores, fsdp, x_ref, o_ref, send_sem, recv_sem):
    plane = line_of(fsdp)
    lines = fsdp // plane
    core = lax.axis_index("seq")
    spot = lax.axis_index("fsdp")
    high, low = spot // plane, spot % plane
    line_peers = [((high + k) % lines) * plane + low for k in range(1, lines)]
    plane_peers = [high * plane + (low + k) % plane for k in range(1, plane)]
    core_peers = [(core + k) % cores for k in range(1, cores)]
    peers = [(core, p) for p in line_peers + plane_peers] + [(c, spot) for c in core_peers]

    barrier = pltpu.get_barrier_semaphore()
    for peer in peers:
        pl.semaphore_signal(barrier, inc=1, device_id=peer, device_id_type=MESH)
    pl.semaphore_wait(barrier, len(peers))

    sent = []

    def send(source_ref, block, peer):
        copy = pltpu.make_async_remote_copy(
            src_ref=source_ref,
            dst_ref=o_ref.at[block],
            send_sem=send_sem.at[len(sent)],
            recv_sem=recv_sem.at[block],
            device_id=peer,
            device_id_type=MESH,
        )
        copy.start()
        sent.append(copy)

    def arrived(block):
        pltpu.make_async_copy(o_ref.at[block], o_ref.at[block], recv_sem.at[block]).wait()

    mine = core * fsdp + spot
    for p in line_peers:
        send(x_ref, mine, (core, p))
    for p in plane_peers:
        send(x_ref, mine, (core, p))
    for c in core_peers:
        send(x_ref, mine, (c, spot))
    o_ref[mine] = x_ref[...]
    for k in range(1, lines):
        block = core * fsdp + ((high + lines - k) % lines) * plane + low
        arrived(block)
        for p in plane_peers:
            send(o_ref.at[block], block, (core, p))
        for c in core_peers:
            send(o_ref.at[block], block, (c, spot))
    for m in range(lines):
        for k in range(1, plane):
            block = core * fsdp + ((high + lines - m) % lines) * plane + (low + plane - k) % plane
            arrived(block)
            for c in core_peers:
                send(o_ref.at[block], block, (c, spot))
    for c in core_peers:
        for m in range(lines):
            for k in range(plane):
                block = c * fsdp + ((high + lines - m) % lines) * plane + (low + plane - k) % plane
                arrived(block)
    for copy in sent:
        copy.wait_send()


def label_kernel(
    cores, fsdp, tokens_ref, lengths_ref, places_ref, targets_ref, o_ref, packed, send_sem, recv_sem
):
    micros, half = tokens_ref.shape
    chunks = half // 128
    start = lax.axis_index("seq") * half
    packed[...] = jnp.zeros_like(packed)
    for m in range(micros):
        for c in range(chunks):
            packed[pl.ds(m * chunks + c, 1), :] = tokens_ref[pl.ds(m, 1), pl.ds(c * 128, 128)]
    base = micros * chunks
    length = lengths_ref[...]
    counted = (start + places_ref[...] < length).astype(jnp.int32)
    live = jnp.clip(length - start, 0, half)
    count = places_ref.shape[1]
    packed[pl.ds(base, micros), pl.ds(0, count)] = targets_ref[...]
    packed[pl.ds(base + micros, micros), pl.ds(0, count)] = counted
    packed[pl.ds(base + 2 * micros, micros), :] = jnp.broadcast_to(live, (micros, 128))
    gather_kernel(cores, fsdp, packed, o_ref, send_sem, recv_sem)


def gather_labels(tokens, lengths, places, targets, collective):
    cores, fsdp = lax.axis_size("seq"), lax.axis_size("fsdp")
    count = cores * fsdp
    micros, half = tokens.shape
    rows = micros * (half // 128) + 3 * micros
    rows = -(-rows // 8) * 8
    result = jax.ShapeDtypeStruct((count, rows, 128), jnp.int32)
    return pl.pallas_call(
        functools.partial(label_kernel, cores, fsdp),
        out_shape=result,
        in_specs=[pl.BlockSpec(memory_space=pltpu.VMEM)] * 4,
        out_specs=pl.BlockSpec(memory_space=pltpu.VMEM),
        scratch_shapes=[
            pltpu.VMEM((rows, 128), jnp.int32),
            pltpu.SemaphoreType.DMA((count,)),
            pltpu.SemaphoreType.DMA((count,)),
        ],
        compiler_params=pltpu.CompilerParams(
            collective_id=collective, has_side_effects=True, vmem_limit_bytes=room(result)
        ),
        name="gather_labels",
    )(tokens, lengths, places, targets)


def gather_rows(array, collective):
    cores, fsdp = lax.axis_size("seq"), lax.axis_size("fsdp")
    count = cores * fsdp
    result = jax.ShapeDtypeStruct((count,) + array.shape, array.dtype)
    return pl.pallas_call(
        functools.partial(gather_kernel, cores, fsdp),
        out_shape=result,
        in_specs=[pl.BlockSpec(memory_space=pltpu.VMEM)],
        out_specs=pl.BlockSpec(memory_space=pltpu.VMEM),
        scratch_shapes=[
            pltpu.SemaphoreType.DMA((count,)),
            pltpu.SemaphoreType.DMA((count,)),
        ],
        compiler_params=pltpu.CompilerParams(
            collective_id=collective,
            has_side_effects=True,
            vmem_limit_bytes=room(array, result),
        ),
        name="gather_rows",
    )(array)


def exchange_kernel(cores, fsdp, x_ref, o_ref, send_sem, recv_sem, own_sem):
    count = cores * fsdp
    mine = lax.axis_index("seq") * fsdp + lax.axis_index("fsdp")

    def place(step):
        other = lax.rem(mine + step, count)
        return other, (other // fsdp, lax.rem(other, fsdp))

    barrier = pltpu.get_barrier_semaphore()

    def greet(step, _):
        pl.semaphore_signal(barrier, inc=1, device_id=place(step)[1], device_id_type=MESH)
        return 0

    lax.fori_loop(1, count, greet, 0)
    pl.semaphore_wait(barrier, count - 1)
    own = pltpu.make_async_copy(x_ref.at[mine], o_ref.at[mine], own_sem)
    own.start()

    def copy_to(step):
        other, peer = place(step)
        return pltpu.make_async_remote_copy(
            src_ref=x_ref.at[other],
            dst_ref=o_ref.at[mine],
            send_sem=send_sem.at[step],
            recv_sem=recv_sem.at[step],
            device_id=peer,
            device_id_type=MESH,
        )

    def start(step, _):
        copy_to(step).start()
        return 0

    lax.fori_loop(1, count, start, 0)
    own.wait()

    def finish(step, _):
        source = lax.rem(mine + count - step, count)
        pltpu.make_async_copy(o_ref.at[source], o_ref.at[source], recv_sem.at[step]).wait()
        copy_to(step).wait_send()
        return 0

    lax.fori_loop(1, count, finish, 0)


def exchange(array, collective):
    cores, fsdp = lax.axis_size("seq"), lax.axis_size("fsdp")
    return pl.pallas_call(
        functools.partial(exchange_kernel, cores, fsdp),
        out_shape=jax.ShapeDtypeStruct(array.shape, array.dtype),
        in_specs=[pl.BlockSpec(memory_space=pltpu.VMEM)],
        out_specs=pl.BlockSpec(memory_space=pltpu.VMEM),
        scratch_shapes=[
            pltpu.SemaphoreType.DMA((cores * fsdp,)),
            pltpu.SemaphoreType.DMA((cores * fsdp,)),
            pltpu.SemaphoreType.DMA,
        ],
        compiler_params=pltpu.CompilerParams(
            collective_id=collective,
            has_side_effects=True,
            vmem_limit_bytes=room(array, array),
        ),
        name="exchange",
    )(array)


def reduce_kernel(
    fsdp, x_ref, o_ref, from_core, from_plane, from_line, core_sum, plane_sum, send_sem, recv_sem
):
    plane = line_of(fsdp)
    lines = fsdp // plane
    core = lax.axis_index("seq")
    spot = lax.axis_index("fsdp")
    high, low = spot // plane, lax.rem(spot, plane)
    far = 1 - core
    peers = [(far, spot)]
    peers += [(core, lax.rem(high + k, lines) * plane + low) for k in range(1, lines)]
    peers += [(core, high * plane + lax.rem(low + k, plane)) for k in range(1, plane)]
    barrier = pltpu.get_barrier_semaphore()
    for peer in peers:
        pl.semaphore_signal(barrier, inc=1, device_id=peer, device_id_type=MESH)
    pl.semaphore_wait(barrier, len(peers))
    sent = []

    def send(source_ref, target_ref, slot, peer):
        copy = pltpu.make_async_remote_copy(
            src_ref=source_ref,
            dst_ref=target_ref,
            send_sem=send_sem.at[slot],
            recv_sem=recv_sem.at[slot],
            device_id=peer,
            device_id_type=MESH,
        )
        copy.start()
        sent.append(copy)
        return copy

    first = []
    for k in list(range(1, plane)) + [0]:
        spot_low = lax.rem(low + k, plane)
        first.append(
            (k, spot_low, send(x_ref.at[far, :, spot_low], from_core.at[spot_low], k, (far, spot)))
        )
    second = []
    for k, spot_low, copy in first:
        copy.wait_recv()
        core_sum[spot_low] = x_ref[core, :, spot_low] + from_core[spot_low]
        if k:
            target = from_plane.at[k - 1]
            peer = (core, high * plane + spot_low)
            second.append((k, send(core_sum.at[spot_low], target, plane + k - 1, peer)))
    plane_sum[...] = core_sum[low]
    for k, copy in second:
        copy.wait_recv()
        plane_sum[...] += from_plane[k - 1]
    third = []
    for k in range(1, lines):
        line = lax.rem(high + k, lines)
        slot = 2 * plane + k - 2
        peer = (core, line * plane + low)
        third.append((k, send(plane_sum.at[line], from_line.at[k - 1], slot, peer)))
    total = plane_sum[high]
    for k, copy in third:
        copy.wait_recv()
        total = total + from_line[k - 1]
    o_ref[...] = total
    for copy in sent:
        copy.wait_send()


def reduce_rows(array, collective):
    cores, fsdp = lax.axis_size("seq"), lax.axis_size("fsdp")
    plane = line_of(fsdp)
    lines = fsdp // plane
    rows, columns = array.shape[0] // (cores * fsdp), array.shape[1]
    kind = array.dtype
    slots = 2 * plane + lines - 2
    return pl.pallas_call(
        functools.partial(reduce_kernel, fsdp),
        out_shape=jax.ShapeDtypeStruct((rows, columns), kind),
        in_specs=[pl.BlockSpec(memory_space=pltpu.VMEM)],
        out_specs=pl.BlockSpec(memory_space=pltpu.VMEM),
        scratch_shapes=[
            pltpu.VMEM((plane, lines, rows, columns), kind),
            pltpu.VMEM((plane - 1, lines, rows, columns), kind),
            pltpu.VMEM((lines - 1, rows, columns), kind),
            pltpu.VMEM((plane, lines, rows, columns), kind),
            pltpu.VMEM((lines, rows, columns), kind),
            pltpu.SemaphoreType.DMA((slots,)),
            pltpu.SemaphoreType.DMA((slots,)),
        ],
        compiler_params=pltpu.CompilerParams(
            collective_id=collective,
            has_side_effects=True,
            vmem_limit_bytes=room(array, array, array),
        ),
        name="reduce_rows",
    )(array.reshape(cores, lines, plane, rows, columns))


def lookup_kernel(unroll, builds, live_ref, ids_ref, own_ref, o_ref, table, stage):
    sources, features, tokens = o_ref.shape
    micros = live_ref.shape[0] // sources
    half = tokens // micros

    def build(step, _):
        for u in range(builds):
            at = pl.multiple_of((step * builds + u) * 128, 128)
            block = own_ref[:, pl.ds(at, 128)].astype(jnp.bfloat16).astype(jnp.float32)
            table[pl.ds(at, 128), pl.ds(0, features)] = block.T
        return 0

    lax.fori_loop(0, table.shape[0] // 128 // builds, build, 0)
    stage[...] = jnp.zeros_like(stage)

    def source(which, _):
        def fetch(first, step, _):
            at = first + step * unroll
            ids = [ids_ref[which * tokens + at + u] for u in range(unroll)]
            for u in range(unroll):
                stage[pl.ds(at + u, 1), :] = table[pl.ds(ids[u], 1), :]
            return 0

        for m in range(micros):
            live = live_ref[which * micros + m]
            lax.fori_loop(
                0, (live + unroll - 1) // unroll, functools.partial(fetch, m * half), 0
            )
        for c in range(tokens // 128):
            block = stage[pl.ds(c * 128, 128), :].T
            o_ref[which, :, pl.ds(c * 128, 128)] = block[:features].astype(jnp.bfloat16)
        return 0

    lax.fori_loop(0, sources, source, 0)


def lookup(live, ids, table_t):
    sources, tokens = ids.shape
    features, vocab = table_t.shape
    return pl.pallas_call(
        functools.partial(lookup_kernel, 64, 10),
        out_shape=jax.ShapeDtypeStruct((sources, features, tokens), jnp.bfloat16),
        in_specs=[
            pl.BlockSpec(memory_space=pltpu.SMEM),
            pl.BlockSpec(memory_space=pltpu.SMEM),
            pl.BlockSpec(memory_space=pltpu.VMEM),
        ],
        out_specs=pl.BlockSpec(memory_space=pltpu.VMEM),
        scratch_shapes=[
            pltpu.VMEM((vocab, 128), jnp.float32),
            pltpu.VMEM((tokens, 128), jnp.float32),
        ],
        compiler_params=pltpu.CompilerParams(vmem_limit_bytes=32 * 1024 * 1024),
        name="lookup",
    )(live.reshape(-1), ids.reshape(-1), table_t)


row_bits = 13
row_count = 1 << row_bits


def scatter_kernel(unroll, live_ref, rows_ref, ids_ref, g_ref, o_ref, spread, *sums):
    sources, features, tokens = g_ref.shape
    micros = live_ref.shape[0] // sources
    half = tokens // micros
    vocab = o_ref.shape[1]
    groups = 4

    def clear(step, _):
        for one in sums:
            one[pl.ds(pl.multiple_of(step * 256, 256), 256)] = jnp.zeros((256, 128), jnp.float32)
        return 0

    lax.fori_loop(0, row_count // 256, clear, 0)
    blank = jnp.zeros((128 // groups - features, 128), jnp.float32)
    group = lax.broadcasted_iota(jnp.int32, (128, 128), 0) // (128 // groups)

    def source(which, _):
        for c in range(tokens // 128):
            block = g_ref[which, :, pl.ds(c * 128, 128)].astype(jnp.float32)
            block = jnp.concatenate([block, blank] * groups, axis=0)
            chosen = ids_ref[which, :, pl.ds(c * 128, 128)] >> row_bits
            spread[pl.ds(c * 128, 128), :] = jnp.where(group == chosen, block, 0.0).T

        def add(first, step, _):
            at = first + step * unroll
            rows = [rows_ref[which * tokens + at + u] for u in range(unroll)]
            for u in range(unroll):
                one = sums[u % len(sums)]
                one[pl.ds(rows[u], 1), :] += spread[pl.ds(at + u, 1), :]
            return 0

        for m in range(micros):
            live = live_ref[which * micros + m]
            lax.fori_loop(0, (live + unroll - 1) // unroll, functools.partial(add, m * half), 0)
        return 0

    lax.fori_loop(0, sources, source, 0)

    def finish(step, _):
        for u in range(2):
            at = pl.multiple_of((step * 2 + u) * 128, 128)
            total = sums[0][pl.ds(at, 128)]
            for one in sums[1:]:
                total = total + one[pl.ds(at, 128)]
            total = total.T
            for k in range(groups):
                part = total[k * (128 // groups) : k * (128 // groups) + features]
                if (k + 1) * row_count <= vocab:
                    o_ref[:, pl.ds(k * row_count + at, 128)] = part
                elif k * row_count < vocab:

                    @pl.when(k * row_count + at + 128 <= vocab)
                    def _():
                        o_ref[:, pl.ds(k * row_count + at, 128)] = part

        return 0

    lax.fori_loop(0, row_count // 256, finish, 0)


def scatter_add(live, ids, grads, vocab):
    sources, features, tokens = grads.shape
    return pl.pallas_call(
        functools.partial(scatter_kernel, 32),
        out_shape=jax.ShapeDtypeStruct((features, vocab), jnp.float32),
        in_specs=[
            pl.BlockSpec(memory_space=pltpu.SMEM),
            pl.BlockSpec(memory_space=pltpu.SMEM),
            pl.BlockSpec(memory_space=pltpu.VMEM),
            pl.BlockSpec(memory_space=pltpu.VMEM),
        ],
        out_specs=pl.BlockSpec(memory_space=pltpu.VMEM),
        scratch_shapes=[pltpu.VMEM((tokens, 128), jnp.float32)]
        + [pltpu.VMEM((row_count, 128), jnp.float32)] * 8,
        compiler_params=pltpu.CompilerParams(vmem_limit_bytes=44 * 1024 * 1024),
        cost_estimate=pl.CostEstimate(
            flops=40 * 10**9, bytes_accessed=8 * 10**6, transcendentals=0
        ),
        name="scatter_add",
    )(
        live.reshape(-1),
        (ids & (row_count - 1)).reshape(-1),
        ids.reshape(sources, 1, tokens),
        grads,
    )


def spread_kernel(count, hidden_ref, spread_ref):
    per = hidden_ref.shape[1] // count
    features = spread_ref.shape[1] // (-(-per // (D // count)) * count)
    spread_ref[...] = jnp.zeros_like(spread_ref)
    for d in range(count):
        block = hidden_ref[:, pl.ds(d * per, per)]
        for k in range(-(-per // features)):
            width = min(features, per - k * features)
            at = (k * count + d) * features
            spread_ref[:, pl.ds(at, width)] = block[:, k * features : k * features + width]


def spread_columns(hidden, count):
    rows = hidden.shape[0]
    pieces = -(-(hidden.shape[1] // count) // (D // count))
    result = jax.ShapeDtypeStruct((rows, pieces * D), hidden.dtype)
    return pl.pallas_call(
        functools.partial(spread_kernel, count),
        out_shape=result,
        in_specs=[pl.BlockSpec(memory_space=pltpu.VMEM)],
        out_specs=pl.BlockSpec(memory_space=pltpu.VMEM),
        compiler_params=pltpu.CompilerParams(vmem_limit_bytes=room(hidden, result)),
        name="spread_columns",
    )(hidden)


def pack_kernel(*refs):
    packed_ref = refs[-1]
    count = packed_ref.shape[0]
    packed_ref[...] = jnp.zeros_like(packed_ref)
    at = 0
    for x_ref in refs[:-1]:
        width = x_ref.shape[1] // count
        for d in range(count):
            packed_ref[d, :, pl.ds(at, width)] = x_ref[:, pl.ds(d * width, width)]
        at += width


def pack_columns(arrays, count):
    width = -(-sum(array.shape[1] for array in arrays) // (128 * count)) * 128
    result = jax.ShapeDtypeStruct((count, arrays[0].shape[0], width), arrays[0].dtype)
    return pl.pallas_call(
        pack_kernel,
        out_shape=result,
        in_specs=[pl.BlockSpec(memory_space=pltpu.VMEM)] * len(arrays),
        out_specs=pl.BlockSpec(memory_space=pltpu.VMEM),
        compiler_params=pltpu.CompilerParams(vmem_limit_bytes=room(*arrays, result)),
        name="pack_columns",
    )(*arrays)


def collect_kernel(count, spread_ref, o_ref):
    per = o_ref.shape[1] // count
    features = spread_ref.shape[2] // count
    for d in range(count):
        for k in range(spread_ref.shape[0]):
            width = min(features, per - k * features)
            part = spread_ref[k, :, pl.ds(d * features, width)]
            o_ref[:, pl.ds(d * per + k * features, width)] = part


def collect_columns(parts, columns, count):
    return pl.pallas_call(
        functools.partial(collect_kernel, count),
        out_shape=jax.ShapeDtypeStruct((parts.shape[1], columns), parts.dtype),
        in_specs=[pl.BlockSpec(memory_space=pltpu.VMEM)],
        out_specs=pl.BlockSpec(memory_space=pltpu.VMEM),
        compiler_params=pltpu.CompilerParams(vmem_limit_bytes=room(parts, parts)),
        name="collect_columns",
    )(parts)


def unpack_kernel(widths, x_ref, *o_refs):
    count = x_ref.shape[0]
    at = 0
    for width, o_ref in zip(widths, o_refs):
        for d in range(count):
            o_ref[:, pl.ds(d * width, width)] = x_ref[d, :, pl.ds(at, width)]
        at += width
    last = x_ref.shape[2] - at
    total = x_ref[0, :, pl.ds(at, last)]
    for d in range(1, count):
        total = total + x_ref[d, :, pl.ds(at, last)]
    o_refs[-1][...] = total


def unpack_columns(blocks, widths, summed):
    count, rows, _ = blocks.shape
    results = tuple(jax.ShapeDtypeStruct((rows, count * w), blocks.dtype) for w in widths)
    results += (jax.ShapeDtypeStruct((rows, summed), blocks.dtype),)
    return pl.pallas_call(
        functools.partial(unpack_kernel, widths),
        out_shape=results,
        in_specs=[pl.BlockSpec(memory_space=pltpu.VMEM)],
        out_specs=tuple(pl.BlockSpec(memory_space=pltpu.VMEM) for _ in results),
        compiler_params=pltpu.CompilerParams(vmem_limit_bytes=room(blocks, *results)),
        name="unpack_columns",
    )(blocks)


def parts_of(rows, columns):
    if columns % 6400 == 0:
        return True, 6400, columns // 6400
    if rows % 200 == 0:
        return False, 200, rows // 200
    return False, rows, 1


def update_kernel(rates, factor_ref, *refs):
    count = len(rates)
    olds, grads = refs[: 3 * count], refs[3 * count : 4 * count]
    outputs, staged = refs[4 * count : 7 * count], refs[7 * count : 10 * count]
    load_sem, store_sem = refs[10 * count], refs[10 * count + 1]
    factor = factor_ref[0]
    plan = []
    for p in range(count):
        columnwise, size, parts = parts_of(*grads[p].shape)
        for part in range(parts):
            at = pl.ds(part * size, size)
            plan.append((p, (slice(None), at) if columnwise else (at, slice(None)), columnwise, size))

    def move(step, k, source, target, sem):
        p, where, _, _ = plan[step]
        refs_at = (source[3 * p + k].at[where], target[3 * p + k].at[where])
        return pltpu.make_async_copy(*refs_at, sem.at[3 * step + k])

    for step in range(len(plan)):
        for k in range(3):
            move(step, k, olds, staged, load_sem).start()
    for step, (p, where, columnwise, size) in enumerate(plan):
        for k in range(3):
            move(step, k, olds, staged, load_sem).wait()
        base = (where[1] if columnwise else where[0]).start
        grain = 640 if columnwise else (40 if size % 40 == 0 else size)

        def body(piece, _, p=p, columnwise=columnwise, base=base, grain=grain):
            at = pl.ds(pl.multiple_of(base + piece * grain, 128 if columnwise else 8), grain)
            spot = (slice(None), at) if columnwise else (at, slice(None))
            old = [staged[3 * p + k][spot] for k in range(3)]
            new = apply_update(old[0], grads[p][spot], old[1], old[2], factor, rates[p])
            for k in range(3):
                staged[3 * p + k][spot] = new[k]
            return 0

        if size == grain:
            whole = (slice(None), slice(None))
            old = [staged[3 * p + k][whole] for k in range(3)]
            new = apply_update(old[0], grads[p][whole], old[1], old[2], factor, rates[p])
            for k in range(3):
                staged[3 * p + k][whole] = new[k]
        else:
            lax.fori_loop(0, size // grain, body, 0)
        for k in range(3):
            move(step, k, staged, outputs, store_sem).start()
    for step in range(len(plan)):
        for k in range(3):
            move(step, k, staged, outputs, store_sem).wait()


def update_all(factor, params, rates):
    olds = [array for param in params for array in param[:3]]
    grads = [param[3] for param in params]
    results = tuple(jax.ShapeDtypeStruct(array.shape, jnp.float32) for array in olds)
    copies = 3 * sum(parts_of(*grad.shape)[2] for grad in grads)
    hbm = pl.BlockSpec(memory_space=pl.ANY)
    new = pl.pallas_call(
        functools.partial(update_kernel, rates),
        out_shape=results,
        in_specs=[pl.BlockSpec(memory_space=pltpu.SMEM)]
        + [hbm] * len(olds)
        + [pl.BlockSpec(memory_space=pltpu.VMEM)] * len(grads),
        out_specs=(hbm,) * len(olds),
        scratch_shapes=[pltpu.VMEM(array.shape, jnp.float32) for array in olds]
        + [pltpu.SemaphoreType.DMA((copies,))] * 2,
        compiler_params=pltpu.CompilerParams(vmem_limit_bytes=room(*results, *grads)),
        name="update_all",
    )(factor.reshape(1), *olds, *grads)
    return [new[3 * p : 3 * p + 3] for p in range(len(params))]


def other_core(arrays):
    return lax.ppermute(arrays, "seq", [(0, 1), (1, 0)])


def norm_forward(values, gain_row):
    inverse = lax.rsqrt(jnp.mean(values * values, axis=-1, keepdims=True) + epsilon)
    return (values * inverse * gain_row, inverse)


def norm_backward(values, inverse, gain_row, grad_out):
    scaled = grad_out * gain_row
    grad_gain = jnp.sum(grad_out * values * inverse, axis=0)
    grad_in = inverse * scaled - values * inverse**3 * jnp.mean(
        values * scaled, axis=-1, keepdims=True
    )
    return (grad_in, grad_gain)


def apply_update(weight_old, grad_full, moment_old, average_old, factor, rate):
    clipped = factor * grad_full
    moment_new = moment * moment_old + clipped
    weight_new = weight_old - rate * (clipped + moment * moment_new)
    average_new = average * average_old + (1.0 - average) * weight_new
    return (weight_new, moment_new, average_new)


def step(
    token_ids,
    lengths,
    loss_positions,
    loss_targets,
    attention_in,
    attention_in_moment,
    attention_in_average,
    attention_out,
    attention_out_moment,
    attention_out_average,
    feed_in,
    feed_in_moment,
    feed_in_average,
    feed_out,
    feed_out_moment,
    feed_out_average,
    embedding,
    embedding_moment,
    embedding_average,
    unembedding,
    unembedding_moment,
    unembedding_average,
    gains_biases,
    gains_biases_moment,
    gains_biases_average,
):
    low = jnp.bfloat16
    wide = jnp.float32
    devices_all = lax.axis_size(both)
    seq_index = lax.axis_index("seq")
    device = lax.axis_index(both)
    micros, _, half = token_ids.shape
    loss_dev = loss_positions.shape[2]
    tokens = micros * half
    rows = micros * loss_dev
    rows_all = devices_all * rows
    vocab_here = unembedding.shape[0]
    features = D // devices_all
    gate_here = FF // devices_all
    gain_rows = gains_biases[: 3 * D].reshape(3, D)
    bias_row = gains_biases[3 * D :]
    second = seq_index.astype(wide)

    positions = loss_positions[:, 0]
    targets = loss_targets[:, 0]
    ids_all = gather_labels(token_ids[:, 0], lengths, positions, targets, 1)
    base = tokens // 128
    all_tokens = ids_all[:, :base].reshape(devices_all, tokens)
    all_targets = ids_all[:, base : base + micros, :loss_dev].reshape(-1)
    all_counted = ids_all[:, base + micros : base + 2 * micros, :loss_dev]
    all_live = ids_all[:, base + 2 * micros : base + 3 * micros, 0]

    down_here = feed_out.shape[1]
    pieces = -(-down_here // features)
    down_pad = jnp.pad(feed_out[0], ((0, pieces * features - down_here), (0, 0)))
    down_pad = [down_pad[k * features : (k + 1) * features] for k in range(pieces)]
    packed = jnp.concatenate([feed_in[0]] + down_pad + [attention_out[0], attention_in[0]], axis=1)
    w_all = lax.all_gather(packed.astype(low), both, axis=0, tiled=True)
    down_at = 2 * FF
    out_at = down_at + pieces * D
    w_feed = w_all[:, :down_at]
    w_out = w_all[:, out_at : out_at + D]
    w_in = w_all[:, out_at + D :]
    w_down = [w_all[:, down_at + k * D : down_at + (k + 1) * D] for k in range(pieces)]
    head_low = unembedding.astype(low)

    arrived = exchange(lookup(all_live, all_tokens, embedding.T), 5)
    x_t = arrived.reshape(D, tokens)
    pick = [
        (positions[m][:, None] == jnp.arange(half)[None, :]).astype(low) for m in range(micros)
    ]
    x_wide, inverse_one, normed_t, keys_t, values_t, forget_t = [], [], [], [], [], []
    for m in range(micros):
        x_wide.append(x_t[:, m * half : (m + 1) * half].astype(wide))
        inverse_one.append(
            lax.rsqrt(jnp.mean(x_wide[m] * x_wide[m], axis=0, keepdims=True) + epsilon)
        )
        normed_t.append((x_wide[m] * inverse_one[m] * gain_rows[0][:, None]).astype(low))

        project_t = dot(w_in[:, D:], normed_t[m], 0, 0)
        keys_t.append(project_t[:D].astype(low).reshape(H, HD, half))
        values_t.append(project_t[D : 2 * D].astype(low).reshape(H, HD, half))
        forget_t.append((project_t[2 * D :] + bias_row[:, None]).astype(low).astype(wide))
    x_rows = jnp.concatenate([dot(pick[m], x_wide[m].astype(low), 1, 1) for m in range(micros)])
    normed_rows = jnp.concatenate(
        [dot(pick[m], normed_t[m], 1, 1) for m in range(micros)]
    ).astype(low)
    q_rows = dot(normed_rows, w_in[:, :D], 1, 0).astype(low)

    upper = (jnp.arange(half)[:, None] <= jnp.arange(half)[None, :]).astype(wide)
    log_gate = jax.nn.log_sigmoid(jnp.stack(forget_t, axis=1))
    decay_own = lax.dot_general(
        log_gate, upper, (((2,), (0,)), ((), ())), precision=highest, preferred_element_type=wide
    )
    total_own = decay_own[:, :, -1]
    decay_rows = jnp.stack(
        [dot(pick[m].astype(wide), decay_own[:, m], 1, 1, highest) for m in range(micros)]
    )
    q_own = q_rows.reshape(micros, loss_dev, H, HD)
    q_far, decay_far, total_far, place_far = other_core((q_own, decay_rows, total_own, positions))
    shift_own = second * total_far
    shift_far = (1.0 - second) * total_own
    key_decay = decay_own + shift_own[:, :, None]
    row_decay = jnp.concatenate(
        [decay_rows + shift_own.T[:, None], decay_far + shift_far.T[:, None]], axis=1
    )
    q_all = jnp.concatenate([q_own, q_far], axis=1)
    places = jnp.concatenate(
        [positions + seq_index * half, place_far + (1 - seq_index) * half], axis=1
    )
    key_places = seq_index * half + jnp.arange(half)

    scores = []
    for m in range(micros):
        raw = jnp.einsum("rhd,hdj->hrj", q_all[m], keys_t[m], preferred_element_type=wide)
        part = raw * HD ** (-0.5) + row_decay[m].T[:, :, None] - key_decay[:, m][:, None, :]
        causal = places[m][:, None] >= key_places[None, :]
        scores.append(jnp.where(causal[None], part, negative))
    scores = jnp.stack(scores)
    peak_own = jnp.max(scores, axis=-1)
    spread_own = jnp.sum(jnp.exp(scores - peak_own[..., None]), axis=-1)
    peak_far, spread_far = other_core((peak_own, spread_own))

    def swap_rows(array):
        return jnp.concatenate([array[:, :, loss_dev:], array[:, :, :loss_dev]], axis=2)

    peak_far, spread_far = swap_rows(peak_far), swap_rows(spread_far)
    peak = jnp.maximum(peak_own, peak_far)
    log_total = peak + jnp.log(
        spread_own * jnp.exp(peak_own - peak) + spread_far * jnp.exp(peak_far - peak)
    )
    probs = jnp.exp(scores - log_total[..., None])
    probs_low = probs.astype(low)
    probs_rest = (probs - probs_low.astype(wide)).astype(low)

    def mix(weights):
        return jnp.stack(
            [
                jnp.einsum(
                    "hrj,hdj->rhd",
                    weights[m],
                    values_t[m],
                    preferred_element_type=wide,
                )
                for m in range(micros)
            ]
        )

    mixed_part = mix(probs_low)
    rest_part = mix(probs_rest)
    mixed_far, rest_far = other_core((mixed_part[:, loss_dev:], rest_part[:, loss_dev:]))
    mixed_sum = mixed_part[:, :loss_dev] + mixed_far
    mixed_full = mixed_sum + rest_part[:, :loss_dev] + rest_far
    mixed_rows = mixed_sum.reshape(rows, D).astype(low)

    middle = x_rows + dot(mixed_rows, w_out, 1, 0)
    normed_two, inverse_two = norm_forward(middle, gain_rows[1])
    normed_two = normed_two.astype(low)
    gate_up = dot(normed_two, w_feed, 1, 0)
    gate_half, up_half = gate_up[:, :FF], gate_up[:, FF:]
    gate_sigmoid = jax.nn.sigmoid(gate_half)
    hidden = (gate_half * gate_sigmoid * up_half).astype(low)
    hidden_spread = spread_columns(hidden, devices_all)
    early_packed = lax.all_gather(
        jnp.concatenate([normed_two, mixed_rows, normed_rows], axis=1),
        both,
        axis=0,
        tiled=True,
    )
    final_in = middle
    for k in range(pieces):
        final_in = final_in + dot(hidden_spread[:, k * D : (k + 1) * D], w_down[k], 1, 0)
    final_normed, final_inverse = norm_forward(final_in, gain_rows[2])

    final_all = gather_rows(final_normed.astype(low), 2).reshape(rows_all, D)
    logits = dot(final_all, head_low, 1, 1)
    vocab_ids = device * vocab_here + jnp.arange(vocab_here)
    target_hits = all_targets[:, None] == vocab_ids[None, :]
    row_peak = jnp.max(logits, axis=1)
    exp_sum = jnp.sum(jnp.exp(logits - row_peak[:, None]), axis=1)
    target_part = jnp.sum(jnp.where(target_hits, logits, 0.0), axis=1)
    logit_sum = jnp.sum(logits, axis=1)
    stats = jnp.stack([row_peak, exp_sum, target_part, logit_sum])
    stats_all = gather_rows(stats.reshape(-1, 128), 3).reshape(devices_all, 4, rows_all)
    peak_all = jnp.max(stats_all[:, 0], axis=0)
    spread_all = jnp.sum(stats_all[:, 1] * jnp.exp(stats_all[:, 0] - peak_all), axis=0)
    target_all = jnp.sum(stats_all[:, 2], axis=0)
    logit_all = jnp.sum(stats_all[:, 3], axis=0)
    total_all = peak_all + jnp.log(spread_all)
    per_row = (
        total_all
        - (1.0 - smooth) * target_all
        - smooth * logit_all / V
        + z_weight * total_all * total_all
    )
    weights_row = all_counted.astype(wide).reshape(devices_all, micros, loss_dev)
    counts = jnp.sum(weights_row, axis=(0, 2))
    weights_row = (weights_row / (micros * counts)[None, :, None]).reshape(-1)
    loss_value = jnp.sum(weights_row * per_row)
    soft_rows = jnp.exp(logits - total_all[:, None])
    grad_logits = (
        weights_row[:, None]
        * (
            soft_rows * (1.0 + 2.0 * z_weight * total_all)[:, None]
            - (1.0 - smooth) * target_hits.astype(wide)
            - smooth / V
        )
    ).astype(low)
    grad_final = reduce_rows(dot(grad_logits, head_low, 1, 0), 7)

    grad_rows, gain_grad_final = norm_backward(final_in, final_inverse, gain_rows[2], grad_final)
    grad_branch = grad_rows.astype(low)
    grad_hidden = jnp.stack([dot(grad_branch, w_down[k], 1, 1) for k in range(pieces)])
    grad_hidden = collect_columns(grad_hidden, FF, devices_all)
    grad_gate = grad_hidden * up_half * gate_sigmoid * (1.0 + gate_half * (1.0 - gate_sigmoid))
    grad_up = grad_hidden * gate_half * gate_sigmoid
    grad_gate_up = jnp.concatenate([grad_gate, grad_up], axis=1).astype(low)
    grad_two, gain_grad_two = norm_backward(
        middle, inverse_two, gain_rows[1], dot(grad_gate_up, w_feed, 1, 1)
    )
    grad_middle = grad_rows + grad_two
    grad_mid_low = grad_middle.astype(low)
    grad_mixed = dot(grad_mid_low, w_out, 1, 1).astype(low)

    branch_all = lax.all_gather(grad_branch, both, axis=0, tiled=True)
    feed_here = 2 * FF // devices_all
    grad_own = grad_mixed.reshape(micros, loss_dev, H, HD)
    inner_own = jnp.sum(grad_own.astype(wide) * mixed_full, axis=-1)
    grad_far, inner_far = other_core((grad_own, inner_own))
    grad_heads = jnp.concatenate([grad_own, grad_far], axis=1)
    inner_sum = jnp.concatenate([inner_own, inner_far], axis=1)
    query_parts, score_rows = [], []
    grad_keys, grad_values, score_columns = [], [], []
    for m in range(micros):
        grad_probs = jnp.einsum(
            "rhd,hdj->hrj", grad_heads[m], values_t[m], preferred_element_type=wide
        )
        grad_scores = (probs[m] * (grad_probs - inner_sum[m].T[:, :, None])).astype(low)
        query_parts.append(
            jnp.einsum("hrj,hdj->rhd", grad_scores, keys_t[m], preferred_element_type=wide)
        )
        grad_keys.append(
            jnp.einsum("hrj,rhd->hdj", grad_scores, q_all[m], preferred_element_type=wide)
            * HD ** (-0.5)
        )
        grad_values.append(
            jnp.einsum("hrj,rhd->hdj", probs_low[m], grad_heads[m], preferred_element_type=wide)
        )
        score_wide = grad_scores.astype(wide)
        score_rows.append(jnp.sum(score_wide, axis=-1))
        score_columns.append(jnp.sum(score_wide, axis=1))
    query_parts = jnp.stack(query_parts)
    score_rows = jnp.stack(score_rows).transpose(0, 2, 1)
    query_far, score_far = other_core((query_parts[:, loss_dev:], score_rows[:, loss_dev:]))
    grad_query = ((query_parts[:, :loss_dev] + query_far) * HD ** (-0.5)).astype(low)
    grad_query = grad_query.reshape(rows, D)
    columns_packed = lax.all_to_all(
        pack_columns((grad_gate_up, hidden, grad_mid_low, grad_query), devices_all),
        both,
        split_axis=0,
        concat_axis=0,
        tiled=True,
    )
    rows_sum = score_rows[:, :loss_dev] + score_far
    later = (1.0 - second) * jnp.sum(score_rows[:, loss_dev:], axis=1)
    grad_in_sum, forget_sum, gain_grad_one, grad_bias, grad_embed = 0.0, 0.0, 0.0, 0.0, []
    projects = []
    for m in range(micros):
        placed = dot(rows_sum[m], pick[m].astype(wide), 0, 0, highest)
        change = placed - score_columns[m]
        grad_log = dot(change, upper, 1, 1, highest) + later[m][:, None]
        grad_forget = (grad_log * jax.nn.sigmoid(-forget_t[m])).astype(low)
        grad_bias = grad_bias + jnp.sum(grad_forget.astype(wide), axis=1)
        query_t = dot(grad_query[m * loss_dev : (m + 1) * loss_dev], pick[m], 0, 0).astype(low)
        keys_part = grad_keys[m].astype(low).reshape(D, half)
        values_part = grad_values[m].astype(low).reshape(D, half)
        grad_forget = lax.optimization_barrier(jnp.pad(grad_forget, ((0, -H % 128), (0, 0))))
        projects.append(jnp.concatenate([query_t, keys_part, values_part, grad_forget], axis=0))
        grad_in_sum = grad_in_sum + dot(normed_t[m], projects[m][D : 3 * D], 1, 1)
        forget_sum = forget_sum + dot(normed_t[m], grad_forget, 1, 1)
    grad_in = lax.psum_scatter(grad_in_sum, both, scatter_dimension=0, tiled=True)
    for m in range(micros):
        grad_normed = dot(w_in, projects[m][: 3 * D + H], 1, 0)
        scaled = grad_normed * gain_rows[0][:, None]
        gain_grad_one = gain_grad_one + jnp.sum(grad_normed * x_wide[m] * inverse_one[m], axis=1)
        grad_one = inverse_one[m] * scaled - x_wide[m] * inverse_one[m] ** 3 * jnp.mean(
            x_wide[m] * scaled, axis=0, keepdims=True
        )
        middle_t = dot(
            grad_middle[m * loss_dev : (m + 1) * loss_dev], pick[m].astype(wide), 0, 0, highest
        )
        grad_embed.append((middle_t + grad_one).astype(low))
    grad_embed = jnp.concatenate(grad_embed, axis=1).reshape(devices_all, features, tokens)
    moved = lax.all_to_all(grad_embed, both, split_axis=0, concat_axis=0, tiled=True)
    early_packed, branch_all, columns_packed, _ = lax.optimization_barrier(
        (early_packed, branch_all, columns_packed, grad_embed[:1, :1, :1])
    )
    late_logits, _ = lax.optimization_barrier((grad_logits, grad_embed[:1, :1, :1]))
    head_grad = lax.optimization_barrier(dot(late_logits, final_all, 0, 0))
    columns_packed = columns_packed.reshape(rows_all, -1)

    def columns_of(first, width):
        return columns_packed[:, first : first + width]

    feed_columns = dot(early_packed[:, :D], columns_of(0, feed_here), 0, 0)
    out_columns = columns_of(feed_here + gate_here, features)
    out_columns = dot(early_packed[:, D : 2 * D], out_columns, 0, 0)
    query_columns = columns_of(feed_here + gate_here + features, features)
    query_columns = dot(early_packed[:, 2 * D :], query_columns, 0, 0)
    grad_down = lax.optimization_barrier(dot(columns_of(feed_here, gate_here), branch_all, 0, 0))
    grad_feed = lax.all_to_all(
        jnp.concatenate(
            [feed_columns, out_columns, query_columns, forget_sum[:, :H]], axis=1
        ).reshape(devices_all, features, feed_here + 2 * features + H),
        both,
        split_axis=0,
        concat_axis=0,
        tiled=True,
    )
    grad_feed, grad_out, grad_q, grad_f = unpack_columns(
        grad_feed, (feed_here, features, features), H
    )
    embed_grad = scatter_add(all_live, all_tokens, moved, V)

    grad_in, _ = lax.optimization_barrier((grad_in, embed_grad[:1, :1]))
    grad_in = jnp.concatenate([grad_q, grad_in, grad_f], axis=1)
    owned_grads = [grad_in, grad_out, grad_feed, grad_down, embed_grad, head_grad]
    square_sum = jnp.zeros((), wide)
    for grad_part in owned_grads:
        square_sum = square_sum + jnp.sum(grad_part * grad_part)
    small_grad = jnp.concatenate(
        [gain_grad_one, gain_grad_two, gain_grad_final, grad_bias, square_sum[None]]
    )
    small_count = small_grad.shape[0]
    small_grad = jnp.pad(small_grad, (0, -small_count % 1024)).reshape(-1, 128)
    small_sum = jnp.sum(gather_rows(small_grad, 4), axis=0).reshape(-1)
    small_total, square_total = small_sum[: small_count - 1], small_sum[small_count - 1]
    grad_norm = jnp.sqrt(square_total + jnp.sum(small_total * small_total))
    factor = jnp.minimum(1.0, clip_limit / grad_norm)
    layer = rate_layer
    news = update_all(
        factor,
        (
            (attention_in[0], attention_in_moment[0], attention_in_average[0], grad_in),
            (attention_out[0], attention_out_moment[0], attention_out_average[0], grad_out),
            (feed_in[0], feed_in_moment[0], feed_in_average[0], grad_feed),
            (feed_out[0], feed_out_moment[0], feed_out_average[0], grad_down),
            (embedding.T, embedding_moment.T, embedding_average.T, embed_grad),
            (unembedding, unembedding_moment, unembedding_average, head_grad),
        ),
        (layer, layer, layer, layer, rate_embed, rate_head),
    )
    results = [loss_value, grad_norm]
    for new in news[:4]:
        results.extend(array[None] for array in new)
    results.extend(array.T for array in news[4])
    results.extend(news[5])
    results.extend(
        apply_update(
            gains_biases, small_total, gains_biases_moment, gains_biases_average, factor, layer
        )
    )
    return tuple(results)


def solution(mesh):
    rows = P(None, both, None)
    tables = (rows,) * 12 + (P(None, both),) * 3 + (P(both, None),) * 3 + (P(),) * 3
    return jax.shard_map(
        step,
        mesh=mesh,
        in_specs=(
            P(None, "fsdp", "seq"),
            P(None, "fsdp"),
            P(None, "fsdp", "seq"),
            P(None, "fsdp", "seq"),
        )
        + tables,
        out_specs=(P(), P()) + tables,
        check_vma=False,
    )
```

```python
import functools
import math

import jax
import jax.numpy as jnp
from jax import lax
from jax.experimental import pallas as pl
from jax.experimental.pallas import tpu as pltpu
from jax.sharding import PartitionSpec as P

D = 768
H = 12
HD = 64
FF = 2048
V = 32000


epsilon = 1e-06
smooth = 0.1
z_weight = 0.005
clip_limit = 0.5
moment = 0.9
average = 0.9
rate_layer = 200.0
rate_head = 1000.0
rate_embed = 5000.0
negative = -1e30
both = ("seq", "fsdp")
highest = lax.Precision.HIGHEST
MESH = pl.DeviceIdType.MESH


def dot(left_side, right_side, left_axis, right_axis, precision=None):
    return lax.dot_general(
        left_side,
        right_side,
        (((left_axis,), (right_axis,)), ((), ())),
        precision=precision,
        preferred_element_type=jnp.float32,
    )


def room(*arrays):
    total = 1 << 20
    for array in arrays:
        shape, size = array.shape, jnp.dtype(array.dtype).itemsize
        tile = 32 // size
        total += (
            math.prod(shape[:-2]) * (-(-shape[-2] // tile) * tile) * (-(-shape[-1] // 128) * 128)
        ) * size
    return total


def line_of(fsdp_count):
    return 4 if fsdp_count % 4 == 0 else 1


def gather_kernel(cores, fsdp, x_ref, o_ref, send_sem, recv_sem):
    plane = line_of(fsdp)
    lines = fsdp // plane
    core = lax.axis_index("seq")
    spot = lax.axis_index("fsdp")
    high, low = spot // plane, spot % plane
    line_peers = [((high + k) % lines) * plane + low for k in range(1, lines)]
    plane_peers = [high * plane + (low + k) % plane for k in range(1, plane)]
    core_peers = [(core + k) % cores for k in range(1, cores)]
    peers = [(core, p) for p in line_peers + plane_peers] + [(c, spot) for c in core_peers]

    barrier = pltpu.get_barrier_semaphore()
    for peer in peers:
        pl.semaphore_signal(barrier, inc=1, device_id=peer, device_id_type=MESH)
    pl.semaphore_wait(barrier, len(peers))

    sent = []

    def send(source_ref, block, peer):
        copy = pltpu.make_async_remote_copy(
            src_ref=source_ref,
            dst_ref=o_ref.at[block],
            send_sem=send_sem.at[len(sent)],
            recv_sem=recv_sem.at[block],
            device_id=peer,
            device_id_type=MESH,
        )
        copy.start()
        sent.append(copy)

    def arrived(block):
        pltpu.make_async_copy(o_ref.at[block], o_ref.at[block], recv_sem.at[block]).wait()

    mine = core * fsdp + spot
    for p in line_peers:
        send(x_ref, mine, (core, p))
    for p in plane_peers:
        send(x_ref, mine, (core, p))
    for c in core_peers:
        send(x_ref, mine, (c, spot))
    o_ref[mine] = x_ref[...]
    for k in range(1, lines):
        block = core * fsdp + ((high + lines - k) % lines) * plane + low
        arrived(block)
        for p in plane_peers:
            send(o_ref.at[block], block, (core, p))
        for c in core_peers:
            send(o_ref.at[block], block, (c, spot))
    for m in range(lines):
        for k in range(1, plane):
            block = core * fsdp + ((high + lines - m) % lines) * plane + (low + plane - k) % plane
            arrived(block)
            for c in core_peers:
                send(o_ref.at[block], block, (c, spot))
    for c in core_peers:
        for m in range(lines):
            for k in range(plane):
                block = c * fsdp + ((high + lines - m) % lines) * plane + (low + plane - k) % plane
                arrived(block)
    for copy in sent:
        copy.wait_send()


def label_kernel(
    cores, fsdp, tokens_ref, lengths_ref, places_ref, targets_ref, o_ref, packed, send_sem, recv_sem
):
    micros, half = tokens_ref.shape
    chunks = half // 128
    start = lax.axis_index("seq") * half
    packed[...] = jnp.zeros_like(packed)
    for m in range(micros):
        for c in range(chunks):
            packed[pl.ds(m * chunks + c, 1), :] = tokens_ref[pl.ds(m, 1), pl.ds(c * 128, 128)]
    base = micros * chunks
    length = lengths_ref[...]
    counted = (start + places_ref[...] < length).astype(jnp.int32)
    live = jnp.clip(length - start, 0, half)
    count = places_ref.shape[1]
    packed[pl.ds(base, micros), pl.ds(0, count)] = targets_ref[...]
    packed[pl.ds(base + micros, micros), pl.ds(0, count)] = counted
    packed[pl.ds(base + 2 * micros, micros), :] = jnp.broadcast_to(live, (micros, 128))
    gather_kernel(cores, fsdp, packed, o_ref, send_sem, recv_sem)


def gather_labels(tokens, lengths, places, targets, collective):
    cores, fsdp = lax.axis_size("seq"), lax.axis_size("fsdp")
    count = cores * fsdp
    micros, half = tokens.shape
    rows = micros * (half // 128) + 3 * micros
    rows = -(-rows // 8) * 8
    result = jax.ShapeDtypeStruct((count, rows, 128), jnp.int32)
    return pl.pallas_call(
        functools.partial(label_kernel, cores, fsdp),
        out_shape=result,
        in_specs=[pl.BlockSpec(memory_space=pltpu.VMEM)] * 4,
        out_specs=pl.BlockSpec(memory_space=pltpu.VMEM),
        scratch_shapes=[
            pltpu.VMEM((rows, 128), jnp.int32),
            pltpu.SemaphoreType.DMA((count,)),
            pltpu.SemaphoreType.DMA((count,)),
        ],
        compiler_params=pltpu.CompilerParams(
            collective_id=collective, has_side_effects=True, vmem_limit_bytes=room(result)
        ),
        name="gather_labels",
    )(tokens, lengths, places, targets)


def gather_rows(array, collective):
    cores, fsdp = lax.axis_size("seq"), lax.axis_size("fsdp")
    count = cores * fsdp
    result = jax.ShapeDtypeStruct((count,) + array.shape, array.dtype)
    return pl.pallas_call(
        functools.partial(gather_kernel, cores, fsdp),
        out_shape=result,
        in_specs=[pl.BlockSpec(memory_space=pltpu.VMEM)],
        out_specs=pl.BlockSpec(memory_space=pltpu.VMEM),
        scratch_shapes=[
            pltpu.SemaphoreType.DMA((count,)),
            pltpu.SemaphoreType.DMA((count,)),
        ],
        compiler_params=pltpu.CompilerParams(
            collective_id=collective,
            has_side_effects=True,
            vmem_limit_bytes=room(array, result),
        ),
        name="gather_rows",
    )(array)


def exchange_kernel(cores, fsdp, x_ref, o_ref, send_sem, recv_sem, own_sem):
    count = cores * fsdp
    mine = lax.axis_index("seq") * fsdp + lax.axis_index("fsdp")

    def place(step):
        other = lax.rem(mine + step, count)
        return other, (other // fsdp, lax.rem(other, fsdp))

    barrier = pltpu.get_barrier_semaphore()

    def greet(step, _):
        pl.semaphore_signal(barrier, inc=1, device_id=place(step)[1], device_id_type=MESH)
        return 0

    lax.fori_loop(1, count, greet, 0)
    pl.semaphore_wait(barrier, count - 1)
    own = pltpu.make_async_copy(x_ref.at[mine], o_ref.at[mine], own_sem)
    own.start()

    def copy_to(step):
        other, peer = place(step)
        return pltpu.make_async_remote_copy(
            src_ref=x_ref.at[other],
            dst_ref=o_ref.at[mine],
            send_sem=send_sem.at[step],
            recv_sem=recv_sem.at[step],
            device_id=peer,
            device_id_type=MESH,
        )

    def start(step, _):
        copy_to(step).start()
        return 0

    lax.fori_loop(1, count, start, 0)
    own.wait()

    def finish(step, _):
        source = lax.rem(mine + count - step, count)
        pltpu.make_async_copy(o_ref.at[source], o_ref.at[source], recv_sem.at[step]).wait()
        copy_to(step).wait_send()
        return 0

    lax.fori_loop(1, count, finish, 0)


def exchange(array, collective):
    cores, fsdp = lax.axis_size("seq"), lax.axis_size("fsdp")
    return pl.pallas_call(
        functools.partial(exchange_kernel, cores, fsdp),
        out_shape=jax.ShapeDtypeStruct(array.shape, array.dtype),
        in_specs=[pl.BlockSpec(memory_space=pltpu.VMEM)],
        out_specs=pl.BlockSpec(memory_space=pltpu.VMEM),
        scratch_shapes=[
            pltpu.SemaphoreType.DMA((cores * fsdp,)),
            pltpu.SemaphoreType.DMA((cores * fsdp,)),
            pltpu.SemaphoreType.DMA,
        ],
        compiler_params=pltpu.CompilerParams(
            collective_id=collective,
            has_side_effects=True,
            vmem_limit_bytes=room(array, array),
        ),
        name="exchange",
    )(array)


def reduce_kernel(
    fsdp, x_ref, o_ref, from_core, from_plane, from_line, core_sum, plane_sum, send_sem, recv_sem
):
    plane = line_of(fsdp)
    lines = fsdp // plane
    core = lax.axis_index("seq")
    spot = lax.axis_index("fsdp")
    high, low = spot // plane, lax.rem(spot, plane)
    far = 1 - core
    peers = [(far, spot)]
    peers += [(core, lax.rem(high + k, lines) * plane + low) for k in range(1, lines)]
    peers += [(core, high * plane + lax.rem(low + k, plane)) for k in range(1, plane)]
    barrier = pltpu.get_barrier_semaphore()
    for peer in peers:
        pl.semaphore_signal(barrier, inc=1, device_id=peer, device_id_type=MESH)
    pl.semaphore_wait(barrier, len(peers))
    sent = []

    def send(source_ref, target_ref, slot, peer):
        copy = pltpu.make_async_remote_copy(
            src_ref=source_ref,
            dst_ref=target_ref,
            send_sem=send_sem.at[slot],
            recv_sem=recv_sem.at[slot],
            device_id=peer,
            device_id_type=MESH,
        )
        copy.start()
        sent.append(copy)
        return copy

    first = []
    for k in list(range(1, plane)) + [0]:
        spot_low = lax.rem(low + k, plane)
        first.append(
            (k, spot_low, send(x_ref.at[far, :, spot_low], from_core.at[spot_low], k, (far, spot)))
        )
    second = []
    for k, spot_low, copy in first:
        copy.wait_recv()
        core_sum[spot_low] = x_ref[core, :, spot_low] + from_core[spot_low]
        if k:
            target = from_plane.at[k - 1]
            peer = (core, high * plane + spot_low)
            second.append((k, send(core_sum.at[spot_low], target, plane + k - 1, peer)))
    plane_sum[...] = core_sum[low]
    for k, copy in second:
        copy.wait_recv()
        plane_sum[...] += from_plane[k - 1]
    third = []
    for k in range(1, lines):
        line = lax.rem(high + k, lines)
        slot = 2 * plane + k - 2
        peer = (core, line * plane + low)
        third.append((k, send(plane_sum.at[line], from_line.at[k - 1], slot, peer)))
    total = plane_sum[high]
    for k, copy in third:
        copy.wait_recv()
        total = total + from_line[k - 1]
    o_ref[...] = total
    for copy in sent:
        copy.wait_send()


def reduce_rows(array, collective):
    cores, fsdp = lax.axis_size("seq"), lax.axis_size("fsdp")
    plane = line_of(fsdp)
    lines = fsdp // plane
    rows, columns = array.shape[0] // (cores * fsdp), array.shape[1]
    kind = array.dtype
    slots = 2 * plane + lines - 2
    return pl.pallas_call(
        functools.partial(reduce_kernel, fsdp),
        out_shape=jax.ShapeDtypeStruct((rows, columns), kind),
        in_specs=[pl.BlockSpec(memory_space=pltpu.VMEM)],
        out_specs=pl.BlockSpec(memory_space=pltpu.VMEM),
        scratch_shapes=[
            pltpu.VMEM((plane, lines, rows, columns), kind),
            pltpu.VMEM((plane - 1, lines, rows, columns), kind),
            pltpu.VMEM((lines - 1, rows, columns), kind),
            pltpu.VMEM((plane, lines, rows, columns), kind),
            pltpu.VMEM((lines, rows, columns), kind),
            pltpu.SemaphoreType.DMA((slots,)),
            pltpu.SemaphoreType.DMA((slots,)),
        ],
        compiler_params=pltpu.CompilerParams(
            collective_id=collective,
            has_side_effects=True,
            vmem_limit_bytes=room(array, array, array),
        ),
        name="reduce_rows",
    )(array.reshape(cores, lines, plane, rows, columns))


def lookup_kernel(unroll, builds, live_ref, ids_ref, own_ref, o_ref, table, stage):
    sources, features, tokens = o_ref.shape
    micros = live_ref.shape[0] // sources
    half = tokens // micros

    def build(step, _):
        for u in range(builds):
            at = pl.multiple_of((step * builds + u) * 128, 128)
            block = own_ref[:, pl.ds(at, 128)].astype(jnp.bfloat16).astype(jnp.float32)
            table[pl.ds(at, 128), pl.ds(0, features)] = block.T
        return 0

    lax.fori_loop(0, table.shape[0] // 128 // builds, build, 0)
    stage[...] = jnp.zeros_like(stage)

    def source(which, _):
        def fetch(first, step, _):
            at = first + step * unroll
            ids = [ids_ref[which * tokens + at + u] for u in range(unroll)]
            for u in range(unroll):
                stage[pl.ds(at + u, 1), :] = table[pl.ds(ids[u], 1), :]
            return 0

        for m in range(micros):
            live = live_ref[which * micros + m]
            lax.fori_loop(
                0, (live + unroll - 1) // unroll, functools.partial(fetch, m * half), 0
            )
        for c in range(tokens // 128):
            block = stage[pl.ds(c * 128, 128), :].T
            o_ref[which, :, pl.ds(c * 128, 128)] = block[:features].astype(jnp.bfloat16)
        return 0

    lax.fori_loop(0, sources, source, 0)


def lookup(live, ids, table_t):
    sources, tokens = ids.shape
    features, vocab = table_t.shape
    return pl.pallas_call(
        functools.partial(lookup_kernel, 64, 10),
        out_shape=jax.ShapeDtypeStruct((sources, features, tokens), jnp.bfloat16),
        in_specs=[
            pl.BlockSpec(memory_space=pltpu.SMEM),
            pl.BlockSpec(memory_space=pltpu.SMEM),
            pl.BlockSpec(memory_space=pltpu.VMEM),
        ],
        out_specs=pl.BlockSpec(memory_space=pltpu.VMEM),
        scratch_shapes=[
            pltpu.VMEM((vocab, 128), jnp.float32),
            pltpu.VMEM((tokens, 128), jnp.float32),
        ],
        compiler_params=pltpu.CompilerParams(vmem_limit_bytes=32 * 1024 * 1024),
        name="lookup",
    )(live.reshape(-1), ids.reshape(-1), table_t)


row_bits = 13
row_count = 1 << row_bits


def scatter_kernel(unroll, live_ref, rows_ref, ids_ref, g_ref, o_ref, spread, *sums):
    sources, features, tokens = g_ref.shape
    micros = live_ref.shape[0] // sources
    half = tokens // micros
    vocab = o_ref.shape[1]
    groups = 4

    def clear(step, _):
        for one in sums:
            one[pl.ds(pl.multiple_of(step * 256, 256), 256)] = jnp.zeros((256, 128), jnp.float32)
        return 0

    lax.fori_loop(0, row_count // 256, clear, 0)
    blank = jnp.zeros((128 // groups - features, 128), jnp.float32)
    group = lax.broadcasted_iota(jnp.int32, (128, 128), 0) // (128 // groups)

    def source(which, _):
        for c in range(tokens // 128):
            block = g_ref[which, :, pl.ds(c * 128, 128)].astype(jnp.float32)
            block = jnp.concatenate([block, blank] * groups, axis=0)
            chosen = ids_ref[which, :, pl.ds(c * 128, 128)] >> row_bits
            spread[pl.ds(c * 128, 128), :] = jnp.where(group == chosen, block, 0.0).T

        def add(first, step, _):
            at = first + step * unroll
            rows = [rows_ref[which * tokens + at + u] for u in range(unroll)]
            for u in range(unroll):
                one = sums[u % len(sums)]
                one[pl.ds(rows[u], 1), :] += spread[pl.ds(at + u, 1), :]
            return 0

        for m in range(micros):
            live = live_ref[which * micros + m]
            lax.fori_loop(0, (live + unroll - 1) // unroll, functools.partial(add, m * half), 0)
        return 0

    lax.fori_loop(0, sources, source, 0)

    def finish(step, _):
        for u in range(2):
            at = pl.multiple_of((step * 2 + u) * 128, 128)
            total = sums[0][pl.ds(at, 128)]
            for one in sums[1:]:
                total = total + one[pl.ds(at, 128)]
            total = total.T
            for k in range(groups):
                part = total[k * (128 // groups) : k * (128 // groups) + features]
                if (k + 1) * row_count <= vocab:
                    o_ref[:, pl.ds(k * row_count + at, 128)] = part
                elif k * row_count < vocab:

                    @pl.when(k * row_count + at + 128 <= vocab)
                    def _():
                        o_ref[:, pl.ds(k * row_count + at, 128)] = part

        return 0

    lax.fori_loop(0, row_count // 256, finish, 0)


def scatter_add(live, ids, grads, vocab):
    sources, features, tokens = grads.shape
    return pl.pallas_call(
        functools.partial(scatter_kernel, 32),
        out_shape=jax.ShapeDtypeStruct((features, vocab), jnp.float32),
        in_specs=[
            pl.BlockSpec(memory_space=pltpu.SMEM),
            pl.BlockSpec(memory_space=pltpu.SMEM),
            pl.BlockSpec(memory_space=pltpu.VMEM),
            pl.BlockSpec(memory_space=pltpu.VMEM),
        ],
        out_specs=pl.BlockSpec(memory_space=pltpu.VMEM),
        scratch_shapes=[pltpu.VMEM((tokens, 128), jnp.float32)]
        + [pltpu.VMEM((row_count, 128), jnp.float32)] * 8,
        compiler_params=pltpu.CompilerParams(vmem_limit_bytes=44 * 1024 * 1024),
        cost_estimate=pl.CostEstimate(
            flops=40 * 10**9, bytes_accessed=8 * 10**6, transcendentals=0
        ),
        name="scatter_add",
    )(
        live.reshape(-1),
        (ids & (row_count - 1)).reshape(-1),
        ids.reshape(sources, 1, tokens),
        grads,
    )


def spread_kernel(count, hidden_ref, spread_ref):
    per = hidden_ref.shape[1] // count
    features = spread_ref.shape[1] // (-(-per // (D // count)) * count)
    spread_ref[...] = jnp.zeros_like(spread_ref)
    for d in range(count):
        block = hidden_ref[:, pl.ds(d * per, per)]
        for k in range(-(-per // features)):
            width = min(features, per - k * features)
            at = (k * count + d) * features
            spread_ref[:, pl.ds(at, width)] = block[:, k * features : k * features + width]


def spread_columns(hidden, count):
    rows = hidden.shape[0]
    pieces = -(-(hidden.shape[1] // count) // (D // count))
    result = jax.ShapeDtypeStruct((rows, pieces * D), hidden.dtype)
    return pl.pallas_call(
        functools.partial(spread_kernel, count),
        out_shape=result,
        in_specs=[pl.BlockSpec(memory_space=pltpu.VMEM)],
        out_specs=pl.BlockSpec(memory_space=pltpu.VMEM),
        compiler_params=pltpu.CompilerParams(vmem_limit_bytes=room(hidden, result)),
        name="spread_columns",
    )(hidden)


def pack_kernel(*refs):
    packed_ref = refs[-1]
    count = packed_ref.shape[0]
    packed_ref[...] = jnp.zeros_like(packed_ref)
    at = 0
    for x_ref in refs[:-1]:
        width = x_ref.shape[1] // count
        for d in range(count):
            packed_ref[d, :, pl.ds(at, width)] = x_ref[:, pl.ds(d * width, width)]
        at += width


def pack_columns(arrays, count):
    width = -(-sum(array.shape[1] for array in arrays) // (128 * count)) * 128
    result = jax.ShapeDtypeStruct((count, arrays[0].shape[0], width), arrays[0].dtype)
    return pl.pallas_call(
        pack_kernel,
        out_shape=result,
        in_specs=[pl.BlockSpec(memory_space=pltpu.VMEM)] * len(arrays),
        out_specs=pl.BlockSpec(memory_space=pltpu.VMEM),
        compiler_params=pltpu.CompilerParams(vmem_limit_bytes=room(*arrays, result)),
        name="pack_columns",
    )(*arrays)


def collect_kernel(count, spread_ref, o_ref):
    per = o_ref.shape[1] // count
    features = spread_ref.shape[2] // count
    for d in range(count):
        for k in range(spread_ref.shape[0]):
            width = min(features, per - k * features)
            part = spread_ref[k, :, pl.ds(d * features, width)]
            o_ref[:, pl.ds(d * per + k * features, width)] = part


def collect_columns(parts, columns, count):
    return pl.pallas_call(
        functools.partial(collect_kernel, count),
        out_shape=jax.ShapeDtypeStruct((parts.shape[1], columns), parts.dtype),
        in_specs=[pl.BlockSpec(memory_space=pltpu.VMEM)],
        out_specs=pl.BlockSpec(memory_space=pltpu.VMEM),
        compiler_params=pltpu.CompilerParams(vmem_limit_bytes=room(parts, parts)),
        name="collect_columns",
    )(parts)


def unpack_kernel(widths, x_ref, *o_refs):
    count = x_ref.shape[0]
    at = 0
    for width, o_ref in zip(widths, o_refs):
        for d in range(count):
            o_ref[:, pl.ds(d * width, width)] = x_ref[d, :, pl.ds(at, width)]
        at += width
    last = x_ref.shape[2] - at
    total = x_ref[0, :, pl.ds(at, last)]
    for d in range(1, count):
        total = total + x_ref[d, :, pl.ds(at, last)]
    o_refs[-1][...] = total


def unpack_columns(blocks, widths, summed):
    count, rows, _ = blocks.shape
    results = tuple(jax.ShapeDtypeStruct((rows, count * w), blocks.dtype) for w in widths)
    results += (jax.ShapeDtypeStruct((rows, summed), blocks.dtype),)
    return pl.pallas_call(
        functools.partial(unpack_kernel, widths),
        out_shape=results,
        in_specs=[pl.BlockSpec(memory_space=pltpu.VMEM)],
        out_specs=tuple(pl.BlockSpec(memory_space=pltpu.VMEM) for _ in results),
        compiler_params=pltpu.CompilerParams(vmem_limit_bytes=room(blocks, *results)),
        name="unpack_columns",
    )(blocks)


def parts_of(rows, columns):
    if columns % 6400 == 0:
        return True, 6400, columns // 6400
    if rows % 200 == 0:
        return False, 200, rows // 200
    return False, rows, 1


def update_kernel(rates, factor_ref, *refs):
    count = len(rates)
    olds, grads = refs[: 3 * count], refs[3 * count : 4 * count]
    outputs, staged = refs[4 * count : 7 * count], refs[7 * count : 10 * count]
    load_sem, store_sem = refs[10 * count], refs[10 * count + 1]
    factor = factor_ref[0]
    plan = []
    for p in range(count):
        columnwise, size, parts = parts_of(*grads[p].shape)
        for part in range(parts):
            at = pl.ds(part * size, size)
            plan.append((p, (slice(None), at) if columnwise else (at, slice(None)), columnwise, size))

    def move(step, k, source, target, sem):
        p, where, _, _ = plan[step]
        refs_at = (source[3 * p + k].at[where], target[3 * p + k].at[where])
        return pltpu.make_async_copy(*refs_at, sem.at[3 * step + k])

    for step in range(len(plan)):
        for k in range(3):
            move(step, k, olds, staged, load_sem).start()
    for step, (p, where, columnwise, size) in enumerate(plan):
        for k in range(3):
            move(step, k, olds, staged, load_sem).wait()
        base = (where[1] if columnwise else where[0]).start
        grain = 640 if columnwise else (40 if size % 40 == 0 else size)

        def body(piece, _, p=p, columnwise=columnwise, base=base, grain=grain):
            at = pl.ds(pl.multiple_of(base + piece * grain, 128 if columnwise else 8), grain)
            spot = (slice(None), at) if columnwise else (at, slice(None))
            old = [staged[3 * p + k][spot] for k in range(3)]
            new = apply_update(old[0], grads[p][spot], old[1], old[2], factor, rates[p])
            for k in range(3):
                staged[3 * p + k][spot] = new[k]
            return 0

        if size == grain:
            whole = (slice(None), slice(None))
            old = [staged[3 * p + k][whole] for k in range(3)]
            new = apply_update(old[0], grads[p][whole], old[1], old[2], factor, rates[p])
            for k in range(3):
                staged[3 * p + k][whole] = new[k]
        else:
            lax.fori_loop(0, size // grain, body, 0)
        for k in range(3):
            move(step, k, staged, outputs, store_sem).start()
    for step in range(len(plan)):
        for k in range(3):
            move(step, k, staged, outputs, store_sem).wait()


def update_all(factor, params, rates):
    olds = [array for param in params for array in param[:3]]
    grads = [param[3] for param in params]
    results = tuple(jax.ShapeDtypeStruct(array.shape, jnp.float32) for array in olds)
    copies = 3 * sum(parts_of(*grad.shape)[2] for grad in grads)
    hbm = pl.BlockSpec(memory_space=pltpu.HBM)
    new = pl.pallas_call(
        functools.partial(update_kernel, rates),
        out_shape=results,
        in_specs=[pl.BlockSpec(memory_space=pltpu.SMEM)]
        + [hbm] * len(olds)
        + [pl.BlockSpec(memory_space=pltpu.VMEM)] * len(grads),
        out_specs=(hbm,) * len(olds),
        scratch_shapes=[pltpu.VMEM(array.shape, jnp.float32) for array in olds]
        + [pltpu.SemaphoreType.DMA((copies,))] * 2,
        compiler_params=pltpu.CompilerParams(vmem_limit_bytes=62 * 1024 * 1024),
        name="update_all",
    )(factor.reshape(1), *olds, *grads)
    return [new[3 * p : 3 * p + 3] for p in range(len(params))]


def other_core(arrays):
    return lax.ppermute(arrays, "seq", [(0, 1), (1, 0)])


def norm_forward(values, gain_row):
    inverse = lax.rsqrt(jnp.mean(values * values, axis=-1, keepdims=True) + epsilon)
    return (values * inverse * gain_row, inverse)


def norm_backward(values, inverse, gain_row, grad_out):
    scaled = grad_out * gain_row
    grad_gain = jnp.sum(grad_out * values * inverse, axis=0)
    grad_in = inverse * scaled - values * inverse**3 * jnp.mean(
        values * scaled, axis=-1, keepdims=True
    )
    return (grad_in, grad_gain)


def apply_update(weight_old, grad_full, moment_old, average_old, factor, rate):
    clipped = factor * grad_full
    moment_new = moment * moment_old + clipped
    weight_new = weight_old - rate * (clipped + moment * moment_new)
    average_new = average * average_old + (1.0 - average) * weight_new
    return (weight_new, moment_new, average_new)


def step(
    token_ids,
    lengths,
    loss_positions,
    loss_targets,
    attention_in,
    attention_in_moment,
    attention_in_average,
    attention_out,
    attention_out_moment,
    attention_out_average,
    feed_in,
    feed_in_moment,
    feed_in_average,
    feed_out,
    feed_out_moment,
    feed_out_average,
    embedding,
    embedding_moment,
    embedding_average,
    unembedding,
    unembedding_moment,
    unembedding_average,
    gains_biases,
    gains_biases_moment,
    gains_biases_average,
):
    low = jnp.bfloat16
    wide = jnp.float32
    devices_all = lax.axis_size(both)
    seq_index = lax.axis_index("seq")
    device = lax.axis_index(both)
    micros, _, half = token_ids.shape
    loss_dev = loss_positions.shape[2]
    tokens = micros * half
    rows = micros * loss_dev
    rows_all = devices_all * rows
    vocab_here = unembedding.shape[0]
    features = D // devices_all
    gate_here = FF // devices_all
    gain_rows = gains_biases[: 3 * D].reshape(3, D)
    bias_row = gains_biases[3 * D :]
    second = seq_index.astype(wide)

    positions = loss_positions[:, 0]
    targets = loss_targets[:, 0]
    ids_all = gather_labels(token_ids[:, 0], lengths, positions, targets, 1)
    base = tokens // 128
    all_tokens = ids_all[:, :base].reshape(devices_all, tokens)
    all_targets = ids_all[:, base : base + micros, :loss_dev].reshape(-1)
    all_counted = ids_all[:, base + micros : base + 2 * micros, :loss_dev]
    all_live = ids_all[:, base + 2 * micros : base + 3 * micros, 0]

    down_here = feed_out.shape[1]
    pieces = -(-down_here // features)
    down_pad = jnp.pad(feed_out[0], ((0, pieces * features - down_here), (0, 0)))
    down_pad = [down_pad[k * features : (k + 1) * features] for k in range(pieces)]
    packed = jnp.concatenate([feed_in[0]] + down_pad + [attention_out[0], attention_in[0]], axis=1)
    w_all = lax.all_gather(packed.astype(low), both, axis=0, tiled=True)
    down_at = 2 * FF
    out_at = down_at + pieces * D
    w_feed = w_all[:, :down_at]
    w_out = w_all[:, out_at : out_at + D]
    w_in = w_all[:, out_at + D :]
    w_down = [w_all[:, down_at + k * D : down_at + (k + 1) * D] for k in range(pieces)]
    head_low = unembedding.astype(low)

    arrived = exchange(lookup(all_live, all_tokens, embedding.T), 5)
    x_t = arrived.reshape(D, tokens)
    pick = [
        (positions[m][:, None] == jnp.arange(half)[None, :]).astype(low) for m in range(micros)
    ]
    x_wide, inverse_one, normed_t, keys_t, values_t, forget_t = [], [], [], [], [], []
    for m in range(micros):
        x_wide.append(x_t[:, m * half : (m + 1) * half].astype(wide))
        inverse_one.append(
            lax.rsqrt(jnp.mean(x_wide[m] * x_wide[m], axis=0, keepdims=True) + epsilon)
        )
        normed_t.append((x_wide[m] * inverse_one[m] * gain_rows[0][:, None]).astype(low))

        project_t = dot(w_in[:, D:], normed_t[m], 0, 0)
        keys_t.append(project_t[:D].astype(low).reshape(H, HD, half))
        values_t.append(project_t[D : 2 * D].astype(low).reshape(H, HD, half))
        forget_t.append((project_t[2 * D :] + bias_row[:, None]).astype(low).astype(wide))
    x_rows = jnp.concatenate([dot(pick[m], x_wide[m].astype(low), 1, 1) for m in range(micros)])
    normed_rows = jnp.concatenate(
        [dot(pick[m], normed_t[m], 1, 1) for m in range(micros)]
    ).astype(low)
    q_rows = dot(normed_rows, w_in[:, :D], 1, 0).astype(low)

    upper = (jnp.arange(half)[:, None] <= jnp.arange(half)[None, :]).astype(wide)
    log_gate = jax.nn.log_sigmoid(jnp.stack(forget_t, axis=1))
    decay_own = lax.dot_general(
        log_gate, upper, (((2,), (0,)), ((), ())), precision=highest, preferred_element_type=wide
    )
    total_own = decay_own[:, :, -1]
    decay_rows = jnp.stack(
        [dot(pick[m].astype(wide), decay_own[:, m], 1, 1, highest) for m in range(micros)]
    )
    q_own = q_rows.reshape(micros, loss_dev, H, HD)
    q_far, decay_far, total_far, place_far = other_core((q_own, decay_rows, total_own, positions))
    shift_own = second * total_far
    shift_far = (1.0 - second) * total_own
    key_decay = decay_own + shift_own[:, :, None]
    row_decay = jnp.concatenate(
        [decay_rows + shift_own.T[:, None], decay_far + shift_far.T[:, None]], axis=1
    )
    q_all = jnp.concatenate([q_own, q_far], axis=1)
    places = jnp.concatenate(
        [positions + seq_index * half, place_far + (1 - seq_index) * half], axis=1
    )
    key_places = seq_index * half + jnp.arange(half)

    scores = []
    for m in range(micros):
        raw = jnp.einsum("rhd,hdj->hrj", q_all[m], keys_t[m], preferred_element_type=wide)
        part = raw * HD ** (-0.5) + row_decay[m].T[:, :, None] - key_decay[:, m][:, None, :]
        causal = places[m][:, None] >= key_places[None, :]
        scores.append(jnp.where(causal[None], part, negative))
    scores = jnp.stack(scores)
    peak_own = jnp.max(scores, axis=-1)
    spread_own = jnp.sum(jnp.exp(scores - peak_own[..., None]), axis=-1)
    peak_far, spread_far = other_core((peak_own, spread_own))

    def swap_rows(array):
        return jnp.concatenate([array[:, :, loss_dev:], array[:, :, :loss_dev]], axis=2)

    peak_far, spread_far = swap_rows(peak_far), swap_rows(spread_far)
    peak = jnp.maximum(peak_own, peak_far)
    log_total = peak + jnp.log(
        spread_own * jnp.exp(peak_own - peak) + spread_far * jnp.exp(peak_far - peak)
    )
    probs = jnp.exp(scores - log_total[..., None])
    probs_low = probs.astype(low)
    probs_rest = (probs - probs_low.astype(wide)).astype(low)

    def mix(weights):
        return jnp.stack(
            [
                jnp.einsum(
                    "hrj,hdj->rhd",
                    weights[m],
                    values_t[m],
                    preferred_element_type=wide,
                )
                for m in range(micros)
            ]
        )

    mixed_part = mix(probs_low)
    rest_part = mix(probs_rest)
    mixed_far, rest_far = other_core((mixed_part[:, loss_dev:], rest_part[:, loss_dev:]))
    mixed_sum = mixed_part[:, :loss_dev] + mixed_far
    mixed_full = mixed_sum + rest_part[:, :loss_dev] + rest_far
    mixed_rows = mixed_sum.reshape(rows, D).astype(low)

    middle = x_rows + dot(mixed_rows, w_out, 1, 0)
    normed_two, inverse_two = norm_forward(middle, gain_rows[1])
    normed_two = normed_two.astype(low)
    gate_up = dot(normed_two, w_feed, 1, 0)
    gate_half, up_half = gate_up[:, :FF], gate_up[:, FF:]
    gate_sigmoid = jax.nn.sigmoid(gate_half)
    hidden = (gate_half * gate_sigmoid * up_half).astype(low)
    hidden_spread = spread_columns(hidden, devices_all)
    early_packed = lax.all_gather(
        jnp.concatenate([normed_two, mixed_rows, normed_rows], axis=1),
        both,
        axis=0,
        tiled=True,
    )
    final_in = middle
    for k in range(pieces):
        final_in = final_in + dot(hidden_spread[:, k * D : (k + 1) * D], w_down[k], 1, 0)
    final_normed, final_inverse = norm_forward(final_in, gain_rows[2])

    final_all = gather_rows(final_normed.astype(low), 2).reshape(rows_all, D)
    logits = dot(final_all, head_low, 1, 1)
    vocab_ids = device * vocab_here + jnp.arange(vocab_here)
    target_hits = all_targets[:, None] == vocab_ids[None, :]
    row_peak = jnp.max(logits, axis=1)
    exp_sum = jnp.sum(jnp.exp(logits - row_peak[:, None]), axis=1)
    target_part = jnp.sum(jnp.where(target_hits, logits, 0.0), axis=1)
    logit_sum = jnp.sum(logits, axis=1)
    stats = jnp.stack([row_peak, exp_sum, target_part, logit_sum])
    stats_all = gather_rows(stats.reshape(-1, 128), 3).reshape(devices_all, 4, rows_all)
    peak_all = jnp.max(stats_all[:, 0], axis=0)
    spread_all = jnp.sum(stats_all[:, 1] * jnp.exp(stats_all[:, 0] - peak_all), axis=0)
    target_all = jnp.sum(stats_all[:, 2], axis=0)
    logit_all = jnp.sum(stats_all[:, 3], axis=0)
    total_all = peak_all + jnp.log(spread_all)
    per_row = (
        total_all
        - (1.0 - smooth) * target_all
        - smooth * logit_all / V
        + z_weight * total_all * total_all
    )
    weights_row = all_counted.astype(wide).reshape(devices_all, micros, loss_dev)
    counts = jnp.sum(weights_row, axis=(0, 2))
    weights_row = (weights_row / (micros * counts)[None, :, None]).reshape(-1)
    loss_value = jnp.sum(weights_row * per_row)
    soft_rows = jnp.exp(logits - total_all[:, None])
    grad_logits = (
        weights_row[:, None]
        * (
            soft_rows * (1.0 + 2.0 * z_weight * total_all)[:, None]
            - (1.0 - smooth) * target_hits.astype(wide)
            - smooth / V
        )
    ).astype(low)
    grad_final = reduce_rows(dot(grad_logits, head_low, 1, 0), 7)

    grad_rows, gain_grad_final = norm_backward(final_in, final_inverse, gain_rows[2], grad_final)
    grad_branch = grad_rows.astype(low)
    grad_hidden = jnp.stack([dot(grad_branch, w_down[k], 1, 1) for k in range(pieces)])
    grad_hidden = collect_columns(grad_hidden, FF, devices_all)
    grad_gate = grad_hidden * up_half * gate_sigmoid * (1.0 + gate_half * (1.0 - gate_sigmoid))
    grad_up = grad_hidden * gate_half * gate_sigmoid
    grad_gate_up = jnp.concatenate([grad_gate, grad_up], axis=1).astype(low)
    grad_two, gain_grad_two = norm_backward(
        middle, inverse_two, gain_rows[1], dot(grad_gate_up, w_feed, 1, 1)
    )
    grad_middle = grad_rows + grad_two
    grad_mid_low = grad_middle.astype(low)
    grad_mixed = dot(grad_mid_low, w_out, 1, 1).astype(low)

    feed_here = 2 * FF // devices_all
    grad_own = grad_mixed.reshape(micros, loss_dev, H, HD)
    inner_own = jnp.sum(grad_own.astype(wide) * mixed_full, axis=-1)
    grad_far, inner_far = other_core((grad_own, inner_own))
    grad_heads = jnp.concatenate([grad_own, grad_far], axis=1)
    inner_sum = jnp.concatenate([inner_own, inner_far], axis=1)
    query_parts, score_rows = [], []
    grad_keys, grad_values, score_columns = [], [], []
    for m in range(micros):
        grad_probs = jnp.einsum(
            "rhd,hdj->hrj", grad_heads[m], values_t[m], preferred_element_type=wide
        )
        grad_scores = (probs[m] * (grad_probs - inner_sum[m].T[:, :, None])).astype(low)
        query_parts.append(
            jnp.einsum("hrj,hdj->rhd", grad_scores, keys_t[m], preferred_element_type=wide)
        )
        grad_keys.append(
            jnp.einsum("hrj,rhd->hdj", grad_scores, q_all[m], preferred_element_type=wide)
            * HD ** (-0.5)
        )
        grad_values.append(
            jnp.einsum("hrj,rhd->hdj", probs_low[m], grad_heads[m], preferred_element_type=wide)
        )
        score_wide = grad_scores.astype(wide)
        score_rows.append(jnp.sum(score_wide, axis=-1))
        score_columns.append(jnp.sum(score_wide, axis=1))
    query_parts = jnp.stack(query_parts)
    score_rows = jnp.stack(score_rows).transpose(0, 2, 1)
    query_far, score_far = other_core((query_parts[:, loss_dev:], score_rows[:, loss_dev:]))
    grad_query = ((query_parts[:, :loss_dev] + query_far) * HD ** (-0.5)).astype(low)
    grad_query = grad_query.reshape(rows, D)
    columns_packed = lax.all_to_all(
        pack_columns((grad_gate_up, hidden, grad_mid_low, grad_query), devices_all),
        both,
        split_axis=0,
        concat_axis=0,
        tiled=True,
    )
    rows_sum = score_rows[:, :loss_dev] + score_far
    later = (1.0 - second) * jnp.sum(score_rows[:, loss_dev:], axis=1)
    grad_in_sum, forget_sum, gain_grad_one, grad_bias, grad_embed = 0.0, 0.0, 0.0, 0.0, []
    projects = []
    for m in range(micros):
        placed = dot(rows_sum[m], pick[m].astype(wide), 0, 0, highest)
        change = placed - score_columns[m]
        grad_log = dot(change, upper, 1, 1, highest) + later[m][:, None]
        grad_forget = (grad_log * jax.nn.sigmoid(-forget_t[m])).astype(low)
        grad_bias = grad_bias + jnp.sum(grad_forget.astype(wide), axis=1)
        query_t = dot(grad_query[m * loss_dev : (m + 1) * loss_dev], pick[m], 0, 0).astype(low)
        keys_part = grad_keys[m].astype(low).reshape(D, half)
        values_part = grad_values[m].astype(low).reshape(D, half)
        grad_forget = lax.optimization_barrier(jnp.pad(grad_forget, ((0, -H % 128), (0, 0))))
        projects.append(jnp.concatenate([query_t, keys_part, values_part, grad_forget], axis=0))
        grad_in_sum = grad_in_sum + dot(normed_t[m], projects[m][D : 3 * D], 1, 1)
        forget_sum = forget_sum + dot(normed_t[m], grad_forget, 1, 1)
    grad_in = lax.psum_scatter(grad_in_sum, both, scatter_dimension=0, tiled=True)
    for m in range(micros):
        grad_normed = dot(w_in, projects[m][: 3 * D + H], 1, 0)
        scaled = grad_normed * gain_rows[0][:, None]
        gain_grad_one = gain_grad_one + jnp.sum(grad_normed * x_wide[m] * inverse_one[m], axis=1)
        grad_one = inverse_one[m] * scaled - x_wide[m] * inverse_one[m] ** 3 * jnp.mean(
            x_wide[m] * scaled, axis=0, keepdims=True
        )
        middle_t = dot(
            grad_middle[m * loss_dev : (m + 1) * loss_dev], pick[m].astype(wide), 0, 0, highest
        )
        grad_embed.append((middle_t + grad_one).astype(low))
    grad_embed = jnp.concatenate(grad_embed, axis=1).reshape(devices_all, features, tokens)
    moved = lax.all_to_all(grad_embed, both, split_axis=0, concat_axis=0, tiled=True)
    early_packed, late_branch, columns_packed, _ = lax.optimization_barrier(
        (early_packed, grad_branch, columns_packed, grad_embed[:1, :1, :1])
    )
    branch_all = gather_rows(late_branch, 8).reshape(rows_all, D)
    late_logits, _ = lax.optimization_barrier((grad_logits, grad_embed[:1, :1, :1]))
    head_grad = lax.optimization_barrier(dot(late_logits, final_all, 0, 0))
    columns_packed = columns_packed.reshape(rows_all, -1)

    def columns_of(first, width):
        return columns_packed[:, first : first + width]

    feed_columns = dot(early_packed[:, :D], columns_of(0, feed_here), 0, 0)
    out_columns = columns_of(feed_here + gate_here, features)
    out_columns = dot(early_packed[:, D : 2 * D], out_columns, 0, 0)
    query_columns = columns_of(feed_here + gate_here + features, features)
    query_columns = dot(early_packed[:, 2 * D :], query_columns, 0, 0)
    grad_down = lax.optimization_barrier(dot(columns_of(feed_here, gate_here), branch_all, 0, 0))
    grad_feed = lax.all_to_all(
        jnp.concatenate(
            [feed_columns, out_columns, query_columns, forget_sum[:, :H]], axis=1
        ).reshape(devices_all, features, feed_here + 2 * features + H),
        both,
        split_axis=0,
        concat_axis=0,
        tiled=True,
    )
    grad_feed, grad_out, grad_q, grad_f = unpack_columns(
        grad_feed, (feed_here, features, features), H
    )
    embed_grad = scatter_add(all_live, all_tokens, moved, V)

    grad_in, _ = lax.optimization_barrier((grad_in, embed_grad[:1, :1]))
    grad_in = jnp.concatenate([grad_q, grad_in, grad_f], axis=1)
    owned_grads = [grad_in, grad_out, grad_feed, grad_down, embed_grad, head_grad]
    square_sum = jnp.zeros((), wide)
    for grad_part in owned_grads:
        square_sum = square_sum + jnp.sum(grad_part * grad_part)
    small_grad = jnp.concatenate(
        [gain_grad_one, gain_grad_two, gain_grad_final, grad_bias, square_sum[None]]
    )
    small_count = small_grad.shape[0]
    small_grad = jnp.pad(small_grad, (0, -small_count % 1024)).reshape(-1, 128)
    small_sum = jnp.sum(gather_rows(small_grad, 4), axis=0).reshape(-1)
    small_total, square_total = small_sum[: small_count - 1], small_sum[small_count - 1]
    grad_norm = jnp.sqrt(square_total + jnp.sum(small_total * small_total))
    factor = jnp.minimum(1.0, clip_limit / grad_norm)
    layer = rate_layer
    news = update_all(
        factor,
        (
            (attention_in[0], attention_in_moment[0], attention_in_average[0], grad_in),
            (attention_out[0], attention_out_moment[0], attention_out_average[0], grad_out),
            (feed_in[0], feed_in_moment[0], feed_in_average[0], grad_feed),
            (feed_out[0], feed_out_moment[0], feed_out_average[0], grad_down),
            (embedding.T, embedding_moment.T, embedding_average.T, embed_grad),
            (unembedding, unembedding_moment, unembedding_average, head_grad),
        ),
        (layer, layer, layer, layer, rate_embed, rate_head),
    )
    results = [loss_value, grad_norm]
    for new in news[:4]:
        results.extend(array[None] for array in new)
    results.extend(array.T for array in news[4])
    results.extend(news[5])
    results.extend(
        apply_update(
            gains_biases, small_total, gains_biases_moment, gains_biases_average, factor, layer
        )
    )
    return tuple(results)


def solution(mesh):
    rows = P(None, both, None)
    tables = (rows,) * 12 + (P(None, both),) * 3 + (P(both, None),) * 3 + (P(),) * 3
    return jax.shard_map(
        step,
        mesh=mesh,
        in_specs=(
            P(None, "fsdp", "seq"),
            P(None, "fsdp"),
            P(None, "fsdp", "seq"),
            P(None, "fsdp", "seq"),
        )
        + tables,
        out_specs=(P(), P()) + tables,
        check_vma=False,
    )
```

```python
import functools
import math

import jax
import jax.numpy as jnp
from jax import lax
from jax.experimental import pallas as pl
from jax.experimental.pallas import tpu as pltpu
from jax.sharding import PartitionSpec as P

D = 768
H = 12
HD = 64
FF = 2048
V = 32000


epsilon = 1e-06
smooth = 0.1
z_weight = 0.005
clip_limit = 0.5
moment = 0.9
average = 0.9
rate_layer = 200.0
rate_head = 1000.0
rate_embed = 5000.0
negative = -1e30
both = ("seq", "fsdp")
highest = lax.Precision.HIGHEST
MESH = pl.DeviceIdType.MESH


def dot(left_side, right_side, left_axis, right_axis, precision=None):
    return lax.dot_general(
        left_side,
        right_side,
        (((left_axis,), (right_axis,)), ((), ())),
        precision=precision,
        preferred_element_type=jnp.float32,
    )


def room(*arrays):
    total = 1 << 20
    for array in arrays:
        shape, size = array.shape, jnp.dtype(array.dtype).itemsize
        tile = 32 // size
        total += (
            math.prod(shape[:-2]) * (-(-shape[-2] // tile) * tile) * (-(-shape[-1] // 128) * 128)
        ) * size
    return total


def line_of(fsdp_count):
    return 4 if fsdp_count % 4 == 0 else 1


def gather_kernel(cores, fsdp, x_ref, o_ref, send_sem, recv_sem):
    plane = line_of(fsdp)
    lines = fsdp // plane
    core = lax.axis_index("seq")
    spot = lax.axis_index("fsdp")
    high, low = spot // plane, spot % plane
    line_peers = [((high + k) % lines) * plane + low for k in range(1, lines)]
    plane_peers = [high * plane + (low + k) % plane for k in range(1, plane)]
    core_peers = [(core + k) % cores for k in range(1, cores)]
    peers = [(core, p) for p in line_peers + plane_peers] + [(c, spot) for c in core_peers]

    barrier = pltpu.get_barrier_semaphore()
    for peer in peers:
        pl.semaphore_signal(barrier, inc=1, device_id=peer, device_id_type=MESH)
    pl.semaphore_wait(barrier, len(peers))

    sent = []

    def send(source_ref, block, peer):
        copy = pltpu.make_async_remote_copy(
            src_ref=source_ref,
            dst_ref=o_ref.at[block],
            send_sem=send_sem.at[len(sent)],
            recv_sem=recv_sem.at[block],
            device_id=peer,
            device_id_type=MESH,
        )
        copy.start()
        sent.append(copy)

    def arrived(block):
        pltpu.make_async_copy(o_ref.at[block], o_ref.at[block], recv_sem.at[block]).wait()

    mine = core * fsdp + spot
    for p in line_peers:
        send(x_ref, mine, (core, p))
    for p in plane_peers:
        send(x_ref, mine, (core, p))
    for c in core_peers:
        send(x_ref, mine, (c, spot))
    o_ref[mine] = x_ref[...]
    for k in range(1, lines):
        block = core * fsdp + ((high + lines - k) % lines) * plane + low
        arrived(block)
        for p in plane_peers:
            send(o_ref.at[block], block, (core, p))
        for c in core_peers:
            send(o_ref.at[block], block, (c, spot))
    for m in range(lines):
        for k in range(1, plane):
            block = core * fsdp + ((high + lines - m) % lines) * plane + (low + plane - k) % plane
            arrived(block)
            for c in core_peers:
                send(o_ref.at[block], block, (c, spot))
    for c in core_peers:
        for m in range(lines):
            for k in range(plane):
                block = c * fsdp + ((high + lines - m) % lines) * plane + (low + plane - k) % plane
                arrived(block)
    for copy in sent:
        copy.wait_send()


def label_kernel(
    cores, fsdp, tokens_ref, lengths_ref, places_ref, targets_ref, o_ref, packed, send_sem, recv_sem
):
    micros, half = tokens_ref.shape
    chunks = half // 128
    start = lax.axis_index("seq") * half
    packed[...] = jnp.zeros_like(packed)
    for m in range(micros):
        for c in range(chunks):
            packed[pl.ds(m * chunks + c, 1), :] = tokens_ref[pl.ds(m, 1), pl.ds(c * 128, 128)]
    base = micros * chunks
    length = lengths_ref[...]
    counted = (start + places_ref[...] < length).astype(jnp.int32)
    live = jnp.clip(length - start, 0, half)
    count = places_ref.shape[1]
    packed[pl.ds(base, micros), pl.ds(0, count)] = targets_ref[...]
    packed[pl.ds(base + micros, micros), pl.ds(0, count)] = counted
    packed[pl.ds(base + 2 * micros, micros), :] = jnp.broadcast_to(live, (micros, 128))
    gather_kernel(cores, fsdp, packed, o_ref, send_sem, recv_sem)


def gather_labels(tokens, lengths, places, targets, collective):
    cores, fsdp = lax.axis_size("seq"), lax.axis_size("fsdp")
    count = cores * fsdp
    micros, half = tokens.shape
    rows = micros * (half // 128) + 3 * micros
    rows = -(-rows // 8) * 8
    result = jax.ShapeDtypeStruct((count, rows, 128), jnp.int32)
    return pl.pallas_call(
        functools.partial(label_kernel, cores, fsdp),
        out_shape=result,
        in_specs=[pl.BlockSpec(memory_space=pltpu.VMEM)] * 4,
        out_specs=pl.BlockSpec(memory_space=pltpu.VMEM),
        scratch_shapes=[
            pltpu.VMEM((rows, 128), jnp.int32),
            pltpu.SemaphoreType.DMA((count,)),
            pltpu.SemaphoreType.DMA((count,)),
        ],
        compiler_params=pltpu.CompilerParams(
            collective_id=collective, has_side_effects=True, vmem_limit_bytes=room(result)
        ),
        name="gather_labels",
    )(tokens, lengths, places, targets)


def gather_rows(array, collective):
    cores, fsdp = lax.axis_size("seq"), lax.axis_size("fsdp")
    count = cores * fsdp
    result = jax.ShapeDtypeStruct((count,) + array.shape, array.dtype)
    return pl.pallas_call(
        functools.partial(gather_kernel, cores, fsdp),
        out_shape=result,
        in_specs=[pl.BlockSpec(memory_space=pltpu.VMEM)],
        out_specs=pl.BlockSpec(memory_space=pltpu.VMEM),
        scratch_shapes=[
            pltpu.SemaphoreType.DMA((count,)),
            pltpu.SemaphoreType.DMA((count,)),
        ],
        compiler_params=pltpu.CompilerParams(
            collective_id=collective,
            has_side_effects=True,
            vmem_limit_bytes=room(array, result),
        ),
        name="gather_rows",
    )(array)


def exchange_kernel(cores, fsdp, x_ref, o_ref, send_sem, recv_sem, own_sem):
    count = cores * fsdp
    mine = lax.axis_index("seq") * fsdp + lax.axis_index("fsdp")

    def place(step):
        other = lax.rem(mine + step, count)
        return other, (other // fsdp, lax.rem(other, fsdp))

    barrier = pltpu.get_barrier_semaphore()

    def greet(step, _):
        pl.semaphore_signal(barrier, inc=1, device_id=place(step)[1], device_id_type=MESH)
        return 0

    lax.fori_loop(1, count, greet, 0)
    pl.semaphore_wait(barrier, count - 1)
    own = pltpu.make_async_copy(x_ref.at[mine], o_ref.at[mine], own_sem)
    own.start()

    def copy_to(step):
        other, peer = place(step)
        return pltpu.make_async_remote_copy(
            src_ref=x_ref.at[other],
            dst_ref=o_ref.at[mine],
            send_sem=send_sem.at[step],
            recv_sem=recv_sem.at[step],
            device_id=peer,
            device_id_type=MESH,
        )

    def start(step, _):
        copy_to(step).start()
        return 0

    lax.fori_loop(1, count, start, 0)
    own.wait()

    def finish(step, _):
        source = lax.rem(mine + count - step, count)
        pltpu.make_async_copy(o_ref.at[source], o_ref.at[source], recv_sem.at[step]).wait()
        copy_to(step).wait_send()
        return 0

    lax.fori_loop(1, count, finish, 0)


def exchange(array, collective):
    cores, fsdp = lax.axis_size("seq"), lax.axis_size("fsdp")
    return pl.pallas_call(
        functools.partial(exchange_kernel, cores, fsdp),
        out_shape=jax.ShapeDtypeStruct(array.shape, array.dtype),
        in_specs=[pl.BlockSpec(memory_space=pltpu.VMEM)],
        out_specs=pl.BlockSpec(memory_space=pltpu.VMEM),
        scratch_shapes=[
            pltpu.SemaphoreType.DMA((cores * fsdp,)),
            pltpu.SemaphoreType.DMA((cores * fsdp,)),
            pltpu.SemaphoreType.DMA,
        ],
        compiler_params=pltpu.CompilerParams(
            collective_id=collective,
            has_side_effects=True,
            vmem_limit_bytes=room(array, array),
        ),
        name="exchange",
    )(array)


def reduce_kernel(
    fsdp, x_ref, o_ref, from_core, from_plane, from_line, core_sum, plane_sum, send_sem, recv_sem
):
    plane = line_of(fsdp)
    lines = fsdp // plane
    core = lax.axis_index("seq")
    spot = lax.axis_index("fsdp")
    high, low = spot // plane, lax.rem(spot, plane)
    far = 1 - core
    peers = [(far, spot)]
    peers += [(core, lax.rem(high + k, lines) * plane + low) for k in range(1, lines)]
    peers += [(core, high * plane + lax.rem(low + k, plane)) for k in range(1, plane)]
    barrier = pltpu.get_barrier_semaphore()
    for peer in peers:
        pl.semaphore_signal(barrier, inc=1, device_id=peer, device_id_type=MESH)
    pl.semaphore_wait(barrier, len(peers))
    sent = []

    def send(source_ref, target_ref, slot, peer):
        copy = pltpu.make_async_remote_copy(
            src_ref=source_ref,
            dst_ref=target_ref,
            send_sem=send_sem.at[slot],
            recv_sem=recv_sem.at[slot],
            device_id=peer,
            device_id_type=MESH,
        )
        copy.start()
        sent.append(copy)
        return copy

    first = []
    for k in list(range(1, plane)) + [0]:
        spot_low = lax.rem(low + k, plane)
        first.append(
            (k, spot_low, send(x_ref.at[far, :, spot_low], from_core.at[spot_low], k, (far, spot)))
        )
    second = []
    for k, spot_low, copy in first:
        copy.wait_recv()
        core_sum[spot_low] = x_ref[core, :, spot_low] + from_core[spot_low]
        if k:
            target = from_plane.at[k - 1]
            peer = (core, high * plane + spot_low)
            second.append((k, send(core_sum.at[spot_low], target, plane + k - 1, peer)))
    plane_sum[...] = core_sum[low]
    for k, copy in second:
        copy.wait_recv()
        plane_sum[...] += from_plane[k - 1]
    third = []
    for k in range(1, lines):
        line = lax.rem(high + k, lines)
        slot = 2 * plane + k - 2
        peer = (core, line * plane + low)
        third.append((k, send(plane_sum.at[line], from_line.at[k - 1], slot, peer)))
    total = plane_sum[high]
    for k, copy in third:
        copy.wait_recv()
        total = total + from_line[k - 1]
    o_ref[...] = total
    for copy in sent:
        copy.wait_send()


def reduce_rows(array, collective):
    cores, fsdp = lax.axis_size("seq"), lax.axis_size("fsdp")
    plane = line_of(fsdp)
    lines = fsdp // plane
    rows, columns = array.shape[0] // (cores * fsdp), array.shape[1]
    kind = array.dtype
    slots = 2 * plane + lines - 2
    return pl.pallas_call(
        functools.partial(reduce_kernel, fsdp),
        out_shape=jax.ShapeDtypeStruct((rows, columns), kind),
        in_specs=[pl.BlockSpec(memory_space=pltpu.VMEM)],
        out_specs=pl.BlockSpec(memory_space=pltpu.VMEM),
        scratch_shapes=[
            pltpu.VMEM((plane, lines, rows, columns), kind),
            pltpu.VMEM((plane - 1, lines, rows, columns), kind),
            pltpu.VMEM((lines - 1, rows, columns), kind),
            pltpu.VMEM((plane, lines, rows, columns), kind),
            pltpu.VMEM((lines, rows, columns), kind),
            pltpu.SemaphoreType.DMA((slots,)),
            pltpu.SemaphoreType.DMA((slots,)),
        ],
        compiler_params=pltpu.CompilerParams(
            collective_id=collective,
            has_side_effects=True,
            vmem_limit_bytes=room(array, array, array),
        ),
        name="reduce_rows",
    )(array.reshape(cores, lines, plane, rows, columns))


def lookup_kernel(unroll, builds, live_ref, ids_ref, own_ref, o_ref, table, stage):
    sources, features, tokens = o_ref.shape
    micros = live_ref.shape[0] // sources
    half = tokens // micros

    def build(step, _):
        for u in range(builds):
            at = pl.multiple_of((step * builds + u) * 128, 128)
            block = own_ref[:, pl.ds(at, 128)].astype(jnp.bfloat16).astype(jnp.float32)
            table[pl.ds(at, 128), pl.ds(0, features)] = block.T
        return 0

    lax.fori_loop(0, table.shape[0] // 128 // builds, build, 0)
    stage[...] = jnp.zeros_like(stage)

    def source(which, _):
        def fetch(first, step, _):
            at = first + step * unroll
            ids = [ids_ref[which * tokens + at + u] for u in range(unroll)]
            for u in range(unroll):
                stage[pl.ds(at + u, 1), :] = table[pl.ds(ids[u], 1), :]
            return 0

        for m in range(micros):
            live = live_ref[which * micros + m]
            lax.fori_loop(
                0, (live + unroll - 1) // unroll, functools.partial(fetch, m * half), 0
            )
        for c in range(tokens // 128):
            block = stage[pl.ds(c * 128, 128), :].T
            o_ref[which, :, pl.ds(c * 128, 128)] = block[:features].astype(jnp.bfloat16)
        return 0

    lax.fori_loop(0, sources, source, 0)


def lookup(live, ids, table_t):
    sources, tokens = ids.shape
    features, vocab = table_t.shape
    return pl.pallas_call(
        functools.partial(lookup_kernel, 64, 10),
        out_shape=jax.ShapeDtypeStruct((sources, features, tokens), jnp.bfloat16),
        in_specs=[
            pl.BlockSpec(memory_space=pltpu.SMEM),
            pl.BlockSpec(memory_space=pltpu.SMEM),
            pl.BlockSpec(memory_space=pltpu.VMEM),
        ],
        out_specs=pl.BlockSpec(memory_space=pltpu.VMEM),
        scratch_shapes=[
            pltpu.VMEM((vocab, 128), jnp.float32),
            pltpu.VMEM((tokens, 128), jnp.float32),
        ],
        compiler_params=pltpu.CompilerParams(vmem_limit_bytes=32 * 1024 * 1024),
        name="lookup",
    )(live.reshape(-1), ids.reshape(-1), table_t)


row_bits = 13
row_count = 1 << row_bits


def scatter_kernel(unroll, live_ref, rows_ref, ids_ref, g_ref, o_ref, spread, *sums):
    sources, features, tokens = g_ref.shape
    micros = live_ref.shape[0] // sources
    half = tokens // micros
    vocab = o_ref.shape[1]
    groups = 4

    def clear(step, _):
        for one in sums:
            one[pl.ds(pl.multiple_of(step * 256, 256), 256)] = jnp.zeros((256, 128), jnp.float32)
        return 0

    lax.fori_loop(0, row_count // 256, clear, 0)
    blank = jnp.zeros((128 // groups - features, 128), jnp.float32)
    group = lax.broadcasted_iota(jnp.int32, (128, 128), 0) // (128 // groups)

    def source(which, _):
        for c in range(tokens // 128):
            block = g_ref[which, :, pl.ds(c * 128, 128)].astype(jnp.float32)
            block = jnp.concatenate([block, blank] * groups, axis=0)
            chosen = ids_ref[which, :, pl.ds(c * 128, 128)] >> row_bits
            spread[pl.ds(c * 128, 128), :] = jnp.where(group == chosen, block, 0.0).T

        def add(first, step, _):
            at = first + step * unroll
            rows = [rows_ref[which * tokens + at + u] for u in range(unroll)]
            for u in range(unroll):
                one = sums[u % len(sums)]
                one[pl.ds(rows[u], 1), :] += spread[pl.ds(at + u, 1), :]
            return 0

        for m in range(micros):
            live = live_ref[which * micros + m]
            lax.fori_loop(0, (live + unroll - 1) // unroll, functools.partial(add, m * half), 0)
        return 0

    lax.fori_loop(0, sources, source, 0)

    def finish(step, _):
        for u in range(2):
            at = pl.multiple_of((step * 2 + u) * 128, 128)
            total = sums[0][pl.ds(at, 128)]
            for one in sums[1:]:
                total = total + one[pl.ds(at, 128)]
            total = total.T
            for k in range(groups):
                part = total[k * (128 // groups) : k * (128 // groups) + features]
                if (k + 1) * row_count <= vocab:
                    o_ref[:, pl.ds(k * row_count + at, 128)] = part
                elif k * row_count < vocab:

                    @pl.when(k * row_count + at + 128 <= vocab)
                    def _():
                        o_ref[:, pl.ds(k * row_count + at, 128)] = part

        return 0

    lax.fori_loop(0, row_count // 256, finish, 0)


def scatter_add(live, ids, grads, vocab):
    sources, features, tokens = grads.shape
    return pl.pallas_call(
        functools.partial(scatter_kernel, 32),
        out_shape=jax.ShapeDtypeStruct((features, vocab), jnp.float32),
        in_specs=[
            pl.BlockSpec(memory_space=pltpu.SMEM),
            pl.BlockSpec(memory_space=pltpu.SMEM),
            pl.BlockSpec(memory_space=pltpu.VMEM),
            pl.BlockSpec(memory_space=pltpu.VMEM),
        ],
        out_specs=pl.BlockSpec(memory_space=pltpu.VMEM),
        scratch_shapes=[pltpu.VMEM((tokens, 128), jnp.float32)]
        + [pltpu.VMEM((row_count, 128), jnp.float32)] * 8,
        compiler_params=pltpu.CompilerParams(vmem_limit_bytes=44 * 1024 * 1024),
        cost_estimate=pl.CostEstimate(
            flops=40 * 10**9, bytes_accessed=8 * 10**6, transcendentals=0
        ),
        name="scatter_add",
    )(
        live.reshape(-1),
        (ids & (row_count - 1)).reshape(-1),
        ids.reshape(sources, 1, tokens),
        grads,
    )


def spread_kernel(count, hidden_ref, spread_ref):
    per = hidden_ref.shape[1] // count
    features = spread_ref.shape[1] // (-(-per // (D // count)) * count)
    spread_ref[...] = jnp.zeros_like(spread_ref)
    for d in range(count):
        block = hidden_ref[:, pl.ds(d * per, per)]
        for k in range(-(-per // features)):
            width = min(features, per - k * features)
            at = (k * count + d) * features
            spread_ref[:, pl.ds(at, width)] = block[:, k * features : k * features + width]


def spread_columns(hidden, count):
    rows = hidden.shape[0]
    pieces = -(-(hidden.shape[1] // count) // (D // count))
    result = jax.ShapeDtypeStruct((rows, pieces * D), hidden.dtype)
    return pl.pallas_call(
        functools.partial(spread_kernel, count),
        out_shape=result,
        in_specs=[pl.BlockSpec(memory_space=pltpu.VMEM)],
        out_specs=pl.BlockSpec(memory_space=pltpu.VMEM),
        compiler_params=pltpu.CompilerParams(vmem_limit_bytes=room(hidden, result)),
        name="spread_columns",
    )(hidden)


def pack_kernel(*refs):
    packed_ref = refs[-1]
    count = packed_ref.shape[0]
    packed_ref[...] = jnp.zeros_like(packed_ref)
    at = 0
    for x_ref in refs[:-1]:
        width = x_ref.shape[1] // count
        for d in range(count):
            packed_ref[d, :, pl.ds(at, width)] = x_ref[:, pl.ds(d * width, width)]
        at += width


def pack_columns(arrays, count):
    width = -(-sum(array.shape[1] for array in arrays) // (128 * count)) * 128
    result = jax.ShapeDtypeStruct((count, arrays[0].shape[0], width), arrays[0].dtype)
    return pl.pallas_call(
        pack_kernel,
        out_shape=result,
        in_specs=[pl.BlockSpec(memory_space=pltpu.VMEM)] * len(arrays),
        out_specs=pl.BlockSpec(memory_space=pltpu.VMEM),
        compiler_params=pltpu.CompilerParams(vmem_limit_bytes=room(*arrays, result)),
        name="pack_columns",
    )(*arrays)


def collect_kernel(count, spread_ref, o_ref):
    per = o_ref.shape[1] // count
    features = spread_ref.shape[2] // count
    for d in range(count):
        for k in range(spread_ref.shape[0]):
            width = min(features, per - k * features)
            part = spread_ref[k, :, pl.ds(d * features, width)]
            o_ref[:, pl.ds(d * per + k * features, width)] = part


def collect_columns(parts, columns, count):
    return pl.pallas_call(
        functools.partial(collect_kernel, count),
        out_shape=jax.ShapeDtypeStruct((parts.shape[1], columns), parts.dtype),
        in_specs=[pl.BlockSpec(memory_space=pltpu.VMEM)],
        out_specs=pl.BlockSpec(memory_space=pltpu.VMEM),
        compiler_params=pltpu.CompilerParams(vmem_limit_bytes=room(parts, parts)),
        name="collect_columns",
    )(parts)


def unpack_kernel(widths, x_ref, *o_refs):
    count = x_ref.shape[0]
    at = 0
    for width, o_ref in zip(widths, o_refs):
        for d in range(count):
            o_ref[:, pl.ds(d * width, width)] = x_ref[d, :, pl.ds(at, width)]
        at += width
    last = x_ref.shape[2] - at
    total = x_ref[0, :, pl.ds(at, last)]
    for d in range(1, count):
        total = total + x_ref[d, :, pl.ds(at, last)]
    o_refs[-1][...] = total


def unpack_columns(blocks, widths, summed):
    count, rows, _ = blocks.shape
    results = tuple(jax.ShapeDtypeStruct((rows, count * w), blocks.dtype) for w in widths)
    results += (jax.ShapeDtypeStruct((rows, summed), blocks.dtype),)
    return pl.pallas_call(
        functools.partial(unpack_kernel, widths),
        out_shape=results,
        in_specs=[pl.BlockSpec(memory_space=pltpu.VMEM)],
        out_specs=tuple(pl.BlockSpec(memory_space=pltpu.VMEM) for _ in results),
        compiler_params=pltpu.CompilerParams(vmem_limit_bytes=room(blocks, *results)),
        name="unpack_columns",
    )(blocks)


def parts_of(rows, columns):
    if columns % 6400 == 0:
        return True, 6400, columns // 6400
    if rows % 200 == 0:
        return False, 200, rows // 200
    return False, rows, 1


def update_kernel(rates, factor_ref, *refs):
    count = len(rates)
    olds, grads = refs[: 3 * count], refs[3 * count : 4 * count]
    outputs, staged = refs[4 * count : 7 * count], refs[7 * count : 10 * count]
    load_sem, store_sem = refs[10 * count], refs[10 * count + 1]
    factor = factor_ref[0]
    plan = []
    for p in range(count):
        columnwise, size, parts = parts_of(*grads[p].shape)
        for part in range(parts):
            at = pl.ds(part * size, size)
            plan.append((p, (slice(None), at) if columnwise else (at, slice(None)), columnwise, size))

    def move(step, k, source, target, sem):
        p, where, _, _ = plan[step]
        refs_at = (source[3 * p + k].at[where], target[3 * p + k].at[where])
        return pltpu.make_async_copy(*refs_at, sem.at[3 * step + k])

    for step in range(len(plan)):
        for k in range(3):
            move(step, k, olds, staged, load_sem).start()
    for step, (p, where, columnwise, size) in enumerate(plan):
        for k in range(3):
            move(step, k, olds, staged, load_sem).wait()
        base = (where[1] if columnwise else where[0]).start
        grain = 640 if columnwise else (40 if size % 40 == 0 else size)

        def body(piece, _, p=p, columnwise=columnwise, base=base, grain=grain):
            at = pl.ds(pl.multiple_of(base + piece * grain, 128 if columnwise else 8), grain)
            spot = (slice(None), at) if columnwise else (at, slice(None))
            old = [staged[3 * p + k][spot] for k in range(3)]
            new = apply_update(old[0], grads[p][spot], old[1], old[2], factor, rates[p])
            for k in range(3):
                staged[3 * p + k][spot] = new[k]
            return 0

        if size == grain:
            whole = (slice(None), slice(None))
            old = [staged[3 * p + k][whole] for k in range(3)]
            new = apply_update(old[0], grads[p][whole], old[1], old[2], factor, rates[p])
            for k in range(3):
                staged[3 * p + k][whole] = new[k]
        else:
            lax.fori_loop(0, size // grain, body, 0)
        for k in range(3):
            move(step, k, staged, outputs, store_sem).start()
    for step in range(len(plan)):
        for k in range(3):
            move(step, k, staged, outputs, store_sem).wait()


def update_all(factor, params, rates):
    olds = [array for param in params for array in param[:3]]
    grads = [param[3] for param in params]
    results = tuple(jax.ShapeDtypeStruct(array.shape, jnp.float32) for array in olds)
    copies = 3 * sum(parts_of(*grad.shape)[2] for grad in grads)
    hbm = pl.BlockSpec(memory_space=pltpu.HBM)
    new = pl.pallas_call(
        functools.partial(update_kernel, rates),
        out_shape=results,
        in_specs=[pl.BlockSpec(memory_space=pltpu.SMEM)]
        + [hbm] * len(olds)
        + [pl.BlockSpec(memory_space=pltpu.VMEM)] * len(grads),
        out_specs=(hbm,) * len(olds),
        scratch_shapes=[pltpu.VMEM(array.shape, jnp.float32) for array in olds]
        + [pltpu.SemaphoreType.DMA((copies,))] * 2,
        compiler_params=pltpu.CompilerParams(vmem_limit_bytes=62 * 1024 * 1024),
        name="update_all",
    )(factor.reshape(1), *olds, *grads)
    return [new[3 * p : 3 * p + 3] for p in range(len(params))]


def other_core(arrays):
    return lax.ppermute(arrays, "seq", [(0, 1), (1, 0)])


def norm_forward(values, gain_row):
    inverse = lax.rsqrt(jnp.mean(values * values, axis=-1, keepdims=True) + epsilon)
    return (values * inverse * gain_row, inverse)


def norm_backward(values, inverse, gain_row, grad_out):
    scaled = grad_out * gain_row
    grad_gain = jnp.sum(grad_out * values * inverse, axis=0)
    grad_in = inverse * scaled - values * inverse**3 * jnp.mean(
        values * scaled, axis=-1, keepdims=True
    )
    return (grad_in, grad_gain)


def apply_update(weight_old, grad_full, moment_old, average_old, factor, rate):
    clipped = factor * grad_full
    moment_new = moment * moment_old + clipped
    weight_new = weight_old - rate * (clipped + moment * moment_new)
    average_new = average * average_old + (1.0 - average) * weight_new
    return (weight_new, moment_new, average_new)


def step(
    token_ids,
    lengths,
    loss_positions,
    loss_targets,
    attention_in,
    attention_in_moment,
    attention_in_average,
    attention_out,
    attention_out_moment,
    attention_out_average,
    feed_in,
    feed_in_moment,
    feed_in_average,
    feed_out,
    feed_out_moment,
    feed_out_average,
    embedding,
    embedding_moment,
    embedding_average,
    unembedding,
    unembedding_moment,
    unembedding_average,
    gains_biases,
    gains_biases_moment,
    gains_biases_average,
):
    low = jnp.bfloat16
    wide = jnp.float32
    devices_all = lax.axis_size(both)
    seq_index = lax.axis_index("seq")
    device = lax.axis_index(both)
    micros, _, half = token_ids.shape
    loss_dev = loss_positions.shape[2]
    tokens = micros * half
    rows = micros * loss_dev
    rows_all = devices_all * rows
    vocab_here = unembedding.shape[0]
    features = D // devices_all
    gate_here = FF // devices_all
    gain_rows = gains_biases[: 3 * D].reshape(3, D)
    bias_row = gains_biases[3 * D :]
    second = seq_index.astype(wide)

    positions = loss_positions[:, 0]
    targets = loss_targets[:, 0]
    ids_all = gather_labels(token_ids[:, 0], lengths, positions, targets, 1)
    base = tokens // 128
    all_tokens = ids_all[:, :base].reshape(devices_all, tokens)
    all_targets = ids_all[:, base : base + micros, :loss_dev].reshape(-1)
    all_counted = ids_all[:, base + micros : base + 2 * micros, :loss_dev]
    all_live = ids_all[:, base + 2 * micros : base + 3 * micros, 0]

    down_here = feed_out.shape[1]
    pieces = -(-down_here // features)
    down_pad = jnp.pad(feed_out[0], ((0, pieces * features - down_here), (0, 0)))
    down_pad = [down_pad[k * features : (k + 1) * features] for k in range(pieces)]
    packed = jnp.concatenate([feed_in[0]] + down_pad + [attention_out[0], attention_in[0]], axis=1)
    w_all = lax.all_gather(packed.astype(low), both, axis=0, tiled=True)
    down_at = 2 * FF
    out_at = down_at + pieces * D
    w_feed = w_all[:, :down_at]
    w_out = w_all[:, out_at : out_at + D]
    w_in = w_all[:, out_at + D :]
    w_down = [w_all[:, down_at + k * D : down_at + (k + 1) * D] for k in range(pieces)]
    head_low = unembedding.astype(low)

    arrived = exchange(lookup(all_live, all_tokens, embedding.T), 5)
    x_t = arrived.reshape(D, tokens)
    pick = [
        (positions[m][:, None] == jnp.arange(half)[None, :]).astype(low) for m in range(micros)
    ]
    x_wide, inverse_one, normed_t, keys_t, values_t, forget_t = [], [], [], [], [], []
    for m in range(micros):
        x_wide.append(x_t[:, m * half : (m + 1) * half].astype(wide))
        inverse_one.append(
            lax.rsqrt(jnp.mean(x_wide[m] * x_wide[m], axis=0, keepdims=True) + epsilon)
        )
        normed_t.append((x_wide[m] * inverse_one[m] * gain_rows[0][:, None]).astype(low))

        project_t = dot(w_in[:, D:], normed_t[m], 0, 0)
        keys_t.append(project_t[:D].astype(low).reshape(H, HD, half))
        values_t.append(project_t[D : 2 * D].astype(low).reshape(H, HD, half))
        forget_t.append((project_t[2 * D :] + bias_row[:, None]).astype(low).astype(wide))
    x_rows = jnp.concatenate([dot(pick[m], x_wide[m].astype(low), 1, 1) for m in range(micros)])
    normed_rows = jnp.concatenate(
        [dot(pick[m], normed_t[m], 1, 1) for m in range(micros)]
    ).astype(low)
    q_rows = dot(normed_rows, w_in[:, :D], 1, 0).astype(low)

    upper = (jnp.arange(half)[:, None] <= jnp.arange(half)[None, :]).astype(wide)
    log_gate = jax.nn.log_sigmoid(jnp.stack(forget_t, axis=1))
    decay_own = lax.dot_general(
        log_gate, upper, (((2,), (0,)), ((), ())), precision=highest, preferred_element_type=wide
    )
    total_own = decay_own[:, :, -1]
    decay_rows = jnp.stack(
        [dot(pick[m].astype(wide), decay_own[:, m], 1, 1, highest) for m in range(micros)]
    )
    q_own = q_rows.reshape(micros, loss_dev, H, HD)
    q_far, decay_far, total_far, place_far = other_core((q_own, decay_rows, total_own, positions))
    shift_own = second * total_far
    shift_far = (1.0 - second) * total_own
    key_decay = decay_own + shift_own[:, :, None]
    row_decay = jnp.concatenate(
        [decay_rows + shift_own.T[:, None], decay_far + shift_far.T[:, None]], axis=1
    )
    q_all = jnp.concatenate([q_own, q_far], axis=1)
    places = jnp.concatenate(
        [positions + seq_index * half, place_far + (1 - seq_index) * half], axis=1
    )
    key_places = seq_index * half + jnp.arange(half)

    scores = []
    for m in range(micros):
        raw = jnp.einsum("rhd,hdj->hrj", q_all[m], keys_t[m], preferred_element_type=wide)
        part = raw * HD ** (-0.5) + row_decay[m].T[:, :, None] - key_decay[:, m][:, None, :]
        causal = places[m][:, None] >= key_places[None, :]
        scores.append(jnp.where(causal[None], part, negative))
    scores = jnp.stack(scores)
    peak_own = jnp.max(scores, axis=-1)
    spread_own = jnp.sum(jnp.exp(scores - peak_own[..., None]), axis=-1)
    peak_far, spread_far = other_core((peak_own, spread_own))

    def swap_rows(array):
        return jnp.concatenate([array[:, :, loss_dev:], array[:, :, :loss_dev]], axis=2)

    peak_far, spread_far = swap_rows(peak_far), swap_rows(spread_far)
    peak = jnp.maximum(peak_own, peak_far)
    log_total = peak + jnp.log(
        spread_own * jnp.exp(peak_own - peak) + spread_far * jnp.exp(peak_far - peak)
    )
    probs = jnp.exp(scores - log_total[..., None])
    probs_low = probs.astype(low)
    probs_rest = (probs - probs_low.astype(wide)).astype(low)

    def mix(weights):
        return jnp.stack(
            [
                jnp.einsum(
                    "hrj,hdj->rhd",
                    weights[m],
                    values_t[m],
                    preferred_element_type=wide,
                )
                for m in range(micros)
            ]
        )

    mixed_part = mix(probs_low)
    rest_part = mix(probs_rest)
    mixed_far, rest_far = other_core((mixed_part[:, loss_dev:], rest_part[:, loss_dev:]))
    mixed_sum = mixed_part[:, :loss_dev] + mixed_far
    mixed_full = mixed_sum + rest_part[:, :loss_dev] + rest_far
    mixed_rows = mixed_sum.reshape(rows, D).astype(low)

    middle = x_rows + dot(mixed_rows, w_out, 1, 0)
    normed_two, inverse_two = norm_forward(middle, gain_rows[1])
    normed_two = normed_two.astype(low)
    gate_up = dot(normed_two, w_feed, 1, 0)
    gate_half, up_half = gate_up[:, :FF], gate_up[:, FF:]
    gate_sigmoid = jax.nn.sigmoid(gate_half)
    hidden = (gate_half * gate_sigmoid * up_half).astype(low)
    hidden_spread = spread_columns(hidden, devices_all)
    early_packed = lax.all_gather(
        jnp.concatenate([normed_two, mixed_rows, normed_rows], axis=1),
        both,
        axis=0,
        tiled=True,
    )
    final_in = middle
    for k in range(pieces):
        final_in = final_in + dot(hidden_spread[:, k * D : (k + 1) * D], w_down[k], 1, 0)
    final_normed, final_inverse = norm_forward(final_in, gain_rows[2])

    final_all = gather_rows(final_normed.astype(low), 2).reshape(rows_all, D)
    logits = dot(final_all, head_low, 1, 1)
    vocab_ids = device * vocab_here + jnp.arange(vocab_here)
    target_hits = all_targets[:, None] == vocab_ids[None, :]
    row_peak = jnp.max(logits, axis=1)
    exp_sum = jnp.sum(jnp.exp(logits - row_peak[:, None]), axis=1)
    target_part = jnp.sum(jnp.where(target_hits, logits, 0.0), axis=1)
    logit_sum = jnp.sum(logits, axis=1)
    stats = jnp.stack([row_peak, exp_sum, target_part, logit_sum])
    stats_all = gather_rows(stats.reshape(-1, 128), 3).reshape(devices_all, 4, rows_all)
    peak_all = jnp.max(stats_all[:, 0], axis=0)
    spread_all = jnp.sum(stats_all[:, 1] * jnp.exp(stats_all[:, 0] - peak_all), axis=0)
    target_all = jnp.sum(stats_all[:, 2], axis=0)
    logit_all = jnp.sum(stats_all[:, 3], axis=0)
    total_all = peak_all + jnp.log(spread_all)
    per_row = (
        total_all
        - (1.0 - smooth) * target_all
        - smooth * logit_all / V
        + z_weight * total_all * total_all
    )
    weights_row = all_counted.astype(wide).reshape(devices_all, micros, loss_dev)
    counts = jnp.sum(weights_row, axis=(0, 2))
    weights_row = (weights_row / (micros * counts)[None, :, None]).reshape(-1)
    loss_value = jnp.sum(weights_row * per_row)
    soft_rows = jnp.exp(logits - total_all[:, None])
    grad_logits = (
        weights_row[:, None]
        * (
            soft_rows * (1.0 + 2.0 * z_weight * total_all)[:, None]
            - (1.0 - smooth) * target_hits.astype(wide)
            - smooth / V
        )
    ).astype(low)
    grad_final = reduce_rows(dot(grad_logits, head_low, 1, 0), 7)

    grad_rows, gain_grad_final = norm_backward(final_in, final_inverse, gain_rows[2], grad_final)
    branch_all = gather_rows(grad_rows.astype(low), 8).reshape(rows_all, D)
    grad_branch, _ = lax.optimization_barrier((grad_rows.astype(low), branch_all[:1, :1]))
    grad_hidden = jnp.stack([dot(grad_branch, w_down[k], 1, 1) for k in range(pieces)])
    grad_hidden = collect_columns(grad_hidden, FF, devices_all)
    grad_gate = grad_hidden * up_half * gate_sigmoid * (1.0 + gate_half * (1.0 - gate_sigmoid))
    grad_up = grad_hidden * gate_half * gate_sigmoid
    grad_gate_up = jnp.concatenate([grad_gate, grad_up], axis=1).astype(low)
    grad_two, gain_grad_two = norm_backward(
        middle, inverse_two, gain_rows[1], dot(grad_gate_up, w_feed, 1, 1)
    )
    grad_middle = grad_rows + grad_two
    grad_mid_low = grad_middle.astype(low)
    grad_mixed = dot(grad_mid_low, w_out, 1, 1).astype(low)

    feed_here = 2 * FF // devices_all
    grad_own = grad_mixed.reshape(micros, loss_dev, H, HD)
    inner_own = jnp.sum(grad_own.astype(wide) * mixed_full, axis=-1)
    grad_far, inner_far = other_core((grad_own, inner_own))
    grad_heads = jnp.concatenate([grad_own, grad_far], axis=1)
    inner_sum = jnp.concatenate([inner_own, inner_far], axis=1)
    query_parts, score_rows = [], []
    grad_keys, grad_values, score_columns = [], [], []
    for m in range(micros):
        grad_probs = jnp.einsum(
            "rhd,hdj->hrj", grad_heads[m], values_t[m], preferred_element_type=wide
        )
        grad_scores = (probs[m] * (grad_probs - inner_sum[m].T[:, :, None])).astype(low)
        query_parts.append(
            jnp.einsum("hrj,hdj->rhd", grad_scores, keys_t[m], preferred_element_type=wide)
        )
        grad_keys.append(
            jnp.einsum("hrj,rhd->hdj", grad_scores, q_all[m], preferred_element_type=wide)
            * HD ** (-0.5)
        )
        grad_values.append(
            jnp.einsum("hrj,rhd->hdj", probs_low[m], grad_heads[m], preferred_element_type=wide)
        )
        score_wide = grad_scores.astype(wide)
        score_rows.append(jnp.sum(score_wide, axis=-1))
        score_columns.append(jnp.sum(score_wide, axis=1))
    query_parts = jnp.stack(query_parts)
    score_rows = jnp.stack(score_rows).transpose(0, 2, 1)
    query_far, score_far = other_core((query_parts[:, loss_dev:], score_rows[:, loss_dev:]))
    grad_query = ((query_parts[:, :loss_dev] + query_far) * HD ** (-0.5)).astype(low)
    grad_query = grad_query.reshape(rows, D)
    columns_packed = lax.all_to_all(
        pack_columns((grad_gate_up, hidden, grad_mid_low, grad_query), devices_all),
        both,
        split_axis=0,
        concat_axis=0,
        tiled=True,
    )
    rows_sum = score_rows[:, :loss_dev] + score_far
    later = (1.0 - second) * jnp.sum(score_rows[:, loss_dev:], axis=1)
    grad_in_sum, forget_sum, gain_grad_one, grad_bias, grad_embed = 0.0, 0.0, 0.0, 0.0, []
    projects = []
    for m in range(micros):
        placed = dot(rows_sum[m], pick[m].astype(wide), 0, 0, highest)
        change = placed - score_columns[m]
        grad_log = dot(change, upper, 1, 1, highest) + later[m][:, None]
        grad_forget = (grad_log * jax.nn.sigmoid(-forget_t[m])).astype(low)
        grad_bias = grad_bias + jnp.sum(grad_forget.astype(wide), axis=1)
        query_t = dot(grad_query[m * loss_dev : (m + 1) * loss_dev], pick[m], 0, 0).astype(low)
        keys_part = grad_keys[m].astype(low).reshape(D, half)
        values_part = grad_values[m].astype(low).reshape(D, half)
        grad_forget = lax.optimization_barrier(jnp.pad(grad_forget, ((0, -H % 128), (0, 0))))
        projects.append(jnp.concatenate([query_t, keys_part, values_part, grad_forget], axis=0))
        grad_in_sum = grad_in_sum + dot(normed_t[m], projects[m][D : 3 * D], 1, 1)
        forget_sum = forget_sum + dot(normed_t[m], grad_forget, 1, 1)
    grad_in = lax.psum_scatter(grad_in_sum, both, scatter_dimension=0, tiled=True)
    for m in range(micros):
        grad_normed = dot(w_in, projects[m][: 3 * D + H], 1, 0)
        scaled = grad_normed * gain_rows[0][:, None]
        gain_grad_one = gain_grad_one + jnp.sum(grad_normed * x_wide[m] * inverse_one[m], axis=1)
        grad_one = inverse_one[m] * scaled - x_wide[m] * inverse_one[m] ** 3 * jnp.mean(
            x_wide[m] * scaled, axis=0, keepdims=True
        )
        middle_t = dot(
            grad_middle[m * loss_dev : (m + 1) * loss_dev], pick[m].astype(wide), 0, 0, highest
        )
        grad_embed.append((middle_t + grad_one).astype(low))
    grad_embed = jnp.concatenate(grad_embed, axis=1).reshape(devices_all, features, tokens)
    moved = lax.all_to_all(grad_embed, both, split_axis=0, concat_axis=0, tiled=True)
    early_packed, columns_packed, _ = lax.optimization_barrier(
        (early_packed, columns_packed, grad_embed[:1, :1, :1])
    )
    late_logits, _ = lax.optimization_barrier((grad_logits, grad_embed[:1, :1, :1]))
    head_grad = lax.optimization_barrier(dot(late_logits, final_all, 0, 0))
    columns_packed = columns_packed.reshape(rows_all, -1)

    def columns_of(first, width):
        return columns_packed[:, first : first + width]

    feed_columns = dot(early_packed[:, :D], columns_of(0, feed_here), 0, 0)
    out_columns = columns_of(feed_here + gate_here, features)
    out_columns = dot(early_packed[:, D : 2 * D], out_columns, 0, 0)
    query_columns = columns_of(feed_here + gate_here + features, features)
    query_columns = dot(early_packed[:, 2 * D :], query_columns, 0, 0)
    grad_down = lax.optimization_barrier(dot(columns_of(feed_here, gate_here), branch_all, 0, 0))
    grad_feed = lax.all_to_all(
        jnp.concatenate(
            [feed_columns, out_columns, query_columns, forget_sum[:, :H]], axis=1
        ).reshape(devices_all, features, feed_here + 2 * features + H),
        both,
        split_axis=0,
        concat_axis=0,
        tiled=True,
    )
    grad_feed, grad_out, grad_q, grad_f = unpack_columns(
        grad_feed, (feed_here, features, features), H
    )
    embed_grad = scatter_add(all_live, all_tokens, moved, V)

    grad_in, _ = lax.optimization_barrier((grad_in, embed_grad[:1, :1]))
    grad_in = jnp.concatenate([grad_q, grad_in, grad_f], axis=1)
    owned_grads = [grad_in, grad_out, grad_feed, grad_down, embed_grad, head_grad]
    square_sum = jnp.zeros((), wide)
    for grad_part in owned_grads:
        square_sum = square_sum + jnp.sum(grad_part * grad_part)
    small_grad = jnp.concatenate(
        [gain_grad_one, gain_grad_two, gain_grad_final, grad_bias, square_sum[None]]
    )
    small_count = small_grad.shape[0]
    small_grad = jnp.pad(small_grad, (0, -small_count % 1024)).reshape(-1, 128)
    small_sum = jnp.sum(gather_rows(small_grad, 4), axis=0).reshape(-1)
    small_total, square_total = small_sum[: small_count - 1], small_sum[small_count - 1]
    grad_norm = jnp.sqrt(square_total + jnp.sum(small_total * small_total))
    factor = jnp.minimum(1.0, clip_limit / grad_norm)
    layer = rate_layer
    news = update_all(
        factor,
        (
            (attention_in[0], attention_in_moment[0], attention_in_average[0], grad_in),
            (attention_out[0], attention_out_moment[0], attention_out_average[0], grad_out),
            (feed_in[0], feed_in_moment[0], feed_in_average[0], grad_feed),
            (feed_out[0], feed_out_moment[0], feed_out_average[0], grad_down),
            (embedding.T, embedding_moment.T, embedding_average.T, embed_grad),
            (unembedding, unembedding_moment, unembedding_average, head_grad),
        ),
        (layer, layer, layer, layer, rate_embed, rate_head),
    )
    results = [loss_value, grad_norm]
    for new in news[:4]:
        results.extend(array[None] for array in new)
    results.extend(array.T for array in news[4])
    results.extend(news[5])
    results.extend(
        apply_update(
            gains_biases, small_total, gains_biases_moment, gains_biases_average, factor, layer
        )
    )
    return tuple(results)


def solution(mesh):
    rows = P(None, both, None)
    tables = (rows,) * 12 + (P(None, both),) * 3 + (P(both, None),) * 3 + (P(),) * 3
    return jax.shard_map(
        step,
        mesh=mesh,
        in_specs=(
            P(None, "fsdp", "seq"),
            P(None, "fsdp"),
            P(None, "fsdp", "seq"),
            P(None, "fsdp", "seq"),
        )
        + tables,
        out_specs=(P(), P()) + tables,
        check_vma=False,
    )
```
